32 devices in a mesh: dp: 2 (over z, core), tp: 16 (over x, y).
Axes of the slice: x: 4, y: 4, z: 1, core: 2. Of those that a mesh axis runs over, the one named last changes fastest.
The devices are a block of a 4x4x8 slice.
Arguments:
- x: bfloat16 [4096, 8192], P(('dp', 'tp')), parts along dimension 0
- gain_a: bfloat16 [8192], replicated
- wq: bfloat16 [8192, 8192], P(None, 'tp')
- wk: bfloat16 [8192, 8192], P(None, 'tp')
- wv: bfloat16 [8192, 8192], P(None, 'tp')
- wo: bfloat16 [8192, 8192], P('tp')
- gain_m: bfloat16 [8192], replicated
- w_gate: bfloat16 [8192, 24576], P(None, 'tp')
- w_up: bfloat16 [8192, 24576], P(None, 'tp')
- w_down: bfloat16 [24576, 8192], P('tp')
Outputs:
- output: bfloat16 [4096, 8192], P(('dp', 'tp')), parts along dimension 0
There are 2 independent parts. The reference program is written for one: setup_inputs(seed, part) draws one part's arguments, and reference() takes and returns one part's arrays. A program takes and returns all parts, laid end to end along the dimension named above; an argument that names none is the same for every part.
All inputs are finite; a program needn't handle non-finite values.
Results may differ from the reference program's by a relative error of at most 0.017.
Values are sent between devices in bfloat16 or wider.
A program may use at most 768 MiB of HBM per device.

```python
import jax
import jax.numpy as jnp
from jax import lax

ROWS = 2048
D = 8192
HEADS = 64
KV_HEADS = 64
HEAD = 128
FF = 24576
THETA = 10000


def setup_inputs(seed: int = 0, part: int = 0) -> dict:
    kx, kn, kq, kk, kv, ko, km, kg, ku, kd = jax.random.split(jax.random.key(seed), 10)

    def weights(key, rows, columns):
        return jax.random.normal(key, (rows, columns), jnp.float32) * rows**-0.5

    drawn = {
        "x": jax.random.normal(jax.random.fold_in(kx, part), (ROWS, D), jnp.float32),
        "gain_a": 1 + 0.1 * jax.random.normal(kn, (D,), jnp.float32),
        "wq": 2 * weights(kq, D, HEADS * HEAD),
        "wk": 2 * weights(kk, D, KV_HEADS * HEAD),
        "wv": 4 * weights(kv, D, KV_HEADS * HEAD),
        "wo": weights(ko, HEADS * HEAD, D),
        "gain_m": 1 + 0.1 * jax.random.normal(km, (D,), jnp.float32),
        "w_gate": weights(kg, D, FF),
        "w_up": weights(ku, D, FF),
        "w_down": 2 * weights(kd, FF, D),
    }
    return {k: v.astype(jnp.bfloat16) for k, v in drawn.items()}


def normed(x, gain):
    wide = x.astype(jnp.float32)
    scale = lax.rsqrt(jnp.mean(wide * wide, -1, keepdims=True) + 1e-6)
    return (wide * scale * gain.astype(jnp.float32)).astype(jnp.bfloat16)


def turned(t, place, theta):
    half = t.shape[-1] // 2
    angle = place.astype(jnp.float32)[:, None] * theta ** (-jnp.arange(half, dtype=jnp.float32) / half)
    cos, sin = jnp.cos(angle)[:, None], jnp.sin(angle)[:, None]
    a, b = t[..., :half].astype(jnp.float32), t[..., half:].astype(jnp.float32)
    return jnp.concatenate([a * cos - b * sin, b * cos + a * sin], -1).astype(jnp.bfloat16)


def matmul(a, w):
    return jnp.dot(a, w, preferred_element_type=jnp.float32).astype(jnp.bfloat16)


def einsum(form, a, b):
    return jnp.einsum(form, a.astype(jnp.float32), b.astype(jnp.float32))


def attention(q, k, v):
    scores = einsum("tgsd,ugd->gstu", q, k) * q.shape[-1] ** -0.5
    token = jnp.arange(q.shape[0])
    scores = jnp.where(token[:, None] >= token, scores, -jnp.inf)
    weights = jax.nn.softmax(scores, -1).astype(jnp.bfloat16)
    return einsum("gstu,ugd->tgsd", weights, v).astype(jnp.bfloat16)


def reference(x, gain_a, wq, wk, wv, wo, gain_m, w_gate, w_up, w_down):
    a, place = normed(x, gain_a), jnp.arange(ROWS)
    q = turned(matmul(a, wq).reshape(ROWS, HEADS, HEAD), place, THETA).reshape(ROWS, KV_HEADS, -1, HEAD)
    k = turned(matmul(a, wk).reshape(ROWS, KV_HEADS, HEAD), place, THETA)
    v = matmul(a, wv).reshape(ROWS, KV_HEADS, HEAD)
    seen = attention(q, k, v).reshape(ROWS, HEADS * HEAD)
    h = (x.astype(jnp.float32) + jnp.dot(seen, wo, preferred_element_type=jnp.float32)).astype(jnp.bfloat16)
    b = normed(h, gain_m)
    gate = jnp.dot(b, w_gate, preferred_element_type=jnp.float32)
    up = jnp.dot(b, w_up, preferred_element_type=jnp.float32)
    hidden = (jax.nn.silu(gate) * up).astype(jnp.bfloat16)
    return (h.astype(jnp.float32) + jnp.dot(hidden, w_down, preferred_element_type=jnp.float32)).astype(jnp.bfloat16)
```

```python
import functools

import jax
import jax.numpy as jnp
import numpy as np
from jax import lax
from jax.experimental import pallas as pl
from jax.experimental.pallas import tpu as pltpu
from jax.sharding import PartitionSpec as P

MESH = pl.DeviceIdType.MESH
HEAD = 128
THETA = 10000
NEG = -1e30
HIDDEN = 2 * NEG
LOG2E = 1.4426950408889634
VMEM = 62 * 2**20
STRIP = 512
BLOCK = 256
TILE = 512
RING = 8

A, B = 0, 1
UP, DOWN = (0, -1), (1, 2)
LINKS = (("y", 1), ("y", -1), ("x", 1), ("x", -1))


def piece(half, along, across):
    return (half, across, along) if half == A else (half, along, across)


def both(along, across):
    return [piece(A, along, across), piece(B, along, across)]


SLOTS = (
    both(0, 0)
    + [piece(A, 0, -1), piece(A, 0, 1), piece(B, 0, -1), piece(B, 0, 1), piece(A, -1, 0), piece(A, 1, 0)]
    + [piece(B, -1, 0), piece(B, 1, 0), *both(0, 2), piece(A, -1, -1), piece(A, 1, -1), piece(B, -1, -1), piece(B, 1, -1)]
    + [piece(A, -1, 1), piece(A, 1, 1), piece(B, -1, 1), piece(B, 1, 1), *both(2, 0), *both(1, 2)]
    + [*both(-1, 2), *both(2, 1)]
    + [*both(2, -1), *both(2, 2)]
)
SLOT = {p: n for n, p in enumerate(SLOTS)}

def _by_link(along, pick):
    return [
        piece(half, along if along == 2 else sign * along, across)
        for (axis, sign) in LINKS
        for half in [A if axis == "y" else B]
        for across in (UP if (sign > 0) == pick else DOWN)
    ]


ORDER = _by_link(2, True) + _by_link(1, False) + _by_link(1, True) + [piece(half, 0, across) for half in (A, B) for across in UP + DOWN]


def _place(side):
    me = lax.axis_index("tp")
    return lax.div(me, side), lax.rem(me, side)


def _device(side, dx, dy):
    x, y = _place(side)
    return lax.rem(x + (dx + side), side) * side + lax.rem(y + (dy + side), side)


def _meet(side):
    barrier = pltpu.get_barrier_semaphore()
    for dx, dy in ((1, 0), (-1, 0), (0, 1), (0, -1)):
        pl.semaphore_signal(barrier, inc=1, device_id={"tp": _device(side, dx, dy)}, device_id_type=MESH)
    pl.semaphore_wait(barrier, 4)


def _step(link):
    axis, sign = link
    return (sign, 0) if axis == "x" else (0, sign)


def _copy(side, link, src, dst, send_sem, recv_sem):
    return pltpu.make_async_remote_copy(src_ref=src, dst_ref=dst, send_sem=send_sem, recv_sem=recv_sem,
                                        device_id={"tp": _device(side, *_step(link))}, device_id_type=MESH)


def _dot(a, b, ca=1, cb=0):
    return lax.dot_general(a, b, (((ca,), (cb,)), ((), ())), preferred_element_type=jnp.float32)


def _plan():
    start, first, second, third, fourth, fifth = [], [], [], [], [], []
    for half in (A, B):
        inner, outer = ("x", "y") if half == A else ("y", "x")
        at = lambda along, across: SLOT[piece(half, along, across)]
        for sign in (1, -1):
            start.append(((inner, sign), at(0, 0), at(0, -sign), 0, 1))
            first.append(((inner, sign), at(0, -sign), at(0, 2), 0 if sign > 0 else 1, 2))
    for half in (B, A):
        outer = "y" if half == A else "x"
        at = lambda along, across: SLOT[piece(half, along, across)]
        for sign in (1, -1):
            start.append(((outer, sign), at(0, 0), at(-sign, 0), 0, 1))
    for across in (-1, 1):
        for half in (A, B):
            outer = "y" if half == A else "x"
            at = lambda along, across: SLOT[piece(half, along, across)]
            for sign in (1, -1):
                first.append(((outer, sign), at(0, across), at(-sign, across), 0, 1))
    for half in (A, B):
        outer = "y" if half == A else "x"
        at = lambda along, across: SLOT[piece(half, along, across)]
        second.append(((outer, 1), at(-1, 0), at(2, 0), 0, 1))
        for sign in (1, -1):
            third.append(((outer, sign), at(0, 2), at(-sign, 2), 0, 1))
        fourth.append(((outer, 1), at(-1, -1), at(2, -1), 0, 1))
        fifth.append(((outer, -1), at(1, 1), at(2, 1), 0, 1))
    sixth = []
    for half in (A, B):
        outer = "y" if half == A else "x"
        at = lambda along, across: SLOT[piece(half, along, across)]
        sixth.append(((outer, -1), at(1, 2), at(2, 2), 0, 1))
    return [start, first, second, third, fourth, fifth, sixth]


PLAN = _plan()
COPIES = [c for group in PLAN for c in group]
_S = lambda *pieces: [SLOT[p] for p in pieces]
EVENTS = [
    [(SLOTS[2:6], 1), (SLOTS[6:10], 2)],
    [(SLOTS[10:12], 3), (SLOTS[12:16], 4)],
    [(SLOTS[16:20], 5), (SLOTS[20:24], 6)],
    [(SLOTS[24:28], None)],
    [(SLOTS[28:32], None)],
]


def _gather_kernel(x_ref, gain_ref, *refs, side, per_step, columns, finish, extra):
    extra_refs, refs = refs[:extra], refs[extra:]
    n_weights = len(columns)
    w_refs, refs = refs[:n_weights], refs[n_weights:]
    out_ref, g, w, stage, sems_x, sems_w, sems_o, send, recv = refs[:9]
    more = refs[9:]
    rows = x_ref.shape[0]
    size = rows // 2
    ring = w.shape[0]
    tiles = sum(columns) // per_step
    total = len(EVENTS) * tiles

    def weights(s, start):
        slot, n = lax.rem(s, ring), lax.rem(s, tiles)
        if per_step == 1:
            before = 0
            for ref, count in zip(w_refs, columns):

                @pl.when((n >= before) & (n < before + count))
                def _(ref=ref, before=before):
                    c = pltpu.make_async_copy(ref.at[:, pl.ds(pl.multiple_of((n - before) * BLOCK, BLOCK), BLOCK)], w.at[slot, 0],
                                              sems_w.at[slot, 0])
                    c.start() if start else c.wait()

                before += count
        else:
            for at, ref in enumerate(w_refs):
                c = pltpu.make_async_copy(ref.at[:, pl.ds(pl.multiple_of(n * BLOCK, BLOCK), BLOCK)], w.at[slot, at], sems_w.at[slot, at])
                c.start() if start else c.wait()

    def remote(number):
        link, src, dst, part, parts = COPIES[number]
        height = size // parts
        return _copy(side, link, g.at[pl.ds(src * size + part * height, height)], g.at[pl.ds(dst * size + part * height, height)],
                     send.at[number], recv.at[dst, part])

    def begin(group):
        first = sum(len(p) for p in PLAN[:group])
        for number in range(first, first + len(PLAN[group])):
            remote(number).start()

    def arrived(slots):
        for number, (_, _, dst, _, _) in enumerate(COPIES):
            if SLOTS[dst] in slots:
                remote(number).wait_recv()

    own = pltpu.make_async_copy(x_ref, g.at[pl.ds(0, rows)], sems_x.at[0])
    own.start()
    for s in range(ring - 1):
        weights(s, True)
    after = finish.prepare(extra_refs, more) if finish.prepare else None
    _meet(side)
    own.wait()

    def norm(i, _):
        here = pl.ds(pl.multiple_of(i * 16, 16), 16)
        wide = g[here, :].astype(jnp.float32)
        scale = lax.rsqrt(jnp.mean(wide * wide, -1, keepdims=True) + 1e-6)
        g[here, :] = (wide * scale * gain_ref[...].astype(jnp.float32)).astype(jnp.bfloat16)

    lax.fori_loop(0, rows // 16, norm, None)
    begin(0)
    if after:
        after()

    def block(b, _):
        for k, events in enumerate(EVENTS):

            @pl.when(b == k)
            def _(events=events):
                for slots, group in events:
                    arrived(slots)
                    if group is not None:
                        begin(group)

        first = 2 * b - lax.div(b, 4)
        count = 2 - lax.div(b, 3)

        def tile(n, _):
            s = b * tiles + n

            @pl.when(s + (ring - 1) < total)
            def _():
                weights(s + (ring - 1), True)

            weights(s, False)
            slot = lax.rem(s, ring)

            def product(m, _):
                at = first + m
                lhs = g.at[pl.ds(pl.multiple_of(at * BLOCK, BLOCK), BLOCK)]
                to = lax.rem(n * count + m, 2)

                @pl.when((b > 0) | (n > 0))
                def _():
                    finish.store(stage, out_ref, sems_o, to, at, n, size, side, start=False)

                finish.compute(lhs, w.at[slot], stage.at[to], at, n, more)
                finish.store(stage, out_ref, sems_o, to, at, n, size, side, start=True)

            lax.fori_loop(0, count, product, None)

        lax.fori_loop(0, tiles, tile, None)

    lax.fori_loop(0, len(EVENTS), block, None)
    for to in range(2):
        finish.store(stage, out_ref, sems_o, to, 0, 0, size, side, start=False)
    for number in range(len(COPIES)):
        remote(number).wait_send()


class _Heads:
    def __init__(self, turned_steps):
        self.turned_steps = turned_steps

    def prepare(self, extra_refs, more):
        (table_ref,) = extra_refs
        table, sems = more
        size = table.shape[0] // len(SLOTS)
        side = int(round((len(SLOTS) // 2) ** 0.5))
        copies = []
        for n, (half, dx, dy) in enumerate(SLOTS):
            row = _device(side, dx, dy) * (2 * size) + half * size
            copies.append(pltpu.make_async_copy(table_ref.at[pl.ds(pl.multiple_of(row, size), size)], table.at[pl.ds(n * size, size)],
                                                sems.at[n]))
        for c in copies:
            c.start()

        def after():
            for c in copies:
                c.wait()

        return after

    def compute(self, lhs, w, to, at, n, more):
        table = more[0]
        got = _dot(lhs[...], w[0]).astype(jnp.bfloat16)

        @pl.when(n < self.turned_steps)
        def _():
            t = table[pl.ds(pl.multiple_of(at * BLOCK, BLOCK), BLOCK), :]
            swapped = pltpu.roll(t, HEAD // 2, 1)
            low = lax.broadcasted_iota(jnp.int32, t.shape, 1) < HEAD // 2
            cos, sin = jnp.where(low, t, swapped), jnp.where(low, -swapped, t)
            for i in range(BLOCK // HEAD):
                one = got[:, i * HEAD : (i + 1) * HEAD].astype(jnp.float32)
                to[:, i * HEAD : (i + 1) * HEAD] = (one * cos + pltpu.roll(one, HEAD // 2, 1) * sin).astype(jnp.bfloat16)

        @pl.when(n >= self.turned_steps)
        def _():
            to[...] = got

    def store(self, stage, out_ref, sems, to, at, n, size, side, start):
        per = BLOCK // size

        def copies(pieces):
            for p, (half, dx, dy) in enumerate(pieces):
                row = pl.multiple_of(_device(side, dx, dy) * (2 * size) + half * size, size)
                for i in range(BLOCK // HEAD):
                    yield pltpu.make_async_copy(stage.at[to, pl.ds(p * size, size), pl.ds(i * HEAD, HEAD)],
                                                out_ref.at[n * (BLOCK // HEAD) + i, pl.ds(row, size)], sems.at[to, p * (BLOCK // HEAD) + i])

        if not start:
            for c in copies(SLOTS[:per]):
                c.wait()
            return
        for k in range(len(SLOTS) // per):

            @pl.when(at == k)
            def _(k=k):
                for c in copies(SLOTS[k * per : (k + 1) * per]):
                    c.start()


class _Hidden:
    prepare = None

    def compute(self, lhs, w, to, at, n, more):
        gate = _dot(lhs[...], w[0])
        up = _dot(lhs[...], w[1])
        to[...] = (jax.nn.silu(gate) * up).astype(jnp.bfloat16)

    def store(self, stage, out_ref, sems, to, at, n, size, side, start):
        c = pltpu.make_async_copy(stage.at[to], out_ref.at[pl.ds(pl.multiple_of(at * BLOCK, BLOCK), BLOCK),
                                                           pl.ds(pl.multiple_of(n * BLOCK, BLOCK), BLOCK)], sems.at[to, 0])
        c.start() if start else c.wait()


def gathered(x, gain, weights, finish, per_step, ring, out_shape, number, name, extra=(), scratch=(), copies=1):
    rows, depth = x.shape
    n = lax.axis_size("tp")
    side = int(round(n**0.5))
    columns = [w.shape[1] // BLOCK for w in weights]
    width = sum(w.shape[1] for w in weights)
    return pl.pallas_call(
        functools.partial(_gather_kernel, side=side, per_step=per_step, columns=columns, finish=finish, extra=len(extra)),
        out_shape=out_shape,
        in_specs=[pl.BlockSpec(memory_space=pl.ANY), pl.BlockSpec(memory_space=pltpu.VMEM)]
        + [pl.BlockSpec(memory_space=pl.ANY)] * (len(extra) + len(weights)),
        out_specs=pl.BlockSpec(memory_space=pl.ANY),
        scratch_shapes=[
            pltpu.VMEM((n * rows, depth), jnp.bfloat16),
            pltpu.VMEM((ring, per_step, depth, BLOCK), jnp.bfloat16),
            pltpu.VMEM((2, BLOCK, BLOCK), jnp.bfloat16),
            pltpu.SemaphoreType.DMA((1,)),
            pltpu.SemaphoreType.DMA((ring, per_step)),
            pltpu.SemaphoreType.DMA((2, copies)),
            pltpu.SemaphoreType.DMA((len(COPIES),)),
            pltpu.SemaphoreType.DMA((len(SLOTS), 2)),
            *scratch,
        ],
        compiler_params=pltpu.CompilerParams(collective_id=number, has_side_effects=True, vmem_limit_bytes=VMEM),
        cost_estimate=pl.CostEstimate(flops=2 * n * rows * depth * width, transcendentals=0, bytes_accessed=2 * len(EVENTS) * depth * width),
        name=name,
    )(x, gain.reshape(1, depth), *extra, *weights)


def _scatter_kernel(rows_ref, x_ref, w_ref, out_ref, hid, res, out, w, far, plain, summed, near, keep, own, r_far, r_plain, r_summed,
                    r_half, r_near, sems_h, sems_x, sems_w, sems_o, s_far, s_plain, s_summed, s_half, s_near, t_far, t_plain, t_summed,
                    t_half, t_near, *, side, where):
    rows, width = out_ref.shape
    size = rows // 2
    low = size // 2
    tile = w.shape[2]
    tiles = width // tile
    ring = r_far.shape[0]
    group = hid.shape[0] // 4

    def fetch(n):
        return pltpu.make_async_copy(rows_ref.at[pl.ds(where(ORDER[n], size, side), size)], hid.at[pl.ds(n * size, size)], sems_h.at[n])

    def fetched(g):
        for n in range(g * 8, g * 8 + 8):
            fetch(n).wait()

    def weights(j):
        slot = lax.rem(j, 4)
        return pltpu.make_async_copy(w_ref.at[:, pl.ds(pl.multiple_of(j * tile, tile), tile)], w.at[slot], sems_w.at[slot])

    def term(g, j):
        return _dot(hid[pl.ds(g * group, group), :], w[lax.rem(j, 4)]).reshape(8, size, tile)

    def move(l, src, dst, s_sem, t_sem, j):
        return _copy(side, LINKS[l], src, dst, s_sem, t_sem)

    def pairs(src, dst, s_sem, t_sem, j):
        a, b = lax.rem(j, 2), lax.rem(j, ring)
        return [_copy(side, LINKS[l], src.at[a, pl.ds(2 * l, 2)], dst.at[b, pl.ds(2 * l, 2)], s_sem.at[a, l], t_sem.at[b, l])
                for l in range(4)]

    def spot(l):
        return (A if l >= 2 else B), l % 2

    def halves(j):
        a, b = lax.rem(j, 2), lax.rem(j, ring)
        return [_copy(side, LINKS[l], near.at[a, 0, l], r_half.at[b, l], s_half.at[a, l], t_half.at[b, l]) for l in range(4)]

    def lasts(j, part):
        a, b = lax.rem(j, 2), lax.rem(j, ring)
        got = []
        for l in range(4):
            at = spot(l)[1] if part else 1 - spot(l)[1]
            got.append(_copy(side, LINKS[l], near.at[a, 1 + part, l], r_near.at[b, l, pl.ds(at * low, low)], s_near.at[a, part, l],
                             t_near.at[b, part, l]))
        return got

    def each(copies, what):
        for c in copies:
            getattr(c, what)()

    def out_copy(j):
        here = pl.ds(pl.multiple_of(j * tile, tile), tile)
        return pltpu.make_async_copy(out.at[:, here], out_ref.at[:, here], sems_o.at[j])

    for n in range(8):
        fetch(n).start()
    weights(0).start()
    for n in range(8, len(ORDER)):
        fetch(n).start()
    residual = pltpu.make_async_copy(x_ref, res, sems_x.at[0])
    residual.start()
    _meet(side)

    def step(i, _):
        @pl.when(i < tiles)
        def _():
            j = i

            @pl.when(j == 0)
            def _():
                fetched(0)

            @pl.when(j + 1 < tiles)
            def _():
                weights(j + 1).start()

            weights(j).wait()

            @pl.when(j >= 2)
            def _():
                each(pairs(far, r_far, s_far, t_far, j), "wait_send")
                each(pairs(plain, r_plain, s_plain, t_plain, j), "wait_send")

            far[lax.rem(j, 2)] = term(0, j).astype(jnp.bfloat16)
            each(pairs(far, r_far, s_far, t_far, j), "start")

            @pl.when(j == 0)
            def _():
                fetched(1)

            plain[lax.rem(j, 2)] = term(1, j).astype(jnp.bfloat16)
            each(pairs(plain, r_plain, s_plain, t_plain, j), "start")

        @pl.when((i >= 1) & (i < tiles + 1))
        def _():
            j = i - 1

            @pl.when(j == 0)
            def _():
                fetched(2)

            @pl.when(j >= 2)
            def _():
                each(pairs(summed, r_summed, s_summed, t_summed, j), "wait_send")

            each(pairs(far, r_far, s_far, t_far, j), "wait_recv")
            summed[lax.rem(j, 2)] = (term(2, j) + r_far[lax.rem(j, ring)].astype(jnp.float32)).astype(jnp.bfloat16)
            each(pairs(summed, r_summed, s_summed, t_summed, j), "start")

        @pl.when((i >= 2) & (i < tiles + 2))
        def _():
            j = i - 2
            a, b = lax.rem(j, 2), lax.rem(j, ring)

            @pl.when(j == 0)
            def _():
                fetched(3)

            @pl.when(j >= 2)
            def _():
                each(halves(j), "wait_send")
                each(lasts(j, 0), "wait_send")

            each(pairs(plain, r_plain, s_plain, t_plain, j), "wait_recv")
            each(pairs(summed, r_summed, s_summed, t_summed, j), "wait_recv")
            mine = term(3, j)
            for half in (A, B):
                l = 2 * half
                from_up = [r_summed[b, 2 * l + k] for k in range(2)] + [r_plain[b, 2 * l + k] for k in range(2)]
                from_down = [r_plain[b, 2 * l + 2 + k] for k in range(2)] + [r_summed[b, 2 * l + 2 + k] for k in range(2)]
                sums = {across: mine[4 * half + k] + from_up[k].astype(jnp.float32) + from_down[k].astype(jnp.float32)
                        for k, across in enumerate(UP + DOWN)}
                own[lax.rem(j, 4), half] = sums[0]
                l = 2 if half == A else 0
                near[a, 0, l] = sums[2][:low].astype(jnp.bfloat16)
                near[a, 0, l + 1] = sums[2][low:].astype(jnp.bfloat16)
                near[a, 1, l] = sums[1][low:].astype(jnp.bfloat16)
                near[a, 1, l + 1] = sums[-1][:low].astype(jnp.bfloat16)
                keep[a, l] = sums[1][:low]
                keep[a, l + 1] = sums[-1][low:]
            each(halves(j), "start")
            each(lasts(j, 0), "start")

        @pl.when((i >= 3) & (i < tiles + 3))
        def _():
            j = i - 3
            a, b = lax.rem(j, 2), lax.rem(j, ring)

            @pl.when(j >= 2)
            def _():
                each(lasts(j, 1), "wait_send")

            each(halves(j), "wait_recv")
            for l in range(4):
                near[a, 2, l] = (keep[a, l] + r_half[b, l].astype(jnp.float32)).astype(jnp.bfloat16)
            each(lasts(j, 1), "start")

        @pl.when(i >= 4)
        def _():
            j = i - 4
            b = lax.rem(j, ring)

            @pl.when(j == 0)
            def _():
                residual.wait()

            each(lasts(j, 0), "wait_recv")
            each(lasts(j, 1), "wait_recv")
            here = pl.ds(pl.multiple_of(j * tile, tile), tile)
            for half in (A, B):
                l = 2 if half == A else 0
                total = own[lax.rem(j, 4), half] + r_near[b, l].astype(jnp.float32) + r_near[b, l + 1].astype(jnp.float32)
                mine = pl.ds(half * size, size)
                out[mine, here] = (res[mine, here].astype(jnp.float32) + total).astype(jnp.bfloat16)
            out_copy(j).start()

    lax.fori_loop(0, tiles + 4, step, None)
    for j in range(tiles - 2, tiles):
        each(pairs(far, r_far, s_far, t_far, j), "wait_send")
        each(pairs(plain, r_plain, s_plain, t_plain, j), "wait_send")
        each(pairs(summed, r_summed, s_summed, t_summed, j), "wait_send")
        each(halves(j), "wait_send")
        each(lasts(j, 0), "wait_send")
        each(lasts(j, 1), "wait_send")
    for j in range(tiles):
        out_copy(j).wait()


def _in_sequence(p, size, side):
    half, dx, dy = p
    return pl.multiple_of(_device(side, dx, dy) * (2 * size) + half * size, size)


def _in_slots(p, size, side):
    return SLOT[p] * size


def scattered(terms, x, w, where, number, name):
    rows, width = x.shape
    depth = w.shape[0]
    n = lax.axis_size("tp")
    side = int(round(n**0.5))
    size, low = rows // 2, rows // 4
    tile = min(TILE, width)
    tiles = width // tile
    bf, f32, dma = jnp.bfloat16, jnp.float32, pltpu.SemaphoreType.DMA
    return pl.pallas_call(
        functools.partial(_scatter_kernel, side=side, where=where),
        out_shape=jax.ShapeDtypeStruct((rows, width), bf),
        in_specs=[pl.BlockSpec(memory_space=pl.ANY)] * 3,
        out_specs=pl.BlockSpec(memory_space=pl.ANY),
        scratch_shapes=[
            pltpu.VMEM((n * rows, depth), bf),
            pltpu.VMEM((rows, width), bf),
            pltpu.VMEM((rows, width), bf),
            pltpu.VMEM((4, depth, tile), bf),
            pltpu.VMEM((2, 8, size, tile), bf),
            pltpu.VMEM((2, 8, size, tile), bf),
            pltpu.VMEM((2, 8, size, tile), bf),
            pltpu.VMEM((2, 3, 4, low, tile), bf),
            pltpu.VMEM((2, 4, low, tile), f32),
            pltpu.VMEM((4, 2, size, tile), f32),
            pltpu.VMEM((RING, 8, size, tile), bf),
            pltpu.VMEM((RING, 8, size, tile), bf),
            pltpu.VMEM((RING, 8, size, tile), bf),
            pltpu.VMEM((RING, 4, low, tile), bf),
            pltpu.VMEM((RING, 4, size, tile), bf),
            dma((len(ORDER),)), dma((1,)), dma((4,)), dma((tiles,)),
            dma((2, 4)), dma((2, 4)), dma((2, 4)), dma((2, 4)), dma((2, 2, 4)),
            dma((RING, 4)), dma((RING, 4)), dma((RING, 4)), dma((RING, 4)), dma((RING, 2, 4)),
        ],
        compiler_params=pltpu.CompilerParams(collective_id=number, has_side_effects=True, vmem_limit_bytes=VMEM),
        cost_estimate=pl.CostEstimate(flops=2 * n * rows * depth * width, transcendentals=0, bytes_accessed=2 * depth * width),
        name=name,
    )(terms, x, w)


def _attend_kernel(q_ref, k_ref, v_ref, o_ref, top_s, mix_s, gap_s, *, scale, bk):
    heads, bq, d = q_ref.shape
    cols, low = bq, k_ref.dtype
    iq = pl.program_id(0)
    e = scale * LOG2E
    wide = min(cols, STRIP)
    pieces = [(i, at) for i in range(heads) for at in range(0, cols, wide)]
    gap_s[...] = lax.broadcasted_iota(jnp.int32, gap_s.shape, 1) - lax.broadcasted_iota(jnp.int32, gap_s.shape, 0)
    top_s[...] = jnp.full(top_s.shape, NEG, jnp.float32)
    mix_s[...] = jnp.zeros(mix_s.shape, jnp.float32)
    ones = jnp.ones((8, bk), low)

    def block(j, masked):
        here = pl.ds(pl.multiple_of(j * bk, bk), bk)
        scores = [_dot(k_ref[i, here, :], q_ref[i, at : at + wide, :], 1, 1) for i, at in pieces]
        ok = gap_s[...] >= j * bk - iq * bq if masked else None
        weights, keeps = [], []
        for (i, at), s in zip(pieces, scores):
            if masked:
                s = jnp.where(ok[:, at : at + wide], s, HIDDEN)
            old = top_s[i : i + 1, at : at + wide]
            top = jnp.maximum(old, s.max(axis=0, keepdims=True))
            top_s[i : i + 1, at : at + wide] = top
            weights.append(jnp.exp2((s - top) * e).astype(low))
            keeps.append(jnp.exp2((old - top) * e))
        for (i, at), p, keep in zip(pieces, weights, keeps):
            values = jnp.concatenate([v_ref[i, here, :].T, ones], axis=0)
            mix_s[i, :, at : at + wide] = mix_s[i, :, at : at + wide] * keep + _dot(values, p, 1, 0)

    whole = lax.div(iq * bq, bk)
    last = lax.div((iq + 1) * bq, bk)
    lax.fori_loop(0, whole, lambda j, _: block(j, False), None)
    lax.fori_loop(whole, last, lambda j, _: block(j, True), None)
    for i in range(heads):
        total = mix_s[i, d : d + 1, :]
        o_ref[:, i * d : (i + 1) * d] = (mix_s[i, :d, :] * (1 / total)).T.astype(o_ref.dtype)


def attended(qkv, bq=1024, bk=512):
    heads, tokens, d = qkv.shape[0] // 3, *qkv.shape[1:]
    bq, bk = min(bq, tokens), min(bk, tokens)
    return pl.pallas_call(
        functools.partial(_attend_kernel, scale=d**-0.5, bk=bk),
        grid=(tokens // bq,),
        in_specs=[pl.BlockSpec((heads, bq, d), lambda i: (0, i, 0)), pl.BlockSpec((heads, tokens, d), lambda i: (1, 0, 0)),
                  pl.BlockSpec((heads, tokens, d), lambda i: (2, 0, 0))],
        out_specs=pl.BlockSpec((bq, heads * d), lambda i: (i, 0)),
        out_shape=jax.ShapeDtypeStruct((tokens, heads * d), qkv.dtype),
        scratch_shapes=[pltpu.VMEM((heads, bq), jnp.float32), pltpu.VMEM((heads, d + 8, bq), jnp.float32), pltpu.VMEM((bk, bq), jnp.int32)],
        compiler_params=pltpu.CompilerParams(dimension_semantics=("arbitrary",), vmem_limit_bytes=VMEM),
        cost_estimate=pl.CostEstimate(flops=4 * heads * tokens * tokens * d, transcendentals=heads * tokens * tokens,
                                      bytes_accessed=8 * heads * tokens * d),
        name="attended",
    )(qkv, qkv, qkv)


def _angles(tokens):
    half = HEAD // 2
    rate = np.power(np.float32(THETA), -np.arange(half, dtype=np.float32) / np.float32(half)).astype(np.float32)
    angle = (np.arange(tokens, dtype=np.float32)[:, None] * rate).astype(np.float64)
    return np.concatenate([np.cos(angle), np.sin(angle)], 1).astype(np.float32)


def solution(mesh):
    n = mesh.shape["tp"]

    def step(x, gain_a, wq, wk, wv, wo, gain_m, w_gate, w_up, w_down):
        rows = n * x.shape[0]
        heads = wq.shape[1] // HEAD
        turned_steps = 2 * wq.shape[1] // BLOCK
        qkv = gathered(
            x, gain_a, (wq, wk, wv), _Heads(turned_steps), 1, 3, jax.ShapeDtypeStruct((3 * heads, rows, HEAD), jnp.bfloat16), 0, "gather_qkv",
            extra=(jnp.asarray(_angles(rows)),),
            scratch=(pltpu.VMEM((rows, HEAD), jnp.float32), pltpu.SemaphoreType.DMA((len(SLOTS),))),
            copies=(BLOCK // (x.shape[0] // 2)) * (BLOCK // HEAD),
        )
        h = scattered(attended(qkv), x, wo, _in_sequence, 1, "scatter_o")
        hidden = gathered(h, gain_m, (w_gate, w_up), _Hidden(), 2, 2, jax.ShapeDtypeStruct((rows, w_gate.shape[1]), jnp.bfloat16), 2,
                          "gather_hidden")
        return scattered(hidden, h, w_down, _in_slots, 3, "scatter_down")

    tokens, columns, rows_of = P(("dp", "tp"), None), P(None, "tp"), P("tp", None)
    return jax.shard_map(
        step,
        mesh=mesh,
        in_specs=(tokens, P(None), columns, columns, columns, rows_of, P(None), columns, columns, rows_of),
        out_specs=tokens,
        check_vma=False,
    )
```

```python
import functools

import jax
import jax.numpy as jnp
import numpy as np
from jax import lax
from jax.experimental import pallas as pl
from jax.experimental.pallas import tpu as pltpu
from jax.sharding import PartitionSpec as P

MESH = pl.DeviceIdType.MESH
HEAD = 128
THETA = 10000
NEG = -1e30
HIDDEN = 2 * NEG
LOG2E = 1.4426950408889634
VMEM = 62 * 2**20
STRIP = 512
BLOCK = 256
TILE = 512
TURN = 4
RING = 8

A, B = 0, 1
UP, DOWN = (0, -1), (1, 2)
LINKS = (("y", 1), ("y", -1), ("x", 1), ("x", -1))


def piece(half, along, across):
    return (half, across, along) if half == A else (half, along, across)


def both(along, across):
    return [piece(A, along, across), piece(B, along, across)]


SLOTS = (
    both(0, 0)
    + [piece(A, 0, -1), piece(A, 0, 1), piece(B, 0, -1), piece(B, 0, 1), piece(A, -1, 0), piece(A, 1, 0)]
    + [piece(B, -1, 0), piece(B, 1, 0), *both(0, 2), piece(A, -1, -1), piece(A, 1, -1), piece(B, -1, -1), piece(B, 1, -1)]
    + [piece(A, -1, 1), piece(A, 1, 1), piece(B, -1, 1), piece(B, 1, 1), *both(2, 0), *both(1, 2)]
    + [*both(-1, 2), *both(2, 1)]
    + [*both(2, -1), *both(2, 2)]
)
SLOT = {p: n for n, p in enumerate(SLOTS)}

def _by_link(along, pick):
    return [
        piece(half, along if along == 2 else sign * along, across)
        for (axis, sign) in LINKS
        for half in [A if axis == "y" else B]
        for across in (UP if (sign > 0) == pick else DOWN)
    ]


ORDER = _by_link(2, True) + _by_link(1, False) + _by_link(1, True) + [piece(half, 0, across) for half in (A, B) for across in UP + DOWN]


def _place(side):
    me = lax.axis_index("tp")
    return lax.div(me, side), lax.rem(me, side)


def _device(side, dx, dy):
    x, y = _place(side)
    return lax.rem(x + (dx + side), side) * side + lax.rem(y + (dy + side), side)


def _meet(side, twin=False):
    barrier = pltpu.get_barrier_semaphore()
    for dx, dy in ((1, 0), (-1, 0), (0, 1), (0, -1)):
        pl.semaphore_signal(barrier, inc=1, device_id={"tp": _device(side, dx, dy)}, device_id_type=MESH)
    if twin:
        pl.semaphore_signal(barrier, inc=1, device_id=_twin(), device_id_type=MESH)
    pl.semaphore_wait(barrier, 5 if twin else 4)


def _twin():
    group = lax.axis_index("dp")
    return {"dp": group + 1 - 2 * lax.rem(group, 2), "tp": lax.axis_index("tp")}


def _step(link):
    axis, sign = link
    return (sign, 0) if axis == "x" else (0, sign)


def _copy(side, link, src, dst, send_sem, recv_sem):
    return pltpu.make_async_remote_copy(src_ref=src, dst_ref=dst, send_sem=send_sem, recv_sem=recv_sem,
                                        device_id={"tp": _device(side, *_step(link))}, device_id_type=MESH)


def _dot(a, b, ca=1, cb=0):
    return lax.dot_general(a, b, (((ca,), (cb,)), ((), ())), preferred_element_type=jnp.float32)


def _plan():
    start, first, second, third, fourth, fifth = [], [], [], [], [], []
    for half in (A, B):
        inner, outer = ("x", "y") if half == A else ("y", "x")
        at = lambda along, across: SLOT[piece(half, along, across)]
        for sign in (1, -1):
            start.append(((inner, sign), at(0, 0), at(0, -sign), 0, 1))
            first.append(((inner, sign), at(0, -sign), at(0, 2), 0 if sign > 0 else 1, 2))
    for half in (B, A):
        outer = "y" if half == A else "x"
        at = lambda along, across: SLOT[piece(half, along, across)]
        for sign in (1, -1):
            start.append(((outer, sign), at(0, 0), at(-sign, 0), 0, 1))
    for across in (-1, 1):
        for half in (A, B):
            outer = "y" if half == A else "x"
            at = lambda along, across: SLOT[piece(half, along, across)]
            for sign in (1, -1):
                first.append(((outer, sign), at(0, across), at(-sign, across), 0, 1))
    for half in (A, B):
        outer = "y" if half == A else "x"
        at = lambda along, across: SLOT[piece(half, along, across)]
        second.append(((outer, 1), at(-1, 0), at(2, 0), 0, 1))
        for sign in (1, -1):
            third.append(((outer, sign), at(0, 2), at(-sign, 2), 0, 1))
        fourth.append(((outer, 1), at(-1, -1), at(2, -1), 0, 1))
        fifth.append(((outer, -1), at(1, 1), at(2, 1), 0, 1))
    sixth = []
    for half in (A, B):
        outer = "y" if half == A else "x"
        at = lambda along, across: SLOT[piece(half, along, across)]
        sixth.append(((outer, -1), at(1, 2), at(2, 2), 0, 1))
    return [start, first, second, third, fourth, fifth, sixth]


PLAN = _plan()
COPIES = [c for group in PLAN for c in group]
_S = lambda *pieces: [SLOT[p] for p in pieces]
EVENTS = [
    [(SLOTS[2:6], 1), (SLOTS[6:10], 2)],
    [(SLOTS[10:12], 3), (SLOTS[12:16], 4)],
    [(SLOTS[16:20], 5), (SLOTS[20:24], 6)],
    [(SLOTS[24:28], None)],
    [(SLOTS[28:32], None)],
]


def _gather_kernel(x_ref, gain_ref, *refs, side, per_step, columns, finish, extra, turns):
    extra_refs, refs = refs[:extra], refs[extra:]
    n_weights = len(columns)
    w_refs, refs = refs[:n_weights], refs[n_weights:]
    out_ref, g, w, stage, sems_x, sems_w, sems_o, send, recv, turn = refs[:10]
    more = refs[10:]
    rows = x_ref.shape[0]
    size = rows // 2
    ring = w.shape[0]
    tiles = sum(columns) // per_step
    total = len(EVENTS) * tiles

    def weights(s, start):
        slot, n = lax.rem(s, ring), lax.rem(s, tiles)
        if per_step == 1:
            before = 0
            for ref, count in zip(w_refs, columns):

                @pl.when((n >= before) & (n < before + count))
                def _(ref=ref, before=before):
                    c = pltpu.make_async_copy(ref.at[:, pl.ds(pl.multiple_of((n - before) * BLOCK, BLOCK), BLOCK)], w.at[slot, 0],
                                              sems_w.at[slot, 0])
                    c.start() if start else c.wait()

                before += count
        else:
            for at, ref in enumerate(w_refs):
                c = pltpu.make_async_copy(ref.at[:, pl.ds(pl.multiple_of(n * BLOCK, BLOCK), BLOCK)], w.at[slot, at], sems_w.at[slot, at])
                c.start() if start else c.wait()

    def remote(number):
        link, src, dst, part, parts = COPIES[number]
        height = size // parts
        return _copy(side, link, g.at[pl.ds(src * size + part * height, height)], g.at[pl.ds(dst * size + part * height, height)],
                     send.at[number], recv.at[dst, part])

    def begin(group):
        first = sum(len(p) for p in PLAN[:group])
        for number in range(first, first + len(PLAN[group])):
            remote(number).start()

    def arrived(slots):
        for number, (_, _, dst, _, _) in enumerate(COPIES):
            if SLOTS[dst] in slots:
                remote(number).wait_recv()

    own = pltpu.make_async_copy(x_ref, g.at[pl.ds(0, rows)], sems_x.at[0])
    own.start()
    for s in range(ring - 1):
        weights(s, True)
    after = finish.prepare(extra_refs, more) if finish.prepare else None
    _meet(side, turns)
    own.wait()

    def norm(i, _):
        here = pl.ds(pl.multiple_of(i * 16, 16), 16)
        wide = g[here, :].astype(jnp.float32)
        scale = lax.rsqrt(jnp.mean(wide * wide, -1, keepdims=True) + 1e-6)
        g[here, :] = (wide * scale * gain_ref[...].astype(jnp.float32)[None]).astype(jnp.bfloat16)

    lax.fori_loop(0, rows // 16, norm, None)
    if turns:
        @pl.when(lax.rem(lax.axis_index("dp"), 2) == 0)
        def _():
            pl.semaphore_wait(turn, 1)

    begin(0)
    if after:
        after()

    def block(b, _):
        for k, events in enumerate(EVENTS):

            @pl.when(b == k)
            def _(events=events):
                for slots, group in events:
                    arrived(slots)
                    if group is not None:
                        begin(group)
                    if turns and group == turns:

                        @pl.when(lax.rem(lax.axis_index("dp"), 2) == 1)
                        def _():
                            pl.semaphore_signal(turn, inc=1, device_id=_twin(), device_id_type=MESH)

        first = 2 * b - lax.div(b, 4)
        count = 2 - lax.div(b, 3)

        def tile(n, _):
            s = b * tiles + n

            @pl.when(s + (ring - 1) < total)
            def _():
                weights(s + (ring - 1), True)

            weights(s, False)
            slot = lax.rem(s, ring)

            def product(m, _):
                at = first + m
                lhs = g.at[pl.ds(pl.multiple_of(at * BLOCK, BLOCK), BLOCK)]
                to = lax.rem(n * count + m, 2)

                @pl.when((b > 0) | (n > 0))
                def _():
                    finish.store(stage, out_ref, sems_o, to, at, n, size, side, start=False)

                finish.compute(lhs, w.at[slot], stage.at[to], at, n, more)
                finish.store(stage, out_ref, sems_o, to, at, n, size, side, start=True)

            lax.fori_loop(0, count, product, None)

        lax.fori_loop(0, tiles, tile, None)

    lax.fori_loop(0, len(EVENTS), block, None)
    for to in range(2):
        finish.store(stage, out_ref, sems_o, to, 0, 0, size, side, start=False)
    for number in range(len(COPIES)):
        remote(number).wait_send()


class _Heads:
    def __init__(self, turned_steps):
        self.turned_steps = turned_steps

    def prepare(self, extra_refs, more):
        (table_ref,) = extra_refs
        table, sems = more
        size = table.shape[0] // len(SLOTS)
        side = int(round((len(SLOTS) // 2) ** 0.5))
        copies = []
        for n, (half, dx, dy) in enumerate(SLOTS):
            row = _device(side, dx, dy) * (2 * size) + half * size
            copies.append(pltpu.make_async_copy(table_ref.at[pl.ds(pl.multiple_of(row, size), size)], table.at[pl.ds(n * size, size)],
                                                sems.at[n]))
        for c in copies:
            c.start()

        def after():
            for c in copies:
                c.wait()

        return after

    def compute(self, lhs, w, to, at, n, more):
        table = more[0]
        got = _dot(lhs[...], w[0]).astype(jnp.bfloat16)

        @pl.when(n < self.turned_steps)
        def _():
            t = table[pl.ds(pl.multiple_of(at * BLOCK, BLOCK), BLOCK), :]
            swapped = pltpu.roll(t, HEAD // 2, 1)
            low = lax.broadcasted_iota(jnp.int32, t.shape, 1) < HEAD // 2
            cos, sin = jnp.where(low, t, swapped), jnp.where(low, -swapped, t)
            for i in range(BLOCK // HEAD):
                one = got[:, i * HEAD : (i + 1) * HEAD].astype(jnp.float32)
                to[:, i * HEAD : (i + 1) * HEAD] = (one * cos + pltpu.roll(one, HEAD // 2, 1) * sin).astype(jnp.bfloat16)

        @pl.when(n >= self.turned_steps)
        def _():
            to[...] = got

    def store(self, stage, out_ref, sems, to, at, n, size, side, start):
        per = BLOCK // size

        def copies(pieces):
            for p, (half, dx, dy) in enumerate(pieces):
                row = pl.multiple_of(_device(side, dx, dy) * (2 * size) + half * size, size)
                for i in range(BLOCK // HEAD):
                    yield pltpu.make_async_copy(stage.at[to, pl.ds(p * size, size), pl.ds(i * HEAD, HEAD)],
                                                out_ref.at[n * (BLOCK // HEAD) + i, pl.ds(row, size)], sems.at[to, p * (BLOCK // HEAD) + i])

        if not start:
            for c in copies(SLOTS[:per]):
                c.wait()
            return
        for k in range(len(SLOTS) // per):

            @pl.when(at == k)
            def _(k=k):
                for c in copies(SLOTS[k * per : (k + 1) * per]):
                    c.start()


class _Hidden:
    prepare = None

    def compute(self, lhs, w, to, at, n, more):
        gate = _dot(lhs[...], w[0])
        up = _dot(lhs[...], w[1])
        to[...] = (jax.nn.silu(gate) * up).astype(jnp.bfloat16)

    def store(self, stage, out_ref, sems, to, at, n, size, side, start):
        c = pltpu.make_async_copy(stage.at[to], out_ref.at[pl.ds(pl.multiple_of(at * BLOCK, BLOCK), BLOCK),
                                                           pl.ds(pl.multiple_of(n * BLOCK, BLOCK), BLOCK)], sems.at[to, 0])
        c.start() if start else c.wait()


def gathered(x, gain, weights, finish, per_step, ring, out_shape, number, name, extra=(), scratch=(), copies=1, turns=None):
    rows, depth = x.shape
    n = lax.axis_size("tp")
    side = int(round(n**0.5))
    columns = [w.shape[1] // BLOCK for w in weights]
    width = sum(w.shape[1] for w in weights)
    return pl.pallas_call(
        functools.partial(_gather_kernel, side=side, per_step=per_step, columns=columns, finish=finish, extra=len(extra), turns=turns),
        out_shape=out_shape,
        in_specs=[pl.BlockSpec(memory_space=pl.ANY), pl.BlockSpec(memory_space=pltpu.VMEM)]
        + [pl.BlockSpec(memory_space=pl.ANY)] * (len(extra) + len(weights)),
        out_specs=pl.BlockSpec(memory_space=pl.ANY),
        scratch_shapes=[
            pltpu.VMEM((n * rows, depth), jnp.bfloat16),
            pltpu.VMEM((ring, per_step, depth, BLOCK), jnp.bfloat16),
            pltpu.VMEM((2, BLOCK, BLOCK), jnp.bfloat16),
            pltpu.SemaphoreType.DMA((1,)),
            pltpu.SemaphoreType.DMA((ring, per_step)),
            pltpu.SemaphoreType.DMA((2, copies)),
            pltpu.SemaphoreType.DMA((len(COPIES),)),
            pltpu.SemaphoreType.DMA((len(SLOTS), 2)),
            pltpu.SemaphoreType.REGULAR,
            *scratch,
        ],
        compiler_params=pltpu.CompilerParams(collective_id=number, has_side_effects=True, vmem_limit_bytes=VMEM),
        cost_estimate=pl.CostEstimate(flops=2 * n * rows * depth * width, transcendentals=0, bytes_accessed=2 * len(EVENTS) * depth * width),
        name=name,
    )(x, gain, *extra, *weights)


def _scatter_kernel(rows_ref, x_ref, w_ref, out_ref, hid, res, out, w, far, plain, summed, near, keep, own, r_far, r_plain, r_summed,
                    r_half, r_near, sems_h, sems_x, sems_w, sems_o, s_far, s_plain, s_summed, s_half, s_near, t_far, t_plain, t_summed,
                    t_half, t_near, *, side, where):
    rows, width = out_ref.shape
    size = rows // 2
    low = size // 2
    tile = w.shape[2]
    tiles = width // tile
    ring = r_far.shape[0]
    group = hid.shape[0] // 4

    def fetch(n):
        return pltpu.make_async_copy(rows_ref.at[pl.ds(where(ORDER[n], size, side), size)], hid.at[pl.ds(n * size, size)], sems_h.at[n])

    def fetched(g):
        for n in range(g * 8, g * 8 + 8):
            fetch(n).wait()

    def weights(j):
        slot = lax.rem(j, 4)
        return pltpu.make_async_copy(w_ref.at[:, pl.ds(pl.multiple_of(j * tile, tile), tile)], w.at[slot], sems_w.at[slot])

    def term(g, j):
        return _dot(hid[pl.ds(g * group, group), :], w[lax.rem(j, 4)]).reshape(8, size, tile)

    def move(l, src, dst, s_sem, t_sem, j):
        return _copy(side, LINKS[l], src, dst, s_sem, t_sem)

    def pairs(src, dst, s_sem, t_sem, j):
        a, b = lax.rem(j, 2), lax.rem(j, ring)
        return [_copy(side, LINKS[l], src.at[a, pl.ds(2 * l, 2)], dst.at[b, pl.ds(2 * l, 2)], s_sem.at[a, l], t_sem.at[b, l])
                for l in range(4)]

    def spot(l):
        return (A if l >= 2 else B), l % 2

    def halves(j):
        a, b = lax.rem(j, 2), lax.rem(j, ring)
        return [_copy(side, LINKS[l], near.at[a, 0, l], r_half.at[b, l], s_half.at[a, l], t_half.at[b, l]) for l in range(4)]

    def lasts(j, part):
        a, b = lax.rem(j, 2), lax.rem(j, ring)
        got = []
        for l in range(4):
            at = spot(l)[1] if part else 1 - spot(l)[1]
            got.append(_copy(side, LINKS[l], near.at[a, 1 + part, l], r_near.at[b, l, pl.ds(at * low, low)], s_near.at[a, part, l],
                             t_near.at[b, part, l]))
        return got

    def each(copies, what):
        for c in copies:
            getattr(c, what)()

    def out_copy(j):
        here = pl.ds(pl.multiple_of(j * tile, tile), tile)
        return pltpu.make_async_copy(out.at[:, here], out_ref.at[:, here], sems_o.at[j])

    for n in range(8):
        fetch(n).start()
    weights(0).start()
    for n in range(8, len(ORDER)):
        fetch(n).start()
    residual = pltpu.make_async_copy(x_ref, res, sems_x.at[0])
    residual.start()
    _meet(side)

    def step(i, _):
        @pl.when(i < tiles)
        def _():
            j = i

            @pl.when(j == 0)
            def _():
                fetched(0)

            @pl.when(j + 1 < tiles)
            def _():
                weights(j + 1).start()

            weights(j).wait()

            @pl.when(j >= 2)
            def _():
                each(pairs(far, r_far, s_far, t_far, j), "wait_send")
                each(pairs(plain, r_plain, s_plain, t_plain, j), "wait_send")

            far[lax.rem(j, 2)] = term(0, j).astype(jnp.bfloat16)
            each(pairs(far, r_far, s_far, t_far, j), "start")

            @pl.when(j == 0)
            def _():
                fetched(1)

            plain[lax.rem(j, 2)] = term(1, j).astype(jnp.bfloat16)
            each(pairs(plain, r_plain, s_plain, t_plain, j), "start")

        @pl.when((i >= 1) & (i < tiles + 1))
        def _():
            j = i - 1

            @pl.when(j == 0)
            def _():
                fetched(2)

            @pl.when(j >= 2)
            def _():
                each(pairs(summed, r_summed, s_summed, t_summed, j), "wait_send")

            each(pairs(far, r_far, s_far, t_far, j), "wait_recv")
            summed[lax.rem(j, 2)] = (term(2, j) + r_far[lax.rem(j, ring)].astype(jnp.float32)).astype(jnp.bfloat16)
            each(pairs(summed, r_summed, s_summed, t_summed, j), "start")

        @pl.when((i >= 2) & (i < tiles + 2))
        def _():
            j = i - 2
            a, b = lax.rem(j, 2), lax.rem(j, ring)

            @pl.when(j == 0)
            def _():
                fetched(3)

            @pl.when(j >= 2)
            def _():
                each(halves(j), "wait_send")
                each(lasts(j, 0), "wait_send")

            each(pairs(plain, r_plain, s_plain, t_plain, j), "wait_recv")
            each(pairs(summed, r_summed, s_summed, t_summed, j), "wait_recv")
            mine = term(3, j)
            for half in (A, B):
                l = 2 * half
                from_up = [r_summed[b, 2 * l + k] for k in range(2)] + [r_plain[b, 2 * l + k] for k in range(2)]
                from_down = [r_plain[b, 2 * l + 2 + k] for k in range(2)] + [r_summed[b, 2 * l + 2 + k] for k in range(2)]
                sums = {across: mine[4 * half + k] + from_up[k].astype(jnp.float32) + from_down[k].astype(jnp.float32)
                        for k, across in enumerate(UP + DOWN)}
                own[lax.rem(j, 4), half] = sums[0]
                l = 2 if half == A else 0
                near[a, 0, l] = sums[2][:low].astype(jnp.bfloat16)
                near[a, 0, l + 1] = sums[2][low:].astype(jnp.bfloat16)
                near[a, 1, l] = sums[1][low:].astype(jnp.bfloat16)
                near[a, 1, l + 1] = sums[-1][:low].astype(jnp.bfloat16)
                keep[a, l] = sums[1][:low]
                keep[a, l + 1] = sums[-1][low:]
            each(halves(j), "start")
            each(lasts(j, 0), "start")

        @pl.when((i >= 3) & (i < tiles + 3))
        def _():
            j = i - 3
            a, b = lax.rem(j, 2), lax.rem(j, ring)

            @pl.when(j >= 2)
            def _():
                each(lasts(j, 1), "wait_send")

            each(halves(j), "wait_recv")
            for l in range(4):
                near[a, 2, l] = (keep[a, l] + r_half[b, l].astype(jnp.float32)).astype(jnp.bfloat16)
            each(lasts(j, 1), "start")

        @pl.when(i >= 4)
        def _():
            j = i - 4
            b = lax.rem(j, ring)

            @pl.when(j == 0)
            def _():
                residual.wait()

            each(lasts(j, 0), "wait_recv")
            each(lasts(j, 1), "wait_recv")
            here = pl.ds(pl.multiple_of(j * tile, tile), tile)
            for half in (A, B):
                l = 2 if half == A else 0
                total = own[lax.rem(j, 4), half] + r_near[b, l].astype(jnp.float32) + r_near[b, l + 1].astype(jnp.float32)
                mine = pl.ds(half * size, size)
                out[mine, here] = (res[mine, here].astype(jnp.float32) + total).astype(jnp.bfloat16)
            out_copy(j).start()

    lax.fori_loop(0, tiles + 4, step, None)
    for j in range(tiles - 2, tiles):
        each(pairs(far, r_far, s_far, t_far, j), "wait_send")
        each(pairs(plain, r_plain, s_plain, t_plain, j), "wait_send")
        each(pairs(summed, r_summed, s_summed, t_summed, j), "wait_send")
        each(halves(j), "wait_send")
        each(lasts(j, 0), "wait_send")
        each(lasts(j, 1), "wait_send")
    for j in range(tiles):
        out_copy(j).wait()


def _in_sequence(p, size, side):
    half, dx, dy = p
    return pl.multiple_of(_device(side, dx, dy) * (2 * size) + half * size, size)


def _in_slots(p, size, side):
    return SLOT[p] * size


def scattered(terms, x, w, where, number, name):
    rows, width = x.shape
    depth = w.shape[0]
    n = lax.axis_size("tp")
    side = int(round(n**0.5))
    size, low = rows // 2, rows // 4
    tile = min(TILE, width)
    tiles = width // tile
    bf, f32, dma = jnp.bfloat16, jnp.float32, pltpu.SemaphoreType.DMA
    return pl.pallas_call(
        functools.partial(_scatter_kernel, side=side, where=where),
        out_shape=jax.ShapeDtypeStruct((rows, width), bf),
        in_specs=[pl.BlockSpec(memory_space=pl.ANY)] * 3,
        out_specs=pl.BlockSpec(memory_space=pl.ANY),
        scratch_shapes=[
            pltpu.VMEM((n * rows, depth), bf),
            pltpu.VMEM((rows, width), bf),
            pltpu.VMEM((rows, width), bf),
            pltpu.VMEM((4, depth, tile), bf),
            pltpu.VMEM((2, 8, size, tile), bf),
            pltpu.VMEM((2, 8, size, tile), bf),
            pltpu.VMEM((2, 8, size, tile), bf),
            pltpu.VMEM((2, 3, 4, low, tile), bf),
            pltpu.VMEM((2, 4, low, tile), f32),
            pltpu.VMEM((4, 2, size, tile), f32),
            pltpu.VMEM((RING, 8, size, tile), bf),
            pltpu.VMEM((RING, 8, size, tile), bf),
            pltpu.VMEM((RING, 8, size, tile), bf),
            pltpu.VMEM((RING, 4, low, tile), bf),
            pltpu.VMEM((RING, 4, size, tile), bf),
            dma((len(ORDER),)), dma((1,)), dma((4,)), dma((tiles,)),
            dma((2, 4)), dma((2, 4)), dma((2, 4)), dma((2, 4)), dma((2, 2, 4)),
            dma((RING, 4)), dma((RING, 4)), dma((RING, 4)), dma((RING, 4)), dma((RING, 2, 4)),
        ],
        compiler_params=pltpu.CompilerParams(collective_id=number, has_side_effects=True, vmem_limit_bytes=VMEM),
        cost_estimate=pl.CostEstimate(flops=2 * n * rows * depth * width, transcendentals=0, bytes_accessed=2 * depth * width),
        name=name,
    )(terms, x, w)


def _attend_kernel(q_ref, k_ref, v_ref, o_ref, top_s, mix_s, gap_s, *, scale, bk):
    heads, bq, d = q_ref.shape
    cols, low = bq, k_ref.dtype
    iq = pl.program_id(0)
    e = scale * LOG2E
    wide = min(cols, STRIP)
    pieces = [(i, at) for i in range(heads) for at in range(0, cols, wide)]
    gap_s[...] = lax.broadcasted_iota(jnp.int32, gap_s.shape, 1) - lax.broadcasted_iota(jnp.int32, gap_s.shape, 0)
    top_s[...] = jnp.full(top_s.shape, NEG, jnp.float32)
    mix_s[...] = jnp.zeros(mix_s.shape, jnp.float32)
    ones = jnp.ones((8, bk), low)

    def block(j, masked):
        here = pl.ds(pl.multiple_of(j * bk, bk), bk)
        scores = [_dot(k_ref[i, here, :], q_ref[i, at : at + wide, :], 1, 1) for i, at in pieces]
        ok = gap_s[...] >= j * bk - iq * bq if masked else None
        weights, keeps = [], []
        for (i, at), s in zip(pieces, scores):
            if masked:
                s = jnp.where(ok[:, at : at + wide], s, HIDDEN)
            old = top_s[i : i + 1, at : at + wide]
            top = jnp.maximum(old, s.max(axis=0, keepdims=True))
            top_s[i : i + 1, at : at + wide] = top
            weights.append(jnp.exp2((s - top) * e).astype(low))
            keeps.append(jnp.exp2((old - top) * e))
        for (i, at), p, keep in zip(pieces, weights, keeps):
            values = jnp.concatenate([v_ref[i, here, :].T, ones], axis=0)
            mix_s[i, :, at : at + wide] = mix_s[i, :, at : at + wide] * keep + _dot(values, p, 1, 0)

    whole = lax.div(iq * bq, bk)
    last = lax.div((iq + 1) * bq, bk)
    lax.fori_loop(0, whole, lambda j, _: block(j, False), None)
    lax.fori_loop(whole, last, lambda j, _: block(j, True), None)
    for i in range(heads):
        total = mix_s[i, d : d + 1, :]
        o_ref[:, i * d : (i + 1) * d] = (mix_s[i, :d, :] * (1 / total)).T.astype(o_ref.dtype)


def attended(qkv, bq=1024, bk=512):
    heads, tokens, d = qkv.shape[0] // 3, *qkv.shape[1:]
    bq, bk = min(bq, tokens), min(bk, tokens)
    return pl.pallas_call(
        functools.partial(_attend_kernel, scale=d**-0.5, bk=bk),
        grid=(tokens // bq,),
        in_specs=[pl.BlockSpec((heads, bq, d), lambda i: (0, i, 0)), pl.BlockSpec((heads, tokens, d), lambda i: (1, 0, 0)),
                  pl.BlockSpec((heads, tokens, d), lambda i: (2, 0, 0))],
        out_specs=pl.BlockSpec((bq, heads * d), lambda i: (i, 0)),
        out_shape=jax.ShapeDtypeStruct((tokens, heads * d), qkv.dtype),
        scratch_shapes=[pltpu.VMEM((heads, bq), jnp.float32), pltpu.VMEM((heads, d + 8, bq), jnp.float32), pltpu.VMEM((bk, bq), jnp.int32)],
        compiler_params=pltpu.CompilerParams(dimension_semantics=("arbitrary",), vmem_limit_bytes=VMEM),
        cost_estimate=pl.CostEstimate(flops=4 * heads * tokens * tokens * d, transcendentals=heads * tokens * tokens,
                                      bytes_accessed=8 * heads * tokens * d),
        name="attended",
    )(qkv, qkv, qkv)


def _angles(tokens):
    half = HEAD // 2
    rate = np.power(np.float32(THETA), -np.arange(half, dtype=np.float32) / np.float32(half)).astype(np.float32)
    angle = (np.arange(tokens, dtype=np.float32)[:, None] * rate).astype(np.float64)
    return np.concatenate([np.cos(angle), np.sin(angle)], 1).astype(np.float32)


def solution(mesh):
    n = mesh.shape["tp"]

    def step(x, gain_a, wq, wk, wv, wo, gain_m, w_gate, w_up, w_down):
        rows = n * x.shape[0]
        heads = wq.shape[1] // HEAD
        turned_steps = 2 * wq.shape[1] // BLOCK
        qkv = gathered(
            x, gain_a, (wq, wk, wv), _Heads(turned_steps), 1, 3, jax.ShapeDtypeStruct((3 * heads, rows, HEAD), jnp.bfloat16), 0, "gather_qkv",
            extra=(jnp.asarray(_angles(rows)),),
            scratch=(pltpu.VMEM((rows, HEAD), jnp.float32), pltpu.SemaphoreType.DMA((len(SLOTS),))),
            copies=(BLOCK // (x.shape[0] // 2)) * (BLOCK // HEAD),
            turns=TURN if mesh.shape["dp"] % 2 == 0 else None,
        )
        h = scattered(attended(qkv), x, wo, _in_sequence, 1, "scatter_o")
        hidden = gathered(h, gain_m, (w_gate, w_up), _Hidden(), 2, 2, jax.ShapeDtypeStruct((rows, w_gate.shape[1]), jnp.bfloat16), 2,
                          "gather_hidden")
        return scattered(hidden, h, w_down, _in_slots, 3, "scatter_down")

    tokens, columns, rows_of = P(("dp", "tp"), None), P(None, "tp"), P("tp", None)
    return jax.shard_map(
        step,
        mesh=mesh,
        in_specs=(tokens, P(None), columns, columns, columns, rows_of, P(None), columns, columns, rows_of),
        out_specs=tokens,
        check_vma=False,
    )
```

```python
import functools

import jax
import jax.numpy as jnp
import numpy as np
from jax import lax
from jax.experimental import pallas as pl
from jax.experimental.pallas import tpu as pltpu
from jax.sharding import PartitionSpec as P

MESH = pl.DeviceIdType.MESH
HEAD = 128
THETA = 10000
NEG = -1e30
HIDDEN = 2 * NEG
LOG2E = 1.4426950408889634
VMEM = 62 * 2**20
LAST_VMEM = 44 * 2**20
STRIP = 512
BLOCK = 256
TILE = 512
TURN = 6
RING = 8

A, B = 0, 1
FAR = 2
UP, DOWN = (0, -1), (1, FAR)
LINKS = (("y", 1), ("y", -1), ("x", 1), ("x", -1))


def piece(half, along, across):
    return (half, across, along) if half == A else (half, along, across)


def both(along, across):
    return [piece(A, along, across), piece(B, along, across)]


NEXT = (-1, 1)
SLOTS = [
    p
    for group in (
        [both(0, 0)],
        [[piece(half, 0, d) for d in NEXT] for half in (A, B)],
        [[piece(half, d, 0) for d in NEXT] for half in (A, B)],
        [both(0, FAR)],
        *([[piece(half, d, across) for d in NEXT] for half in (A, B)] for across in NEXT),
        [both(FAR, 0), both(1, FAR), both(-1, FAR), both(FAR, 1), both(FAR, -1), both(FAR, FAR)],
    )
    for some in group
    for p in some
]
SLOT = {p: n for n, p in enumerate(SLOTS)}

def _by_link(along, pick):
    return [
        piece(half, along if along == 2 else sign * along, across)
        for (axis, sign) in LINKS
        for half in [A if axis == "y" else B]
        for across in (UP if (sign > 0) == pick else DOWN)
    ]


ORDER = _by_link(2, True) + _by_link(1, False) + _by_link(1, True) + [piece(half, 0, across) for half in (A, B) for across in UP + DOWN]


def _place(side):
    me = lax.axis_index("tp")
    return lax.div(me, side), lax.rem(me, side)


def _device(side, dx, dy):
    x, y = _place(side)
    return lax.rem(x + (dx + side), side) * side + lax.rem(y + (dy + side), side)


def _meet(side, twin=False):
    barrier = pltpu.get_barrier_semaphore()
    for dx, dy in ((1, 0), (-1, 0), (0, 1), (0, -1)):
        pl.semaphore_signal(barrier, inc=1, device_id={"tp": _device(side, dx, dy)}, device_id_type=MESH)
    if twin:
        pl.semaphore_signal(barrier, inc=1, device_id=_twin(), device_id_type=MESH)
    pl.semaphore_wait(barrier, 5 if twin else 4)


def _twin():
    group = lax.axis_index("dp")
    return {"dp": group + 1 - 2 * lax.rem(group, 2), "tp": lax.axis_index("tp")}


def _step(link):
    axis, sign = link
    return (sign, 0) if axis == "x" else (0, sign)


def _copy(side, link, src, dst, send_sem, recv_sem):
    return pltpu.make_async_remote_copy(src_ref=src, dst_ref=dst, send_sem=send_sem, recv_sem=recv_sem,
                                        device_id={"tp": _device(side, *_step(link))}, device_id_type=MESH)


def _dot(a, b, ca=1, cb=0):
    return lax.dot_general(a, b, (((ca,), (cb,)), ((), ())), preferred_element_type=jnp.float32)


def _plan():
    slot = lambda half, along, across: SLOT[piece(half, along, across)]

    def inner(half, sign, source, target, part=0, parts=1):
        return ("xy"[half], sign), slot(half, 0, source), slot(half, 0, target), part, parts

    def outer(half, sign, source, across):
        target = -sign if source == 0 else FAR
        return ("yx"[half], sign), slot(half, source, across), slot(half, target, across), 0, 1

    halves, signs = (A, B), (1, -1)
    return [
        [inner(A, sign, 0, -sign) for sign in signs],
        [inner(B, sign, 0, -sign) for sign in signs],
        [outer(half, sign, 0, 0) for half in (B, A) for sign in signs],
        [inner(half, sign, -sign, FAR, int(sign < 0), 2) for half in halves for sign in signs]
        + [outer(half, sign, 0, across) for across in NEXT for half in halves for sign in signs],
        [outer(half, 1, -1, 0) for half in halves],
        [outer(half, sign, 0, FAR) for half in halves for sign in signs],
        [outer(half, 1, -1, -1) for half in halves],
        [outer(half, -1, 1, 1) for half in halves],
        [outer(half, -1, 1, FAR) for half in halves],
    ]


PLAN = _plan()
COPIES = [c for group in PLAN for c in group]
EVENTS = [
    [(SLOTS[2:6], 3), (SLOTS[6:10], 4)],
    [(SLOTS[10:12], 5), (SLOTS[12:16], 6)],
    [(SLOTS[16:20], 7), (SLOTS[20:24], 8)],
    [(SLOTS[24:28], None)],
    [(SLOTS[28:], None)],
]


def _gather_kernel(x_ref, gain_ref, *refs, side, n_weights, finish, extra, turns):
    extra_refs, refs = refs[:extra], refs[extra:]
    w_refs, refs = refs[:n_weights], refs[n_weights:]
    out_ref, g, w, stage, sems_x, sems_w, sems_o, send, recv, turn = refs[:10]
    more = refs[10:]
    rows = x_ref.shape[0]
    size = rows // 2
    ring, wide = w.shape[0], w.shape[2]
    tiles = sum(ref.shape[1] for ref in w_refs) // wide
    total = len(EVENTS) * tiles

    def weights(s, start):
        finish.weights(w_refs, lax.rem(s, tiles), w, lax.rem(s, ring), sems_w, "start" if start else "wait")

    def remote(number):
        link, src, dst, part, parts = COPIES[number]
        height = size // parts
        return _copy(side, link, g.at[pl.ds(src * size + part * height, height)], g.at[pl.ds(dst * size + part * height, height)],
                     send.at[number], recv.at[dst, part])

    def begin(group):
        first = sum(len(p) for p in PLAN[:group])
        for number in range(first, first + len(PLAN[group])):
            remote(number).start()

    def arrived(slots):
        for number, (_, _, dst, _, _) in enumerate(COPIES):
            if SLOTS[dst] in slots:
                remote(number).wait_recv()

    own = [pltpu.make_async_copy(x_ref.at[here], g.at[here], sems_x.at[half]) for half in (A, B) for here in [pl.ds(half * size, size)]]
    for c in own:
        c.start()
    for s in range(ring - 1):
        weights(s, True)
    after = finish.prepare(extra_refs, more) if finish.prepare else None
    _meet(side, turns)

    def norm(i, _):
        here = pl.ds(pl.multiple_of(i * 16, 16), 16)
        wide = g[here, :].astype(jnp.float32)
        scale = lax.rsqrt(jnp.mean(wide * wide, -1, keepdims=True) + 1e-6)
        g[here, :] = (wide * scale * gain_ref[...].astype(jnp.float32)[None]).astype(jnp.bfloat16)

    for half in (A, B):
        own[half].wait()
        lax.fori_loop(half * size // 16, (half + 1) * size // 16, norm, None)
        if turns and half == A:
            @pl.when(lax.rem(lax.axis_index("dp"), 2) == 0)
            def _():
                pl.semaphore_wait(turn, 1)

        begin(half)
    begin(2)
    if after:
        after()

    def block(b, _):
        for k, events in enumerate(EVENTS):

            @pl.when(b == k)
            def _(events=events):
                for slots, group in events:
                    arrived(slots)
                    if group is not None:
                        begin(group)
                    if turns and group == turns:

                        @pl.when(lax.rem(lax.axis_index("dp"), 2) == 1)
                        def _():
                            pl.semaphore_signal(turn, inc=1, device_id=_twin(), device_id_type=MESH)

        first = 2 * b - lax.div(b, 4)
        count = 2 - lax.div(b, 3)

        def tile(n, _):
            s = b * tiles + n

            @pl.when(s + (ring - 1) < total)
            def _():
                weights(s + (ring - 1), True)

            weights(s, False)
            slot = lax.rem(s, ring)

            def product(m, _):
                at = first + m
                lhs = g.at[pl.ds(pl.multiple_of(at * BLOCK, BLOCK), BLOCK)]
                to = lax.rem(n * count + m, 2)

                @pl.when((b > 0) | (n > 0))
                def _():
                    finish.store(stage, out_ref, sems_o, to, at, n, size, side, start=False)

                finish.compute(lhs, w.at[slot], stage.at[to], at, n, more)
                finish.store(stage, out_ref, sems_o, to, at, n, size, side, start=True)

            lax.fori_loop(0, count, product, None)

        lax.fori_loop(0, tiles, tile, None)

    lax.fori_loop(0, len(EVENTS), block, None)
    for to in range(2):
        finish.store(stage, out_ref, sems_o, to, 0, 0, size, side, start=False)
    for number in range(len(COPIES)):
        remote(number).wait_send()


class _Heads:
    def __init__(self, turned_steps):
        self.turned_steps = turned_steps

    def weights(self, refs, n, w, slot, sems, what):
        for at, ref in enumerate(refs):

            @pl.when(n == at)
            def _(ref=ref):
                getattr(pltpu.make_async_copy(ref, w.at[slot], sems.at[slot, 0]), what)()

    def prepare(self, extra_refs, more):
        (table_ref,) = extra_refs
        table, sems = more
        size = table.shape[0] // len(SLOTS)
        side = int(round((len(SLOTS) // 2) ** 0.5))
        copies = []
        for n, (half, dx, dy) in enumerate(SLOTS):
            row = _device(side, dx, dy) * (2 * size) + half * size
            copies.append(pltpu.make_async_copy(table_ref.at[pl.ds(pl.multiple_of(row, size), size)], table.at[pl.ds(n * size, size)],
                                                sems.at[n]))
        for c in copies:
            c.start()

        def after():
            for c in copies:
                c.wait()

        return after

    def compute(self, lhs, w, to, at, n, more):
        table = more[0]
        got = _dot(lhs[...], w[...]).astype(jnp.bfloat16)

        @pl.when(n < self.turned_steps)
        def _():
            t = table[pl.ds(pl.multiple_of(at * BLOCK, BLOCK), BLOCK), :]
            swapped = pltpu.roll(t, HEAD // 2, 1)
            low = lax.broadcasted_iota(jnp.int32, t.shape, 1) < HEAD // 2
            cos, sin = jnp.where(low, t, swapped), jnp.where(low, -swapped, t)
            for i in range(0, w.shape[1], HEAD):
                one = got[:, i : i + HEAD].astype(jnp.float32)
                to[:, i : i + HEAD] = (one * cos + pltpu.roll(one, HEAD // 2, 1) * sin).astype(jnp.bfloat16)

        @pl.when(n >= self.turned_steps)
        def _():
            to[...] = got

    def store(self, stage, out_ref, sems, to, at, n, size, side, start):
        per = BLOCK // size

        heads = stage.shape[2] // HEAD

        def copies(pieces):
            for p, (half, dx, dy) in enumerate(pieces):
                row = pl.multiple_of(_device(side, dx, dy) * (2 * size) + half * size, size)
                for i in range(heads):
                    yield pltpu.make_async_copy(stage.at[to, pl.ds(p * size, size), pl.ds(i * HEAD, HEAD)],
                                                out_ref.at[n * heads + i, pl.ds(row, size)], sems.at[to, p * heads + i])

        if not start:
            for c in copies(SLOTS[:per]):
                c.wait()
            return
        for k in range(len(SLOTS) // per):

            @pl.when(at == k)
            def _(k=k):
                for c in copies(SLOTS[k * per : (k + 1) * per]):
                    c.start()


class _Hidden:
    prepare = None

    def weights(self, refs, n, w, slot, sems, what):
        for at, ref in enumerate(refs):
            here = pl.ds(pl.multiple_of(n * BLOCK, BLOCK), BLOCK)
            getattr(pltpu.make_async_copy(ref.at[:, here], w.at[slot, :, pl.ds(at * BLOCK, BLOCK)], sems.at[slot, at]), what)()

    def compute(self, lhs, w, to, at, n, more):
        got = _dot(lhs[...], w[...])
        to[...] = (jax.nn.silu(got[:, :BLOCK]) * got[:, BLOCK:]).astype(jnp.bfloat16)

    def store(self, stage, out_ref, sems, to, at, n, size, side, start):
        c = pltpu.make_async_copy(stage.at[to], out_ref.at[pl.ds(pl.multiple_of(at * BLOCK, BLOCK), BLOCK),
                                                           pl.ds(pl.multiple_of(n * BLOCK, BLOCK), BLOCK)], sems.at[to, 0])
        c.start() if start else c.wait()


def gathered(x, gain, weights, finish, stored, out_shape, number, name, extra=(), scratch=(), turns=None):
    rows, depth = x.shape
    n = lax.axis_size("tp")
    side = int(round(n**0.5))
    width = sum(w.shape[1] for w in weights)
    anywhere, dma = pl.BlockSpec(memory_space=pl.ANY), pltpu.SemaphoreType.DMA
    return pl.pallas_call(
        functools.partial(_gather_kernel, side=side, n_weights=len(weights), finish=finish, extra=len(extra), turns=turns),
        out_shape=out_shape,
        in_specs=[anywhere, pl.BlockSpec(memory_space=pltpu.VMEM)] + [anywhere] * (len(extra) + len(weights)),
        out_specs=anywhere,
        scratch_shapes=[
            pltpu.VMEM((n * rows, depth), jnp.bfloat16),
            pltpu.VMEM((2, depth, 2 * BLOCK), jnp.bfloat16),
            pltpu.VMEM((2, BLOCK, stored), jnp.bfloat16),
            dma((2,)), dma((2, 2)), dma((2, len(SLOTS))), dma((len(COPIES),)), dma((len(SLOTS), 2)),
            pltpu.SemaphoreType.REGULAR,
            *scratch,
        ],
        compiler_params=pltpu.CompilerParams(collective_id=number, has_side_effects=True, vmem_limit_bytes=VMEM),
        cost_estimate=pl.CostEstimate(flops=2 * n * rows * depth * width, transcendentals=0, bytes_accessed=2 * len(EVENTS) * depth * width),
        name=name,
    )(x, gain, *extra, *weights)


def _scatter_kernel(rows_ref, x_ref, w_ref, out_ref, hid, res, out, w, far, plain, summed, near, keep, own, r_far, r_plain, r_summed,
                    r_half, r_near, sems_h, sems_x, sems_w, sems_o, s_far, s_plain, s_summed, s_half, s_near, t_far, t_plain, t_summed,
                    t_half, t_near, *, side, where, last):
    rows, width = out_ref.shape
    out = out_ref if last else out
    size = rows // 2
    low = size // 2
    tile = w.shape[2]
    tiles = width // tile
    ring = r_far.shape[0]
    group = hid.shape[0] // 4

    def fetch(n):
        return pltpu.make_async_copy(rows_ref.at[pl.ds(where(ORDER[n], size, side), size)], hid.at[pl.ds(n * size, size)], sems_h.at[n])

    def fetched(g):
        for n in range(g * 8, g * 8 + 8):
            fetch(n).wait()

    def weights(j):
        slot = lax.rem(j, 4)
        return pltpu.make_async_copy(w_ref.at[:, pl.ds(pl.multiple_of(j * tile, tile), tile)], w.at[slot], sems_w.at[slot])

    def term(g, j):
        return _dot(hid[pl.ds(g * group, group), :], w[lax.rem(j, 4)]).reshape(8, size, tile)

    def move(l, src, dst, s_sem, t_sem, j):
        return _copy(side, LINKS[l], src, dst, s_sem, t_sem)

    def pairs(src, dst, s_sem, t_sem, j):
        a, b = lax.rem(j, 2), lax.rem(j, ring)
        return [_copy(side, LINKS[l], src.at[a, pl.ds(2 * l, 2)], dst.at[b, pl.ds(2 * l, 2)], s_sem.at[a, l], t_sem.at[b, l])
                for l in range(4)]

    def spot(l):
        return (A if l >= 2 else B), l % 2

    def halves(j):
        a, b = lax.rem(j, 2), lax.rem(j, ring)
        return [_copy(side, LINKS[l], near.at[a, 0, l], r_half.at[b, l], s_half.at[a, l], t_half.at[b, l]) for l in range(4)]

    def lasts(j, part):
        a, b = lax.rem(j, 2), lax.rem(j, ring)
        got = []
        for l in range(4):
            at = spot(l)[1] if part else 1 - spot(l)[1]
            got.append(_copy(side, LINKS[l], near.at[a, 1 + part, l], r_near.at[b, l, pl.ds(at * low, low)], s_near.at[a, part, l],
                             t_near.at[b, part, l]))
        return got

    def each(copies, what):
        for c in copies:
            getattr(c, what)()

    def out_copy(j):
        here = pl.ds(pl.multiple_of(j * tile, tile), tile)
        return pltpu.make_async_copy(out.at[:, here], out_ref.at[:, here], sems_o.at[j])

    for n in range(8):
        fetch(n).start()
    weights(0).start()
    for n in range(8, len(ORDER)):
        fetch(n).start()
    residual = pltpu.make_async_copy(x_ref, res, sems_x.at[0])
    residual.start()
    _meet(side)

    def step(i, _):
        @pl.when(i < tiles)
        def _():
            j = i

            @pl.when(j == 0)
            def _():
                fetched(0)

            @pl.when(j + 1 < tiles)
            def _():
                weights(j + 1).start()

            weights(j).wait()

            @pl.when(j >= 2)
            def _():
                each(pairs(far, r_far, s_far, t_far, j), "wait_send")
                each(pairs(plain, r_plain, s_plain, t_plain, j), "wait_send")

            far[lax.rem(j, 2)] = term(0, j).astype(jnp.bfloat16)
            each(pairs(far, r_far, s_far, t_far, j), "start")

            @pl.when(j == 0)
            def _():
                fetched(1)

            plain[lax.rem(j, 2)] = term(1, j).astype(jnp.bfloat16)
            each(pairs(plain, r_plain, s_plain, t_plain, j), "start")

        @pl.when((i >= 1) & (i < tiles + 1))
        def _():
            j = i - 1

            @pl.when(j == 0)
            def _():
                fetched(2)

            @pl.when(j >= 2)
            def _():
                each(pairs(summed, r_summed, s_summed, t_summed, j), "wait_send")

            each(pairs(far, r_far, s_far, t_far, j), "wait_recv")
            summed[lax.rem(j, 2)] = (term(2, j) + r_far[lax.rem(j, ring)].astype(jnp.float32)).astype(jnp.bfloat16)
            each(pairs(summed, r_summed, s_summed, t_summed, j), "start")

        @pl.when((i >= 2) & (i < tiles + 2))
        def _():
            j = i - 2
            a, b = lax.rem(j, 2), lax.rem(j, ring)

            @pl.when(j == 0)
            def _():
                fetched(3)

            @pl.when(j >= 2)
            def _():
                each(halves(j), "wait_send")
                each(lasts(j, 0), "wait_send")

            each(pairs(plain, r_plain, s_plain, t_plain, j), "wait_recv")
            each(pairs(summed, r_summed, s_summed, t_summed, j), "wait_recv")
            mine = term(3, j)
            for half in (A, B):
                l = 2 * half
                from_up = [r_summed[b, 2 * l + k] for k in range(2)] + [r_plain[b, 2 * l + k] for k in range(2)]
                from_down = [r_plain[b, 2 * l + 2 + k] for k in range(2)] + [r_summed[b, 2 * l + 2 + k] for k in range(2)]
                sums = {across: mine[4 * half + k] + from_up[k].astype(jnp.float32) + from_down[k].astype(jnp.float32)
                        for k, across in enumerate(UP + DOWN)}
                own[lax.rem(j, 4), half] = sums[0]
                l = 2 if half == A else 0
                near[a, 0, l] = sums[2][:low].astype(jnp.bfloat16)
                near[a, 0, l + 1] = sums[2][low:].astype(jnp.bfloat16)
                near[a, 1, l] = sums[1][low:].astype(jnp.bfloat16)
                near[a, 1, l + 1] = sums[-1][:low].astype(jnp.bfloat16)
                keep[a, l] = sums[1][:low]
                keep[a, l + 1] = sums[-1][low:]
            each(halves(j), "start")
            each(lasts(j, 0), "start")

        @pl.when((i >= 3) & (i < tiles + 3))
        def _():
            j = i - 3
            a, b = lax.rem(j, 2), lax.rem(j, ring)

            @pl.when(j >= 2)
            def _():
                each(lasts(j, 1), "wait_send")

            each(halves(j), "wait_recv")
            for l in range(4):
                near[a, 2, l] = (keep[a, l] + r_half[b, l].astype(jnp.float32)).astype(jnp.bfloat16)
            each(lasts(j, 1), "start")

        @pl.when(i >= 4)
        def _():
            j = i - 4
            b = lax.rem(j, ring)

            @pl.when(j == 0)
            def _():
                residual.wait()

            each(lasts(j, 0), "wait_recv")
            each(lasts(j, 1), "wait_recv")
            here = pl.ds(pl.multiple_of(j * tile, tile), tile)
            for half in (A, B):
                l = 2 if half == A else 0
                total = own[lax.rem(j, 4), half] + r_near[b, l].astype(jnp.float32) + r_near[b, l + 1].astype(jnp.float32)
                mine = pl.ds(half * size, size)
                out[mine, here] = (res[mine, here].astype(jnp.float32) + total).astype(jnp.bfloat16)
            if not last:
                out_copy(j).start()

    lax.fori_loop(0, tiles + 4, step, None)
    for j in range(tiles - 2, tiles):
        each(pairs(far, r_far, s_far, t_far, j), "wait_send")
        each(pairs(plain, r_plain, s_plain, t_plain, j), "wait_send")
        each(pairs(summed, r_summed, s_summed, t_summed, j), "wait_send")
        each(halves(j), "wait_send")
        each(lasts(j, 0), "wait_send")
        each(lasts(j, 1), "wait_send")
    if not last:
        for j in range(tiles):
            out_copy(j).wait()


def _in_sequence(p, size, side):
    half, dx, dy = p
    return pl.multiple_of(_device(side, dx, dy) * (2 * size) + half * size, size)


def _in_slots(p, size, side):
    return SLOT[p] * size


def scattered(terms, x, w, where, number, name, last=False):
    rows, width = x.shape
    depth = w.shape[0]
    n = lax.axis_size("tp")
    side = int(round(n**0.5))
    size, low = rows // 2, rows // 4
    tile = min(TILE, width)
    tiles = width // tile
    bf, f32, dma = jnp.bfloat16, jnp.float32, pltpu.SemaphoreType.DMA
    return pl.pallas_call(
        functools.partial(_scatter_kernel, side=side, where=where, last=last),
        out_shape=jax.ShapeDtypeStruct((rows, width), bf),
        in_specs=[pl.BlockSpec(memory_space=pl.ANY)] * 3,
        out_specs=pl.BlockSpec(memory_space=pltpu.VMEM if last else pl.ANY),
        scratch_shapes=[
            pltpu.VMEM((n * rows, depth), bf),
            pltpu.VMEM((rows, width), bf),
            pltpu.VMEM((rows, TILE if last else width), bf),
            pltpu.VMEM((4, depth, tile), bf),
            pltpu.VMEM((2, 8, size, tile), bf),
            pltpu.VMEM((2, 8, size, tile), bf),
            pltpu.VMEM((2, 8, size, tile), bf),
            pltpu.VMEM((2, 3, 4, low, tile), bf),
            pltpu.VMEM((2, 4, low, tile), f32),
            pltpu.VMEM((4, 2, size, tile), f32),
            pltpu.VMEM((RING, 8, size, tile), bf),
            pltpu.VMEM((RING, 8, size, tile), bf),
            pltpu.VMEM((RING, 8, size, tile), bf),
            pltpu.VMEM((RING, 4, low, tile), bf),
            pltpu.VMEM((RING, 4, size, tile), bf),
            dma((len(ORDER),)), dma((1,)), dma((4,)), dma((tiles,)),
            dma((2, 4)), dma((2, 4)), dma((2, 4)), dma((2, 4)), dma((2, 2, 4)),
            dma((RING, 4)), dma((RING, 4)), dma((RING, 4)), dma((RING, 4)), dma((RING, 2, 4)),
        ],
        compiler_params=pltpu.CompilerParams(collective_id=number, has_side_effects=True, vmem_limit_bytes=LAST_VMEM if last else VMEM),
        cost_estimate=pl.CostEstimate(flops=2 * n * rows * depth * width, transcendentals=0, bytes_accessed=2 * depth * width),
        name=name,
    )(terms, x, w)


def _attend_kernel(q_ref, k_ref, v_ref, o_ref, top_s, mix_s, gap_s, *, scale, bk):
    heads, bq, d = q_ref.shape
    cols, low = bq, k_ref.dtype
    iq = pl.program_id(0)
    e = scale * LOG2E
    wide = min(cols, STRIP)
    pieces = [(i, at) for i in range(heads) for at in range(0, cols, wide)]
    gap_s[...] = lax.broadcasted_iota(jnp.int32, gap_s.shape, 1) - lax.broadcasted_iota(jnp.int32, gap_s.shape, 0)
    top_s[...] = jnp.full(top_s.shape, NEG, jnp.float32)
    mix_s[...] = jnp.zeros(mix_s.shape, jnp.float32)
    ones = jnp.ones((8, bk), low)

    def block(j, masked):
        here = pl.ds(pl.multiple_of(j * bk, bk), bk)
        scores = [_dot(k_ref[i, here, :], q_ref[i, at : at + wide, :], 1, 1) for i, at in pieces]
        ok = gap_s[...] >= j * bk - iq * bq if masked else None
        weights, keeps = [], []
        for (i, at), s in zip(pieces, scores):
            if masked:
                s = jnp.where(ok[:, at : at + wide], s, HIDDEN)
            old = top_s[i : i + 1, at : at + wide]
            top = jnp.maximum(old, s.max(axis=0, keepdims=True))
            top_s[i : i + 1, at : at + wide] = top
            weights.append(jnp.exp2((s - top) * e).astype(low))
            keeps.append(jnp.exp2((old - top) * e))
        for (i, at), p, keep in zip(pieces, weights, keeps):
            values = jnp.concatenate([v_ref[i, here, :].T, ones], axis=0)
            mix_s[i, :, at : at + wide] = mix_s[i, :, at : at + wide] * keep + _dot(values, p, 1, 0)

    whole = lax.div(iq * bq, bk)
    last = lax.div((iq + 1) * bq, bk)
    lax.fori_loop(0, whole, lambda j, _: block(j, False), None)
    lax.fori_loop(whole, last, lambda j, _: block(j, True), None)
    for i in range(heads):
        total = mix_s[i, d : d + 1, :]
        o_ref[:, i * d : (i + 1) * d] = (mix_s[i, :d, :] * (1 / total)).T.astype(o_ref.dtype)


def attended(qkv, bq=1024, bk=512):
    heads, tokens, d = qkv.shape[0] // 3, *qkv.shape[1:]
    bq, bk = min(bq, tokens), min(bk, tokens)
    return pl.pallas_call(
        functools.partial(_attend_kernel, scale=d**-0.5, bk=bk),
        grid=(tokens // bq,),
        in_specs=[pl.BlockSpec((heads, bq, d), lambda i: (0, i, 0)), pl.BlockSpec((heads, tokens, d), lambda i: (1, 0, 0)),
                  pl.BlockSpec((heads, tokens, d), lambda i: (2, 0, 0))],
        out_specs=pl.BlockSpec((bq, heads * d), lambda i: (i, 0)),
        out_shape=jax.ShapeDtypeStruct((tokens, heads * d), qkv.dtype),
        scratch_shapes=[pltpu.VMEM((heads, bq), jnp.float32), pltpu.VMEM((heads, d + 8, bq), jnp.float32), pltpu.VMEM((bk, bq), jnp.int32)],
        compiler_params=pltpu.CompilerParams(dimension_semantics=("arbitrary",), vmem_limit_bytes=VMEM),
        cost_estimate=pl.CostEstimate(flops=4 * heads * tokens * tokens * d, transcendentals=heads * tokens * tokens,
                                      bytes_accessed=8 * heads * tokens * d),
        name="attended",
    )(qkv, qkv, qkv)


def _angles(tokens):
    half = HEAD // 2
    rate = np.power(np.float32(THETA), -np.arange(half, dtype=np.float32) / np.float32(half)).astype(np.float32)
    angle = (np.arange(tokens, dtype=np.float32)[:, None] * rate).astype(np.float64)
    return np.concatenate([np.cos(angle), np.sin(angle)], 1).astype(np.float32)


def solution(mesh):
    n = mesh.shape["tp"]

    def step(x, gain_a, wq, wk, wv, wo, gain_m, w_gate, w_up, w_down):
        rows = n * x.shape[0]
        heads = wq.shape[1] // HEAD
        qkv = gathered(
            x, gain_a, (wq, wk, wv), _Heads(2), 2 * BLOCK, jax.ShapeDtypeStruct((3 * heads, rows, HEAD), jnp.bfloat16), 0, "gather_qkv",
            extra=(jnp.asarray(_angles(rows)),),
            scratch=(pltpu.VMEM((rows, HEAD), jnp.float32), pltpu.SemaphoreType.DMA((len(SLOTS),))),
            turns=TURN if mesh.shape["dp"] % 2 == 0 else None,
        )
        h = scattered(attended(qkv), x, wo, _in_sequence, 1, "scatter_o")
        hidden = gathered(h, gain_m, (w_gate, w_up), _Hidden(), BLOCK, jax.ShapeDtypeStruct((rows, w_gate.shape[1]), jnp.bfloat16), 2,
                          "gather_hidden")
        return scattered(hidden, h, w_down, _in_slots, 3, "scatter_down", last=True)

    tokens, columns, rows_of = P(("dp", "tp"), None), P(None, "tp"), P("tp", None)
    return jax.shard_map(
        step,
        mesh=mesh,
        in_specs=(tokens, P(None), columns, columns, columns, rows_of, P(None), columns, columns, rows_of),
        out_specs=tokens,
        check_vma=False,
    )
```

```python
import functools

import jax
import jax.numpy as jnp
import numpy as np
from jax import lax
from jax.experimental import pallas as pl
from jax.experimental.pallas import tpu as pltpu
from jax.sharding import PartitionSpec as P

MESH = pl.DeviceIdType.MESH
HEAD = 128
THETA = 10000
NEG = -1e30
HIDDEN = 2 * NEG
LOG2E = 1.4426950408889634
VMEM = 62 * 2**20
LAST_VMEM = 44 * 2**20
STRIP = 512
BLOCK = 256
TILE = 512
TURN = 6
RING = 8

A, B = 0, 1
FAR = 2
UP, DOWN = (0, -1), (1, FAR)
LINKS = (("y", 1), ("y", -1), ("x", 1), ("x", -1))


def piece(half, along, across):
    return (half, across, along) if half == A else (half, along, across)


def both(along, across):
    return [piece(A, along, across), piece(B, along, across)]


NEXT = (-1, 1)
SLOTS = [
    p
    for group in (
        [both(0, 0)],
        [[piece(half, 0, d) for d in NEXT] for half in (A, B)],
        [[piece(half, d, 0) for d in NEXT] for half in (A, B)],
        [both(0, FAR)],
        *([[piece(half, d, across) for d in NEXT] for half in (A, B)] for across in NEXT),
        [both(FAR, 0), both(1, FAR), both(-1, FAR), both(FAR, 1), both(FAR, -1), both(FAR, FAR)],
    )
    for some in group
    for p in some
]
SLOT = {p: n for n, p in enumerate(SLOTS)}

def _by_link(along, pick):
    return [
        piece(half, along if along == 2 else sign * along, across)
        for (axis, sign) in LINKS
        for half in [A if axis == "y" else B]
        for across in (UP if (sign > 0) == pick else DOWN)
    ]


ORDER = _by_link(2, True) + _by_link(1, False) + _by_link(1, True) + [piece(half, 0, across) for half in (A, B) for across in UP + DOWN]


def _place(side):
    me = lax.axis_index("tp")
    return lax.div(me, side), lax.rem(me, side)


def _device(side, dx, dy):
    x, y = _place(side)
    return lax.rem(x + (dx + side), side) * side + lax.rem(y + (dy + side), side)


def _meet(side, twin=False):
    barrier = pltpu.get_barrier_semaphore()
    others = [{"tp": _device(side, *_step(link))} for link in LINKS] + ([_twin()] if twin else [])
    for other in others:
        pl.semaphore_signal(barrier, inc=1, device_id=other, device_id_type=MESH)
    return lambda: pl.semaphore_wait(barrier, len(others))


def _twin():
    group = lax.axis_index("dp")
    return {"dp": group + 1 - 2 * lax.rem(group, 2), "tp": lax.axis_index("tp")}


def _step(link):
    axis, sign = link
    return (sign, 0) if axis == "x" else (0, sign)


def _copy(side, link, src, dst, send_sem, recv_sem):
    return pltpu.make_async_remote_copy(src_ref=src, dst_ref=dst, send_sem=send_sem, recv_sem=recv_sem,
                                        device_id={"tp": _device(side, *_step(link))}, device_id_type=MESH)


def _dot(a, b, ca=1, cb=0):
    return lax.dot_general(a, b, (((ca,), (cb,)), ((), ())), preferred_element_type=jnp.float32)


def _plan():
    slot = lambda half, along, across: SLOT[piece(half, along, across)]

    def inner(half, sign, source, target, part=0, parts=1):
        return ("xy"[half], sign), slot(half, 0, source), slot(half, 0, target), part, parts

    def outer(half, sign, source, across):
        target = -sign if source == 0 else FAR
        return ("yx"[half], sign), slot(half, source, across), slot(half, target, across), 0, 1

    halves, signs = (A, B), (1, -1)
    return [
        [inner(A, sign, 0, -sign) for sign in signs],
        [inner(B, sign, 0, -sign) for sign in signs],
        [outer(half, sign, 0, 0) for half in (B, A) for sign in signs],
        [inner(half, sign, -sign, FAR, int(sign < 0), 2) for half in halves for sign in signs]
        + [outer(half, sign, 0, across) for across in NEXT for half in halves for sign in signs],
        [outer(half, 1, -1, 0) for half in halves],
        [outer(half, sign, 0, FAR) for half in halves for sign in signs],
        [outer(half, 1, -1, -1) for half in halves],
        [outer(half, -1, 1, 1) for half in halves],
        [outer(half, -1, 1, FAR) for half in halves],
    ]


PLAN = _plan()
COPIES = [c for group in PLAN for c in group]
EVENTS = [
    (SLOTS[2:6], 3), (SLOTS[6:10], 4), (SLOTS[10:12], 5), (SLOTS[12:16], 6), (SLOTS[16:20], 7), (SLOTS[20:24], 8), (SLOTS[24:28], None),
    (SLOTS[28:], None),
]


def _gather_kernel(x_ref, gain_ref, *refs, side, n_weights, finish, extra, turns):
    extra_refs, refs = refs[:extra], refs[extra:]
    w_refs, refs = refs[:n_weights], refs[n_weights:]
    out_ref, g, gain, w, stage, sems_x, sems_w, sems_o, send, recv, turn, *more = refs
    rows = x_ref.shape[0]
    size = rows // 2
    ring, wide = w.shape[0], w.shape[2]
    tiles = sum(ref.shape[1] for ref in w_refs) // wide
    loads = tiles if tiles <= ring else len(EVENTS) * tiles

    def weights(s, start):
        finish.weights(w_refs, lax.rem(s, tiles), w, lax.rem(s, ring), sems_w, "start" if start else "wait")

    def remote(number):
        link, src, dst, part, parts = COPIES[number]
        height = size // parts
        return _copy(side, link, g.at[pl.ds(src * size + part * height, height)], g.at[pl.ds(dst * size + part * height, height)],
                     send.at[number], recv.at[dst, part])

    def begin(group):
        first = sum(len(p) for p in PLAN[:group])
        for number in range(first, first + len(PLAN[group])):
            remote(number).start()

    def arrived(slots):
        for number, (_, _, dst, _, _) in enumerate(COPIES):
            if SLOTS[dst] in slots:
                remote(number).wait_recv()

    met = _meet(side, turns)
    own = [pltpu.make_async_copy(x_ref.at[here], g.at[here], sems_x.at[half]) for half in (A, B) for here in [pl.ds(half * size, size)]]
    gains = pltpu.make_async_copy(gain_ref, gain, sems_x.at[2])
    for c in (own[A], gains, own[B]):
        c.start()

    def norm(i, _):
        here = pl.ds(pl.multiple_of(i * 16, 16), 16)
        wide = g[here, :].astype(jnp.float32)
        scale = lax.rsqrt(jnp.mean(wide * wide, -1, keepdims=True) + 1e-6)
        g[here, :] = (wide * scale * gain[...].astype(jnp.float32)[None]).astype(jnp.bfloat16)

    gains.wait()
    for half in (A, B):
        own[half].wait()
        lax.fori_loop(half * size // 16, (half + 1) * size // 16, norm, None)
        if half == A:
            met()
        if turns and half == A:
            @pl.when(lax.rem(lax.axis_index("dp"), 2) == 0)
            def _():
                pl.semaphore_wait(turn, 1)

        begin(half)
    begin(2)
    for s in range(ring - 1):
        weights(s, True)
    if finish.prepare:
        finish.prepare(extra_refs, more)

    def block(b, _):
        for k, (slots, group) in enumerate(EVENTS):

            @pl.when(b == k)
            def _(slots=slots, group=group):
                arrived(slots)
                if group is not None:
                    begin(group)
                if turns and group == turns:

                    @pl.when(lax.rem(lax.axis_index("dp"), 2) == 1)
                    def _():
                        pl.semaphore_signal(turn, inc=1, device_id=_twin(), device_id_type=MESH)

        def tile(n, _):
            s = b * tiles + n

            @pl.when(s + (ring - 1) < loads)
            def _():
                weights(s + (ring - 1), True)

            @pl.when(s < loads)
            def _():
                weights(s, False)

            to = lax.rem(s, 2)

            @pl.when(s >= 2)
            def _():
                finish.store(stage, out_ref, sems_o, to, b, n, size, side, start=False)

            finish.compute(g.at[pl.ds(pl.multiple_of(b * BLOCK, BLOCK), BLOCK)], w.at[lax.rem(s, ring)], stage.at[to], b, n, more)
            finish.store(stage, out_ref, sems_o, to, b, n, size, side, start=True)

        lax.fori_loop(0, tiles, tile, None)

    lax.fori_loop(0, len(EVENTS), block, None)
    for to in range(2):
        finish.store(stage, out_ref, sems_o, to, 0, 0, size, side, start=False)
    for number in range(len(COPIES)):
        remote(number).wait_send()


class _Heads:
    def __init__(self, turned_steps):
        self.turned_steps = turned_steps

    def weights(self, refs, n, w, slot, sems, what):
        for at, ref in enumerate(refs):

            @pl.when(n == at)
            def _(ref=ref):
                getattr(pltpu.make_async_copy(ref, w.at[slot], sems.at[slot, 0]), what)()

    def prepare(self, extra_refs, more):
        (table_ref,) = extra_refs
        table, sems = more
        size = table.shape[0] // len(SLOTS)
        side = int(round((len(SLOTS) // 2) ** 0.5))
        copies = []
        for n, (half, dx, dy) in enumerate(SLOTS):
            row = _device(side, dx, dy) * (2 * size) + half * size
            copies.append(pltpu.make_async_copy(table_ref.at[pl.ds(pl.multiple_of(row, size), size)], table.at[pl.ds(n * size, size)],
                                                sems.at[n]))
        for what in ("start", "wait"):
            for c in copies:
                getattr(c, what)()

    def compute(self, lhs, w, to, at, n, more):
        table = more[0]
        got = _dot(lhs[...], w[...]).astype(jnp.bfloat16)

        @pl.when(n < self.turned_steps)
        def _():
            t = table[pl.ds(pl.multiple_of(at * BLOCK, BLOCK), BLOCK), :]
            swapped = pltpu.roll(t, HEAD // 2, 1)
            low = lax.broadcasted_iota(jnp.int32, t.shape, 1) < HEAD // 2
            cos, sin = jnp.where(low, t, swapped), jnp.where(low, -swapped, t)
            for i in range(0, w.shape[1], HEAD):
                one = got[:, i : i + HEAD].astype(jnp.float32)
                to[:, i : i + HEAD] = (one * cos + pltpu.roll(one, HEAD // 2, 1) * sin).astype(jnp.bfloat16)

        @pl.when(n >= self.turned_steps)
        def _():
            to[...] = got

    def store(self, stage, out_ref, sems, to, at, n, size, side, start):
        per = BLOCK // size

        heads = stage.shape[2] // HEAD

        def copies(pieces):
            for p, (half, dx, dy) in enumerate(pieces):
                row = pl.multiple_of(_device(side, dx, dy) * (2 * size) + half * size, size)
                for i in range(heads):
                    yield pltpu.make_async_copy(stage.at[to, pl.ds(p * size, size), pl.ds(i * HEAD, HEAD)],
                                                out_ref.at[n * heads + i, pl.ds(row, size)], sems.at[to, p * heads + i])

        if not start:
            for c in copies(SLOTS[:per]):
                c.wait()
            return
        for k in range(len(SLOTS) // per):

            @pl.when(at == k)
            def _(k=k):
                for c in copies(SLOTS[k * per : (k + 1) * per]):
                    c.start()


class _Hidden:
    prepare = None

    def weights(self, refs, n, w, slot, sems, what):
        for at, ref in enumerate(refs):
            here = pl.ds(pl.multiple_of(n * BLOCK, BLOCK), BLOCK)
            getattr(pltpu.make_async_copy(ref.at[:, here], w.at[slot, :, pl.ds(at * BLOCK, BLOCK)], sems.at[slot, at]), what)()

    def compute(self, lhs, w, to, at, n, more):
        got = _dot(lhs[...], w[...])
        to[...] = (jax.nn.silu(got[:, :BLOCK]) * got[:, BLOCK:]).astype(jnp.bfloat16)

    def store(self, stage, out_ref, sems, to, at, n, size, side, start):
        c = pltpu.make_async_copy(stage.at[to], out_ref.at[pl.ds(pl.multiple_of(at * BLOCK, BLOCK), BLOCK),
                                                           pl.ds(pl.multiple_of(n * BLOCK, BLOCK), BLOCK)], sems.at[to, 0])
        c.start() if start else c.wait()


def gathered(x, gain, weights, finish, stored, out_shape, number, name, extra=(), scratch=(), turns=None):
    rows, depth = x.shape
    n = lax.axis_size("tp")
    side = int(round(n**0.5))
    width = sum(w.shape[1] for w in weights)
    anywhere, dma = pl.BlockSpec(memory_space=pl.ANY), pltpu.SemaphoreType.DMA
    return pl.pallas_call(
        functools.partial(_gather_kernel, side=side, n_weights=len(weights), finish=finish, extra=len(extra), turns=turns),
        out_shape=out_shape,
        in_specs=[anywhere] * (2 + len(extra) + len(weights)),
        out_specs=anywhere,
        scratch_shapes=[
            pltpu.VMEM((n * rows, depth), jnp.bfloat16),
            pltpu.VMEM((depth,), jnp.bfloat16),
            pltpu.VMEM((3, depth, 2 * BLOCK), jnp.bfloat16),
            pltpu.VMEM((2, BLOCK, stored), jnp.bfloat16),
            dma((3,)), dma((3, 2)), dma((2, len(SLOTS))), dma((len(COPIES),)), dma((len(SLOTS), 2)),
            pltpu.SemaphoreType.REGULAR,
            *scratch,
        ],
        compiler_params=pltpu.CompilerParams(collective_id=number, has_side_effects=True, vmem_limit_bytes=VMEM),
        cost_estimate=pl.CostEstimate(flops=2 * n * rows * depth * width, transcendentals=0, bytes_accessed=2 * len(EVENTS) * depth * width),
        name=name,
    )(x, gain, *extra, *weights)


def _scatter_kernel(rows_ref, x_ref, w_ref, out_ref, hid, res, out, w, far, plain, summed, near, keep, own, r_far, r_plain, r_summed,
                    r_half, r_near, sems_h, sems_x, sems_w, sems_o, s_far, s_plain, s_summed, s_half, s_near, t_far, t_plain, t_summed,
                    t_half, t_near, *, side, where, last):
    rows, width = out_ref.shape
    out = out_ref if last else out
    size = rows // 2
    low = size // 2
    tile = w.shape[2]
    tiles = width // tile
    ring = r_far.shape[0]
    group = hid.shape[0] // 4

    def fetch(n):
        return pltpu.make_async_copy(rows_ref.at[pl.ds(where(ORDER[n], size, side), size)], hid.at[pl.ds(n * size, size)], sems_h.at[n])

    def fetched(g):
        for n in range(g * 8, g * 8 + 8):
            fetch(n).wait()

    def weights(j):
        slot = lax.rem(j, 4)
        return pltpu.make_async_copy(w_ref.at[:, pl.ds(pl.multiple_of(j * tile, tile), tile)], w.at[slot], sems_w.at[slot])

    def term(g, j):
        return _dot(hid[pl.ds(g * group, group), :], w[lax.rem(j, 4)]).reshape(8, size, tile)

    def move(l, src, dst, s_sem, t_sem, j):
        return _copy(side, LINKS[l], src, dst, s_sem, t_sem)

    def pairs(src, dst, s_sem, t_sem, j):
        a, b = lax.rem(j, 2), lax.rem(j, ring)
        return [_copy(side, LINKS[l], src.at[a, pl.ds(2 * l, 2)], dst.at[b, pl.ds(2 * l, 2)], s_sem.at[a, l], t_sem.at[b, l])
                for l in range(4)]

    def spot(l):
        return (A if l >= 2 else B), l % 2

    def halves(j):
        a, b = lax.rem(j, 2), lax.rem(j, ring)
        return [_copy(side, LINKS[l], near.at[a, 0, l], r_half.at[b, l], s_half.at[a, l], t_half.at[b, l]) for l in range(4)]

    def lasts(j, part):
        a, b = lax.rem(j, 2), lax.rem(j, ring)
        got = []
        for l in range(4):
            at = spot(l)[1] if part else 1 - spot(l)[1]
            got.append(_copy(side, LINKS[l], near.at[a, 1 + part, l], r_near.at[b, l, pl.ds(at * low, low)], s_near.at[a, part, l],
                             t_near.at[b, part, l]))
        return got

    def each(copies, what):
        for c in copies:
            getattr(c, what)()

    def out_copy(j):
        here = pl.ds(pl.multiple_of(j * tile, tile), tile)
        return pltpu.make_async_copy(out.at[:, here], out_ref.at[:, here], sems_o.at[j])

    for n in range(8):
        fetch(n).start()
    weights(0).start()
    for n in range(8, len(ORDER)):
        fetch(n).start()
    residual = pltpu.make_async_copy(x_ref, res, sems_x.at[0])
    residual.start()
    _meet(side)()

    def step(i, _):
        @pl.when(i < tiles)
        def _():
            j = i

            @pl.when(j == 0)
            def _():
                fetched(0)

            @pl.when(j + 1 < tiles)
            def _():
                weights(j + 1).start()

            weights(j).wait()

            @pl.when(j >= 2)
            def _():
                each(pairs(far, r_far, s_far, t_far, j), "wait_send")
                each(pairs(plain, r_plain, s_plain, t_plain, j), "wait_send")

            far[lax.rem(j, 2)] = term(0, j).astype(jnp.bfloat16)
            each(pairs(far, r_far, s_far, t_far, j), "start")

            @pl.when(j == 0)
            def _():
                fetched(1)

            plain[lax.rem(j, 2)] = term(1, j).astype(jnp.bfloat16)
            each(pairs(plain, r_plain, s_plain, t_plain, j), "start")

        @pl.when((i >= 1) & (i < tiles + 1))
        def _():
            j = i - 1

            @pl.when(j == 0)
            def _():
                fetched(2)

            @pl.when(j >= 2)
            def _():
                each(pairs(summed, r_summed, s_summed, t_summed, j), "wait_send")

            each(pairs(far, r_far, s_far, t_far, j), "wait_recv")
            summed[lax.rem(j, 2)] = (term(2, j) + r_far[lax.rem(j, ring)].astype(jnp.float32)).astype(jnp.bfloat16)
            each(pairs(summed, r_summed, s_summed, t_summed, j), "start")

        @pl.when((i >= 2) & (i < tiles + 2))
        def _():
            j = i - 2
            a, b = lax.rem(j, 2), lax.rem(j, ring)

            @pl.when(j == 0)
            def _():
                fetched(3)

            @pl.when(j >= 2)
            def _():
                each(halves(j), "wait_send")
                each(lasts(j, 0), "wait_send")

            each(pairs(plain, r_plain, s_plain, t_plain, j), "wait_recv")
            each(pairs(summed, r_summed, s_summed, t_summed, j), "wait_recv")
            mine = term(3, j)
            for half in (A, B):
                l = 2 * half
                from_up = [r_summed[b, 2 * l + k] for k in range(2)] + [r_plain[b, 2 * l + k] for k in range(2)]
                from_down = [r_plain[b, 2 * l + 2 + k] for k in range(2)] + [r_summed[b, 2 * l + 2 + k] for k in range(2)]
                sums = {across: mine[4 * half + k] + from_up[k].astype(jnp.float32) + from_down[k].astype(jnp.float32)
                        for k, across in enumerate(UP + DOWN)}
                own[lax.rem(j, 4), half] = sums[0]
                l = 2 if half == A else 0
                near[a, 0, l] = sums[2][:low].astype(jnp.bfloat16)
                near[a, 0, l + 1] = sums[2][low:].astype(jnp.bfloat16)
                near[a, 1, l] = sums[1][low:].astype(jnp.bfloat16)
                near[a, 1, l + 1] = sums[-1][:low].astype(jnp.bfloat16)
                keep[a, l] = sums[1][:low]
                keep[a, l + 1] = sums[-1][low:]
            each(halves(j), "start")
            each(lasts(j, 0), "start")

        @pl.when((i >= 3) & (i < tiles + 3))
        def _():
            j = i - 3
            a, b = lax.rem(j, 2), lax.rem(j, ring)

            @pl.when(j >= 2)
            def _():
                each(lasts(j, 1), "wait_send")

            each(halves(j), "wait_recv")
            for l in range(4):
                near[a, 2, l] = (keep[a, l] + r_half[b, l].astype(jnp.float32)).astype(jnp.bfloat16)
            each(lasts(j, 1), "start")

        @pl.when(i >= 4)
        def _():
            j = i - 4
            b = lax.rem(j, ring)

            @pl.when(j == 0)
            def _():
                residual.wait()

            each(lasts(j, 0), "wait_recv")
            each(lasts(j, 1), "wait_recv")
            here = pl.ds(pl.multiple_of(j * tile, tile), tile)
            for half in (A, B):
                l = 2 if half == A else 0
                total = own[lax.rem(j, 4), half] + r_near[b, l].astype(jnp.float32) + r_near[b, l + 1].astype(jnp.float32)
                mine = pl.ds(half * size, size)
                out[mine, here] = (res[mine, here].astype(jnp.float32) + total).astype(jnp.bfloat16)
            if not last:
                out_copy(j).start()

    lax.fori_loop(0, tiles + 4, step, None)
    for j in range(tiles - 2, tiles):
        each(pairs(far, r_far, s_far, t_far, j), "wait_send")
        each(pairs(plain, r_plain, s_plain, t_plain, j), "wait_send")
        each(pairs(summed, r_summed, s_summed, t_summed, j), "wait_send")
        each(halves(j), "wait_send")
        each(lasts(j, 0), "wait_send")
        each(lasts(j, 1), "wait_send")
    if not last:
        for j in range(tiles):
            out_copy(j).wait()


def _in_sequence(p, size, side):
    half, dx, dy = p
    return pl.multiple_of(_device(side, dx, dy) * (2 * size) + half * size, size)


def _in_slots(p, size, side):
    return SLOT[p] * size


def scattered(terms, x, w, where, number, name, last=False):
    rows, width = x.shape
    depth = w.shape[0]
    n = lax.axis_size("tp")
    side = int(round(n**0.5))
    size, low = rows // 2, rows // 4
    tile = min(TILE, width)
    tiles = width // tile
    bf, f32, dma = jnp.bfloat16, jnp.float32, pltpu.SemaphoreType.DMA
    return pl.pallas_call(
        functools.partial(_scatter_kernel, side=side, where=where, last=last),
        out_shape=jax.ShapeDtypeStruct((rows, width), bf),
        in_specs=[pl.BlockSpec(memory_space=pl.ANY)] * 3,
        out_specs=pl.BlockSpec(memory_space=pltpu.VMEM if last else pl.ANY),
        scratch_shapes=[
            pltpu.VMEM((n * rows, depth), bf),
            pltpu.VMEM((rows, width), bf),
            pltpu.VMEM((rows, TILE if last else width), bf),
            pltpu.VMEM((4, depth, tile), bf),
            pltpu.VMEM((2, 8, size, tile), bf),
            pltpu.VMEM((2, 8, size, tile), bf),
            pltpu.VMEM((2, 8, size, tile), bf),
            pltpu.VMEM((2, 3, 4, low, tile), bf),
            pltpu.VMEM((2, 4, low, tile), f32),
            pltpu.VMEM((4, 2, size, tile), f32),
            pltpu.VMEM((RING, 8, size, tile), bf),
            pltpu.VMEM((RING, 8, size, tile), bf),
            pltpu.VMEM((RING, 8, size, tile), bf),
            pltpu.VMEM((RING, 4, low, tile), bf),
            pltpu.VMEM((RING, 4, size, tile), bf),
            dma((len(ORDER),)), dma((1,)), dma((4,)), dma((tiles,)),
            dma((2, 4)), dma((2, 4)), dma((2, 4)), dma((2, 4)), dma((2, 2, 4)),
            dma((RING, 4)), dma((RING, 4)), dma((RING, 4)), dma((RING, 4)), dma((RING, 2, 4)),
        ],
        compiler_params=pltpu.CompilerParams(collective_id=number, has_side_effects=True, vmem_limit_bytes=LAST_VMEM if last else VMEM),
        cost_estimate=pl.CostEstimate(flops=2 * n * rows * depth * width, transcendentals=0, bytes_accessed=2 * depth * width),
        name=name,
    )(terms, x, w)


def _attend_kernel(q_ref, k_ref, v_ref, o_ref, top_s, mix_s, gap_s, *, scale, bk):
    heads, bq, d = q_ref.shape
    cols, low = bq, k_ref.dtype
    iq = pl.program_id(0)
    e = scale * LOG2E
    wide = min(cols, STRIP)
    pieces = [(i, at) for i in range(heads) for at in range(0, cols, wide)]
    gap_s[...] = lax.broadcasted_iota(jnp.int32, gap_s.shape, 1) - lax.broadcasted_iota(jnp.int32, gap_s.shape, 0)
    top_s[...] = jnp.full(top_s.shape, NEG, jnp.float32)
    mix_s[...] = jnp.zeros(mix_s.shape, jnp.float32)
    ones = jnp.ones((8, bk), low)

    def block(j, masked):
        here = pl.ds(pl.multiple_of(j * bk, bk), bk)
        scores = [_dot(k_ref[i, here, :], q_ref[i, at : at + wide, :], 1, 1) for i, at in pieces]
        ok = gap_s[...] >= j * bk - iq * bq if masked else None
        weights, keeps = [], []
        for (i, at), s in zip(pieces, scores):
            if masked:
                s = jnp.where(ok[:, at : at + wide], s, HIDDEN)
            old = top_s[i : i + 1, at : at + wide]
            top = jnp.maximum(old, s.max(axis=0, keepdims=True))
            top_s[i : i + 1, at : at + wide] = top
            weights.append(jnp.exp2((s - top) * e).astype(low))
            keeps.append(jnp.exp2((old - top) * e))
        for (i, at), p, keep in zip(pieces, weights, keeps):
            values = jnp.concatenate([v_ref[i, here, :].T, ones], axis=0)
            mix_s[i, :, at : at + wide] = mix_s[i, :, at : at + wide] * keep + _dot(values, p, 1, 0)

    whole = lax.div(iq * bq, bk)
    last = lax.div((iq + 1) * bq, bk)
    lax.fori_loop(0, whole, lambda j, _: block(j, False), None)
    lax.fori_loop(whole, last, lambda j, _: block(j, True), None)
    for i in range(heads):
        total = mix_s[i, d : d + 1, :]
        o_ref[:, i * d : (i + 1) * d] = (mix_s[i, :d, :] * (1 / total)).T.astype(o_ref.dtype)


def attended(qkv, bq=1024, bk=512):
    heads, tokens, d = qkv.shape[0] // 3, *qkv.shape[1:]
    bq, bk = min(bq, tokens), min(bk, tokens)
    return pl.pallas_call(
        functools.partial(_attend_kernel, scale=d**-0.5, bk=bk),
        grid=(tokens // bq,),
        in_specs=[pl.BlockSpec((heads, bq, d), lambda i: (0, i, 0)), pl.BlockSpec((heads, tokens, d), lambda i: (1, 0, 0)),
                  pl.BlockSpec((heads, tokens, d), lambda i: (2, 0, 0))],
        out_specs=pl.BlockSpec((bq, heads * d), lambda i: (i, 0)),
        out_shape=jax.ShapeDtypeStruct((tokens, heads * d), qkv.dtype),
        scratch_shapes=[pltpu.VMEM((heads, bq), jnp.float32), pltpu.VMEM((heads, d + 8, bq), jnp.float32), pltpu.VMEM((bk, bq), jnp.int32)],
        compiler_params=pltpu.CompilerParams(dimension_semantics=("arbitrary",), vmem_limit_bytes=VMEM),
        cost_estimate=pl.CostEstimate(flops=4 * heads * tokens * tokens * d, transcendentals=heads * tokens * tokens,
                                      bytes_accessed=8 * heads * tokens * d),
        name="attended",
    )(qkv, qkv, qkv)


def _angles(tokens):
    half = HEAD // 2
    rate = np.power(np.float32(THETA), -np.arange(half, dtype=np.float32) / np.float32(half)).astype(np.float32)
    angle = (np.arange(tokens, dtype=np.float32)[:, None] * rate).astype(np.float64)
    return np.concatenate([np.cos(angle), np.sin(angle)], 1).astype(np.float32)


def solution(mesh):
    n = mesh.shape["tp"]

    def step(x, gain_a, wq, wk, wv, wo, gain_m, w_gate, w_up, w_down):
        rows = n * x.shape[0]
        heads = wq.shape[1] // HEAD
        qkv = gathered(
            x, gain_a, (wq, wk, wv), _Heads(2), 2 * BLOCK, jax.ShapeDtypeStruct((3 * heads, rows, HEAD), jnp.bfloat16), 0, "gather_qkv",
            extra=(jnp.asarray(_angles(rows)),),
            scratch=(pltpu.VMEM((rows, HEAD), jnp.float32), pltpu.SemaphoreType.DMA((len(SLOTS),))),
            turns=TURN if mesh.shape["dp"] % 2 == 0 else None,
        )
        h = scattered(attended(qkv), x, wo, _in_sequence, 1, "scatter_o")
        hidden = gathered(h, gain_m, (w_gate, w_up), _Hidden(), BLOCK, jax.ShapeDtypeStruct((rows, w_gate.shape[1]), jnp.bfloat16), 2,
                          "gather_hidden")
        return scattered(hidden, h, w_down, _in_slots, 3, "scatter_down", last=True)

    tokens, columns, rows_of = P(("dp", "tp"), None), P(None, "tp"), P("tp", None)
    return jax.shard_map(
        step,
        mesh=mesh,
        in_specs=(tokens, P(None), columns, columns, columns, rows_of, P(None), columns, columns, rows_of),
        out_specs=tokens,
        check_vma=False,
    )
```

```python
import functools

import jax
import jax.numpy as jnp
import numpy as np
from jax import lax
from jax.experimental import pallas as pl
from jax.experimental.pallas import tpu as pltpu
from jax.sharding import PartitionSpec as P

MESH = pl.DeviceIdType.MESH
HEAD = 128
THETA = 10000
NEG = -1e30
HIDDEN = 2 * NEG
LOG2E = 1.4426950408889634
VMEM = 62 * 2**20
LAST_VMEM = 44 * 2**20
STRIP = 512
BLOCK = 256
TILE = 512
RING = 8

A, B = 0, 1
FAR = 2
UP, DOWN = (0, -1), (1, FAR)
LINKS = (("y", 1), ("y", -1), ("x", 1), ("x", -1))


def piece(half, along, across):
    return (half, across, along) if half == A else (half, along, across)


def both(along, across):
    return [piece(A, along, across), piece(B, along, across)]


NEXT = (-1, 1)
SLOTS = [
    p
    for group in (
        [both(0, 0)],
        [[piece(half, 0, d) for d in NEXT] for half in (A, B)],
        [[piece(half, d, 0) for d in NEXT] for half in (A, B)],
        [both(0, FAR)],
        *([[piece(half, d, across) for d in NEXT] for half in (A, B)] for across in NEXT),
        [both(FAR, 0), both(1, FAR), both(-1, FAR), both(FAR, 1), both(FAR, -1), both(FAR, FAR)],
    )
    for some in group
    for p in some
]
SLOT = {p: n for n, p in enumerate(SLOTS)}

def _by_link(along, pick):
    return [
        piece(half, along if along == 2 else sign * along, across)
        for (axis, sign) in LINKS
        for half in [A if axis == "y" else B]
        for across in (UP if (sign > 0) == pick else DOWN)
    ]


ORDER = _by_link(2, True) + _by_link(1, False) + _by_link(1, True) + [piece(half, 0, across) for half in (A, B) for across in UP + DOWN]


def _place(side):
    me = lax.axis_index("tp")
    return lax.div(me, side), lax.rem(me, side)


def _device(side, dx, dy):
    x, y = _place(side)
    return lax.rem(x + (dx + side), side) * side + lax.rem(y + (dy + side), side)


def _meet(side, twin=False):
    barrier = pltpu.get_barrier_semaphore()
    others = [{"tp": _device(side, *_step(link))} for link in LINKS] + ([_twin()] if twin else [])
    for other in others:
        pl.semaphore_signal(barrier, inc=1, device_id=other, device_id_type=MESH)
    return lambda: pl.semaphore_wait(barrier, len(others))


def _twin():
    group = lax.axis_index("dp")
    return {"dp": group + 1 - 2 * lax.rem(group, 2), "tp": lax.axis_index("tp")}


def _step(link):
    axis, sign = link
    return (sign, 0) if axis == "x" else (0, sign)


def _copy(side, link, src, dst, send_sem, recv_sem):
    return pltpu.make_async_remote_copy(src_ref=src, dst_ref=dst, send_sem=send_sem, recv_sem=recv_sem,
                                        device_id={"tp": _device(side, *_step(link))}, device_id_type=MESH)


def _cost(rows, depth, width, passes=1):
    return pl.CostEstimate(flops=2 * rows * depth * width, transcendentals=0, bytes_accessed=2 * passes * depth * width)


def _tile(i, size):
    return pl.ds(pl.multiple_of(i * size, size), size)


def _during(i, late, count):
    return pl.when((i >= late) & (i < count + late))


def _dot(a, b, ca=1, cb=0):
    return lax.dot_general(a, b, (((ca,), (cb,)), ((), ())), preferred_element_type=jnp.float32)


def _plan():
    slot = lambda half, along, across: SLOT[piece(half, along, across)]

    def inner(half, sign, source, target, part=0, parts=1):
        return ("xy"[half], sign), slot(half, 0, source), slot(half, 0, target), part, parts

    def outer(half, sign, source, across):
        target = -sign if source == 0 else FAR
        return ("yx"[half], sign), slot(half, source, across), slot(half, target, across), 0, 1

    halves, signs = (A, B), (1, -1)
    return [
        [inner(A, sign, 0, -sign) for sign in signs],
        [inner(B, sign, 0, -sign) for sign in signs],
        [outer(half, sign, 0, 0) for half in (B, A) for sign in signs],
        [inner(half, sign, -sign, FAR, int(sign < 0), 2) for half in halves for sign in signs]
        + [outer(half, sign, 0, across) for across in NEXT for half in halves for sign in signs],
        [outer(half, 1, -1, 0) for half in halves],
        [outer(half, sign, 0, FAR) for half in halves for sign in signs],
        [outer(half, 1, -1, -1) for half in halves],
        [outer(half, -1, 1, 1) for half in halves],
        [outer(half, -1, 1, FAR) for half in halves],
    ]


PLAN = _plan()
COPIES = [c for group in PLAN for c in group]
EVENTS = [
    (SLOTS[2:6], 3), (SLOTS[6:10], 4), (SLOTS[10:12], 5), (SLOTS[12:16], 6), (SLOTS[16:20], 7), (SLOTS[20:24], 8), (SLOTS[24:28], None),
    (SLOTS[28:], None),
]


def _gather_kernel(x_ref, gain_ref, *refs, side, finish, counts, twins):
    refs = iter(refs)
    take = lambda n: [next(refs) for _ in range(n)]
    extra_refs, w_refs, shared = (take(n) for n in counts[:3])
    (out_ref,), shelves = take(1), take(2 * len(shared))
    g, gain, w, stage, sems_x, sems_w, sems_o, send, recv = take(9)
    more = take(counts[3])
    carry = _Carry(side, twins, shared[0], shelves, *refs) if shared else None
    rows = x_ref.shape[0]
    size = rows // 2
    tiles = sum(ref.shape[1] for ref in w_refs) // w.shape[2]
    ring = min(w.shape[0], tiles)
    loads = tiles if tiles <= ring else len(EVENTS) * tiles

    def weights(s, start):
        finish.weights(w_refs, lax.rem(s, tiles), w, lax.rem(s, ring), sems_w, "start" if start else "wait")

    def remote(number):
        link, src, dst, part, parts = COPIES[number]
        height = size // parts
        return _copy(side, link, g.at[pl.ds(src * size + part * height, height)], g.at[pl.ds(dst * size + part * height, height)],
                     send.at[number], recv.at[dst, part])

    def begin(group):
        first = sum(len(p) for p in PLAN[:group])
        for number in range(first, first + len(PLAN[group])):
            remote(number).start()

    def arrived(slots):
        for number, (_, _, dst, _, _) in enumerate(COPIES):
            if SLOTS[dst] in slots:
                remote(number).wait_recv()

    met = _meet(side, bool(carry and twins))
    own = [pltpu.make_async_copy(x_ref.at[here], g.at[here], sems_x.at[half]) for half in (A, B) for here in [pl.ds(half * size, size)]]
    gains = pltpu.make_async_copy(gain_ref, gain, sems_x.at[2])
    for c in (own[A], gains, own[B]):
        c.start()

    def norm(i, _):
        here = _tile(i, 16)
        wide = g[here, :].astype(jnp.float32)
        scale = lax.rsqrt(jnp.mean(wide * wide, -1, keepdims=True) + 1e-6)
        g[here, :] = (wide * scale * gain[...].astype(jnp.float32)[None]).astype(jnp.bfloat16)

    gains.wait()
    if carry:
        met()
        carry.begin()
    for half in (A, B):
        own[half].wait()
        lax.fori_loop(half * size // 16, (half + 1) * size // 16, norm, None)
        if half == A:
            carry.proceed() if carry else met()
        begin(half)
    begin(2)
    for s in range(ring - 1):
        weights(s, True)
    if finish.prepare:
        finish.prepare(extra_refs, more)

    def block(b, _):
        for k, (slots, group) in enumerate(EVENTS):

            @pl.when(b == k)
            def _(slots=slots, group=group):
                arrived(slots)
                if group is not None:
                    begin(group)
                if carry and k < 2:
                    carry.hand(k)

        def tile(n, _):
            s = b * tiles + n

            @pl.when(s + (ring - 1) < loads)
            def _():
                weights(s + (ring - 1), True)

            @pl.when(s < loads)
            def _():
                weights(s, False)

            to = lax.rem(s, 2)

            @pl.when(s >= 2)
            def _():
                finish.store(stage, out_ref, sems_o, to, b, n, size, side, start=False)

            finish.compute(g.at[_tile(b, BLOCK)], w.at[lax.rem(s, ring)], stage.at[to], b, n, more)
            finish.store(stage, out_ref, sems_o, to, b, n, size, side, start=True)

        lax.fori_loop(0, tiles, tile, None)

    lax.fori_loop(0, len(EVENTS), block, None)
    for to in range(2):
        finish.store(stage, out_ref, sems_o, to, 0, 0, size, side, start=False)
    for number in range(len(COPIES)):
        remote(number).wait_send()
    if carry:
        carry.end()


class _Carry:
    SHELF = {-1: 0, 1: 1, FAR: 2}

    def __init__(self, side, twins, w_ref, shelves, send, recv, give, got):
        self.side, self.twins, self.w_ref, self.shelves = side, twins, w_ref, shelves
        self.send, self.recv, self.give, self.got = send, recv, give, got

    def carrier(self, body):
        if self.twins:
            pl.when(lax.rem(lax.axis_index("dp"), 2) == 0)(body)
        else:
            body()

    def copies(self, step):
        for t, shelf in enumerate(self.shelves):
            for sign in (1, -1):
                depth, width = shelf.shape[1:]
                here = pl.ds((int(sign < 0) ^ (step == 1)) * (depth // 2), depth // 2)
                if step == 2:
                    src, dst = shelf.at[self.SHELF[-sign], here], shelf.at[self.SHELF[FAR], here]
                else:
                    src, dst = self.w_ref.at[here, pl.ds(t * width, width)], shelf.at[self.SHELF[-sign], here]
                sem = t, int(sign < 0), step
                yield _copy(self.side, ("xy"[t], sign), src, dst, self.send.at[sem], self.recv.at[sem])

    def handed(self, k):
        for t, shelf in enumerate(self.shelves):
            for at in ((0, 1), (2,))[k]:
                yield pltpu.make_async_remote_copy(src_ref=shelf.at[at], dst_ref=shelf.at[at], send_sem=self.give.at[t, at],
                                                   recv_sem=self.got.at[t, at], device_id=_twin(), device_id_type=MESH)

    def all(self, copies, what):
        for c in copies:
            getattr(c, what)()

    def begin(self):
        @self.carrier
        def _():
            for step in (0, 1):
                self.all(self.copies(step), "start")

    def proceed(self):
        @self.carrier
        def _():
            self.all(self.copies(0), "wait_recv")
            self.all(self.copies(2), "start")

    def hand(self, k):
        @self.carrier
        def _():
            self.all(self.copies(k + 1), "wait_recv")
            if self.twins:
                self.all(self.handed(k), "start")

    def end(self):
        @self.carrier
        def _():
            for step in range(3):
                self.all(self.copies(step), "wait_send")
            if self.twins:
                for k in (0, 1):
                    self.all(self.handed(k), "wait_send")

        if self.twins:

            @pl.when(lax.rem(lax.axis_index("dp"), 2) == 1)
            def _():
                for k in (0, 1):
                    self.all(self.handed(k), "wait_recv")


class _Heads:
    def __init__(self, turned_steps):
        self.turned_steps = turned_steps

    def weights(self, refs, n, w, slot, sems, what):
        for at, ref in enumerate(refs):

            @pl.when(n == at)
            def _(ref=ref):
                getattr(pltpu.make_async_copy(ref, w.at[slot], sems.at[slot, 0]), what)()

    def prepare(self, extra_refs, more):
        (table_ref,) = extra_refs
        table, sems = more
        size = table.shape[0] // len(SLOTS)
        side = int(round((len(SLOTS) // 2) ** 0.5))
        copies = []
        for n, (half, dx, dy) in enumerate(SLOTS):
            row = _device(side, dx, dy) * (2 * size) + half * size
            copies.append(pltpu.make_async_copy(table_ref.at[pl.ds(pl.multiple_of(row, size), size)], table.at[pl.ds(n * size, size)],
                                                sems.at[n]))
        for what in ("start", "wait"):
            for c in copies:
                getattr(c, what)()

    def compute(self, lhs, w, to, at, n, more):
        table = more[0]
        got = _dot(lhs[...], w[...]).astype(jnp.bfloat16)

        @pl.when(n < self.turned_steps)
        def _():
            t = table[_tile(at, BLOCK), :]
            swapped = pltpu.roll(t, HEAD // 2, 1)
            low = lax.broadcasted_iota(jnp.int32, t.shape, 1) < HEAD // 2
            cos, sin = jnp.where(low, t, swapped), jnp.where(low, -swapped, t)
            for i in range(0, w.shape[1], HEAD):
                one = got[:, i : i + HEAD].astype(jnp.float32)
                to[:, i : i + HEAD] = (one * cos + pltpu.roll(one, HEAD // 2, 1) * sin).astype(jnp.bfloat16)

        @pl.when(n >= self.turned_steps)
        def _():
            to[...] = got

    def store(self, stage, out_ref, sems, to, at, n, size, side, start):
        per = BLOCK // size

        heads = stage.shape[2] // HEAD

        def copies(pieces):
            for p, (half, dx, dy) in enumerate(pieces):
                row = pl.multiple_of(_device(side, dx, dy) * (2 * size) + half * size, size)
                for i in range(heads):
                    yield pltpu.make_async_copy(stage.at[to, pl.ds(p * size, size), pl.ds(i * HEAD, HEAD)],
                                                out_ref.at[n * heads + i, pl.ds(row, size)], sems.at[to, p * heads + i])

        if not start:
            for c in copies(SLOTS[:per]):
                c.wait()
            return
        for k in range(len(SLOTS) // per):

            @pl.when(at == k)
            def _(k=k):
                for c in copies(SLOTS[k * per : (k + 1) * per]):
                    c.start()


class _Hidden:
    prepare = None

    def weights(self, refs, n, w, slot, sems, what):
        for at, ref in enumerate(refs):
            here = _tile(n, BLOCK)
            getattr(pltpu.make_async_copy(ref.at[:, here], w.at[slot, :, pl.ds(at * BLOCK, BLOCK)], sems.at[slot, at]), what)()

    def compute(self, lhs, w, to, at, n, more):
        got = _dot(lhs[...], w[...])
        to[...] = (jax.nn.silu(got[:, :BLOCK]) * got[:, BLOCK:]).astype(jnp.bfloat16)

    def store(self, stage, out_ref, sems, to, at, n, size, side, start):
        c = pltpu.make_async_copy(stage.at[to], out_ref.at[_tile(at, BLOCK),
                                                           _tile(n, BLOCK)], sems.at[to, 0])
        c.start() if start else c.wait()


def gathered(x, gain, weights, finish, stored, out_shape, number, name, extra=(), scratch=(), share=None, twins=False):
    rows, depth = x.shape
    n = lax.axis_size("tp")
    side = int(round(n**0.5))
    width = sum(w.shape[1] for w in weights)
    anywhere, dma = pl.BlockSpec(memory_space=pl.ANY), pltpu.SemaphoreType.DMA
    shared = [] if share is None else [share]
    shelves = [jax.ShapeDtypeStruct((side - 1, w.shape[0], w.shape[1] // 2), w.dtype) for w in 2 * shared]
    operands = [x, gain, *extra, *weights, *shared]
    return pl.pallas_call(
        functools.partial(_gather_kernel, side=side, finish=finish, counts=(len(extra), len(weights), len(shared), len(scratch)), twins=twins),
        out_shape=[out_shape, *shelves] if shared else out_shape,
        in_specs=[anywhere] * len(operands),
        out_specs=[anywhere] * 3 if shared else anywhere,
        scratch_shapes=[
            pltpu.VMEM((n * rows, depth), jnp.bfloat16),
            pltpu.VMEM((depth,), jnp.bfloat16),
            pltpu.VMEM((3, depth, 2 * BLOCK), jnp.bfloat16),
            pltpu.VMEM((2, BLOCK, stored), jnp.bfloat16),
            dma((3,)), dma((3, 2)), dma((2, len(SLOTS))), dma((len(COPIES),)), dma((len(SLOTS), 2)),
            *scratch,
            *([dma((2, 2, 3))] * 2 + [dma((2, 3))] * 2 if shared else []),
        ],
        compiler_params=pltpu.CompilerParams(collective_id=number, has_side_effects=True, vmem_limit_bytes=VMEM),
        cost_estimate=_cost(n * rows, depth, width, len(EVENTS)),
        name=name,
    )(*operands)


class _Sum:
    def __init__(self, side, near, keep, own, r_half, r_near, s_half, s_near, t_half, t_near):
        self.side, self.near, self.keep, self.own = side, near, keep, own
        self.r_half, self.r_near, self.s_half, self.s_near, self.t_half, self.t_near = r_half, r_near, s_half, s_near, t_half, t_near
        self.low = keep.shape[2]

    def halves(self, j):
        a, b = lax.rem(j, 2), lax.rem(j, self.r_half.shape[0])
        return [_copy(self.side, link, self.near.at[a, 0, l], self.r_half.at[b, l], self.s_half.at[a, l], self.t_half.at[b, l])
                for l, link in enumerate(LINKS)]

    def lasts(self, j, part):
        a, b = lax.rem(j, 2), lax.rem(j, self.r_near.shape[0])
        got = []
        for l, link in enumerate(LINKS):
            at = l % 2 if part else 1 - l % 2
            got.append(_copy(self.side, link, self.near.at[a, 1 + part, l], self.r_near.at[b, l, pl.ds(at * self.low, self.low)],
                             self.s_near.at[a, part, l], self.t_near.at[b, part, l]))
        return got

    def each(self, what, *groups):
        for c in sum(groups, []):
            getattr(c, what)()

    def freed(self, j):
        @pl.when(j >= 2)
        def _():
            self.each("wait_send", self.halves(j), self.lasts(j, 0))

    def put(self, j, t, l, pieces):
        a, low, bf = lax.rem(j, 2), self.low, jnp.bfloat16
        self.own[lax.rem(j, 4), t] = pieces[0]
        self.near[a, 0, l] = pieces[FAR][:low].astype(bf)
        self.near[a, 0, l + 1] = pieces[FAR][low:].astype(bf)
        self.near[a, 1, l] = pieces[1][low:].astype(bf)
        self.near[a, 1, l + 1] = pieces[-1][:low].astype(bf)
        self.keep[a, l] = pieces[1][:low]
        self.keep[a, l + 1] = pieces[-1][low:]

    def leave(self, j):
        self.each("start", self.halves(j), self.lasts(j, 0))

    def merge(self, j):
        a, b = lax.rem(j, 2), lax.rem(j, self.r_half.shape[0])

        @pl.when(j >= 2)
        def _():
            self.each("wait_send", self.lasts(j, 1))

        self.each("wait_recv", self.halves(j))
        for l in range(len(LINKS)):
            self.near[a, 2, l] = (self.keep[a, l] + self.r_half[b, l].astype(jnp.float32)).astype(jnp.bfloat16)
        self.each("start", self.lasts(j, 1))

    def arrived(self, j):
        self.each("wait_recv", self.lasts(j, 0), self.lasts(j, 1))

    def total(self, j, t, l):
        b = lax.rem(j, self.r_near.shape[0])
        return self.own[lax.rem(j, 4), t] + self.r_near[b, l].astype(jnp.float32) + self.r_near[b, l + 1].astype(jnp.float32)

    def left(self, j):
        self.each("wait_send", self.halves(j), self.lasts(j, 0), self.lasts(j, 1))

    @staticmethod
    def scratch(rings, low, tile):
        bf, f32, dma = jnp.bfloat16, jnp.float32, pltpu.SemaphoreType.DMA
        return [pltpu.VMEM((2, 3, 4, low, tile), bf), pltpu.VMEM((2, 4, low, tile), f32), pltpu.VMEM((4, 2, 2 * low, tile), f32),
                pltpu.VMEM((rings, 4, low, tile), bf), pltpu.VMEM((rings, 4, 2 * low, tile), bf),
                dma((2, 4)), dma((2, 2, 4)), dma((rings, 4)), dma((rings, 2, 4))]


def _scatter_kernel(rows_ref, x_ref, w_ref, out, hid, res, w, far, plain, summed, r_far, r_plain, r_summed, sems_h, sems_x, sems_w,
                    s_far, s_plain, s_summed, t_far, t_plain, t_summed, *second, side):
    rows, width = out.shape
    size = rows // 2
    tile = w.shape[2]
    tiles = width // tile
    ring = r_far.shape[0]
    group = hid.shape[0] // 4

    def fetch(n):
        return pltpu.make_async_copy(rows_ref.at[pl.ds(SLOT[ORDER[n]] * size, size)], hid.at[pl.ds(n * size, size)], sems_h.at[n])

    def weights(j):
        slot = lax.rem(j, 4)
        return pltpu.make_async_copy(w_ref.at[:, _tile(j, tile)], w.at[slot], sems_w.at[slot])

    def term(g, j):
        return _dot(hid[pl.ds(g * group, group), :], w[lax.rem(j, 4)]).reshape(8, size, tile)

    def move(l, src, dst, s_sem, t_sem, j):
        return _copy(side, LINKS[l], src, dst, s_sem, t_sem)

    def pairs(src, dst, s_sem, t_sem, j):
        a, b = lax.rem(j, 2), lax.rem(j, ring)
        return [_copy(side, LINKS[l], src.at[a, pl.ds(2 * l, 2)], dst.at[b, pl.ds(2 * l, 2)], s_sem.at[a, l], t_sem.at[b, l])
                for l in range(4)]

    ring2 = _Sum(side, *second)

    def each(copies, what):
        for c in copies:
            getattr(c, what)()

    weights(0).start()
    for n in range(len(ORDER)):
        fetch(n).start()
    residual = pltpu.make_async_copy(x_ref, res, sems_x.at[0])
    residual.start()
    _meet(side)()
    for n in range(len(ORDER)):
        fetch(n).wait()
    residual.wait()

    def step(i, _):
        @_during(i, 0, tiles)
        def _():
            j = i

            @pl.when(j + 1 < tiles)
            def _():
                weights(j + 1).start()

            weights(j).wait()

            @pl.when(j >= 2)
            def _():
                each(pairs(far, r_far, s_far, t_far, j), "wait_send")
                each(pairs(plain, r_plain, s_plain, t_plain, j), "wait_send")

            far[lax.rem(j, 2)] = term(0, j).astype(jnp.bfloat16)
            each(pairs(far, r_far, s_far, t_far, j), "start")

            plain[lax.rem(j, 2)] = term(1, j).astype(jnp.bfloat16)
            each(pairs(plain, r_plain, s_plain, t_plain, j), "start")

        @_during(i, 1, tiles)
        def _():
            j = i - 1

            @pl.when(j >= 2)
            def _():
                each(pairs(summed, r_summed, s_summed, t_summed, j), "wait_send")

            each(pairs(far, r_far, s_far, t_far, j), "wait_recv")
            summed[lax.rem(j, 2)] = (term(2, j) + r_far[lax.rem(j, ring)].astype(jnp.float32)).astype(jnp.bfloat16)
            each(pairs(summed, r_summed, s_summed, t_summed, j), "start")

        @_during(i, 2, tiles)
        def _():
            j = i - 2
            b = lax.rem(j, ring)

            ring2.freed(j)
            each(pairs(plain, r_plain, s_plain, t_plain, j), "wait_recv")
            each(pairs(summed, r_summed, s_summed, t_summed, j), "wait_recv")
            mine = term(3, j)
            for half in (A, B):
                l = 2 * half
                up, down = pl.ds(2 * l, 2), pl.ds(2 * l + 2, 2)
                from_up = jnp.concatenate([r_summed[b, up], r_plain[b, up]]).astype(jnp.float32)
                from_down = jnp.concatenate([r_plain[b, down], r_summed[b, down]]).astype(jnp.float32)
                both_ways = mine[4 * half : 4 * half + 4] + from_up + from_down
                sums = {across: both_ways[k] for k, across in enumerate(UP + DOWN)}
                ring2.put(j, half, 2 - l, sums)
            ring2.leave(j)

        @_during(i, 3, tiles)
        def _():
            ring2.merge(i - 3)

        @pl.when(i >= 4)
        def _():
            j = i - 4

            ring2.arrived(j)
            here = _tile(j, tile)
            for half in (A, B):
                mine = pl.ds(half * size, size)
                out[mine, here] = (res[mine, here].astype(jnp.float32) + ring2.total(j, half, 2 - 2 * half)).astype(jnp.bfloat16)

    lax.fori_loop(0, tiles + 4, step, None)
    for j in range(tiles - 2, tiles):
        each(pairs(far, r_far, s_far, t_far, j), "wait_send")
        each(pairs(plain, r_plain, s_plain, t_plain, j), "wait_send")
        each(pairs(summed, r_summed, s_summed, t_summed, j), "wait_send")
        ring2.left(j)


def scattered(terms, x, w, number, name):
    rows, width = x.shape
    depth = w.shape[0]
    n = lax.axis_size("tp")
    side = int(round(n**0.5))
    size, low = rows // 2, rows // 4
    tile = min(TILE, width)
    tiles = width // tile
    bf, dma = jnp.bfloat16, pltpu.SemaphoreType.DMA
    return pl.pallas_call(
        functools.partial(_scatter_kernel, side=side),
        out_shape=jax.ShapeDtypeStruct((rows, width), bf),
        in_specs=[pl.BlockSpec(memory_space=pl.ANY)] * 3,
        out_specs=pl.BlockSpec(memory_space=pltpu.VMEM),
        scratch_shapes=[
            pltpu.VMEM((n * rows, depth), bf),
            pltpu.VMEM((rows, width), bf),
            pltpu.VMEM((4, depth, tile), bf),
            pltpu.VMEM((2, 8, size, tile), bf),
            pltpu.VMEM((2, 8, size, tile), bf),
            pltpu.VMEM((2, 8, size, tile), bf),
            pltpu.VMEM((RING, 8, size, tile), bf),
            pltpu.VMEM((RING, 8, size, tile), bf),
            pltpu.VMEM((RING, 8, size, tile), bf),
            dma((len(ORDER),)), dma((1,)), dma((4,)),
            *[dma((2, 4))] * 3, *[dma((RING, 4))] * 3,
            *_Sum.scratch(RING, low, tile),
        ],
        compiler_params=pltpu.CompilerParams(collective_id=number, has_side_effects=True, vmem_limit_bytes=LAST_VMEM),
        cost_estimate=_cost(n * rows, depth, width),
        name=name,
    )(terms, x, w)


AROUND = (0, 1, -1, FAR)
ORIGIN = (0, -1, 1, FAR)


def _share_kernel(seen_ref, x_ref, w_ref, left_ref, right_ref, out_ref, s, relay, w, res, out, sems_own, sems_x, sems_w, sems_o, s_next, s_far,
                  s_pass, t_next, t_far, t_pass, *second, side):
    rows, width = out_ref.shape
    depth, tile = w_ref.shape[0], w.shape[3]
    half, tiles = width // 2, width // 2 // tile
    slots = w.shape[0]
    ring = _Sum(side, *second)

    def block(t, along, across):
        dx, dy = (along, across) if t == 0 else (across, along)
        return seen_ref.at[_tile(_device(side, dx, dy), rows)]

    def place(t, i, origin, count=1):
        return s.at[t, pl.ds(i * rows, count * rows), pl.ds(ORIGIN.index(origin) * depth, depth)]

    def own():
        return [pltpu.make_async_copy(block(t, 0, across), place(t, i, 0), sems_own.at[t, i])
                for t in range(2) for i, across in enumerate(AROUND)]

    ways = [(t, n, sign) for t in range(2) for n, sign in enumerate((1, -1))]

    def far():
        return [_copy(side, ("xy"[t], sign), block(t, FAR, AROUND[2 * n + i]), relay.at[t, n, pl.ds(i * rows, rows)], s_far.at[t, n, i],
                      t_far.at[t, n, i]) for t, n, sign in ways for i in range(2)]

    def nexts():
        return [_copy(side, ("xy"[t], sign), block(t, sign, across), place(t, i, -sign), s_next.at[t, n, i], t_next.at[t, n, i])
                for t, n, sign in ways for i, across in enumerate(AROUND)]

    def passed():
        return [_copy(side, ("xy"[t], sign), relay.at[t, n], place(t, 2 * n, FAR, 2), s_pass.at[t, n], t_pass.at[t, n]) for t, n, sign in ways]

    def each(what, *groups):
        for c in sum(groups, []):
            getattr(c, what)()

    def weights(j):
        got = []
        for t, shelf in enumerate((left_ref, right_ref)):
            here = _tile(j, tile)
            there = _tile(t * tiles + j, tile)
            for i in range(side):
                src = shelf.at[i - 1, :, here] if i else w_ref.at[:, there]
                got.append(pltpu.make_async_copy(src, w.at[lax.rem(j, slots), t, pl.ds(i * depth, depth)], sems_w.at[lax.rem(j, slots), t, i]))
        return got

    def out_copy(t, j):
        here = _tile(t * tiles + j, tile)
        return pltpu.make_async_copy(out.at[:, here], out_ref.at[:, here], sems_o.at[t, j])

    met = _meet(side)
    each("start", own())
    for j in range(slots - 1):
        each("start", weights(j))
    residual = pltpu.make_async_copy(x_ref, res, sems_x.at[0])
    residual.start()
    met()
    each("start", far(), nexts())
    each("wait_recv", far())
    each("start", passed())
    each("wait", own())
    each("wait_recv", nexts(), passed())
    residual.wait()

    def step(i, _):
        @_during(i, 0, tiles)
        def _():
            j = i

            @pl.when(j + (slots - 1) < tiles)
            def _():
                each("start", weights(j + (slots - 1)))

            each("wait", weights(j))
            ring.freed(j)
            for t in range(2):
                got = _dot(s[t], w[lax.rem(j, slots), t])
                ring.put(j, t, 2 * t, {across: got[k * rows : (k + 1) * rows] for k, across in enumerate(AROUND)})
            ring.leave(j)

        @_during(i, 1, tiles)
        def _():
            ring.merge(i - 1)

        @pl.when(i >= 2)
        def _():
            j = i - 2

            ring.arrived(j)
            for t in range(2):
                here = _tile(t * tiles + j, tile)
                out[:, here] = (res[:, here].astype(jnp.float32) + ring.total(j, t, 2 * t)).astype(jnp.bfloat16)
                out_copy(t, j).start()

    lax.fori_loop(0, tiles + 2, step, None)
    for j in range(tiles - 2, tiles):
        ring.left(j)
    each("wait_send", far(), nexts(), passed())
    for t in range(2):
        for j in range(tiles):
            out_copy(t, j).wait()


def projected(seen, x, w, left, right, number, name):
    rows, width = x.shape
    depth = w.shape[0]
    n = lax.axis_size("tp")
    side = int(round(n**0.5))
    tile = min(TILE, width // 2)
    tiles = width // 2 // tile
    bf, dma = jnp.bfloat16, pltpu.SemaphoreType.DMA
    anywhere = pl.BlockSpec(memory_space=pl.ANY)
    return pl.pallas_call(
        functools.partial(_share_kernel, side=side),
        out_shape=jax.ShapeDtypeStruct((rows, width), bf),
        in_specs=[anywhere] * 5,
        out_specs=anywhere,
        scratch_shapes=[
            pltpu.VMEM((2, side * rows, side * depth), bf),
            pltpu.VMEM((2, 2, 2 * rows, depth), bf),
            pltpu.VMEM((3, 2, side * depth, tile), bf),
            pltpu.VMEM((rows, width), bf),
            pltpu.VMEM((rows, width), bf),
            dma((2, 4)), dma((1,)), dma((3, 2, side)), dma((2, tiles)),
            *[dma((2, 2, 4)), dma((2, 2, 2)), dma((2, 2))] * 2,
            *_Sum.scratch(tiles, rows // 2, tile),
        ],
        compiler_params=pltpu.CompilerParams(collective_id=number, has_side_effects=True, vmem_limit_bytes=VMEM),
        cost_estimate=_cost(n * rows, depth, width, side),
        name=name,
    )(seen, x, w, left, right)


def _attend_kernel(q_ref, k_ref, v_ref, o_ref, top_s, mix_s, *, scale):
    heads, size, d = q_ref.shape
    low = k_ref.dtype
    mine = pl.program_id(0)
    e = scale * LOG2E
    top_s[...] = jnp.full(top_s.shape, NEG, jnp.float32)
    mix_s[...] = jnp.zeros(mix_s.shape, jnp.float32)
    ones = jnp.ones((8, size), low)

    def block(j, masked):
        here = _tile(j, size)
        scores = [_dot(k_ref[i, here, :], q_ref[i], 1, 1) for i in range(heads)]
        if masked:
            seen = lax.broadcasted_iota(jnp.int32, (size, size), 1) >= lax.broadcasted_iota(jnp.int32, (size, size), 0)
        weights, keeps = [], []
        for i, s in enumerate(scores):
            s = jnp.where(seen, s, HIDDEN) if masked else s
            old = top_s[i : i + 1, :]
            top = jnp.maximum(old, s.max(axis=0, keepdims=True))
            top_s[i : i + 1, :] = top
            weights.append(jnp.exp2((s - top) * e).astype(low))
            keeps.append(jnp.exp2((old - top) * e))
        for i, (p, keep) in enumerate(zip(weights, keeps)):
            values = jnp.concatenate([v_ref[i, here, :].T, ones], axis=0)
            mix_s[i] = mix_s[i] * keep + _dot(values, p, 1, 0)

    lax.fori_loop(0, mine, lambda j, _: block(j, False), None)
    block(mine, True)
    for i in range(heads):
        total = mix_s[i, d : d + 1, :]
        o_ref[:, i * d : (i + 1) * d] = (mix_s[i, :d, :] * (1 / total)).T.astype(o_ref.dtype)


def attended(qkv):
    heads, tokens, d = qkv.shape[0] // 3, *qkv.shape[1:]
    size = min(STRIP, tokens)
    return pl.pallas_call(
        functools.partial(_attend_kernel, scale=d**-0.5),
        grid=(tokens // size,),
        in_specs=[pl.BlockSpec((heads, size, d), lambda i: (0, i, 0)), pl.BlockSpec((heads, tokens, d), lambda i: (1, 0, 0)),
                  pl.BlockSpec((heads, tokens, d), lambda i: (2, 0, 0))],
        out_specs=pl.BlockSpec((size, heads * d), lambda i: (i, 0)),
        out_shape=jax.ShapeDtypeStruct((tokens, heads * d), qkv.dtype),
        scratch_shapes=[pltpu.VMEM((heads, size), jnp.float32), pltpu.VMEM((heads, d + 8, size), jnp.float32)],
        compiler_params=pltpu.CompilerParams(dimension_semantics=("arbitrary",), vmem_limit_bytes=VMEM),
        cost_estimate=pl.CostEstimate(flops=4 * heads * tokens * tokens * d, transcendentals=heads * tokens * tokens,
                                      bytes_accessed=8 * heads * tokens * d),
        name="attended",
    )(qkv, qkv, qkv)


def _angles(tokens):
    half = HEAD // 2
    rate = np.power(np.float32(THETA), -np.arange(half, dtype=np.float32) / np.float32(half)).astype(np.float32)
    angle = (np.arange(tokens, dtype=np.float32)[:, None] * rate).astype(np.float64)
    return np.concatenate([np.cos(angle), np.sin(angle)], 1).astype(np.float32)


def solution(mesh):
    n = mesh.shape["tp"]

    def step(x, gain_a, wq, wk, wv, wo, gain_m, w_gate, w_up, w_down):
        rows = n * x.shape[0]
        heads = wq.shape[1] // HEAD
        qkv, left, right = gathered(
            x, gain_a, (wq, wk, wv), _Heads(2), 2 * BLOCK, jax.ShapeDtypeStruct((3 * heads, rows, HEAD), jnp.bfloat16), 0, "gather_qkv",
            extra=(jnp.asarray(_angles(rows)),),
            scratch=(pltpu.VMEM((rows, HEAD), jnp.float32), pltpu.SemaphoreType.DMA((len(SLOTS),))),
            share=wo, twins=mesh.shape["dp"] % 2 == 0,
        )
        h = projected(attended(qkv), x, wo, left, right, 1, "project")
        hidden = gathered(h, gain_m, (w_gate, w_up), _Hidden(), BLOCK, jax.ShapeDtypeStruct((rows, w_gate.shape[1]), jnp.bfloat16), 2,
                          "gather_hidden")
        return scattered(hidden, h, w_down, 3, "scatter_down")

    tokens, columns, rows_of = P(("dp", "tp"), None), P(None, "tp"), P("tp", None)
    return jax.shard_map(
        step,
        mesh=mesh,
        in_specs=(tokens, P(None), columns, columns, columns, rows_of, P(None), columns, columns, rows_of),
        out_specs=tokens,
        check_vma=False,
    )
```

```python
import functools

import jax
import jax.numpy as jnp
import numpy as np
from jax import lax
from jax.experimental import pallas as pl
from jax.experimental.pallas import tpu as pltpu
from jax.sharding import PartitionSpec as P

MESH = pl.DeviceIdType.MESH
HEAD = 128
THETA = 10000
NEG = -1e30
HIDDEN = 2 * NEG
LOG2E = 1.4426950408889634
VMEM = 62 * 2**20
LAST_VMEM = 44 * 2**20
STRIP = 512
BLOCK = 256
TILE = 512
RING = 8

A, B = 0, 1
FAR = 2
UP, DOWN = (0, -1), (1, FAR)
LINKS = (("y", 1), ("y", -1), ("x", 1), ("x", -1))


def piece(half, along, across):
    return (half, across, along) if half == A else (half, along, across)


def both(along, across):
    return [piece(A, along, across), piece(B, along, across)]


NEXT = (-1, 1)
SLOTS = [
    p
    for group in (
        [both(0, 0)],
        [[piece(half, 0, d) for d in NEXT] for half in (A, B)],
        [[piece(half, d, 0) for d in NEXT] for half in (A, B)],
        [both(0, FAR)],
        *([[piece(half, d, across) for d in NEXT] for half in (A, B)] for across in NEXT),
        [both(FAR, 0), both(1, FAR), both(-1, FAR), both(FAR, 1), both(FAR, -1), both(FAR, FAR)],
    )
    for some in group
    for p in some
]
SLOT = {p: n for n, p in enumerate(SLOTS)}

def _by_link(along, pick):
    return [
        piece(half, along if along == 2 else sign * along, across)
        for (axis, sign) in LINKS
        for half in [A if axis == "y" else B]
        for across in (UP if (sign > 0) == pick else DOWN)
    ]


ORDER = _by_link(2, True) + _by_link(1, False) + _by_link(1, True) + [piece(half, 0, across) for half in (A, B) for across in UP + DOWN]


def _place(side):
    me = lax.axis_index("tp")
    return lax.div(me, side), lax.rem(me, side)


def _device(side, dx, dy):
    x, y = _place(side)
    return lax.rem(x + (dx + side), side) * side + lax.rem(y + (dy + side), side)


def _meet(side, twin=False):
    barrier = pltpu.get_barrier_semaphore()
    others = [{"tp": _device(side, *_step(link))} for link in LINKS] + ([_twin()] if twin else [])
    for other in others:
        pl.semaphore_signal(barrier, inc=1, device_id=other, device_id_type=MESH)
    return lambda: pl.semaphore_wait(barrier, len(others))


def _twin():
    group = lax.axis_index("dp")
    return {"dp": group + 1 - 2 * lax.rem(group, 2), "tp": lax.axis_index("tp")}


def _step(link):
    axis, sign = link
    return (sign, 0) if axis == "x" else (0, sign)


def _copy(side, link, src, dst, send_sem, recv_sem):
    return pltpu.make_async_remote_copy(src_ref=src, dst_ref=dst, send_sem=send_sem, recv_sem=recv_sem,
                                        device_id={"tp": _device(side, *_step(link))}, device_id_type=MESH)


def _cost(rows, depth, width, passes=1):
    return pl.CostEstimate(flops=2 * rows * depth * width, transcendentals=0, bytes_accessed=2 * passes * depth * width)


def _tile(i, size):
    return pl.ds(pl.multiple_of(i * size, size), size)


def _during(i, late, count):
    return pl.when((i >= late) & (i < count + late))


def _dot(a, b, ca=1, cb=0):
    return lax.dot_general(a, b, (((ca,), (cb,)), ((), ())), preferred_element_type=jnp.float32)


def _plan():
    slot = lambda half, along, across: SLOT[piece(half, along, across)]

    def inner(half, sign, source, target, part=0, parts=1):
        return ("xy"[half], sign), slot(half, 0, source), slot(half, 0, target), part, parts

    def outer(half, sign, source, across):
        target = -sign if source == 0 else FAR
        return ("yx"[half], sign), slot(half, source, across), slot(half, target, across), 0, 1

    halves, signs = (A, B), (1, -1)
    return [
        [inner(A, sign, 0, -sign) for sign in signs],
        [inner(B, sign, 0, -sign) for sign in signs],
        [outer(half, sign, 0, 0) for half in (B, A) for sign in signs],
        [inner(half, sign, -sign, FAR, int(sign < 0), 2) for half in halves for sign in signs]
        + [outer(half, sign, 0, across) for across in NEXT for half in halves for sign in signs],
        [outer(half, 1, -1, 0) for half in halves],
        [outer(half, sign, 0, FAR) for half in halves for sign in signs],
        [outer(half, 1, -1, -1) for half in halves],
        [outer(half, -1, 1, 1) for half in halves],
        [outer(half, -1, 1, FAR) for half in halves],
    ]


PLAN = _plan()
COPIES = [c for group in PLAN for c in group]
EVENTS = [
    (SLOTS[2:6], 3), (SLOTS[6:10], 4), (SLOTS[10:12], 5), (SLOTS[12:16], 6), (SLOTS[16:20], 7), (SLOTS[20:24], 8), (SLOTS[24:28], None),
    (SLOTS[28:], None),
]


def _gather_kernel(x_ref, gain_ref, *refs, side, finish, counts, twins):
    refs = iter(refs)
    take = lambda n: [next(refs) for _ in range(n)]
    extra_refs, w_refs, shared = (take(n) for n in counts[:3])
    (out_ref,), shelves = take(1), take(2 * len(shared))
    g, gain, w, stage, sems_x, sems_w, sems_o, send, recv = take(9)
    more = take(counts[3])
    carry = _Carry(side, twins, shared[0], shelves, *refs) if shared else None
    rows = x_ref.shape[0]
    size = rows // 2
    tiles = sum(ref.shape[1] for ref in w_refs) // w.shape[2]
    ring = min(w.shape[0], tiles)
    loads = tiles if tiles <= ring else len(EVENTS) * tiles

    def weights(s, start):
        finish.weights(w_refs, lax.rem(s, tiles), w, lax.rem(s, ring), sems_w, "start" if start else "wait")

    def remote(number):
        link, src, dst, part, parts = COPIES[number]
        height = size // parts
        return _copy(side, link, g.at[pl.ds(src * size + part * height, height)], g.at[pl.ds(dst * size + part * height, height)],
                     send.at[number], recv.at[dst, part])

    def begin(group):
        first = sum(len(p) for p in PLAN[:group])
        for number in range(first, first + len(PLAN[group])):
            remote(number).start()

    def arrived(slots):
        for number, (_, _, dst, _, _) in enumerate(COPIES):
            if SLOTS[dst] in slots:
                remote(number).wait_recv()

    met = _meet(side, bool(carry and twins))
    own = [pltpu.make_async_copy(x_ref.at[here], g.at[here], sems_x.at[half]) for half in (A, B) for here in [pl.ds(half * size, size)]]
    gains = pltpu.make_async_copy(gain_ref, gain, sems_x.at[2])
    for c in (own[A], gains, own[B]):
        c.start()

    def norm(i, _):
        here = _tile(i, 16)
        wide = g[here, :].astype(jnp.float32)
        scale = lax.rsqrt(jnp.mean(wide * wide, -1, keepdims=True) + 1e-6)
        g[here, :] = (wide * scale * gain[...].astype(jnp.float32)[None]).astype(jnp.bfloat16)

    gains.wait()
    if carry:
        met()
        carry.begin()
    for half in (A, B):
        own[half].wait()
        lax.fori_loop(half * size // 16, (half + 1) * size // 16, norm, None)
        if half == A:
            carry.proceed() if carry else met()
        begin(half)
    begin(2)
    for s in range(ring - 1):
        weights(s, True)
    if finish.prepare:
        finish.prepare(extra_refs, more)
    if carry:
        for k in (0, 1):
            carry.hand(k)

    def block(b, _):
        for k, (slots, group) in enumerate(EVENTS):

            @pl.when(b == k)
            def _(slots=slots, group=group):
                arrived(slots)
                if group is not None:
                    begin(group)
        def tile(n, _):
            s = b * tiles + n

            @pl.when(s + (ring - 1) < loads)
            def _():
                weights(s + (ring - 1), True)

            @pl.when(s < loads)
            def _():
                weights(s, False)

            to = lax.rem(s, 2)

            @pl.when(s >= 2)
            def _():
                finish.store(stage, out_ref, sems_o, to, b, n, size, side, start=False)

            finish.compute(g.at[_tile(b, BLOCK)], w.at[lax.rem(s, ring)], stage.at[to], b, n, more)
            finish.store(stage, out_ref, sems_o, to, b, n, size, side, start=True)

        lax.fori_loop(0, tiles, tile, None)

    lax.fori_loop(0, len(EVENTS), block, None)
    for to in range(2):
        finish.store(stage, out_ref, sems_o, to, 0, 0, size, side, start=False)
    for number in range(len(COPIES)):
        remote(number).wait_send()
    if carry:
        carry.end()


class _Carry:
    SHELF = {-1: 0, 1: 1, FAR: 2}

    def __init__(self, side, twins, w_ref, shelves, send, recv, give, got):
        self.side, self.twins, self.w_ref, self.shelves = side, twins, w_ref, shelves
        self.send, self.recv, self.give, self.got = send, recv, give, got

    def carrier(self, body):
        if self.twins:
            pl.when(lax.rem(lax.axis_index("dp"), 2) == 0)(body)
        else:
            body()

    def copies(self, step):
        for t, shelf in enumerate(self.shelves):
            for sign in (1, -1):
                depth, width = shelf.shape[1:]
                here = pl.ds((int(sign < 0) ^ (step == 1)) * (depth // 2), depth // 2)
                if step == 2:
                    src, dst = shelf.at[self.SHELF[-sign], here], shelf.at[self.SHELF[FAR], here]
                else:
                    src, dst = self.w_ref.at[here, pl.ds(t * width, width)], shelf.at[self.SHELF[-sign], here]
                sem = t, int(sign < 0), step
                yield _copy(self.side, ("xy"[t], sign), src, dst, self.send.at[sem], self.recv.at[sem])

    def handed(self, k):
        for t, shelf in enumerate(self.shelves):
            for at in ((0, 1), (2,))[k]:
                yield pltpu.make_async_remote_copy(src_ref=shelf.at[at], dst_ref=shelf.at[at], send_sem=self.give.at[t, at],
                                                   recv_sem=self.got.at[t, at], device_id=_twin(), device_id_type=MESH)

    def all(self, copies, what):
        for c in copies:
            getattr(c, what)()

    def begin(self):
        @self.carrier
        def _():
            for step in (0, 1):
                self.all(self.copies(step), "start")

    def proceed(self):
        @self.carrier
        def _():
            self.all(self.copies(0), "wait_recv")
            self.all(self.copies(2), "start")

    def hand(self, k):
        @self.carrier
        def _():
            self.all(self.copies(k + 1), "wait_recv")
            if self.twins:
                self.all(self.handed(k), "start")

    def end(self):
        @self.carrier
        def _():
            for step in range(3):
                self.all(self.copies(step), "wait_send")
            if self.twins:
                for k in (0, 1):
                    self.all(self.handed(k), "wait_send")

        if self.twins:

            @pl.when(lax.rem(lax.axis_index("dp"), 2) == 1)
            def _():
                for k in (0, 1):
                    self.all(self.handed(k), "wait_recv")


class _Heads:
    def __init__(self, turned_steps):
        self.turned_steps = turned_steps

    def weights(self, refs, n, w, slot, sems, what):
        for at, ref in enumerate(refs):

            @pl.when(n == at)
            def _(ref=ref):
                getattr(pltpu.make_async_copy(ref, w.at[slot], sems.at[slot, 0]), what)()

    def prepare(self, extra_refs, more):
        (table_ref,) = extra_refs
        table, sems = more
        size = table.shape[0] // len(SLOTS)
        side = int(round((len(SLOTS) // 2) ** 0.5))
        copies = []
        for n, (half, dx, dy) in enumerate(SLOTS):
            row = _device(side, dx, dy) * (2 * size) + half * size
            copies.append(pltpu.make_async_copy(table_ref.at[pl.ds(pl.multiple_of(row, size), size)], table.at[pl.ds(n * size, size)],
                                                sems.at[n]))
        for what in ("start", "wait"):
            for c in copies:
                getattr(c, what)()

    def compute(self, lhs, w, to, at, n, more):
        table = more[0]
        got = _dot(lhs[...], w[...]).astype(jnp.bfloat16)

        @pl.when(n < self.turned_steps)
        def _():
            t = table[_tile(at, BLOCK), :]
            swapped = pltpu.roll(t, HEAD // 2, 1)
            low = lax.broadcasted_iota(jnp.int32, t.shape, 1) < HEAD // 2
            cos, sin = jnp.where(low, t, swapped), jnp.where(low, -swapped, t)
            for i in range(0, w.shape[1], HEAD):
                one = got[:, i : i + HEAD].astype(jnp.float32)
                to[:, i : i + HEAD] = (one * cos + pltpu.roll(one, HEAD // 2, 1) * sin).astype(jnp.bfloat16)

        @pl.when(n >= self.turned_steps)
        def _():
            to[...] = got

    def store(self, stage, out_ref, sems, to, at, n, size, side, start):
        per = BLOCK // size

        heads = stage.shape[2] // HEAD

        def copies(pieces):
            for p, (half, dx, dy) in enumerate(pieces):
                row = pl.multiple_of(_device(side, dx, dy) * (2 * size) + half * size, size)
                for i in range(heads):
                    yield pltpu.make_async_copy(stage.at[to, pl.ds(p * size, size), pl.ds(i * HEAD, HEAD)],
                                                out_ref.at[n * heads + i, pl.ds(row, size)], sems.at[to, p * heads + i])

        if not start:
            for c in copies(SLOTS[:per]):
                c.wait()
            return
        for k in range(len(SLOTS) // per):

            @pl.when(at == k)
            def _(k=k):
                for c in copies(SLOTS[k * per : (k + 1) * per]):
                    c.start()


class _Hidden:
    prepare = None

    def weights(self, refs, n, w, slot, sems, what):
        for at, ref in enumerate(refs):
            here = _tile(n, BLOCK)
            getattr(pltpu.make_async_copy(ref.at[:, here], w.at[slot, :, pl.ds(at * BLOCK, BLOCK)], sems.at[slot, at]), what)()

    def compute(self, lhs, w, to, at, n, more):
        got = _dot(lhs[...], w[...])
        to[...] = (jax.nn.silu(got[:, :BLOCK]) * got[:, BLOCK:]).astype(jnp.bfloat16)

    def store(self, stage, out_ref, sems, to, at, n, size, side, start):
        c = pltpu.make_async_copy(stage.at[to], out_ref.at[_tile(at, BLOCK),
                                                           _tile(n, BLOCK)], sems.at[to, 0])
        c.start() if start else c.wait()


def gathered(x, gain, weights, finish, stored, out_shape, number, name, extra=(), scratch=(), share=None, twins=False):
    rows, depth = x.shape
    n = lax.axis_size("tp")
    side = int(round(n**0.5))
    width = sum(w.shape[1] for w in weights)
    anywhere, dma = pl.BlockSpec(memory_space=pl.ANY), pltpu.SemaphoreType.DMA
    shared = [] if share is None else [share]
    shelves = [jax.ShapeDtypeStruct((side - 1, w.shape[0], w.shape[1] // 2), w.dtype) for w in 2 * shared]
    operands = [x, gain, *extra, *weights, *shared]
    return pl.pallas_call(
        functools.partial(_gather_kernel, side=side, finish=finish, counts=(len(extra), len(weights), len(shared), len(scratch)), twins=twins),
        out_shape=[out_shape, *shelves] if shared else out_shape,
        in_specs=[anywhere] * len(operands),
        out_specs=[anywhere] * 3 if shared else anywhere,
        scratch_shapes=[
            pltpu.VMEM((n * rows, depth), jnp.bfloat16),
            pltpu.VMEM((depth,), jnp.bfloat16),
            pltpu.VMEM((3, depth, 2 * BLOCK), jnp.bfloat16),
            pltpu.VMEM((2, BLOCK, stored), jnp.bfloat16),
            dma((3,)), dma((3, 2)), dma((2, len(SLOTS))), dma((len(COPIES),)), dma((len(SLOTS), 2)),
            *scratch,
            *([dma((2, 2, 3))] * 2 + [dma((2, 3))] * 2 if shared else []),
        ],
        compiler_params=pltpu.CompilerParams(collective_id=number, has_side_effects=True, vmem_limit_bytes=VMEM),
        cost_estimate=_cost(n * rows, depth, width, len(EVENTS)),
        name=name,
    )(*operands)


class _Sum:
    def __init__(self, side, near, keep, own, r_half, r_near, s_half, s_near, t_half, t_near):
        self.side, self.near, self.keep, self.own = side, near, keep, own
        self.r_half, self.r_near, self.s_half, self.s_near, self.t_half, self.t_near = r_half, r_near, s_half, s_near, t_half, t_near
        self.low = keep.shape[2]

    def halves(self, j):
        a, b = lax.rem(j, 2), lax.rem(j, self.r_half.shape[0])
        return [_copy(self.side, link, self.near.at[a, 0, l], self.r_half.at[b, l], self.s_half.at[a, l], self.t_half.at[b, l])
                for l, link in enumerate(LINKS)]

    def lasts(self, j, part):
        a, b = lax.rem(j, 2), lax.rem(j, self.r_near.shape[0])
        got = []
        for l, link in enumerate(LINKS):
            at = l % 2 if part else 1 - l % 2
            got.append(_copy(self.side, link, self.near.at[a, 1 + part, l], self.r_near.at[b, l, pl.ds(at * self.low, self.low)],
                             self.s_near.at[a, part, l], self.t_near.at[b, part, l]))
        return got

    def each(self, what, *groups):
        for c in sum(groups, []):
            getattr(c, what)()

    def freed(self, j):
        @pl.when(j >= 2)
        def _():
            self.each("wait_send", self.halves(j), self.lasts(j, 0))

    def put(self, j, t, l, pieces):
        a, low, bf = lax.rem(j, 2), self.low, jnp.bfloat16
        self.own[lax.rem(j, 4), t] = pieces[0]
        self.near[a, 0, l] = pieces[FAR][:low].astype(bf)
        self.near[a, 0, l + 1] = pieces[FAR][low:].astype(bf)
        self.near[a, 1, l] = pieces[1][low:].astype(bf)
        self.near[a, 1, l + 1] = pieces[-1][:low].astype(bf)
        self.keep[a, l] = pieces[1][:low]
        self.keep[a, l + 1] = pieces[-1][low:]

    def leave(self, j):
        self.each("start", self.halves(j), self.lasts(j, 0))

    def merge(self, j):
        a, b = lax.rem(j, 2), lax.rem(j, self.r_half.shape[0])

        @pl.when(j >= 2)
        def _():
            self.each("wait_send", self.lasts(j, 1))

        self.each("wait_recv", self.halves(j))
        for l in range(len(LINKS)):
            self.near[a, 2, l] = (self.keep[a, l] + self.r_half[b, l].astype(jnp.float32)).astype(jnp.bfloat16)
        self.each("start", self.lasts(j, 1))

    def arrived(self, j):
        self.each("wait_recv", self.lasts(j, 0), self.lasts(j, 1))

    def total(self, j, t, l):
        b = lax.rem(j, self.r_near.shape[0])
        return self.own[lax.rem(j, 4), t] + self.r_near[b, l].astype(jnp.float32) + self.r_near[b, l + 1].astype(jnp.float32)

    def left(self, j):
        self.each("wait_send", self.halves(j), self.lasts(j, 0), self.lasts(j, 1))

    @staticmethod
    def scratch(rings, low, tile):
        bf, f32, dma = jnp.bfloat16, jnp.float32, pltpu.SemaphoreType.DMA
        return [pltpu.VMEM((2, 3, 4, low, tile), bf), pltpu.VMEM((2, 4, low, tile), f32), pltpu.VMEM((4, 2, 2 * low, tile), f32),
                pltpu.VMEM((rings, 4, low, tile), bf), pltpu.VMEM((rings, 4, 2 * low, tile), bf),
                dma((2, 4)), dma((2, 2, 4)), dma((rings, 4)), dma((rings, 2, 4))]


def _scatter_kernel(rows_ref, x_ref, w_ref, out, hid, res, w, far, plain, summed, r_far, r_plain, r_summed, sems_h, sems_x, sems_w,
                    s_far, s_plain, s_summed, t_far, t_plain, t_summed, *second, side):
    rows, width = out.shape
    size = rows // 2
    tile = w.shape[2]
    tiles = width // tile
    ring = r_far.shape[0]
    group = hid.shape[0] // 4

    def fetch(n):
        return pltpu.make_async_copy(rows_ref.at[pl.ds(SLOT[ORDER[n]] * size, size)], hid.at[pl.ds(n * size, size)], sems_h.at[n])

    def weights(j):
        slot = lax.rem(j, 4)
        return pltpu.make_async_copy(w_ref.at[:, _tile(j, tile)], w.at[slot], sems_w.at[slot])

    def term(g, j):
        return _dot(hid[pl.ds(g * group, group), :], w[lax.rem(j, 4)]).reshape(8, size, tile)

    def move(l, src, dst, s_sem, t_sem, j):
        return _copy(side, LINKS[l], src, dst, s_sem, t_sem)

    def pairs(src, dst, s_sem, t_sem, j):
        a, b = lax.rem(j, 2), lax.rem(j, ring)
        return [_copy(side, LINKS[l], src.at[a, pl.ds(2 * l, 2)], dst.at[b, pl.ds(2 * l, 2)], s_sem.at[a, l], t_sem.at[b, l])
                for l in range(4)]

    ring2 = _Sum(side, *second)

    def each(copies, what):
        for c in copies:
            getattr(c, what)()

    weights(0).start()
    for n in range(len(ORDER)):
        fetch(n).start()
    residual = pltpu.make_async_copy(x_ref, res, sems_x.at[0])
    residual.start()
    _meet(side)()
    for n in range(len(ORDER)):
        fetch(n).wait()
    residual.wait()

    def step(i, _):
        @_during(i, 0, tiles)
        def _():
            j = i

            @pl.when(j + 1 < tiles)
            def _():
                weights(j + 1).start()

            weights(j).wait()

            @pl.when(j >= 2)
            def _():
                each(pairs(far, r_far, s_far, t_far, j), "wait_send")
                each(pairs(plain, r_plain, s_plain, t_plain, j), "wait_send")

            far[lax.rem(j, 2)] = term(0, j).astype(jnp.bfloat16)
            each(pairs(far, r_far, s_far, t_far, j), "start")

            plain[lax.rem(j, 2)] = term(1, j).astype(jnp.bfloat16)
            each(pairs(plain, r_plain, s_plain, t_plain, j), "start")

        @_during(i, 1, tiles)
        def _():
            j = i - 1

            @pl.when(j >= 2)
            def _():
                each(pairs(summed, r_summed, s_summed, t_summed, j), "wait_send")

            each(pairs(far, r_far, s_far, t_far, j), "wait_recv")
            summed[lax.rem(j, 2)] = (term(2, j) + r_far[lax.rem(j, ring)].astype(jnp.float32)).astype(jnp.bfloat16)
            each(pairs(summed, r_summed, s_summed, t_summed, j), "start")

        @_during(i, 2, tiles)
        def _():
            j = i - 2
            b = lax.rem(j, ring)

            ring2.freed(j)
            each(pairs(plain, r_plain, s_plain, t_plain, j), "wait_recv")
            each(pairs(summed, r_summed, s_summed, t_summed, j), "wait_recv")
            mine = term(3, j)
            for half in (A, B):
                l = 2 * half
                up, down = pl.ds(2 * l, 2), pl.ds(2 * l + 2, 2)
                from_up = jnp.concatenate([r_summed[b, up], r_plain[b, up]]).astype(jnp.float32)
                from_down = jnp.concatenate([r_plain[b, down], r_summed[b, down]]).astype(jnp.float32)
                both_ways = mine[4 * half : 4 * half + 4] + from_up + from_down
                sums = {across: both_ways[k] for k, across in enumerate(UP + DOWN)}
                ring2.put(j, half, 2 - l, sums)
            ring2.leave(j)

        @_during(i, 3, tiles)
        def _():
            ring2.merge(i - 3)

        @pl.when(i >= 4)
        def _():
            j = i - 4

            ring2.arrived(j)
            here = _tile(j, tile)
            for half in (A, B):
                mine = pl.ds(half * size, size)
                out[mine, here] = (res[mine, here].astype(jnp.float32) + ring2.total(j, half, 2 - 2 * half)).astype(jnp.bfloat16)

    lax.fori_loop(0, tiles + 4, step, None)
    for j in range(tiles - 2, tiles):
        each(pairs(far, r_far, s_far, t_far, j), "wait_send")
        each(pairs(plain, r_plain, s_plain, t_plain, j), "wait_send")
        each(pairs(summed, r_summed, s_summed, t_summed, j), "wait_send")
        ring2.left(j)


def scattered(terms, x, w, number, name):
    rows, width = x.shape
    depth = w.shape[0]
    n = lax.axis_size("tp")
    side = int(round(n**0.5))
    size, low = rows // 2, rows // 4
    tile = min(TILE, width)
    tiles = width // tile
    bf, dma = jnp.bfloat16, pltpu.SemaphoreType.DMA
    return pl.pallas_call(
        functools.partial(_scatter_kernel, side=side),
        out_shape=jax.ShapeDtypeStruct((rows, width), bf),
        in_specs=[pl.BlockSpec(memory_space=pl.ANY)] * 3,
        out_specs=pl.BlockSpec(memory_space=pltpu.VMEM),
        scratch_shapes=[
            pltpu.VMEM((n * rows, depth), bf),
            pltpu.VMEM((rows, width), bf),
            pltpu.VMEM((4, depth, tile), bf),
            pltpu.VMEM((2, 8, size, tile), bf),
            pltpu.VMEM((2, 8, size, tile), bf),
            pltpu.VMEM((2, 8, size, tile), bf),
            pltpu.VMEM((RING, 8, size, tile), bf),
            pltpu.VMEM((RING, 8, size, tile), bf),
            pltpu.VMEM((RING, 8, size, tile), bf),
            dma((len(ORDER),)), dma((1,)), dma((4,)),
            *[dma((2, 4))] * 3, *[dma((RING, 4))] * 3,
            *_Sum.scratch(RING, low, tile),
        ],
        compiler_params=pltpu.CompilerParams(collective_id=number, has_side_effects=True, vmem_limit_bytes=LAST_VMEM),
        cost_estimate=_cost(n * rows, depth, width),
        name=name,
    )(terms, x, w)


AROUND = (0, 1, -1, FAR)
ORIGIN = (0, -1, 1, FAR)


def _share_kernel(seen_ref, x_ref, w_ref, left_ref, right_ref, out_ref, s, relay, w, res, out, sems_own, sems_x, sems_w, sems_o, s_next, s_far,
                  s_pass, t_next, t_far, t_pass, *second, side):
    rows, width = out_ref.shape
    depth, tile = w_ref.shape[0], w.shape[3]
    half, tiles = width // 2, width // 2 // tile
    slots = w.shape[0]
    ring = _Sum(side, *second)

    def block(t, along, across):
        dx, dy = (along, across) if t == 0 else (across, along)
        return seen_ref.at[_tile(_device(side, dx, dy), rows)]

    def place(t, i, origin, count=1):
        return s.at[t, pl.ds(i * rows, count * rows), pl.ds(ORIGIN.index(origin) * depth, depth)]

    def own():
        return [pltpu.make_async_copy(block(t, 0, across), place(t, i, 0), sems_own.at[t, i])
                for t in range(2) for i, across in enumerate(AROUND)]

    ways = [(t, n, sign) for t in range(2) for n, sign in enumerate((1, -1))]

    def far():
        return [_copy(side, ("xy"[t], sign), block(t, FAR, AROUND[2 * n + i]), relay.at[t, n, pl.ds(i * rows, rows)], s_far.at[t, n, i],
                      t_far.at[t, n, i]) for t, n, sign in ways for i in range(2)]

    def nexts():
        return [_copy(side, ("xy"[t], sign), block(t, sign, across), place(t, i, -sign), s_next.at[t, n, i], t_next.at[t, n, i])
                for t, n, sign in ways for i, across in enumerate(AROUND)]

    def passed():
        return [_copy(side, ("xy"[t], sign), relay.at[t, n], place(t, 2 * n, FAR, 2), s_pass.at[t, n], t_pass.at[t, n]) for t, n, sign in ways]

    def each(what, *groups):
        for c in sum(groups, []):
            getattr(c, what)()

    def weights(j):
        got = []
        for t, shelf in enumerate((left_ref, right_ref)):
            here = _tile(j, tile)
            there = _tile(t * tiles + j, tile)
            for i in range(side):
                src = shelf.at[i - 1, :, here] if i else w_ref.at[:, there]
                got.append(pltpu.make_async_copy(src, w.at[lax.rem(j, slots), t, pl.ds(i * depth, depth)], sems_w.at[lax.rem(j, slots), t, i]))
        return got

    def out_copy(t, j):
        here = _tile(t * tiles + j, tile)
        return pltpu.make_async_copy(out.at[:, here], out_ref.at[:, here], sems_o.at[t, j])

    met = _meet(side)
    each("start", own())
    for j in range(slots - 1):
        each("start", weights(j))
    residual = pltpu.make_async_copy(x_ref, res, sems_x.at[0])
    residual.start()
    met()
    each("start", far(), nexts())
    each("wait_recv", far())
    each("start", passed())
    each("wait", own())
    each("wait_recv", nexts(), passed())
    residual.wait()

    def step(i, _):
        @_during(i, 0, tiles)
        def _():
            j = i

            @pl.when(j + (slots - 1) < tiles)
            def _():
                each("start", weights(j + (slots - 1)))

            each("wait", weights(j))
            ring.freed(j)
            for t in range(2):
                got = _dot(s[t], w[lax.rem(j, slots), t])
                ring.put(j, t, 2 * t, {across: got[k * rows : (k + 1) * rows] for k, across in enumerate(AROUND)})
            ring.leave(j)

        @_during(i, 1, tiles)
        def _():
            ring.merge(i - 1)

        @pl.when(i >= 2)
        def _():
            j = i - 2

            ring.arrived(j)
            for t in range(2):
                here = _tile(t * tiles + j, tile)
                out[:, here] = (res[:, here].astype(jnp.float32) + ring.total(j, t, 2 * t)).astype(jnp.bfloat16)
                out_copy(t, j).start()

    lax.fori_loop(0, tiles + 2, step, None)
    for j in range(tiles - 2, tiles):
        ring.left(j)
    each("wait_send", far(), nexts(), passed())
    for t in range(2):
        for j in range(tiles):
            out_copy(t, j).wait()


def projected(seen, x, w, left, right, number, name):
    rows, width = x.shape
    depth = w.shape[0]
    n = lax.axis_size("tp")
    side = int(round(n**0.5))
    tile = min(TILE, width // 2)
    tiles = width // 2 // tile
    bf, dma = jnp.bfloat16, pltpu.SemaphoreType.DMA
    anywhere = pl.BlockSpec(memory_space=pl.ANY)
    return pl.pallas_call(
        functools.partial(_share_kernel, side=side),
        out_shape=jax.ShapeDtypeStruct((rows, width), bf),
        in_specs=[anywhere] * 5,
        out_specs=anywhere,
        scratch_shapes=[
            pltpu.VMEM((2, side * rows, side * depth), bf),
            pltpu.VMEM((2, 2, 2 * rows, depth), bf),
            pltpu.VMEM((3, 2, side * depth, tile), bf),
            pltpu.VMEM((rows, width), bf),
            pltpu.VMEM((rows, width), bf),
            dma((2, 4)), dma((1,)), dma((3, 2, side)), dma((2, tiles)),
            *[dma((2, 2, 4)), dma((2, 2, 2)), dma((2, 2))] * 2,
            *_Sum.scratch(tiles, rows // 2, tile),
        ],
        compiler_params=pltpu.CompilerParams(collective_id=number, has_side_effects=True, vmem_limit_bytes=VMEM),
        cost_estimate=_cost(n * rows, depth, width, side),
        name=name,
    )(seen, x, w, left, right)


def _attend_kernel(q_ref, k_ref, v_ref, o_ref, top_s, mix_s, *, scale):
    heads, size, d = q_ref.shape
    low = k_ref.dtype
    mine = pl.program_id(0)
    e = scale * LOG2E
    top_s[...] = jnp.full(top_s.shape, NEG, jnp.float32)
    mix_s[...] = jnp.zeros(mix_s.shape, jnp.float32)
    ones = jnp.ones((8, size), low)

    def block(j, masked):
        here = _tile(j, size)
        scores = [_dot(k_ref[i, here, :], q_ref[i], 1, 1) for i in range(heads)]
        if masked:
            seen = lax.broadcasted_iota(jnp.int32, (size, size), 1) >= lax.broadcasted_iota(jnp.int32, (size, size), 0)
        weights, keeps = [], []
        for i, s in enumerate(scores):
            s = jnp.where(seen, s, HIDDEN) if masked else s
            old = top_s[i : i + 1, :]
            top = jnp.maximum(old, s.max(axis=0, keepdims=True))
            top_s[i : i + 1, :] = top
            weights.append(jnp.exp2((s - top) * e).astype(low))
            keeps.append(jnp.exp2((old - top) * e))
        for i, (p, keep) in enumerate(zip(weights, keeps)):
            values = jnp.concatenate([v_ref[i, here, :].T, ones], axis=0)
            mix_s[i] = mix_s[i] * keep + _dot(values, p, 1, 0)

    lax.fori_loop(0, mine, lambda j, _: block(j, False), None)
    block(mine, True)
    for i in range(heads):
        total = mix_s[i, d : d + 1, :]
        o_ref[:, i * d : (i + 1) * d] = (mix_s[i, :d, :] * (1 / total)).T.astype(o_ref.dtype)


def attended(qkv):
    heads, tokens, d = qkv.shape[0] // 3, *qkv.shape[1:]
    size = min(STRIP, tokens)
    return pl.pallas_call(
        functools.partial(_attend_kernel, scale=d**-0.5),
        grid=(tokens // size,),
        in_specs=[pl.BlockSpec((heads, size, d), lambda i: (0, i, 0)), pl.BlockSpec((heads, tokens, d), lambda i: (1, 0, 0)),
                  pl.BlockSpec((heads, tokens, d), lambda i: (2, 0, 0))],
        out_specs=pl.BlockSpec((size, heads * d), lambda i: (i, 0)),
        out_shape=jax.ShapeDtypeStruct((tokens, heads * d), qkv.dtype),
        scratch_shapes=[pltpu.VMEM((heads, size), jnp.float32), pltpu.VMEM((heads, d + 8, size), jnp.float32)],
        compiler_params=pltpu.CompilerParams(dimension_semantics=("arbitrary",), vmem_limit_bytes=VMEM),
        cost_estimate=pl.CostEstimate(flops=4 * heads * tokens * tokens * d, transcendentals=heads * tokens * tokens,
                                      bytes_accessed=8 * heads * tokens * d),
        name="attended",
    )(qkv, qkv, qkv)


def _angles(tokens):
    half = HEAD // 2
    rate = np.power(np.float32(THETA), -np.arange(half, dtype=np.float32) / np.float32(half)).astype(np.float32)
    angle = (np.arange(tokens, dtype=np.float32)[:, None] * rate).astype(np.float64)
    return np.concatenate([np.cos(angle), np.sin(angle)], 1).astype(np.float32)


def solution(mesh):
    n = mesh.shape["tp"]

    def step(x, gain_a, wq, wk, wv, wo, gain_m, w_gate, w_up, w_down):
        rows = n * x.shape[0]
        heads = wq.shape[1] // HEAD
        qkv, left, right = gathered(
            x, gain_a, (wq, wk, wv), _Heads(2), 2 * BLOCK, jax.ShapeDtypeStruct((3 * heads, rows, HEAD), jnp.bfloat16), 0, "gather_qkv",
            extra=(jnp.asarray(_angles(rows)),),
            scratch=(pltpu.VMEM((rows, HEAD), jnp.float32), pltpu.SemaphoreType.DMA((len(SLOTS),))),
            share=wo, twins=mesh.shape["dp"] % 2 == 0,
        )
        h = projected(attended(qkv), x, wo, left, right, 1, "project")
        hidden = gathered(h, gain_m, (w_gate, w_up), _Hidden(), BLOCK, jax.ShapeDtypeStruct((rows, w_gate.shape[1]), jnp.bfloat16), 2,
                          "gather_hidden")
        return scattered(hidden, h, w_down, 3, "scatter_down")

    tokens, columns, rows_of = P(("dp", "tp"), None), P(None, "tp"), P("tp", None)
    return jax.shard_map(
        step,
        mesh=mesh,
        in_specs=(tokens, P(None), columns, columns, columns, rows_of, P(None), columns, columns, rows_of),
        out_specs=tokens,
        check_vma=False,
    )
```

```python
import functools

import jax
import jax.numpy as jnp
import numpy as np
from jax import lax
from jax.experimental import pallas as pl
from jax.experimental.pallas import tpu as pltpu
from jax.sharding import PartitionSpec as P

MESH = pl.DeviceIdType.MESH
HEAD = 128
THETA = 10000
NEG = -1e30
HIDDEN = 2 * NEG
LOG2E = 1.4426950408889634
VMEM = 62 << 20
LAST_VMEM = 44 << 20
BLOCK = 256
TILE = 512
RING = 8

A, B = 0, 1
FAR = 2
UP, DOWN = (0, -1), (1, FAR)
LINKS = (("y", 1), ("y", -1), ("x", 1), ("x", -1))


def piece(half, along, across):
    return (half, across, along) if half == A else (half, along, across)


def both(along, across):
    return [piece(A, along, across), piece(B, along, across)]


NEXT, SIGNS, HALVES = (-1, 1), (1, -1), (A, B)
SLOTS = [
    p
    for group in (
        [both(0, 0)],
        [[piece(half, 0, d) for d in NEXT] for half in HALVES],
        [[piece(half, d, 0) for d in NEXT] for half in HALVES],
        [both(0, FAR)],
        *([[piece(half, d, across) for d in NEXT] for half in HALVES] for across in NEXT),
        [both(FAR, 0), both(1, FAR), both(-1, FAR), both(FAR, 1), both(FAR, -1), both(FAR, FAR)],
    )
    for some in group
    for p in some
]
SLOT = {p: n for n, p in enumerate(SLOTS)}

def _by_link(along, pick):
    return [
        piece(half, along if along == 2 else sign * along, across)
        for (axis, sign) in LINKS
        for half in [A if axis == "y" else B]
        for across in (UP if (sign > 0) == pick else DOWN)
    ]


ORDER = _by_link(2, True) + _by_link(1, False) + _by_link(1, True) + [piece(half, 0, across) for half in HALVES for across in UP + DOWN]


def _place(side):
    me = lax.axis_index("tp")
    return lax.div(me, side), lax.rem(me, side)


def _device(side, dx, dy):
    x, y = _place(side)
    return lax.rem(x + (dx + side), side) * side + lax.rem(y + (dy + side), side)


def _meet(side, twin=False):
    barrier = pltpu.get_barrier_semaphore()
    others = [{"tp": _device(side, *_step(link))} for link in LINKS] + ([_twin()] if twin else [])
    for other in others:
        pl.semaphore_signal(barrier, inc=1, device_id=other, device_id_type=MESH)
    return lambda: pl.semaphore_wait(barrier, len(others))


def _twin():
    group = lax.axis_index("dp")
    return {"dp": group + 1 - 2 * lax.rem(group, 2), "tp": lax.axis_index("tp")}


def _step(link):
    axis, sign = link
    return (sign, 0) if axis == "x" else (0, sign)


def _copy(side, link, src, dst, send_sem, recv_sem):
    return pltpu.make_async_remote_copy(src_ref=src, dst_ref=dst, send_sem=send_sem, recv_sem=recv_sem,
                                        device_id={"tp": _device(side, *_step(link))}, device_id_type=MESH)


def _cost(rows, depth, width, passes=1):
    return pl.CostEstimate(flops=2 * rows * depth * width, transcendentals=0, bytes_accessed=2 * passes * depth * width)


def _tile(i, size):
    return pl.ds(pl.multiple_of(i * size, size), size)


def _during(i, late, count):
    return pl.when((i >= late) & (i < count + late))


def _dot(a, b, ca=1, cb=0):
    return lax.dot_general(a, b, (((ca,), (cb,)), ((), ())), preferred_element_type=jnp.float32)


def _plan():
    slot = lambda half, along, across: SLOT[piece(half, along, across)]

    def inner(half, sign, source, target, part=0, parts=1):
        return ("xy"[half], sign), slot(half, 0, source), slot(half, 0, target), part, parts

    def outer(half, sign, source, across):
        target = -sign if source == 0 else FAR
        return ("yx"[half], sign), slot(half, source, across), slot(half, target, across), 0, 1

    halves, signs = HALVES, SIGNS
    return [
        [inner(A, sign, 0, -sign) for sign in signs],
        [inner(B, sign, 0, -sign) for sign in signs],
        [outer(half, sign, 0, 0) for half in (B, A) for sign in signs],
        [inner(half, sign, -sign, FAR, int(sign < 0), 2) for half in halves for sign in signs]
        + [outer(half, sign, 0, across) for across in NEXT for half in halves for sign in signs],
        [outer(half, 1, -1, 0) for half in halves],
        [outer(half, sign, 0, FAR) for half in halves for sign in signs],
        [outer(half, 1, -1, -1) for half in halves],
        [outer(half, -1, 1, 1) for half in halves],
        [outer(half, -1, 1, FAR) for half in halves],
    ]


PLAN = _plan()
COPIES = [c for group in PLAN for c in group]
EVENTS = [
    (SLOTS[2:6], 3), (SLOTS[6:10], 4), (SLOTS[10:12], 5), (SLOTS[12:16], 6), (SLOTS[16:20], 7), (SLOTS[20:24], 8), (SLOTS[24:28], None),
    (SLOTS[28:], None),
]


def _gather_kernel(x_ref, gain_ref, *refs, side, finish, counts, twins):
    refs = iter(refs)
    take = lambda n: [next(refs) for _ in range(n)]
    extra_refs, w_refs, shared = (take(n) for n in counts[:3])
    (out_ref,), shelves = take(1), take(2 * len(shared))
    g, gain, w, stage, sems_x, sems_w, sems_o, send, recv = take(9)
    more = take(counts[3])
    carry = _Carry(side, twins, shared[0], shelves, *refs) if shared else None
    rows = x_ref.shape[0]
    size = rows // 2
    tiles = sum(ref.shape[1] for ref in w_refs) // w.shape[2]
    ring = min(w.shape[0], tiles)
    loads = tiles if tiles <= ring else len(EVENTS) * tiles

    def weights(s, start):
        finish.weights(w_refs, lax.rem(s, tiles), w, lax.rem(s, ring), sems_w, "start" if start else "wait")

    def remote(number):
        link, src, dst, part, parts = COPIES[number]
        height = size // parts
        return _copy(side, link, g.at[pl.ds(src * size + part * height, height)], g.at[pl.ds(dst * size + part * height, height)],
                     send.at[number], recv.at[dst, part])

    def begin(group):
        first = sum(len(p) for p in PLAN[:group])
        for number in range(first, first + len(PLAN[group])):
            remote(number).start()

    def arrived(slots):
        for number, (_, _, dst, _, _) in enumerate(COPIES):
            if SLOTS[dst] in slots:
                remote(number).wait_recv()

    met = _meet(side, bool(carry and twins))
    own = [pltpu.make_async_copy(x_ref.at[here], g.at[here], sems_x.at[half]) for half in HALVES for here in [pl.ds(half * size, size)]]
    gains = pltpu.make_async_copy(gain_ref, gain, sems_x.at[2])
    for c in (own[A], gains, own[B]):
        c.start()

    def norm(i, _):
        here = _tile(i, 16)
        wide = g[here, :].astype(jnp.float32)
        scale = lax.rsqrt(jnp.mean(wide * wide, -1, keepdims=True) + 1e-6)
        g[here, :] = (wide * scale * gain[...].astype(jnp.float32)[None]).astype(jnp.bfloat16)

    gains.wait()
    if carry:
        met()
        carry.begin()
    for half in HALVES:
        own[half].wait()
        lax.fori_loop(half * size // 16, (half + 1) * size // 16, norm, None)
        if half == A:
            carry.proceed() if carry else met()
        begin(half)
    begin(2)
    for s in range(ring - 1):
        weights(s, True)
    if finish.prepare:
        finish.prepare(extra_refs, more)
    if carry:
        for k in HALVES:
            carry.hand(k)

    def block(b, _):
        for k, (slots, group) in enumerate(EVENTS):

            @pl.when(b == k)
            def _(slots=slots, group=group):
                arrived(slots)
                if group is not None:
                    begin(group)
        def tile(n, _):
            s = b * tiles + n

            @pl.when(s + (ring - 1) < loads)
            def _():
                weights(s + (ring - 1), True)

            @pl.when(s < loads)
            def _():
                weights(s, False)

            to = lax.rem(s, 2)

            @pl.when(s >= 2)
            def _():
                finish.store(stage, out_ref, sems_o, to, b, n, size, side, start=False)

            finish.compute(g.at[_tile(b, BLOCK)], w.at[lax.rem(s, ring)], stage.at[to], b, n, more)
            finish.store(stage, out_ref, sems_o, to, b, n, size, side, start=True)

        lax.fori_loop(0, tiles, tile, None)

    lax.fori_loop(0, len(EVENTS), block, None)
    for to in range(2):
        finish.store(stage, out_ref, sems_o, to, 0, 0, size, side, start=False)
    for number in range(len(COPIES)):
        remote(number).wait_send()
    if carry:
        carry.end()


class _Carry:
    SHELF = {-1: 0, 1: 1, FAR: 2}

    def __init__(self, side, twins, w_ref, shelves, send, recv, give, got):
        self.side, self.twins, self.w_ref, self.shelves = side, twins, w_ref, shelves
        self.send, self.recv, self.give, self.got = send, recv, give, got

    def carrier(self, body):
        if self.twins:
            pl.when(lax.rem(lax.axis_index("dp"), 2) == 0)(body)
        else:
            body()

    def copies(self, step):
        for t, shelf in enumerate(self.shelves):
            for sign in SIGNS:
                depth, width = shelf.shape[1:]
                here = pl.ds((int(sign < 0) ^ (step == 1)) * (depth // 2), depth // 2)
                if step == 2:
                    src, dst = shelf.at[self.SHELF[-sign], here], shelf.at[self.SHELF[FAR], here]
                else:
                    src, dst = self.w_ref.at[here, pl.ds(t * width, width)], shelf.at[self.SHELF[-sign], here]
                sem = t, int(sign < 0), step
                yield _copy(self.side, ("xy"[t], sign), src, dst, self.send.at[sem], self.recv.at[sem])

    def handed(self, k):
        for t, shelf in enumerate(self.shelves):
            for at in ((0, 1), (2,))[k]:
                yield pltpu.make_async_remote_copy(src_ref=shelf.at[at], dst_ref=shelf.at[at], send_sem=self.give.at[t, at],
                                                   recv_sem=self.got.at[t, at], device_id=_twin(), device_id_type=MESH)

    def all(self, copies, what):
        for c in copies:
            getattr(c, what)()

    def begin(self):
        @self.carrier
        def _():
            for step in HALVES:
                self.all(self.copies(step), "start")

    def proceed(self):
        @self.carrier
        def _():
            self.all(self.copies(0), "wait_recv")
            self.all(self.copies(2), "start")

    def hand(self, k):
        @self.carrier
        def _():
            self.all(self.copies(k + 1), "wait_recv")
            if self.twins:
                self.all(self.handed(k), "start")

    def end(self):
        @self.carrier
        def _():
            for step in range(3):
                self.all(self.copies(step), "wait_send")
            if self.twins:
                for k in HALVES:
                    self.all(self.handed(k), "wait_send")

        if self.twins:

            @pl.when(lax.rem(lax.axis_index("dp"), 2) == 1)
            def _():
                for k in HALVES:
                    self.all(self.handed(k), "wait_recv")


class _Heads:
    def __init__(self, turned_steps):
        self.turned_steps = turned_steps

    def weights(self, refs, n, w, slot, sems, what):
        for at, ref in enumerate(refs):

            @pl.when(n == at)
            def _(ref=ref):
                getattr(pltpu.make_async_copy(ref, w.at[slot], sems.at[slot, 0]), what)()

    def prepare(self, extra_refs, more):
        (table_ref,) = extra_refs
        table, sems = more
        size = table.shape[0] // len(SLOTS)
        side = int(round((len(SLOTS) // 2) ** 0.5))
        copies = []
        for n, (half, dx, dy) in enumerate(SLOTS):
            row = _device(side, dx, dy) * (2 * size) + half * size
            copies.append(pltpu.make_async_copy(table_ref.at[pl.ds(pl.multiple_of(row, size), size)], table.at[pl.ds(n * size, size)],
                                                sems.at[n]))
        for what in ("start", "wait"):
            for c in copies:
                getattr(c, what)()

    def compute(self, lhs, w, to, at, n, more):
        table = more[0]
        got = _dot(lhs[...], w[...]).astype(jnp.bfloat16)

        @pl.when(n < self.turned_steps)
        def _():
            t = table[_tile(at, BLOCK), :]
            swapped = pltpu.roll(t, HEAD // 2, 1)
            low = lax.broadcasted_iota(jnp.int32, t.shape, 1) < HEAD // 2
            cos, sin = jnp.where(low, t, swapped), jnp.where(low, -swapped, t)
            for i in range(0, w.shape[1], HEAD):
                one = got[:, i : i + HEAD].astype(jnp.float32)
                to[:, i : i + HEAD] = (one * cos + pltpu.roll(one, HEAD // 2, 1) * sin).astype(jnp.bfloat16)

        @pl.when(n >= self.turned_steps)
        def _():
            to[...] = got

    def store(self, stage, out_ref, sems, to, at, n, size, side, start):
        per = BLOCK // size

        heads = stage.shape[2] // HEAD

        def copies(pieces):
            for p, (half, dx, dy) in enumerate(pieces):
                row = pl.multiple_of(_device(side, dx, dy) * (2 * size) + half * size, size)
                for i in range(heads):
                    yield pltpu.make_async_copy(stage.at[to, pl.ds(p * size, size), pl.ds(i * HEAD, HEAD)],
                                                out_ref.at[n * heads + i, pl.ds(row, size)], sems.at[to, p * heads + i])

        if not start:
            for c in copies(SLOTS[:per]):
                c.wait()
            return
        for k in range(len(SLOTS) // per):

            @pl.when(at == k)
            def _(k=k):
                for c in copies(SLOTS[k * per : (k + 1) * per]):
                    c.start()


class _Hidden:
    prepare = None

    def weights(self, refs, n, w, slot, sems, what):
        for at, ref in enumerate(refs):
            here = _tile(n, BLOCK)
            getattr(pltpu.make_async_copy(ref.at[:, here], w.at[slot, :, pl.ds(at * BLOCK, BLOCK)], sems.at[slot, at]), what)()

    def compute(self, lhs, w, to, at, n, more):
        got = _dot(lhs[...], w[...])
        to[...] = (jax.nn.silu(got[:, :BLOCK]) * got[:, BLOCK:]).astype(jnp.bfloat16)

    def store(self, stage, out_ref, sems, to, at, n, size, side, start):
        c = pltpu.make_async_copy(stage.at[to], out_ref.at[_tile(at, BLOCK),
                                                           _tile(n, BLOCK)], sems.at[to, 0])
        c.start() if start else c.wait()


def gathered(x, gain, weights, finish, stored, out_shape, number, name, extra=(), scratch=(), share=None, twins=False):
    rows, depth = x.shape
    n = lax.axis_size("tp")
    side = int(round(n**0.5))
    width = sum(w.shape[1] for w in weights)
    anywhere, dma = pl.BlockSpec(memory_space=pl.ANY), pltpu.SemaphoreType.DMA
    shared = [] if share is None else [share]
    shelves = [jax.ShapeDtypeStruct((side - 1, w.shape[0], w.shape[1] // 2), w.dtype) for w in 2 * shared]
    operands = [x, gain, *extra, *weights, *shared]
    return pl.pallas_call(
        functools.partial(_gather_kernel, side=side, finish=finish, counts=(len(extra), len(weights), len(shared), len(scratch)), twins=twins),
        out_shape=[out_shape, *shelves] if shared else out_shape,
        in_specs=[anywhere] * len(operands),
        out_specs=[anywhere] * 3 if shared else anywhere,
        scratch_shapes=[
            pltpu.VMEM((n * rows, depth), jnp.bfloat16),
            pltpu.VMEM((depth,), jnp.bfloat16),
            pltpu.VMEM((3, depth, 2 * BLOCK), jnp.bfloat16),
            pltpu.VMEM((2, BLOCK, stored), jnp.bfloat16),
            dma((3,)), dma((3, 2)), dma((2, len(SLOTS))), dma((len(COPIES),)), dma((len(SLOTS), 2)),
            *scratch,
            *([dma((2, 2, 3))] * 2 + [dma((2, 3))] * 2 if shared else []),
        ],
        compiler_params=pltpu.CompilerParams(collective_id=number, has_side_effects=True, vmem_limit_bytes=VMEM),
        cost_estimate=_cost(n * rows, depth, width, len(EVENTS)),
        name=name,
    )(*operands)


class _Sum:
    def __init__(self, side, near, keep, own, r_half, r_near, s_half, s_near, t_half, t_near):
        self.side, self.near, self.keep, self.own = side, near, keep, own
        self.r_half, self.r_near, self.s_half, self.s_near, self.t_half, self.t_near = r_half, r_near, s_half, s_near, t_half, t_near
        self.low = keep.shape[2]

    def halves(self, j):
        a, b = lax.rem(j, 2), lax.rem(j, self.r_half.shape[0])
        return [_copy(self.side, link, self.near.at[a, 0, l], self.r_half.at[b, l], self.s_half.at[a, l], self.t_half.at[b, l])
                for l, link in enumerate(LINKS)]

    def lasts(self, j, part):
        a, b = lax.rem(j, 2), lax.rem(j, self.r_near.shape[0])
        got = []
        for l, link in enumerate(LINKS):
            at = l % 2 if part else 1 - l % 2
            got.append(_copy(self.side, link, self.near.at[a, 1 + part, l], self.r_near.at[b, l, pl.ds(at * self.low, self.low)],
                             self.s_near.at[a, part, l], self.t_near.at[b, part, l]))
        return got

    def each(self, what, *groups):
        for c in sum(groups, []):
            getattr(c, what)()

    def freed(self, j):
        @pl.when(j >= 2)
        def _():
            self.each("wait_send", self.halves(j), self.lasts(j, 0))

    def put(self, j, t, l, pieces):
        a, low, bf = lax.rem(j, 2), self.low, jnp.bfloat16
        self.own[lax.rem(j, 4), t] = pieces[0]
        self.near[a, 0, l] = pieces[FAR][:low].astype(bf)
        self.near[a, 0, l + 1] = pieces[FAR][low:].astype(bf)
        self.near[a, 1, l] = pieces[1][low:].astype(bf)
        self.near[a, 1, l + 1] = pieces[-1][:low].astype(bf)
        self.keep[a, l] = pieces[1][:low]
        self.keep[a, l + 1] = pieces[-1][low:]

    def leave(self, j):
        self.each("start", self.halves(j), self.lasts(j, 0))

    def merge(self, j):
        a, b = lax.rem(j, 2), lax.rem(j, self.r_half.shape[0])

        @pl.when(j >= 2)
        def _():
            self.each("wait_send", self.lasts(j, 1))

        self.each("wait_recv", self.halves(j))
        for l in range(len(LINKS)):
            self.near[a, 2, l] = (self.keep[a, l] + self.r_half[b, l].astype(jnp.float32)).astype(jnp.bfloat16)
        self.each("start", self.lasts(j, 1))

    def arrived(self, j):
        self.each("wait_recv", self.lasts(j, 0), self.lasts(j, 1))

    def total(self, j, t, l):
        b = lax.rem(j, self.r_near.shape[0])
        return self.own[lax.rem(j, 4), t] + self.r_near[b, l].astype(jnp.float32) + self.r_near[b, l + 1].astype(jnp.float32)

    def left(self, j):
        self.each("wait_send", self.halves(j), self.lasts(j, 0), self.lasts(j, 1))

    @staticmethod
    def scratch(rings, low, tile):
        bf, f32, dma = jnp.bfloat16, jnp.float32, pltpu.SemaphoreType.DMA
        return [pltpu.VMEM((2, 3, 4, low, tile), bf), pltpu.VMEM((2, 4, low, tile), f32), pltpu.VMEM((4, 2, 2 * low, tile), f32),
                pltpu.VMEM((rings, 4, low, tile), bf), pltpu.VMEM((rings, 4, 2 * low, tile), bf),
                dma((2, 4)), dma((2, 2, 4)), dma((rings, 4)), dma((rings, 2, 4))]


def _scatter_kernel(rows_ref, x_ref, w_ref, out, hid, res, w, far, plain, summed, r_far, r_plain, r_summed, sems_h, sems_x, sems_w,
                    s_far, s_plain, s_summed, t_far, t_plain, t_summed, *second, side):
    rows, width = out.shape
    size = rows // 2
    tile = w.shape[2]
    tiles = width // tile
    ring = r_far.shape[0]
    group = hid.shape[0] // 4

    def fetch(n):
        return pltpu.make_async_copy(rows_ref.at[pl.ds(SLOT[ORDER[n]] * size, size)], hid.at[pl.ds(n * size, size)], sems_h.at[n])

    def weights(j):
        slot = lax.rem(j, 4)
        return pltpu.make_async_copy(w_ref.at[:, _tile(j, tile)], w.at[slot], sems_w.at[slot])

    def term(g, j):
        return _dot(hid[pl.ds(g * group, group), :], w[lax.rem(j, 4)]).reshape(8, size, tile)

    def move(l, src, dst, s_sem, t_sem, j):
        return _copy(side, LINKS[l], src, dst, s_sem, t_sem)

    def pairs(src, dst, s_sem, t_sem, j):
        a, b = lax.rem(j, 2), lax.rem(j, ring)
        return [_copy(side, LINKS[l], src.at[a, pl.ds(2 * l, 2)], dst.at[b, pl.ds(2 * l, 2)], s_sem.at[a, l], t_sem.at[b, l])
                for l in range(4)]

    ring2 = _Sum(side, *second)

    def each(copies, what):
        for c in copies:
            getattr(c, what)()

    weights(0).start()
    for n in range(len(ORDER)):
        fetch(n).start()
    residual = pltpu.make_async_copy(x_ref, res, sems_x.at[0])
    residual.start()
    _meet(side)()
    for n in range(len(ORDER)):
        fetch(n).wait()
    residual.wait()

    def step(i, _):
        @_during(i, 0, tiles)
        def _():
            j = i

            @pl.when(j + 1 < tiles)
            def _():
                weights(j + 1).start()

            weights(j).wait()

            @pl.when(j >= 2)
            def _():
                each(pairs(far, r_far, s_far, t_far, j), "wait_send")
                each(pairs(plain, r_plain, s_plain, t_plain, j), "wait_send")

            far[lax.rem(j, 2)] = term(0, j).astype(jnp.bfloat16)
            each(pairs(far, r_far, s_far, t_far, j), "start")

            plain[lax.rem(j, 2)] = term(1, j).astype(jnp.bfloat16)
            each(pairs(plain, r_plain, s_plain, t_plain, j), "start")

        @_during(i, 1, tiles)
        def _():
            j = i - 1

            @pl.when(j >= 2)
            def _():
                each(pairs(summed, r_summed, s_summed, t_summed, j), "wait_send")

            each(pairs(far, r_far, s_far, t_far, j), "wait_recv")
            summed[lax.rem(j, 2)] = (term(2, j) + r_far[lax.rem(j, ring)].astype(jnp.float32)).astype(jnp.bfloat16)
            each(pairs(summed, r_summed, s_summed, t_summed, j), "start")

        @_during(i, 2, tiles)
        def _():
            j = i - 2
            b = lax.rem(j, ring)

            ring2.freed(j)
            each(pairs(plain, r_plain, s_plain, t_plain, j), "wait_recv")
            each(pairs(summed, r_summed, s_summed, t_summed, j), "wait_recv")
            mine = term(3, j)
            for half in HALVES:
                l = 2 * half
                up, down = pl.ds(2 * l, 2), pl.ds(2 * l + 2, 2)
                from_up = jnp.concatenate([r_summed[b, up], r_plain[b, up]]).astype(jnp.float32)
                from_down = jnp.concatenate([r_plain[b, down], r_summed[b, down]]).astype(jnp.float32)
                both_ways = mine[4 * half : 4 * half + 4] + from_up + from_down
                sums = {across: both_ways[k] for k, across in enumerate(UP + DOWN)}
                ring2.put(j, half, 2 - l, sums)
            ring2.leave(j)

        @_during(i, 3, tiles)
        def _():
            ring2.merge(i - 3)

        @pl.when(i >= 4)
        def _():
            j = i - 4

            ring2.arrived(j)
            here = _tile(j, tile)
            for half in HALVES:
                mine = pl.ds(half * size, size)
                out[mine, here] = (res[mine, here].astype(jnp.float32) + ring2.total(j, half, 2 - 2 * half)).astype(jnp.bfloat16)

    lax.fori_loop(0, tiles + 4, step, None)
    for j in range(tiles - 2, tiles):
        each(pairs(far, r_far, s_far, t_far, j), "wait_send")
        each(pairs(plain, r_plain, s_plain, t_plain, j), "wait_send")
        each(pairs(summed, r_summed, s_summed, t_summed, j), "wait_send")
        ring2.left(j)


def scattered(terms, x, w, number, name):
    rows, width = x.shape
    depth = w.shape[0]
    n = lax.axis_size("tp")
    side = int(round(n**0.5))
    size, low = rows // 2, rows // 4
    tile = min(TILE, width)
    tiles = width // tile
    bf, dma = jnp.bfloat16, pltpu.SemaphoreType.DMA
    return pl.pallas_call(
        functools.partial(_scatter_kernel, side=side),
        out_shape=jax.ShapeDtypeStruct((rows, width), bf),
        in_specs=[pl.BlockSpec(memory_space=pl.ANY)] * 3,
        out_specs=pl.BlockSpec(memory_space=pltpu.VMEM),
        scratch_shapes=[
            pltpu.VMEM((n * rows, depth), bf),
            pltpu.VMEM((rows, width), bf),
            pltpu.VMEM((4, depth, tile), bf),
            pltpu.VMEM((2, 8, size, tile), bf),
            pltpu.VMEM((2, 8, size, tile), bf),
            pltpu.VMEM((2, 8, size, tile), bf),
            pltpu.VMEM((RING, 8, size, tile), bf),
            pltpu.VMEM((RING, 8, size, tile), bf),
            pltpu.VMEM((RING, 8, size, tile), bf),
            dma((len(ORDER),)), dma((1,)), dma((4,)),
            *[dma((2, 4))] * 3, *[dma((RING, 4))] * 3,
            *_Sum.scratch(RING, low, tile),
        ],
        compiler_params=pltpu.CompilerParams(collective_id=number, has_side_effects=True, vmem_limit_bytes=LAST_VMEM),
        cost_estimate=_cost(n * rows, depth, width),
        name=name,
    )(terms, x, w)


AROUND = (0, 1, -1, FAR)
ORIGIN = (0, -1, 1, FAR)
TURNS = (FAR, 1, 0, -1)


def _attend(qkv, mine, o, top_s, mix_s):
    size, d = o.shape[0], qkv.shape[2]
    heads = qkv.shape[0] // 3
    e = d**-0.5 * LOG2E
    top_s[...] = jnp.full(top_s.shape, NEG, jnp.float32)
    mix_s[...] = jnp.zeros(mix_s.shape, jnp.float32)
    ones = jnp.ones((8, size), qkv.dtype)

    def block(j, masked):
        here = _tile(j, size)
        scores = [_dot(qkv[heads + i, here, :], qkv[i, _tile(mine, size), :], 1, 1) for i in range(heads)]
        if masked:
            seen = lax.broadcasted_iota(jnp.int32, (size, size), 1) >= lax.broadcasted_iota(jnp.int32, (size, size), 0)
        weights, keeps = [], []
        for i, s in enumerate(scores):
            s = jnp.where(seen, s, HIDDEN) if masked else s
            old = top_s[i : i + 1, :]
            top = jnp.maximum(old, s.max(axis=0, keepdims=True))
            top_s[i : i + 1, :] = top
            weights.append(jnp.exp2((s - top) * e).astype(qkv.dtype))
            keeps.append(jnp.exp2((old - top) * e))
        for i, (p, keep) in enumerate(zip(weights, keeps)):
            values = jnp.concatenate([qkv[2 * heads + i, here, :].T, ones], axis=0)
            mix_s[i] = mix_s[i] * keep + _dot(values, p, 1, 0)

    lax.fori_loop(0, mine, lambda j, _: block(j, False), None)
    block(mine, True)
    for i in range(heads):
        total = mix_s[i, d : d + 1, :]
        o[:, i * d : (i + 1) * d] = (mix_s[i, :d, :] * (1 / total)).T.astype(o.dtype)


def _share_kernel(qkv_ref, x_ref, w_ref, left_ref, right_ref, out_ref, qkv, seen, top_s, mix_s, s, relay, w, res, out, sems_q, sems_x, sems_w,
                  sems_o, s_next, s_far, s_pass, t_next, t_far, t_pass, *second, side):
    rows, width = out_ref.shape
    depth, tile = w_ref.shape[0], w.shape[3]
    half, tiles = width // 2, width // 2 // tile
    slots = w.shape[0]
    ring = _Sum(side, *second)
    x, y = _place(side)

    def block(t, along, across):
        dx, dy = (along, across) if t == 0 else (across, along)
        return seen.at[TURNS.index(dx), _tile(lax.rem(y + (dy + side), side), rows)]

    def place(t, across, origin):
        return s.at[t, _tile(AROUND.index(across), rows), _tile(ORIGIN.index(origin), depth)]

    ways = [(t, n, sign) for t in HALVES for n, sign in enumerate(SIGNS)]

    def far(t, along, across):
        n, i = divmod(AROUND.index(across), 2)
        sign = 1 - 2 * n
        return _copy(side, ("xy"[t], sign), block(t, FAR, across), relay.at[t, n, i], s_far.at[t, n, i], t_far.at[t, n, i])

    def passed(t, across):
        n, i = divmod(AROUND.index(across), 2)
        return _copy(side, ("xy"[t], 1 - 2 * n), relay.at[t, n, i], place(t, across, FAR), s_pass.at[t, n, i], t_pass.at[t, n, i])

    def next_to(t, sign, across):
        at = t, int(sign < 0), AROUND.index(across)
        return _copy(side, ("xy"[t], sign), block(t, sign, across), place(t, across, -sign), s_next.at[at], t_next.at[at])

    def sends(t, along, across):
        if along:
            (far if along == FAR else next_to)(t, along, across).start()
        else:
            place(t, across, 0)[...] = block(t, 0, across)[...]

    def each(what, copies):
        for c in copies:
            getattr(c, what)()

    def weights(j):
        got = []
        for t, shelf in enumerate((left_ref, right_ref)):
            for i in range(side):
                src = shelf.at[i - 1, :, _tile(j, tile)] if i else w_ref.at[:, _tile(t * tiles + j, tile)]
                got.append(pltpu.make_async_copy(src, w.at[lax.rem(j, slots), t, pl.ds(i * depth, depth)], sems_w.at[lax.rem(j, slots), t, i]))
        return got

    def out_copy(t, j):
        here = _tile(t * tiles + j, tile)
        return pltpu.make_async_copy(out.at[:, here], out_ref.at[:, here], sems_o.at[t, j])

    met = _meet(side)
    heads = qkv.shape[0] // 3
    parts = [pltpu.make_async_copy(qkv_ref.at[here], qkv.at[here], sems_q.at[n]) for n in range(3) for here in [pl.ds(n * heads, heads)]]
    each("start", parts)
    for j in range(slots - 1):
        each("start", weights(j))
    residual = pltpu.make_async_copy(x_ref, res, sems_x.at[0])
    residual.start()
    each("wait", parts)
    met()

    def turn(n, _):
        _attend(qkv, lax.rem(x + (FAR + side) - n, side), seen.at[n], top_s, mix_s)
        for k, dx in enumerate(TURNS):

            @pl.when(n == k)
            def _(dx=dx):
                for other in AROUND:
                    sends(0, dx, other)
                    sends(1, other, dx)
                if dx == 1:
                    for across in AROUND:
                        far(0, FAR, across).wait_recv()
                        passed(0, across).start()

    lax.fori_loop(0, len(TURNS), turn, None)
    for dx in TURNS:
        far(1, FAR, dx).wait_recv()
        passed(1, dx).start()
    for t, n, sign in ways:
        each("wait_recv", [next_to(t, sign, across) for across in AROUND])
    residual.wait()
    for t in HALVES:
        each("wait_recv", [passed(t, across) for across in AROUND])

    def step(i, _):
        @_during(i, 0, tiles)
        def _():
            j = i

            @pl.when(j + (slots - 1) < tiles)
            def _():
                each("start", weights(j + (slots - 1)))

            each("wait", weights(j))
            ring.freed(j)
            for t in HALVES:
                got = _dot(s[t], w[lax.rem(j, slots), t])
                ring.put(j, t, 2 * t, {across: got[k * rows : (k + 1) * rows] for k, across in enumerate(AROUND)})
            ring.leave(j)

        @_during(i, 1, tiles)
        def _():
            ring.merge(i - 1)

        @pl.when(i >= 2)
        def _():
            j = i - 2
            ring.arrived(j)
            for t in HALVES:
                here = _tile(t * tiles + j, tile)
                out[:, here] = (res[:, here].astype(jnp.float32) + ring.total(j, t, 2 * t)).astype(jnp.bfloat16)
                out_copy(t, j).start()

    lax.fori_loop(0, tiles + 2, step, None)
    for j in range(tiles - 2, tiles):
        ring.left(j)
    for t, n, sign in ways:
        each("wait_send", [next_to(t, sign, across) for across in AROUND])
    for t in HALVES:
        each("wait_send", [copy for across in AROUND for copy in (far(t, FAR, across), passed(t, across))])
        for j in range(tiles):
            out_copy(t, j).wait()


def projected(qkv, x, w, left, right, number, name):
    rows, width = x.shape
    depth = w.shape[0]
    n = lax.axis_size("tp")
    side = int(round(n**0.5))
    tile = min(TILE, width // 2)
    tiles = width // 2 // tile
    bf, dma = jnp.bfloat16, pltpu.SemaphoreType.DMA
    anywhere = pl.BlockSpec(memory_space=pl.ANY)
    return pl.pallas_call(
        functools.partial(_share_kernel, side=side),
        out_shape=jax.ShapeDtypeStruct((rows, width), bf),
        in_specs=[anywhere] * 5,
        out_specs=anywhere,
        scratch_shapes=[
            pltpu.VMEM(qkv.shape, bf),
            pltpu.VMEM((side, side * rows, depth), bf),
            pltpu.VMEM((qkv.shape[0] // 3, side * rows), jnp.float32),
            pltpu.VMEM((qkv.shape[0] // 3, HEAD + 8, side * rows), jnp.float32),
            pltpu.VMEM((2, side * rows, side * depth), bf),
            pltpu.VMEM((2, 2, 2, rows, depth), bf),
            pltpu.VMEM((3, 2, side * depth, tile), bf),
            pltpu.VMEM((rows, width), bf),
            pltpu.VMEM((rows, width), bf),
            dma((3,)), dma((1,)), dma((3, 2, side)), dma((2, tiles)),
            *[dma((2, 2, 4)), dma((2, 2, 2)), dma((2, 2, 2))] * 2,
            *_Sum.scratch(tiles, rows // 2, tile),
        ],
        compiler_params=pltpu.CompilerParams(collective_id=number, has_side_effects=True, vmem_limit_bytes=VMEM),
        cost_estimate=_cost(n * rows, depth, width, side),
        name=name,
    )(qkv, x, w, left, right)


def _angles(tokens):
    half = HEAD // 2
    rate = np.power(np.float32(THETA), -np.arange(half, dtype=np.float32) / np.float32(half)).astype(np.float32)
    angle = (np.arange(tokens, dtype=np.float32)[:, None] * rate).astype(np.float64)
    return np.concatenate([np.cos(angle), np.sin(angle)], 1).astype(np.float32)


def solution(mesh):
    n = mesh.shape["tp"]

    def step(x, gain_a, wq, wk, wv, wo, gain_m, w_gate, w_up, w_down):
        rows = n * x.shape[0]
        heads = wq.shape[1] // HEAD
        qkv, left, right = gathered(
            x, gain_a, (wq, wk, wv), _Heads(2), 2 * BLOCK, jax.ShapeDtypeStruct((3 * heads, rows, HEAD), jnp.bfloat16), 0, "gather_qkv",
            extra=(jnp.asarray(_angles(rows)),),
            scratch=(pltpu.VMEM((rows, HEAD), jnp.float32), pltpu.SemaphoreType.DMA((len(SLOTS),))),
            share=wo, twins=mesh.shape["dp"] % 2 == 0,
        )
        h = projected(qkv, x, wo, left, right, 1, "project")
        hidden = gathered(h, gain_m, (w_gate, w_up), _Hidden(), BLOCK, jax.ShapeDtypeStruct((rows, w_gate.shape[1]), jnp.bfloat16), 2,
                          "gather_hidden")
        return scattered(hidden, h, w_down, 3, "scatter_down")

    tokens, columns, rows_of = P(("dp", "tp"), None), P(None, "tp"), P("tp", None)
    return jax.shard_map(
        step,
        mesh=mesh,
        in_specs=(tokens, P(None), columns, columns, columns, rows_of, P(None), columns, columns, rows_of),
        out_specs=tokens,
        check_vma=False,
    )
```

```python
import functools

import jax
import jax.numpy as jnp
import numpy as np
from jax import lax
from jax.experimental import pallas as pl
from jax.experimental.pallas import tpu as pltpu
from jax.sharding import PartitionSpec as P

MESH = pl.DeviceIdType.MESH
HEAD = 128
THETA = 10000
NEG = -1e30
HIDDEN = 2 * NEG
LOG2E = 1.4426950408889634
VMEM = 62 << 20
LAST_VMEM = 44 << 20
BLOCK = 256
TILE = 512
RING = 8

A, B = 0, 1
FAR = 2
UP, DOWN = (0, -1), (1, FAR)
LINKS = (("y", 1), ("y", -1), ("x", 1), ("x", -1))


def piece(half, along, across):
    return (half, across, along) if half == A else (half, along, across)


def both(along, across):
    return [piece(A, along, across), piece(B, along, across)]


NEXT, SIGNS, HALVES = (-1, 1), (1, -1), (A, B)
SLOTS = [
    p
    for group in (
        [both(0, 0)],
        [[piece(half, 0, d) for d in NEXT] for half in HALVES],
        [[piece(half, d, 0) for d in NEXT] for half in HALVES],
        [both(0, FAR)],
        *([[piece(half, d, across) for d in NEXT] for half in HALVES] for across in NEXT),
        [both(FAR, 0), both(1, FAR), both(-1, FAR), both(FAR, 1), both(FAR, -1), both(FAR, FAR)],
    )
    for some in group
    for p in some
]
SLOT = {p: n for n, p in enumerate(SLOTS)}

def _by_link(along, pick):
    return [
        piece(half, along if along == 2 else sign * along, across)
        for (axis, sign) in LINKS
        for half in [A if axis == "y" else B]
        for across in (UP if (sign > 0) == pick else DOWN)
    ]


ORDER = _by_link(2, True) + _by_link(1, False) + _by_link(1, True) + [piece(half, 0, across) for half in HALVES for across in UP + DOWN]


def _place(side):
    me = lax.axis_index("tp")
    return lax.div(me, side), lax.rem(me, side)


def _device(side, dx, dy):
    x, y = _place(side)
    return lax.rem(x + (dx + side), side) * side + lax.rem(y + (dy + side), side)


def _meet(side, twin=False):
    barrier = pltpu.get_barrier_semaphore()
    others = [{"tp": _device(side, *_step(link))} for link in LINKS] + ([_twin()] if twin else [])
    for other in others:
        pl.semaphore_signal(barrier, inc=1, device_id=other, device_id_type=MESH)
    return lambda: pl.semaphore_wait(barrier, len(others))


def _twin():
    group = lax.axis_index("dp")
    return {"dp": group + 1 - 2 * lax.rem(group, 2), "tp": lax.axis_index("tp")}


def _step(link):
    axis, sign = link
    return (sign, 0) if axis == "x" else (0, sign)


def _copy(side, link, src, dst, send_sem, recv_sem):
    return pltpu.make_async_remote_copy(src_ref=src, dst_ref=dst, send_sem=send_sem, recv_sem=recv_sem,
                                        device_id={"tp": _device(side, *_step(link))}, device_id_type=MESH)


def _cost(rows, depth, width, passes=1):
    return pl.CostEstimate(flops=2 * rows * depth * width, transcendentals=0, bytes_accessed=2 * passes * depth * width)


def _tile(i, size):
    return pl.ds(pl.multiple_of(i * size, size), size)


def _during(i, late, count):
    return pl.when((i >= late) & (i < count + late))


def _dot(a, b, ca=1, cb=0):
    return lax.dot_general(a, b, (((ca,), (cb,)), ((), ())), preferred_element_type=jnp.float32)


def _plan():
    slot = lambda half, along, across: SLOT[piece(half, along, across)]

    def inner(half, sign, source, target, part=0, parts=1):
        return ("xy"[half], sign), slot(half, 0, source), slot(half, 0, target), part, parts

    def outer(half, sign, source, across):
        target = -sign if source == 0 else FAR
        return ("yx"[half], sign), slot(half, source, across), slot(half, target, across), 0, 1

    halves, signs = HALVES, SIGNS
    return [
        [inner(A, sign, 0, -sign) for sign in signs],
        [inner(B, sign, 0, -sign) for sign in signs],
        [outer(half, sign, 0, 0) for half in (B, A) for sign in signs],
        [inner(half, sign, -sign, FAR, int(sign < 0), 2) for half in halves for sign in signs]
        + [outer(half, sign, 0, across) for across in NEXT for half in halves for sign in signs],
        [outer(half, 1, -1, 0) for half in halves],
        [outer(half, sign, 0, FAR) for half in halves for sign in signs],
        [outer(half, 1, -1, -1) for half in halves],
        [outer(half, -1, 1, 1) for half in halves],
        [outer(half, -1, 1, FAR) for half in halves],
    ]


PLAN = _plan()
COPIES = [c for group in PLAN for c in group]
EVENTS = [
    (SLOTS[2:6], 3), (SLOTS[6:10], 4), (SLOTS[10:12], 5), (SLOTS[12:16], 6), (SLOTS[16:20], 7), (SLOTS[20:24], 8), (SLOTS[24:28], None),
    (SLOTS[28:], None),
]


def _gather_kernel(x_ref, gain_ref, *refs, side, finish, counts, twins):
    refs = iter(refs)
    take = lambda n: [next(refs) for _ in range(n)]
    extra_refs, w_refs, shared = (take(n) for n in counts[:3])
    (out_ref,), shelves = take(1), take(2 * len(shared))
    g, gain, w, stage, sems_x, sems_w, sems_o, send, recv = take(9)
    more = take(counts[3])
    carry = _Carry(side, twins, shared[0], shelves, *refs) if shared else None
    rows = x_ref.shape[0]
    size = rows // 2
    tiles = sum(ref.shape[1] for ref in w_refs) // w.shape[2]
    ring = min(w.shape[0], tiles)
    loads = tiles if tiles <= ring else len(EVENTS) * tiles

    def weights(s, start):
        finish.weights(w_refs, lax.rem(s, tiles), w, lax.rem(s, ring), sems_w, "start" if start else "wait")

    def remote(number):
        link, src, dst, part, parts = COPIES[number]
        height = size // parts
        return _copy(side, link, g.at[pl.ds(src * size + part * height, height)], g.at[pl.ds(dst * size + part * height, height)],
                     send.at[number], recv.at[dst, part])

    def begin(group):
        first = sum(len(p) for p in PLAN[:group])
        for number in range(first, first + len(PLAN[group])):
            remote(number).start()

    def arrived(slots):
        for number, (_, _, dst, _, _) in enumerate(COPIES):
            if SLOTS[dst] in slots:
                remote(number).wait_recv()

    met = _meet(side, bool(carry and twins))
    own = [pltpu.make_async_copy(x_ref.at[here], g.at[here], sems_x.at[half]) for half in HALVES for here in [pl.ds(half * size, size)]]
    gains = pltpu.make_async_copy(gain_ref, gain, sems_x.at[2])
    for c in (own[A], gains, own[B]):
        c.start()

    def norm(i, _):
        here = _tile(i, 16)
        wide = g[here, :].astype(jnp.float32)
        scale = lax.rsqrt(jnp.mean(wide * wide, -1, keepdims=True) + 1e-6)
        g[here, :] = (wide * scale * gain[...].astype(jnp.float32)[None]).astype(jnp.bfloat16)

    gains.wait()
    if carry:
        met()
        carry.begin()
    for half in HALVES:
        own[half].wait()
        lax.fori_loop(half * size // 16, (half + 1) * size // 16, norm, None)
        if half == A:
            carry.proceed() if carry else met()
        begin(half)
    begin(2)
    for s in range(ring - 1):
        weights(s, True)
    if finish.prepare:
        finish.prepare(extra_refs, more)
    if carry:
        for k in HALVES:
            carry.hand(k)

    def block(b, _):
        for k, (slots, group) in enumerate(EVENTS):

            @pl.when(b == k)
            def _(slots=slots, group=group):
                arrived(slots)
                if group is not None:
                    begin(group)
        def tile(n, _):
            s = b * tiles + n

            @pl.when(s + (ring - 1) < loads)
            def _():
                weights(s + (ring - 1), True)

            @pl.when(s < loads)
            def _():
                weights(s, False)

            to = lax.rem(s, 2)

            @pl.when(s >= 2)
            def _():
                finish.store(stage, out_ref, sems_o, to, b, n, size, side, start=False)

            finish.compute(g.at[_tile(b, BLOCK)], w.at[lax.rem(s, ring)], stage.at[to], b, n, more)
            finish.store(stage, out_ref, sems_o, to, b, n, size, side, start=True)

        lax.fori_loop(0, tiles, tile, None)

    lax.fori_loop(0, len(EVENTS), block, None)
    for to in range(2):
        finish.store(stage, out_ref, sems_o, to, 0, 0, size, side, start=False)
    for number in range(len(COPIES)):
        remote(number).wait_send()
    if carry:
        carry.end()


class _Carry:
    SHELF = {-1: 0, 1: 1, FAR: 2}

    def __init__(self, side, twins, w_ref, shelves, send, recv, give, got):
        self.side, self.twins, self.w_ref, self.shelves = side, twins, w_ref, shelves
        self.send, self.recv, self.give, self.got = send, recv, give, got

    def carrier(self, body):
        if self.twins:
            pl.when(lax.rem(lax.axis_index("dp"), 2) == 0)(body)
        else:
            body()

    def copies(self, step):
        for t, shelf in enumerate(self.shelves):
            for sign in SIGNS:
                depth, width = shelf.shape[1:]
                here = pl.ds((int(sign < 0) ^ (step == 1)) * (depth // 2), depth // 2)
                if step == 2:
                    src, dst = shelf.at[self.SHELF[-sign], here], shelf.at[self.SHELF[FAR], here]
                else:
                    src, dst = self.w_ref.at[here, pl.ds(t * width, width)], shelf.at[self.SHELF[-sign], here]
                sem = t, int(sign < 0), step
                yield _copy(self.side, ("xy"[t], sign), src, dst, self.send.at[sem], self.recv.at[sem])

    def handed(self, k):
        for t, shelf in enumerate(self.shelves):
            for at in ((0, 1), (2,))[k]:
                yield pltpu.make_async_remote_copy(src_ref=shelf.at[at], dst_ref=shelf.at[at], send_sem=self.give.at[t, at],
                                                   recv_sem=self.got.at[t, at], device_id=_twin(), device_id_type=MESH)

    def all(self, copies, what):
        for c in copies:
            getattr(c, what)()

    def begin(self):
        @self.carrier
        def _():
            for step in HALVES:
                self.all(self.copies(step), "start")

    def proceed(self):
        @self.carrier
        def _():
            self.all(self.copies(0), "wait_recv")
            self.all(self.copies(2), "start")

    def hand(self, k):
        @self.carrier
        def _():
            self.all(self.copies(k + 1), "wait_recv")
            if self.twins:
                self.all(self.handed(k), "start")

    def end(self):
        @self.carrier
        def _():
            for step in range(3):
                self.all(self.copies(step), "wait_send")
            if self.twins:
                for k in HALVES:
                    self.all(self.handed(k), "wait_send")

        if self.twins:

            @pl.when(lax.rem(lax.axis_index("dp"), 2) == 1)
            def _():
                for k in HALVES:
                    self.all(self.handed(k), "wait_recv")


class _Heads:
    def __init__(self, turned_steps):
        self.turned_steps = turned_steps

    def weights(self, refs, n, w, slot, sems, what):
        for at, ref in enumerate(refs):

            @pl.when(n == at)
            def _(ref=ref):
                getattr(pltpu.make_async_copy(ref, w.at[slot], sems.at[slot, 0]), what)()

    def prepare(self, extra_refs, more):
        (table_ref,) = extra_refs
        table, sems = more
        size = table.shape[0] // len(SLOTS)
        side = int(round((len(SLOTS) // 2) ** 0.5))
        copies = []
        for n, (half, dx, dy) in enumerate(SLOTS):
            row = _device(side, dx, dy) * (2 * size) + half * size
            copies.append(pltpu.make_async_copy(table_ref.at[pl.ds(pl.multiple_of(row, size), size)], table.at[pl.ds(n * size, size)],
                                                sems.at[n]))
        for what in ("start", "wait"):
            for c in copies:
                getattr(c, what)()

    def compute(self, lhs, w, to, at, n, more):
        table = more[0]
        got = _dot(lhs[...], w[...]).astype(jnp.bfloat16)

        @pl.when(n < self.turned_steps)
        def _():
            t = table[_tile(at, BLOCK), :]
            swapped = pltpu.roll(t, HEAD // 2, 1)
            low = lax.broadcasted_iota(jnp.int32, t.shape, 1) < HEAD // 2
            cos, sin = jnp.where(low, t, swapped), jnp.where(low, -swapped, t)
            for i in range(0, w.shape[1], HEAD):
                one = got[:, i : i + HEAD].astype(jnp.float32)
                to[:, i : i + HEAD] = (one * cos + pltpu.roll(one, HEAD // 2, 1) * sin).astype(jnp.bfloat16)

        @pl.when(n >= self.turned_steps)
        def _():
            to[...] = got

    def store(self, stage, out_ref, sems, to, at, n, size, side, start):
        per = BLOCK // size

        heads = stage.shape[2] // HEAD

        def copies(pieces):
            for p, (half, dx, dy) in enumerate(pieces):
                row = pl.multiple_of(_device(side, dx, dy) * (2 * size) + half * size, size)
                for i in range(heads):
                    yield pltpu.make_async_copy(stage.at[to, pl.ds(p * size, size), pl.ds(i * HEAD, HEAD)],
                                                out_ref.at[n * heads + i, pl.ds(row, size)], sems.at[to, p * heads + i])

        if not start:
            for c in copies(SLOTS[:per]):
                c.wait()
            return
        for k in range(len(SLOTS) // per):

            @pl.when(at == k)
            def _(k=k):
                for c in copies(SLOTS[k * per : (k + 1) * per]):
                    c.start()


class _Hidden:
    prepare = None

    def weights(self, refs, n, w, slot, sems, what):
        for at, ref in enumerate(refs):
            here = _tile(n, BLOCK)
            getattr(pltpu.make_async_copy(ref.at[:, here], w.at[slot, :, pl.ds(at * BLOCK, BLOCK)], sems.at[slot, at]), what)()

    def compute(self, lhs, w, to, at, n, more):
        got = _dot(lhs[...], w[...])
        to[...] = (jax.nn.silu(got[:, :BLOCK]) * got[:, BLOCK:]).astype(jnp.bfloat16)

    def store(self, stage, out_ref, sems, to, at, n, size, side, start):
        c = pltpu.make_async_copy(stage.at[to], out_ref.at[_tile(at, BLOCK),
                                                           _tile(n, BLOCK)], sems.at[to, 0])
        c.start() if start else c.wait()


def gathered(x, gain, weights, finish, stored, out_shape, number, name, extra=(), scratch=(), share=None, twins=False):
    rows, depth = x.shape
    n = lax.axis_size("tp")
    side = int(round(n**0.5))
    width = sum(w.shape[1] for w in weights)
    anywhere, dma = pl.BlockSpec(memory_space=pl.ANY), pltpu.SemaphoreType.DMA
    shared = [] if share is None else [share]
    shelves = [jax.ShapeDtypeStruct((side - 1, w.shape[0], w.shape[1] // 2), w.dtype) for w in 2 * shared]
    operands = [x, gain, *extra, *weights, *shared]
    return pl.pallas_call(
        functools.partial(_gather_kernel, side=side, finish=finish, counts=(len(extra), len(weights), len(shared), len(scratch)), twins=twins),
        out_shape=[out_shape, *shelves] if shared else out_shape,
        in_specs=[anywhere] * len(operands),
        out_specs=[anywhere] * 3 if shared else anywhere,
        scratch_shapes=[
            pltpu.VMEM((n * rows, depth), jnp.bfloat16),
            pltpu.VMEM((depth,), jnp.bfloat16),
            pltpu.VMEM((3, depth, 2 * BLOCK), jnp.bfloat16),
            pltpu.VMEM((2, BLOCK, stored), jnp.bfloat16),
            dma((3,)), dma((3, 2)), dma((2, len(SLOTS))), dma((len(COPIES),)), dma((len(SLOTS), 2)),
            *scratch,
            *([dma((2, 2, 3))] * 2 + [dma((2, 3))] * 2 if shared else []),
        ],
        compiler_params=pltpu.CompilerParams(collective_id=number, has_side_effects=True, vmem_limit_bytes=VMEM),
        cost_estimate=_cost(n * rows, depth, width, len(EVENTS)),
        name=name,
    )(*operands)


class _Sum:
    def __init__(self, side, near, keep, own, r_half, r_near, s_half, s_near, t_half, t_near):
        self.side, self.near, self.keep, self.own = side, near, keep, own
        self.r_half, self.r_near, self.s_half, self.s_near, self.t_half, self.t_near = r_half, r_near, s_half, s_near, t_half, t_near
        self.low = keep.shape[2]

    def halves(self, j):
        a, b = lax.rem(j, 2), lax.rem(j, self.r_half.shape[0])
        return [_copy(self.side, link, self.near.at[a, 0, l], self.r_half.at[b, l], self.s_half.at[a, l], self.t_half.at[b, l])
                for l, link in enumerate(LINKS)]

    def lasts(self, j, part):
        a, b = lax.rem(j, 2), lax.rem(j, self.r_near.shape[0])
        got = []
        for l, link in enumerate(LINKS):
            at = l % 2 if part else 1 - l % 2
            got.append(_copy(self.side, link, self.near.at[a, 1 + part, l], self.r_near.at[b, l, pl.ds(at * self.low, self.low)],
                             self.s_near.at[a, part, l], self.t_near.at[b, part, l]))
        return got

    def each(self, what, *groups):
        for c in sum(groups, []):
            getattr(c, what)()

    def freed(self, j):
        @pl.when(j >= 2)
        def _():
            self.each("wait_send", self.halves(j), self.lasts(j, 0))

    def put(self, j, t, l, pieces):
        a, low, bf = lax.rem(j, 2), self.low, jnp.bfloat16
        self.own[lax.rem(j, 4), t] = pieces[0]
        self.near[a, 0, l] = pieces[FAR][:low].astype(bf)
        self.near[a, 0, l + 1] = pieces[FAR][low:].astype(bf)
        self.near[a, 1, l] = pieces[1][low:].astype(bf)
        self.near[a, 1, l + 1] = pieces[-1][:low].astype(bf)
        self.keep[a, l] = pieces[1][:low]
        self.keep[a, l + 1] = pieces[-1][low:]

    def leave(self, j):
        self.each("start", self.halves(j), self.lasts(j, 0))

    def merge(self, j):
        a, b = lax.rem(j, 2), lax.rem(j, self.r_half.shape[0])

        @pl.when(j >= 2)
        def _():
            self.each("wait_send", self.lasts(j, 1))

        self.each("wait_recv", self.halves(j))
        for l in range(len(LINKS)):
            self.near[a, 2, l] = (self.keep[a, l] + self.r_half[b, l].astype(jnp.float32)).astype(jnp.bfloat16)
        self.each("start", self.lasts(j, 1))

    def arrived(self, j):
        self.each("wait_recv", self.lasts(j, 0), self.lasts(j, 1))

    def total(self, j, t, l):
        b = lax.rem(j, self.r_near.shape[0])
        return self.own[lax.rem(j, 4), t] + self.r_near[b, l].astype(jnp.float32) + self.r_near[b, l + 1].astype(jnp.float32)

    def left(self, j):
        self.each("wait_send", self.halves(j), self.lasts(j, 0), self.lasts(j, 1))

    @staticmethod
    def scratch(rings, low, tile):
        bf, f32, dma = jnp.bfloat16, jnp.float32, pltpu.SemaphoreType.DMA
        return [pltpu.VMEM((2, 3, 4, low, tile), bf), pltpu.VMEM((2, 4, low, tile), f32), pltpu.VMEM((4, 2, 2 * low, tile), f32),
                pltpu.VMEM((rings, 4, low, tile), bf), pltpu.VMEM((rings, 4, 2 * low, tile), bf),
                dma((2, 4)), dma((2, 2, 4)), dma((rings, 4)), dma((rings, 2, 4))]


def _scatter_kernel(rows_ref, x_ref, w_ref, out, hid, res, w, far, plain, summed, r_far, r_plain, r_summed, sems_h, sems_x, sems_w,
                    s_far, s_plain, s_summed, t_far, t_plain, t_summed, *second, side):
    rows, width = out.shape
    size = rows // 2
    tile = w.shape[2]
    tiles = width // tile
    ring = r_far.shape[0]
    group = hid.shape[0] // 4

    def fetch(n):
        return pltpu.make_async_copy(rows_ref.at[pl.ds(SLOT[ORDER[n]] * size, size)], hid.at[pl.ds(n * size, size)], sems_h.at[n])

    def weights(j):
        slot = lax.rem(j, 4)
        return pltpu.make_async_copy(w_ref.at[:, _tile(j, tile)], w.at[slot], sems_w.at[slot])

    def term(g, j):
        return _dot(hid[pl.ds(g * group, group), :], w[lax.rem(j, 4)]).reshape(8, size, tile)

    def move(l, src, dst, s_sem, t_sem, j):
        return _copy(side, LINKS[l], src, dst, s_sem, t_sem)

    def pairs(src, dst, s_sem, t_sem, j):
        a, b = lax.rem(j, 2), lax.rem(j, ring)
        return [_copy(side, LINKS[l], src.at[a, pl.ds(2 * l, 2)], dst.at[b, pl.ds(2 * l, 2)], s_sem.at[a, l], t_sem.at[b, l])
                for l in range(4)]

    ring2 = _Sum(side, *second)

    def each(copies, what):
        for c in copies:
            getattr(c, what)()

    weights(0).start()
    for n in range(len(ORDER)):
        fetch(n).start()
    residual = pltpu.make_async_copy(x_ref, res, sems_x.at[0])
    residual.start()
    _meet(side)()
    for n in range(len(ORDER)):
        fetch(n).wait()
    residual.wait()

    def step(i, _):
        @_during(i, 0, tiles)
        def _():
            j = i

            @pl.when(j + 1 < tiles)
            def _():
                weights(j + 1).start()

            weights(j).wait()

            @pl.when(j >= 2)
            def _():
                each(pairs(far, r_far, s_far, t_far, j), "wait_send")
                each(pairs(plain, r_plain, s_plain, t_plain, j), "wait_send")

            far[lax.rem(j, 2)] = term(0, j).astype(jnp.bfloat16)
            each(pairs(far, r_far, s_far, t_far, j), "start")

            plain[lax.rem(j, 2)] = term(1, j).astype(jnp.bfloat16)
            each(pairs(plain, r_plain, s_plain, t_plain, j), "start")

        @_during(i, 1, tiles)
        def _():
            j = i - 1

            @pl.when(j >= 2)
            def _():
                each(pairs(summed, r_summed, s_summed, t_summed, j), "wait_send")

            each(pairs(far, r_far, s_far, t_far, j), "wait_recv")
            summed[lax.rem(j, 2)] = (term(2, j) + r_far[lax.rem(j, ring)].astype(jnp.float32)).astype(jnp.bfloat16)
            each(pairs(summed, r_summed, s_summed, t_summed, j), "start")

        @_during(i, 2, tiles)
        def _():
            j = i - 2
            b = lax.rem(j, ring)

            ring2.freed(j)
            each(pairs(plain, r_plain, s_plain, t_plain, j), "wait_recv")
            each(pairs(summed, r_summed, s_summed, t_summed, j), "wait_recv")
            mine = term(3, j)
            for half in HALVES:
                l = 2 * half
                up, down = pl.ds(2 * l, 2), pl.ds(2 * l + 2, 2)
                from_up = jnp.concatenate([r_summed[b, up], r_plain[b, up]]).astype(jnp.float32)
                from_down = jnp.concatenate([r_plain[b, down], r_summed[b, down]]).astype(jnp.float32)
                both_ways = mine[4 * half : 4 * half + 4] + from_up + from_down
                sums = {across: both_ways[k] for k, across in enumerate(UP + DOWN)}
                ring2.put(j, half, 2 - l, sums)
            ring2.leave(j)

        @_during(i, 3, tiles)
        def _():
            ring2.merge(i - 3)

        @pl.when(i >= 4)
        def _():
            j = i - 4

            ring2.arrived(j)
            here = _tile(j, tile)
            for half in HALVES:
                mine = pl.ds(half * size, size)
                out[mine, here] = (res[mine, here].astype(jnp.float32) + ring2.total(j, half, 2 - 2 * half)).astype(jnp.bfloat16)

    lax.fori_loop(0, tiles + 4, step, None)
    for j in range(tiles - 2, tiles):
        each(pairs(far, r_far, s_far, t_far, j), "wait_send")
        each(pairs(plain, r_plain, s_plain, t_plain, j), "wait_send")
        each(pairs(summed, r_summed, s_summed, t_summed, j), "wait_send")
        ring2.left(j)


def scattered(terms, x, w, number, name):
    rows, width = x.shape
    depth = w.shape[0]
    n = lax.axis_size("tp")
    side = int(round(n**0.5))
    size, low = rows // 2, rows // 4
    tile = min(TILE, width)
    tiles = width // tile
    bf, dma = jnp.bfloat16, pltpu.SemaphoreType.DMA
    return pl.pallas_call(
        functools.partial(_scatter_kernel, side=side),
        out_shape=jax.ShapeDtypeStruct((rows, width), bf),
        in_specs=[pl.BlockSpec(memory_space=pl.ANY)] * 3,
        out_specs=pl.BlockSpec(memory_space=pltpu.VMEM),
        scratch_shapes=[
            pltpu.VMEM((n * rows, depth), bf),
            pltpu.VMEM((rows, width), bf),
            pltpu.VMEM((4, depth, tile), bf),
            pltpu.VMEM((2, 8, size, tile), bf),
            pltpu.VMEM((2, 8, size, tile), bf),
            pltpu.VMEM((2, 8, size, tile), bf),
            pltpu.VMEM((RING, 8, size, tile), bf),
            pltpu.VMEM((RING, 8, size, tile), bf),
            pltpu.VMEM((RING, 8, size, tile), bf),
            dma((len(ORDER),)), dma((1,)), dma((4,)),
            *[dma((2, 4))] * 3, *[dma((RING, 4))] * 3,
            *_Sum.scratch(RING, low, tile),
        ],
        compiler_params=pltpu.CompilerParams(collective_id=number, has_side_effects=True, vmem_limit_bytes=LAST_VMEM),
        cost_estimate=_cost(n * rows, depth, width),
        name=name,
    )(terms, x, w)


AROUND = (0, 1, -1, FAR)
ORIGIN = (0, -1, 1, FAR)
TURNS = (FAR, 1, -1, 0)


def _attend(qkv, mine, o, top_s, mix_s):
    size, d = o.shape[0], qkv.shape[2]
    heads = qkv.shape[0] // 3
    e = d**-0.5 * LOG2E
    top_s[...] = jnp.full(top_s.shape, NEG, jnp.float32)
    mix_s[...] = jnp.zeros(mix_s.shape, jnp.float32)
    ones = jnp.ones((8, size), qkv.dtype)

    def block(j, masked):
        here = _tile(j, size)
        scores = [_dot(qkv[heads + i, here, :], qkv[i, _tile(mine, size), :], 1, 1) for i in range(heads)]
        if masked:
            seen = lax.broadcasted_iota(jnp.int32, (size, size), 1) >= lax.broadcasted_iota(jnp.int32, (size, size), 0)
        weights, keeps = [], []
        for i, s in enumerate(scores):
            s = jnp.where(seen, s, HIDDEN) if masked else s
            old = top_s[i : i + 1, :]
            top = jnp.maximum(old, s.max(axis=0, keepdims=True))
            top_s[i : i + 1, :] = top
            weights.append(jnp.exp2((s - top) * e).astype(qkv.dtype))
            keeps.append(jnp.exp2((old - top) * e))
        for i, (p, keep) in enumerate(zip(weights, keeps)):
            values = jnp.concatenate([qkv[2 * heads + i, here, :].T, ones], axis=0)
            mix_s[i] = mix_s[i] * keep + _dot(values, p, 1, 0)

    lax.fori_loop(0, mine, lambda j, _: block(j, False), None)
    block(mine, True)
    for i in range(heads):
        total = mix_s[i, d : d + 1, :]
        o[:, i * d : (i + 1) * d] = (mix_s[i, :d, :] * (1 / total)).T.astype(o.dtype)


def _share_kernel(qkv_ref, x_ref, w_ref, left_ref, right_ref, out_ref, qkv, seen, top_s, mix_s, s, relay, w, res, out, sems_q, sems_x, sems_w,
                  sems_o, s_next, s_far, s_pass, t_next, t_far, t_pass, *second, side):
    rows, width = out_ref.shape
    depth, tile = w_ref.shape[0], w.shape[3]
    half, tiles = width // 2, width // 2 // tile
    slots = w.shape[0]
    ring = _Sum(side, *second)
    x, y = _place(side)

    def block(t, along, across):
        dx, dy = (along, across) if t == 0 else (across, along)
        return seen.at[TURNS.index(dx), _tile(lax.rem(y + (dy + side), side), rows)]

    def place(t, across, origin):
        return s.at[t, _tile(AROUND.index(across), rows), _tile(ORIGIN.index(origin), depth)]

    ways = [(t, n, sign) for t in HALVES for n, sign in enumerate(SIGNS)]

    def far(t, along, across):
        n, i = divmod(AROUND.index(across), 2)
        sign = 1 - 2 * n
        return _copy(side, ("xy"[t], sign), block(t, FAR, across), relay.at[t, n, i], s_far.at[t, n, i], t_far.at[t, n, i])

    def passed(t, across):
        n, i = divmod(AROUND.index(across), 2)
        return _copy(side, ("xy"[t], 1 - 2 * n), relay.at[t, n, i], place(t, across, FAR), s_pass.at[t, n, i], t_pass.at[t, n, i])

    def next_to(t, sign, across):
        at = t, int(sign < 0), AROUND.index(across)
        return _copy(side, ("xy"[t], sign), block(t, sign, across), place(t, across, -sign), s_next.at[at], t_next.at[at])

    def sends(t, along, across):
        if along:
            (far if along == FAR else next_to)(t, along, across).start()
        else:
            place(t, across, 0)[...] = block(t, 0, across)[...]

    def each(what, copies):
        for c in copies:
            getattr(c, what)()

    def weights(j):
        got = []
        for t, shelf in enumerate((left_ref, right_ref)):
            for i in range(side):
                src = shelf.at[i - 1, :, _tile(j, tile)] if i else w_ref.at[:, _tile(t * tiles + j, tile)]
                got.append(pltpu.make_async_copy(src, w.at[lax.rem(j, slots), t, pl.ds(i * depth, depth)], sems_w.at[lax.rem(j, slots), t, i]))
        return got

    def out_copy(t, j):
        here = _tile(t * tiles + j, tile)
        return pltpu.make_async_copy(out.at[:, here], out_ref.at[:, here], sems_o.at[t, j])

    met = _meet(side)
    heads = qkv.shape[0] // 3
    parts = [pltpu.make_async_copy(qkv_ref.at[here], qkv.at[here], sems_q.at[n]) for n in range(3) for here in [pl.ds(n * heads, heads)]]
    each("start", parts)
    for j in range(slots - 1):
        each("start", weights(j))
    residual = pltpu.make_async_copy(x_ref, res, sems_x.at[0])
    residual.start()
    each("wait", parts)
    met()

    def turn(n, _):
        _attend(qkv, lax.rem(x + (FAR + len(TURNS) * 2) - lax.div(n * (n + 1), 2), side), seen.at[n], top_s, mix_s)
        for k, dx in enumerate(TURNS):

            @pl.when(n == k)
            def _(dx=dx):
                for other in AROUND:
                    sends(0, dx, other)
                    sends(1, other, dx)

    lax.fori_loop(0, len(TURNS), turn, None)
    for t in HALVES:
        for across in TURNS:
            far(t, FAR, across).wait_recv()
            passed(t, across).start()
    for t, n, sign in ways:
        each("wait_recv", [next_to(t, sign, across) for across in AROUND])
    residual.wait()
    for t in HALVES:
        each("wait_recv", [passed(t, across) for across in AROUND])

    def step(i, _):
        @_during(i, 0, tiles)
        def _():
            j = i

            @pl.when(j + (slots - 1) < tiles)
            def _():
                each("start", weights(j + (slots - 1)))

            each("wait", weights(j))
            ring.freed(j)
            for t in HALVES:
                got = _dot(s[t], w[lax.rem(j, slots), t])
                ring.put(j, t, 2 * t, {across: got[k * rows : (k + 1) * rows] for k, across in enumerate(AROUND)})
            ring.leave(j)

        @_during(i, 1, tiles)
        def _():
            ring.merge(i - 1)

        @pl.when(i >= 2)
        def _():
            j = i - 2
            ring.arrived(j)
            for t in HALVES:
                here = _tile(t * tiles + j, tile)
                out[:, here] = (res[:, here].astype(jnp.float32) + ring.total(j, t, 2 * t)).astype(jnp.bfloat16)
                out_copy(t, j).start()

    lax.fori_loop(0, tiles + 2, step, None)
    for j in range(tiles - 2, tiles):
        ring.left(j)
    for t, n, sign in ways:
        each("wait_send", [next_to(t, sign, across) for across in AROUND])
    for t in HALVES:
        each("wait_send", [copy for across in AROUND for copy in (far(t, FAR, across), passed(t, across))])
        for j in range(tiles):
            out_copy(t, j).wait()


def projected(qkv, x, w, left, right, number, name):
    rows, width = x.shape
    depth = w.shape[0]
    n = lax.axis_size("tp")
    side = int(round(n**0.5))
    tile = min(TILE, width // 2)
    tiles = width // 2 // tile
    bf, dma = jnp.bfloat16, pltpu.SemaphoreType.DMA
    anywhere = pl.BlockSpec(memory_space=pl.ANY)
    return pl.pallas_call(
        functools.partial(_share_kernel, side=side),
        out_shape=jax.ShapeDtypeStruct((rows, width), bf),
        in_specs=[anywhere] * 5,
        out_specs=anywhere,
        scratch_shapes=[
            pltpu.VMEM(qkv.shape, bf),
            pltpu.VMEM((side, side * rows, depth), bf),
            pltpu.VMEM((qkv.shape[0] // 3, side * rows), jnp.float32),
            pltpu.VMEM((qkv.shape[0] // 3, HEAD + 8, side * rows), jnp.float32),
            pltpu.VMEM((2, side * rows, side * depth), bf),
            pltpu.VMEM((2, 2, 2, rows, depth), bf),
            pltpu.VMEM((3, 2, side * depth, tile), bf),
            pltpu.VMEM((rows, width), bf),
            pltpu.VMEM((rows, width), bf),
            dma((3,)), dma((1,)), dma((3, 2, side)), dma((2, tiles)),
            *[dma((2, 2, 4)), dma((2, 2, 2)), dma((2, 2, 2))] * 2,
            *_Sum.scratch(tiles, rows // 2, tile),
        ],
        compiler_params=pltpu.CompilerParams(collective_id=number, has_side_effects=True, vmem_limit_bytes=VMEM),
        cost_estimate=_cost(n * rows, depth, width, side),
        name=name,
    )(qkv, x, w, left, right)


def _angles(tokens):
    half = HEAD // 2
    rate = np.power(np.float32(THETA), -np.arange(half, dtype=np.float32) / np.float32(half)).astype(np.float32)
    angle = (np.arange(tokens, dtype=np.float32)[:, None] * rate).astype(np.float64)
    return np.concatenate([np.cos(angle), np.sin(angle)], 1).astype(np.float32)


def solution(mesh):
    n = mesh.shape["tp"]

    def step(x, gain_a, wq, wk, wv, wo, gain_m, w_gate, w_up, w_down):
        rows = n * x.shape[0]
        heads = wq.shape[1] // HEAD
        qkv, left, right = gathered(
            x, gain_a, (wq, wk, wv), _Heads(2), 2 * BLOCK, jax.ShapeDtypeStruct((3 * heads, rows, HEAD), jnp.bfloat16), 0, "gather_qkv",
            extra=(jnp.asarray(_angles(rows)),),
            scratch=(pltpu.VMEM((rows, HEAD), jnp.float32), pltpu.SemaphoreType.DMA((len(SLOTS),))),
            share=wo, twins=mesh.shape["dp"] % 2 == 0,
        )
        h = projected(qkv, x, wo, left, right, 1, "project")
        hidden = gathered(h, gain_m, (w_gate, w_up), _Hidden(), BLOCK, jax.ShapeDtypeStruct((rows, w_gate.shape[1]), jnp.bfloat16), 2,
                          "gather_hidden")
        return scattered(hidden, h, w_down, 3, "scatter_down")

    tokens, columns, rows_of = P(("dp", "tp"), None), P(None, "tp"), P("tp", None)
    return jax.shard_map(
        step,
        mesh=mesh,
        in_specs=(tokens, P(None), columns, columns, columns, rows_of, P(None), columns, columns, rows_of),
        out_specs=tokens,
        check_vma=False,
    )
```

```python
import functools

import jax
import jax.numpy as jnp
import numpy as np
from jax import lax
from jax.experimental import pallas as pl
from jax.experimental.pallas import tpu as pltpu
from jax.sharding import PartitionSpec as P

MESH = pl.DeviceIdType.MESH
HEAD = 128
THETA = 10000
NEG = -1e30
HIDDEN = 2 * NEG
LOG2E = 1.4426950408889634
VMEM = 62 << 20
LAST_VMEM = 48 << 20
BLOCK = 256
TILE = 512
RING = 6

A, B = 0, 1
FAR = 2
UP, DOWN = (0, -1), (1, FAR)
LINKS = (("y", 1), ("y", -1), ("x", 1), ("x", -1))


def piece(half, along, across):
    return (half, across, along) if half == A else (half, along, across)


def both(along, across):
    return [piece(A, along, across), piece(B, along, across)]


NEXT, SIGNS, HALVES = (-1, 1), (1, -1), (A, B)
SLOTS = [
    p
    for group in (
        [both(0, 0)],
        [[piece(half, 0, d) for d in NEXT] for half in HALVES],
        [[piece(half, d, 0) for d in NEXT] for half in HALVES],
        [both(0, FAR)],
        *([[piece(half, d, across) for d in NEXT] for half in HALVES] for across in NEXT),
        [both(FAR, 0), both(1, FAR), both(-1, FAR), both(FAR, 1), both(FAR, -1), both(FAR, FAR)],
    )
    for some in group
    for p in some
]
SLOT = {p: n for n, p in enumerate(SLOTS)}

def _by_link(along, pick):
    return [
        piece(half, along if along == 2 else sign * along, across)
        for (axis, sign) in LINKS
        for half in [A if axis == "y" else B]
        for across in (UP if (sign > 0) == pick else DOWN)
    ]


ORDER = _by_link(2, True) + _by_link(1, False) + _by_link(1, True) + [piece(half, 0, across) for half in HALVES for across in UP + DOWN]


def _place(side):
    me = lax.axis_index("tp")
    return lax.div(me, side), lax.rem(me, side)


def _device(side, dx, dy):
    x, y = _place(side)
    return lax.rem(x + (dx + side), side) * side + lax.rem(y + (dy + side), side)


def _meet(side, twin=False):
    barrier = pltpu.get_barrier_semaphore()
    others = [{"tp": _device(side, *_step(link))} for link in LINKS] + ([_twin()] if twin else [])
    for other in others:
        pl.semaphore_signal(barrier, inc=1, device_id=other, device_id_type=MESH)
    return lambda: pl.semaphore_wait(barrier, len(others))


def _twin():
    group = lax.axis_index("dp")
    return {"dp": group + 1 - 2 * lax.rem(group, 2), "tp": lax.axis_index("tp")}


def _step(link):
    axis, sign = link
    return (sign, 0) if axis == "x" else (0, sign)


def _copy(side, link, src, dst, send_sem, recv_sem):
    return pltpu.make_async_remote_copy(src_ref=src, dst_ref=dst, send_sem=send_sem, recv_sem=recv_sem,
                                        device_id={"tp": _device(side, *_step(link))}, device_id_type=MESH)


def _cost(rows, depth, width, passes=1):
    return pl.CostEstimate(flops=2 * rows * depth * width, transcendentals=0, bytes_accessed=2 * passes * depth * width)


def _tile(i, size):
    return pl.ds(pl.multiple_of(i * size, size), size)


def _during(i, late, count):
    return pl.when((i >= late) & (i < count + late))


def _dot(a, b, ca=1, cb=0):
    return lax.dot_general(a, b, (((ca,), (cb,)), ((), ())), preferred_element_type=jnp.float32)


def _plan():
    slot = lambda half, along, across: SLOT[piece(half, along, across)]

    def inner(half, sign, source, target, part=0, of="all"):
        return ("xy"[half], sign), slot(half, 0, source), slot(half, 0, target), part, of

    def outer(half, sign, source, across, part=0, of="all"):
        target = -sign if source == 0 else FAR
        return ("yx"[half], sign), slot(half, source, across), slot(half, target, across), part, of

    def final(*which):
        return [outer(*which, part, "columns") for part in HALVES]

    halves, signs = HALVES, SIGNS
    return [
        [inner(A, sign, 0, -sign) for sign in signs],
        [inner(B, sign, 0, -sign) for sign in signs],
        [outer(half, sign, 0, 0) for half in (B, A) for sign in signs],
        [inner(half, sign, -sign, FAR, int(sign < 0), "rows") for half in halves for sign in signs]
        + [outer(half, sign, 0, across) for across in NEXT for half in halves for sign in signs],
        [outer(half, 1, -1, 0) for half in halves],
        [outer(half, sign, 0, FAR) for half in halves for sign in signs],
        [copy for half in halves for copy in final(half, 1, -1, -1)],
        [outer(half, -1, 1, 1) for half in halves],
        [copy for half in halves for copy in final(half, -1, 1, FAR)],
    ]


PLAN = _plan()
COPIES = [c for group in PLAN for c in group]
_ENDS = (6, 10, 12, 16, 20, 24, 28, len(SLOTS))
EVENTS = [(SLOTS[a:b], k + 3 if k + 3 < len(PLAN) else None) for k, (a, b) in enumerate(zip((0, *_ENDS), _ENDS))]


def _gather_kernel(x_ref, gain_ref, *refs, side, finish, counts, twins):
    refs = iter(refs)
    take = lambda n: [next(refs) for _ in range(n)]
    extra_refs, w_refs, shared = (take(n) for n in counts[:3])
    (out_ref,), shelves = take(1), take(2 * len(shared))
    g, gain, w, stage, sems_x, sems_w, sems_o, send, recv = take(9)
    more = take(counts[3])
    carry = _Carry(side, twins, shared[0], shelves, *refs) if shared else None
    rows, depth = x_ref.shape
    size = rows // 2
    tiles = sum(ref.shape[1] for ref in w_refs) // w.shape[2]
    ring = min(w.shape[0], tiles)
    loads = tiles if tiles <= ring else len(EVENTS) * tiles

    def weights(s, start):
        finish.weights(w_refs, lax.rem(s, tiles), w, lax.rem(s, ring), sems_w, "start" if start else "wait")

    def remote(number):
        link, src, dst, part, of = COPIES[number]
        height = size // 2 if of == "rows" else size
        width = depth // 2 if of == "columns" else depth
        above, left = (part * height, 0) if of == "rows" else (0, part * width)
        here = [g.at[pl.ds(slot * size + above, height), pl.ds(left, width)] for slot in (src, dst)]
        return _copy(side, link, *here, send.at[number], recv.at[dst, part])

    def begin(group):
        first = sum(len(p) for p in PLAN[:group])
        for number in range(first, first + len(PLAN[group])):
            remote(number).start()

    def arrived(slots, parts=HALVES):
        for number, (_, _, dst, part, _) in enumerate(COPIES):
            if SLOTS[dst] in slots and part in parts:
                remote(number).wait_recv()

    met = _meet(side, bool(carry and twins))
    own = [pltpu.make_async_copy(x_ref.at[here], g.at[here], sems_x.at[half]) for half in HALVES for here in [pl.ds(half * size, size)]]
    gains = pltpu.make_async_copy(gain_ref, gain, sems_x.at[2])
    for c in (own[A], gains, own[B]):
        c.start()

    def norm(i, _):
        here = _tile(i, 16)
        wide = g[here, :].astype(jnp.float32)
        scale = lax.rsqrt(jnp.mean(wide * wide, -1, keepdims=True) + 1e-6)
        g[here, :] = (wide * scale * gain[...].astype(jnp.float32)[None]).astype(jnp.bfloat16)

    gains.wait()
    if carry:
        met()
        carry.begin()
    for half in HALVES:
        own[half].wait()
        lax.fori_loop(half * size // 16, (half + 1) * size // 16, norm, None)
        if half == A:
            carry.proceed() if carry else met()
        begin(half)
    begin(2)
    for s in range(ring - 1):
        weights(s, True)
    if finish.prepare:
        finish.prepare(extra_refs, more)
    if carry:
        for k in HALVES:
            carry.hand(k)

    def block(b, _):
        for k, (slots, group) in enumerate(EVENTS):

            @pl.when(b == k)
            def _(slots=slots, group=group):
                arrived(slots)
                if group is not None:
                    begin(group)
        def tile(n, _):
            s = b * tiles + n

            @pl.when(s + (ring - 1) < loads)
            def _():
                weights(s + (ring - 1), True)

            @pl.when(s < loads)
            def _():
                weights(s, False)

            product(b, n, s, g.at[_tile(b, BLOCK)], w.at[lax.rem(s, ring)])

        lax.fori_loop(0, tiles, tile, None)

    def product(b, n, s, lhs, rhs, *partial):
        to = lax.rem(s, 2)

        @pl.when(s >= 2)
        def _():
            finish.store(stage, out_ref, sems_o, to, b, n, size, side, start=False)

        finish.compute(lhs, rhs, stage.at[to], b, n, more, *partial)
        finish.store(stage, out_ref, sems_o, to, b, n, size, side, start=True)

    final = len(EVENTS) - 1
    whole = final if finish.in_parts else len(EVENTS)
    lax.fori_loop(0, whole, block, None)
    if whole == final:
        for part in HALVES:
            arrived(EVENTS[final][0], [part])
            here = pl.ds(part * (depth // 2), depth // 2)
            lhs = g.at[pl.ds(final * BLOCK, BLOCK), here]

            def tile(n, _, part=part, here=here, lhs=lhs):
                partial, *_ = more
                if part == A:
                    partial[n] = _dot(lhs[...], w[n, here, :])
                else:
                    product(final, n, final * tiles + n, lhs, w.at[n, here], partial)

            lax.fori_loop(0, tiles, tile, None)
    for to in range(2):
        finish.store(stage, out_ref, sems_o, to, 0, 0, size, side, start=False)
    for number in range(len(COPIES)):
        remote(number).wait_send()
    if carry:
        carry.end()


class _Carry:
    SHELF = {-1: 0, 1: 1, FAR: 2}

    def __init__(self, side, twins, w_ref, shelves, send, recv, give, got):
        self.side, self.twins, self.w_ref, self.shelves = side, twins, w_ref, shelves
        self.send, self.recv, self.give, self.got = send, recv, give, got

    def carrier(self, body):
        if self.twins:
            pl.when(lax.rem(lax.axis_index("dp"), 2) == 0)(body)
        else:
            body()

    def copies(self, step):
        for t, shelf in enumerate(self.shelves):
            for sign in SIGNS:
                depth, width = shelf.shape[1:]
                here = pl.ds((int(sign < 0) ^ (step == 1)) * (depth // 2), depth // 2)
                if step == 2:
                    src, dst = shelf.at[self.SHELF[-sign], here], shelf.at[self.SHELF[FAR], here]
                else:
                    src, dst = self.w_ref.at[here, pl.ds(t * width, width)], shelf.at[self.SHELF[-sign], here]
                sem = t, int(sign < 0), step
                yield _copy(self.side, ("xy"[t], sign), src, dst, self.send.at[sem], self.recv.at[sem])

    def handed(self, k):
        for t, shelf in enumerate(self.shelves):
            for at in ((0, 1), (2,))[k]:
                yield pltpu.make_async_remote_copy(src_ref=shelf.at[at], dst_ref=shelf.at[at], send_sem=self.give.at[t, at],
                                                   recv_sem=self.got.at[t, at], device_id=_twin(), device_id_type=MESH)

    def all(self, copies, what):
        for c in copies:
            getattr(c, what)()

    def begin(self):
        @self.carrier
        def _():
            for step in HALVES:
                self.all(self.copies(step), "start")

    def proceed(self):
        @self.carrier
        def _():
            self.all(self.copies(0), "wait_recv")
            self.all(self.copies(2), "start")

    def hand(self, k):
        @self.carrier
        def _():
            self.all(self.copies(k + 1), "wait_recv")
            if self.twins:
                self.all(self.handed(k), "start")

    def end(self):
        @self.carrier
        def _():
            for step in range(3):
                self.all(self.copies(step), "wait_send")
            if self.twins:
                for k in HALVES:
                    self.all(self.handed(k), "wait_send")

        if self.twins:

            @pl.when(lax.rem(lax.axis_index("dp"), 2) == 1)
            def _():
                for k in HALVES:
                    self.all(self.handed(k), "wait_recv")


class _Heads:
    in_parts = True

    def __init__(self, turned_steps):
        self.turned_steps = turned_steps

    def weights(self, refs, n, w, slot, sems, what):
        for at, ref in enumerate(refs):

            @pl.when(n == at)
            def _(ref=ref):
                getattr(pltpu.make_async_copy(ref, w.at[slot], sems.at[slot, 0]), what)()

    def prepare(self, extra_refs, more):
        (table_ref,) = extra_refs
        _, table, sems = more
        size = table.shape[0] // len(SLOTS)
        side = int(round((len(SLOTS) // 2) ** 0.5))
        copies = []
        for n, (half, dx, dy) in enumerate(SLOTS):
            row = _device(side, dx, dy) * (2 * size) + half * size
            copies.append(pltpu.make_async_copy(table_ref.at[pl.ds(pl.multiple_of(row, size), size)], table.at[pl.ds(n * size, size)],
                                                sems.at[n]))
        for what in ("start", "wait"):
            for c in copies:
                getattr(c, what)()

    def compute(self, lhs, w, to, at, n, more, partial=None):
        _, table, _ = more
        got = _dot(lhs[...], w[...])
        got = (got if partial is None else got + partial[n]).astype(jnp.bfloat16)

        @pl.when(n < self.turned_steps)
        def _():
            t = table[_tile(at, BLOCK), :]
            swapped = pltpu.roll(t, HEAD // 2, 1)
            low = lax.broadcasted_iota(jnp.int32, t.shape, 1) < HEAD // 2
            cos, sin = jnp.where(low, t, swapped), jnp.where(low, -swapped, t)
            for i in range(0, w.shape[1], HEAD):
                one = got[:, i : i + HEAD].astype(jnp.float32)
                to[:, i : i + HEAD] = (one * cos + pltpu.roll(one, HEAD // 2, 1) * sin).astype(jnp.bfloat16)

        @pl.when(n >= self.turned_steps)
        def _():
            to[...] = got

    def store(self, stage, out_ref, sems, to, at, n, size, side, start):
        per = BLOCK // size

        heads = stage.shape[2] // HEAD

        def copies(pieces):
            for p, (half, dx, dy) in enumerate(pieces):
                row = pl.multiple_of(_device(side, dx, dy) * (2 * size) + half * size, size)
                for i in range(heads):
                    yield pltpu.make_async_copy(stage.at[to, pl.ds(p * size, size), pl.ds(i * HEAD, HEAD)],
                                                out_ref.at[n * heads + i, pl.ds(row, size)], sems.at[to, p * heads + i])

        if not start:
            for c in copies(SLOTS[:per]):
                c.wait()
            return
        for k in range(len(SLOTS) // per):

            @pl.when(at == k)
            def _(k=k):
                for c in copies(SLOTS[k * per : (k + 1) * per]):
                    c.start()


class _Hidden:
    prepare = None
    in_parts = False

    def weights(self, refs, n, w, slot, sems, what):
        for at, ref in enumerate(refs):
            here = _tile(n, BLOCK)
            getattr(pltpu.make_async_copy(ref.at[:, here], w.at[slot, :, pl.ds(at * BLOCK, BLOCK)], sems.at[slot, at]), what)()

    def compute(self, lhs, w, to, at, n, more):
        got = _dot(lhs[...], w[...])
        to[...] = (jax.nn.silu(got[:, :BLOCK]) * got[:, BLOCK:]).astype(jnp.bfloat16)

    def store(self, stage, out_ref, sems, to, at, n, size, side, start):
        c = pltpu.make_async_copy(stage.at[to], out_ref.at[_tile(at, BLOCK),
                                                           _tile(n, BLOCK)], sems.at[to, 0])
        c.start() if start else c.wait()


def gathered(x, gain, weights, finish, stored, out_shape, number, name, extra=(), scratch=(), share=None, twins=False):
    rows, depth = x.shape
    n = lax.axis_size("tp")
    side = int(round(n**0.5))
    width = sum(w.shape[1] for w in weights)
    anywhere, dma = pl.BlockSpec(memory_space=pl.ANY), pltpu.SemaphoreType.DMA
    shared = [] if share is None else [share]
    shelves = [jax.ShapeDtypeStruct((side - 1, w.shape[0], w.shape[1] // 2), w.dtype) for w in 2 * shared]
    operands = [x, gain, *extra, *weights, *shared]
    return pl.pallas_call(
        functools.partial(_gather_kernel, side=side, finish=finish, counts=(len(extra), len(weights), len(shared), len(scratch)), twins=twins),
        out_shape=[out_shape, *shelves] if shared else out_shape,
        in_specs=[anywhere] * len(operands),
        out_specs=[anywhere] * 3 if shared else anywhere,
        scratch_shapes=[
            pltpu.VMEM((n * rows, depth), jnp.bfloat16),
            pltpu.VMEM((depth,), jnp.bfloat16),
            pltpu.VMEM((3, depth, 2 * BLOCK), jnp.bfloat16),
            pltpu.VMEM((2, BLOCK, stored), jnp.bfloat16),
            dma((3,)), dma((3, 2)), dma((2, len(SLOTS))), dma((len(COPIES),)), dma((len(SLOTS), 2)),
            *scratch,
            *([dma((2, 2, 3))] * 2 + [dma((2, 3))] * 2 if shared else []),
        ],
        compiler_params=pltpu.CompilerParams(collective_id=number, has_side_effects=True, vmem_limit_bytes=VMEM),
        cost_estimate=_cost(n * rows, depth, width, len(EVENTS)),
        name=name,
    )(*operands)


class _Sum:
    def __init__(self, side, near, keep, own, r_half, r_near, s_half, s_near, t_half, t_near):
        self.side, self.near, self.keep, self.own = side, near, keep, own
        self.r_half, self.r_near, self.s_half, self.s_near, self.t_half, self.t_near = r_half, r_near, s_half, s_near, t_half, t_near
        self.low = keep.shape[2]

    def halves(self, j):
        a, b = lax.rem(j, 2), lax.rem(j, self.r_half.shape[0])
        return [_copy(self.side, link, self.near.at[a, 0, l], self.r_half.at[b, l], self.s_half.at[a, l], self.t_half.at[b, l])
                for l, link in enumerate(LINKS)]

    def lasts(self, j, part):
        a, b = lax.rem(j, 2), lax.rem(j, self.r_near.shape[0])
        got = []
        for l, link in enumerate(LINKS):
            at = l % 2 if part else 1 - l % 2
            got.append(_copy(self.side, link, self.near.at[a, 1 + part, l], self.r_near.at[b, l, pl.ds(at * self.low, self.low)],
                             self.s_near.at[a, part, l], self.t_near.at[b, part, l]))
        return got

    def each(self, what, *groups):
        for c in sum(groups, []):
            getattr(c, what)()

    def freed(self, j):
        self.each("wait_send", self.halves(j), self.lasts(j, 0))

    def gone(self, j):
        self.each("wait_send", self.lasts(j, 1))

    def put(self, j, t, l, pieces):
        a, low, bf = lax.rem(j, 2), self.low, jnp.bfloat16
        self.own[lax.rem(j, 4), t] = pieces[0]
        self.near[a, 0, l] = pieces[FAR][:low].astype(bf)
        self.near[a, 0, l + 1] = pieces[FAR][low:].astype(bf)
        self.near[a, 1, l] = pieces[1][low:].astype(bf)
        self.near[a, 1, l + 1] = pieces[-1][:low].astype(bf)
        self.keep[a, l] = pieces[1][:low]
        self.keep[a, l + 1] = pieces[-1][low:]

    def leave(self, j):
        self.each("start", self.halves(j), self.lasts(j, 0))

    def merge(self, j):
        a, b = lax.rem(j, 2), lax.rem(j, self.r_half.shape[0])
        self.each("wait_recv", self.halves(j))
        for l in range(len(LINKS)):
            self.near[a, 2, l] = (self.keep[a, l] + self.r_half[b, l].astype(jnp.float32)).astype(jnp.bfloat16)
        self.each("start", self.lasts(j, 1))

    def arrived(self, j):
        self.each("wait_recv", self.lasts(j, 0), self.lasts(j, 1))

    def total(self, j, t, l):
        b = lax.rem(j, self.r_near.shape[0])
        return self.own[lax.rem(j, 4), t] + self.r_near[b, l].astype(jnp.float32) + self.r_near[b, l + 1].astype(jnp.float32)

    @staticmethod
    def scratch(rings, low, tile):
        bf, f32, dma = jnp.bfloat16, jnp.float32, pltpu.SemaphoreType.DMA
        return [pltpu.VMEM((2, 3, 4, low, tile), bf), pltpu.VMEM((2, 4, low, tile), f32), pltpu.VMEM((4, 2, 2 * low, tile), f32),
                pltpu.VMEM((rings, 4, low, tile), bf), pltpu.VMEM((rings, 4, 2 * low, tile), bf),
                dma((2, 4)), dma((2, 2, 4)), dma((rings, 4)), dma((rings, 2, 4))]


def _scatter_kernel(rows_ref, x_ref, w_ref, out, hid, res, w, far, plain, summed, r_far, r_plain, r_summed, sems_h, sems_x, sems_w,
                    s_far, s_plain, s_summed, t_far, t_plain, t_summed, *second, side):
    rows, width = out.shape
    size = rows // 2
    tile = w.shape[2]
    tiles = width // tile
    ring = r_far.shape[0]
    group = hid.shape[0] // 4

    def fetch(n):
        return pltpu.make_async_copy(rows_ref.at[pl.ds(SLOT[ORDER[n]] * size, size)], hid.at[pl.ds(n * size, size)], sems_h.at[n])

    def weights(j):
        slot = lax.rem(j, 4)
        return pltpu.make_async_copy(w_ref.at[:, _tile(j, tile)], w.at[slot], sems_w.at[slot])

    def terms(g, j, count=1):
        return _dot(hid[pl.ds(g * group, count * group), :], w[lax.rem(j, 4)]).reshape(-1, size, tile)

    def pairs(src, dst, s_sem, t_sem, j):
        a, b = lax.rem(j, 2), lax.rem(j, ring)
        return [_copy(side, LINKS[l], src.at[a, pl.ds(2 * l, 2)], dst.at[b, pl.ds(2 * l, 2)], s_sem.at[a, l], t_sem.at[b, l])
                for l in range(4)]

    ring2 = _Sum(side, *second)

    def each(copies, what):
        for c in copies:
            getattr(c, what)()

    weights(0).start()
    for n in range(len(ORDER)):
        fetch(n).start()
    residual = pltpu.make_async_copy(x_ref, res, sems_x.at[0])
    residual.start()
    _meet(side)()
    for n in range(len(ORDER)):
        fetch(n).wait()
    residual.wait()

    def step(i, _):
        @_during(i, 2, tiles)
        def _():
            each(pairs(far, r_far, s_far, t_far, i - 2), "wait_send")
            each(pairs(plain, r_plain, s_plain, t_plain, i - 2), "wait_send")

        @_during(i, 0, tiles)
        def _():
            j = i

            @pl.when(j + 1 < tiles)
            def _():
                weights(j + 1).start()

            weights(j).wait()
            got = terms(0, j, 2).astype(jnp.bfloat16)
            far[lax.rem(j, 2)] = got[:8]
            plain[lax.rem(j, 2)] = got[8:]
            each(pairs(far, r_far, s_far, t_far, j), "start")
            each(pairs(plain, r_plain, s_plain, t_plain, j), "start")

        @_during(i, 3, tiles)
        def _():
            each(pairs(summed, r_summed, s_summed, t_summed, i - 3), "wait_send")

        @_during(i, 1, tiles)
        def _():
            j = i - 1
            each(pairs(far, r_far, s_far, t_far, j), "wait_recv")
            summed[lax.rem(j, 2)] = (terms(2, j) + r_far[lax.rem(j, ring)].astype(jnp.float32)).astype(jnp.bfloat16)
            each(pairs(summed, r_summed, s_summed, t_summed, j), "start")

        @_during(i, 4, tiles)
        def _():
            ring2.freed(i - 4)

        @_during(i, 2, tiles)
        def _():
            j = i - 2
            b = lax.rem(j, ring)
            each(pairs(plain, r_plain, s_plain, t_plain, j), "wait_recv")
            each(pairs(summed, r_summed, s_summed, t_summed, j), "wait_recv")
            mine = terms(3, j)
            for half in HALVES:
                l = 2 * half
                up, down = pl.ds(2 * l, 2), pl.ds(2 * l + 2, 2)
                from_up = jnp.concatenate([r_summed[b, up], r_plain[b, up]]).astype(jnp.float32)
                from_down = jnp.concatenate([r_plain[b, down], r_summed[b, down]]).astype(jnp.float32)
                both_ways = mine[4 * half : 4 * half + 4] + from_up + from_down
                sums = {across: both_ways[k] for k, across in enumerate(UP + DOWN)}
                ring2.put(j, half, 2 - l, sums)
            ring2.leave(j)

        @_during(i, 5, tiles)
        def _():
            ring2.gone(i - 5)

        @_during(i, 3, tiles)
        def _():
            ring2.merge(i - 3)

        @pl.when(i >= 4)
        def _():
            j = i - 4

            ring2.arrived(j)
            here = _tile(j, tile)
            for half in HALVES:
                mine = pl.ds(half * size, size)
                out[mine, here] = (res[mine, here].astype(jnp.float32) + ring2.total(j, half, 2 - 2 * half)).astype(jnp.bfloat16)

    lax.fori_loop(0, tiles + 4, step, None)
    ring2.gone(tiles - 1)


def scattered(terms, x, w, number, name):
    rows, width = x.shape
    depth = w.shape[0]
    n = lax.axis_size("tp")
    side = int(round(n**0.5))
    size, low = rows // 2, rows // 4
    tile = min(TILE, width)
    tiles = width // tile
    bf, dma = jnp.bfloat16, pltpu.SemaphoreType.DMA
    return pl.pallas_call(
        functools.partial(_scatter_kernel, side=side),
        out_shape=jax.ShapeDtypeStruct((rows, width), bf),
        in_specs=[pl.BlockSpec(memory_space=pl.ANY)] * 3,
        out_specs=pl.BlockSpec(memory_space=pltpu.VMEM),
        scratch_shapes=[
            pltpu.VMEM((n * rows, depth), bf),
            pltpu.VMEM((rows, width), bf),
            pltpu.VMEM((4, depth, tile), bf),
            pltpu.VMEM((2, 8, size, tile), bf),
            pltpu.VMEM((2, 8, size, tile), bf),
            pltpu.VMEM((2, 8, size, tile), bf),
            pltpu.VMEM((RING, 8, size, tile), bf),
            pltpu.VMEM((RING, 8, size, tile), bf),
            pltpu.VMEM((RING, 8, size, tile), bf),
            dma((len(ORDER),)), dma((1,)), dma((4,)),
            *[dma((2, 4))] * 3, *[dma((RING, 4))] * 3,
            *_Sum.scratch(RING, low, tile),
        ],
        compiler_params=pltpu.CompilerParams(collective_id=number, has_side_effects=True, vmem_limit_bytes=LAST_VMEM),
        cost_estimate=_cost(n * rows, depth, width),
        name=name,
    )(terms, x, w)


AROUND = (0, 1, -1, FAR)
ORIGIN = (0, -1, 1, FAR)
TURNS = (FAR, 1, -1, 0)


def _attend(qkv, mine, o, top_s, mix_s):
    size, d = o.shape[0], qkv.shape[2]
    heads = qkv.shape[0] // 3
    e = d**-0.5 * LOG2E
    top_s[...] = jnp.full(top_s.shape, NEG, jnp.float32)
    mix_s[...] = jnp.zeros(mix_s.shape, jnp.float32)
    ones = jnp.ones((8, size), qkv.dtype)

    def block(j, masked):
        here = _tile(j, size)
        scores = [_dot(qkv[heads + i, here, :], qkv[i, _tile(mine, size), :], 1, 1) for i in range(heads)]
        if masked:
            seen = lax.broadcasted_iota(jnp.int32, (size, size), 1) >= lax.broadcasted_iota(jnp.int32, (size, size), 0)
        weights, keeps = [], []
        for i, s in enumerate(scores):
            s = jnp.where(seen, s, HIDDEN) if masked else s
            old = top_s[i : i + 1, :]
            top = jnp.maximum(old, s.max(axis=0, keepdims=True))
            top_s[i : i + 1, :] = top
            weights.append(jnp.exp2((s - top) * e).astype(qkv.dtype))
            keeps.append(jnp.exp2((old - top) * e))
        for i, (p, keep) in enumerate(zip(weights, keeps)):
            values = jnp.concatenate([qkv[2 * heads + i, here, :].T, ones], axis=0)
            mix_s[i] = mix_s[i] * keep + _dot(values, p, 1, 0)

    lax.fori_loop(0, mine, lambda j, _: block(j, False), None)
    block(mine, True)
    for i in range(heads):
        total = mix_s[i, d : d + 1, :]
        o[:, i * d : (i + 1) * d] = (mix_s[i, :d, :] * (1 / total)).T.astype(o.dtype)


def _share_kernel(qkv_ref, x_ref, w_ref, left_ref, right_ref, out_ref, qkv, seen, top_s, mix_s, s, relay, w, res, out, sems_q, sems_x, sems_w,
                  sems_o, s_next, s_far, s_pass, t_next, t_far, t_pass, *second, side):
    rows, width = out_ref.shape
    depth, tile = w_ref.shape[0], w.shape[3]
    half, tiles = width // 2, width // 2 // tile
    slots = w.shape[0]
    ring = _Sum(side, *second)
    x, y = _place(side)

    def block(t, along, across):
        dx, dy = (along, across) if t == 0 else (across, along)
        return seen.at[TURNS.index(dx), _tile(lax.rem(y + (dy + side), side), rows)]

    def place(t, across, origin):
        return s.at[t, _tile(AROUND.index(across), rows), _tile(ORIGIN.index(origin), depth)]

    ways = [(t, n, sign) for t in HALVES for n, sign in enumerate(SIGNS)]

    def far(t, along, across):
        n, i = divmod(AROUND.index(across), 2)
        sign = 1 - 2 * n
        return _copy(side, ("xy"[t], sign), block(t, FAR, across), relay.at[t, n, i], s_far.at[t, n, i], t_far.at[t, n, i])

    def passed(t, across):
        n, i = divmod(AROUND.index(across), 2)
        return _copy(side, ("xy"[t], 1 - 2 * n), relay.at[t, n, i], place(t, across, FAR), s_pass.at[t, n, i], t_pass.at[t, n, i])

    def next_to(t, sign, across):
        at = t, int(sign < 0), AROUND.index(across)
        return _copy(side, ("xy"[t], sign), block(t, sign, across), place(t, across, -sign), s_next.at[at], t_next.at[at])

    def sends(t, along, across):
        if along:
            (far if along == FAR else next_to)(t, along, across).start()
        else:
            place(t, across, 0)[...] = block(t, 0, across)[...]

    def each(what, copies):
        for c in copies:
            getattr(c, what)()

    def weights(j):
        got = []
        for t, shelf in enumerate((left_ref, right_ref)):
            for i in range(side):
                src = shelf.at[i - 1, :, _tile(j, tile)] if i else w_ref.at[:, _tile(t * tiles + j, tile)]
                got.append(pltpu.make_async_copy(src, w.at[lax.rem(j, slots), t, pl.ds(i * depth, depth)], sems_w.at[lax.rem(j, slots), t, i]))
        return got

    def out_copy(t, j):
        here = _tile(t * tiles + j, tile)
        return pltpu.make_async_copy(out.at[:, here], out_ref.at[:, here], sems_o.at[t, j])

    met = _meet(side)
    heads = qkv.shape[0] // 3
    parts = [pltpu.make_async_copy(qkv_ref.at[here], qkv.at[here], sems_q.at[n]) for n in range(3) for here in [pl.ds(n * heads, heads)]]
    each("start", parts)
    for j in range(slots - 1):
        each("start", weights(j))
    residual = pltpu.make_async_copy(x_ref, res, sems_x.at[0])
    residual.start()
    each("wait", parts)
    met()

    def turn(n, _):
        _attend(qkv, lax.rem(x + (FAR + len(TURNS) * 2) - lax.div(n * (n + 1), 2), side), seen.at[n], top_s, mix_s)
        for k, dx in enumerate(TURNS):

            @pl.when(n == k)
            def _(dx=dx):
                for other in AROUND:
                    sends(0, dx, other)
                    sends(1, other, dx)

    lax.fori_loop(0, len(TURNS), turn, None)
    for t in HALVES:
        for across in TURNS:
            far(t, FAR, across).wait_recv()
            passed(t, across).start()
    for t, n, sign in ways:
        each("wait_recv", [next_to(t, sign, across) for across in AROUND])
    residual.wait()
    for t in HALVES:
        each("wait_recv", [passed(t, across) for across in AROUND])

    def step(i, _):
        @_during(i, 2, tiles)
        def _():
            ring.freed(i - 2)

        @_during(i, 0, tiles)
        def _():
            j = i

            @pl.when(j + (slots - 1) < tiles)
            def _():
                each("start", weights(j + (slots - 1)))

            each("wait", weights(j))
            for t in HALVES:
                got = _dot(s[t], w[lax.rem(j, slots), t])
                ring.put(j, t, 2 * t, {across: got[k * rows : (k + 1) * rows] for k, across in enumerate(AROUND)})
            ring.leave(j)

        @_during(i, 3, tiles)
        def _():
            ring.gone(i - 3)

        @_during(i, 1, tiles)
        def _():
            ring.merge(i - 1)

        @pl.when(i >= 2)
        def _():
            j = i - 2
            ring.arrived(j)
            for t in HALVES:
                here = _tile(t * tiles + j, tile)
                out[:, here] = (res[:, here].astype(jnp.float32) + ring.total(j, t, 2 * t)).astype(jnp.bfloat16)
                out_copy(t, j).start()

    lax.fori_loop(0, tiles + 2, step, None)
    ring.gone(tiles - 1)
    for t, n, sign in ways:
        each("wait_send", [next_to(t, sign, across) for across in AROUND])
    for t in HALVES:
        each("wait_send", [copy for across in AROUND for copy in (far(t, FAR, across), passed(t, across))])
        for j in range(tiles):
            out_copy(t, j).wait()


def projected(qkv, x, w, left, right, number, name):
    rows, width = x.shape
    depth = w.shape[0]
    n = lax.axis_size("tp")
    side = int(round(n**0.5))
    tile = min(TILE, width // 2)
    tiles = width // 2 // tile
    bf, dma = jnp.bfloat16, pltpu.SemaphoreType.DMA
    anywhere = pl.BlockSpec(memory_space=pl.ANY)
    return pl.pallas_call(
        functools.partial(_share_kernel, side=side),
        out_shape=jax.ShapeDtypeStruct((rows, width), bf),
        in_specs=[anywhere] * 5,
        out_specs=anywhere,
        scratch_shapes=[
            pltpu.VMEM(qkv.shape, bf),
            pltpu.VMEM((side, side * rows, depth), bf),
            pltpu.VMEM((qkv.shape[0] // 3, side * rows), jnp.float32),
            pltpu.VMEM((qkv.shape[0] // 3, HEAD + 8, side * rows), jnp.float32),
            pltpu.VMEM((2, side * rows, side * depth), bf),
            pltpu.VMEM((2, 2, 2, rows, depth), bf),
            pltpu.VMEM((3, 2, side * depth, tile), bf),
            pltpu.VMEM((rows, width), bf),
            pltpu.VMEM((rows, width), bf),
            dma((3,)), dma((1,)), dma((3, 2, side)), dma((2, tiles)),
            *[dma((2, 2, 4)), dma((2, 2, 2)), dma((2, 2, 2))] * 2,
            *_Sum.scratch(tiles, rows // 2, tile),
        ],
        compiler_params=pltpu.CompilerParams(collective_id=number, has_side_effects=True, vmem_limit_bytes=VMEM),
        cost_estimate=_cost(n * rows, depth, width, side),
        name=name,
    )(qkv, x, w, left, right)


def _angles(tokens):
    half = HEAD // 2
    rate = np.power(np.float32(THETA), -np.arange(half, dtype=np.float32) / np.float32(half)).astype(np.float32)
    angle = (np.arange(tokens, dtype=np.float32)[:, None] * rate).astype(np.float64)
    return np.concatenate([np.cos(angle), np.sin(angle)], 1).astype(np.float32)


def solution(mesh):
    n = mesh.shape["tp"]

    def step(x, gain_a, wq, wk, wv, wo, gain_m, w_gate, w_up, w_down):
        rows = n * x.shape[0]
        heads = wq.shape[1] // HEAD
        qkv, left, right = gathered(
            x, gain_a, (wq, wk, wv), _Heads(2), 2 * BLOCK, jax.ShapeDtypeStruct((3 * heads, rows, HEAD), jnp.bfloat16), 0, "gather_qkv",
            extra=(jnp.asarray(_angles(rows)),),
            scratch=(pltpu.VMEM((3, BLOCK, 2 * BLOCK), jnp.float32), pltpu.VMEM((rows, HEAD), jnp.float32),
                     pltpu.SemaphoreType.DMA((len(SLOTS),))),
            share=wo, twins=mesh.shape["dp"] % 2 == 0,
        )
        h = projected(qkv, x, wo, left, right, 1, "project")
        hidden = gathered(h, gain_m, (w_gate, w_up), _Hidden(), BLOCK, jax.ShapeDtypeStruct((rows, w_gate.shape[1]), jnp.bfloat16), 2,
                          "gather_hidden")
        return scattered(hidden, h, w_down, 3, "scatter_down")

    tokens, columns, rows_of = P(("dp", "tp"), None), P(None, "tp"), P("tp", None)
    return jax.shard_map(
        step,
        mesh=mesh,
        in_specs=(tokens, P(None), columns, columns, columns, rows_of, P(None), columns, columns, rows_of),
        out_specs=tokens,
        check_vma=False,
    )
```

```python
import functools

import jax
import jax.numpy as jnp
import numpy as np
from jax import lax
from jax.experimental import pallas as pl
from jax.experimental.pallas import tpu as pltpu
from jax.sharding import PartitionSpec as P

MESH = pl.DeviceIdType.MESH
HEAD = 128
THETA = 10000
NEG = -1e30
HIDDEN = 2 * NEG
LOG2E = 1.4426950408889634
VMEM = 62 << 20
LAST_VMEM = 48 << 20
BLOCK = 256
TILE = 512
RING = 6

A, B = 0, 1
FAR = 2
UP, DOWN = (0, -1), (1, FAR)
LINKS = (("y", 1), ("y", -1), ("x", 1), ("x", -1))


def piece(half, along, across):
    return (half, across, along) if half == A else (half, along, across)


def both(along, across):
    return [piece(A, along, across), piece(B, along, across)]


NEXT, SIGNS, HALVES = (-1, 1), (1, -1), (A, B)
SLOTS = [
    p
    for group in (
        [both(0, 0)],
        [[piece(half, 0, d) for d in NEXT] for half in HALVES],
        [[piece(half, d, 0) for d in NEXT] for half in HALVES],
        [both(0, FAR)],
        *([[piece(half, d, across) for d in NEXT] for half in HALVES] for across in NEXT),
        [both(FAR, 0), both(1, FAR), both(-1, FAR), both(FAR, 1), both(FAR, -1), both(FAR, FAR)],
    )
    for some in group
    for p in some
]
SLOT = {p: n for n, p in enumerate(SLOTS)}

def _by_link(along, pick):
    return [
        piece(half, along if along == 2 else sign * along, across)
        for (axis, sign) in LINKS
        for half in [A if axis == "y" else B]
        for across in (UP if (sign > 0) == pick else DOWN)
    ]


ORDER = _by_link(2, True) + _by_link(1, False) + _by_link(1, True) + [piece(half, 0, across) for half in HALVES for across in UP + DOWN]


def _place(side):
    me = lax.axis_index("tp")
    return lax.div(me, side), lax.rem(me, side)


def _device(side, dx, dy):
    x, y = _place(side)
    return lax.rem(x + (dx + side), side) * side + lax.rem(y + (dy + side), side)


def _meet(side, twin=False):
    barrier = pltpu.get_barrier_semaphore()
    others = [{"tp": _device(side, *_step(link))} for link in LINKS] + ([_twin()] if twin else [])
    for other in others:
        pl.semaphore_signal(barrier, inc=1, device_id=other, device_id_type=MESH)
    return lambda: pl.semaphore_wait(barrier, len(others))


def _twin():
    group = lax.axis_index("dp")
    return {"dp": group + 1 - 2 * lax.rem(group, 2), "tp": lax.axis_index("tp")}


def _step(link):
    axis, sign = link
    return (sign, 0) if axis == "x" else (0, sign)


def _copy(side, link, src, dst, send_sem, recv_sem):
    return pltpu.make_async_remote_copy(src_ref=src, dst_ref=dst, send_sem=send_sem, recv_sem=recv_sem,
                                        device_id={"tp": _device(side, *_step(link))}, device_id_type=MESH)


def _cost(rows, depth, width, passes=1):
    return pl.CostEstimate(flops=2 * rows * depth * width, transcendentals=0, bytes_accessed=2 * passes * depth * width)


def _tile(i, size):
    return pl.ds(pl.multiple_of(i * size, size), size)


def _during(i, late, count):
    return pl.when((i >= late) & (i < count + late))


def _dot(a, b, ca=1, cb=0):
    return lax.dot_general(a, b, (((ca,), (cb,)), ((), ())), preferred_element_type=jnp.float32)


def _plan():
    slot = lambda half, along, across: SLOT[piece(half, along, across)]

    def inner(half, sign, source, target, part=0, of="all"):
        return ("xy"[half], sign), slot(half, 0, source), slot(half, 0, target), part, of

    def outer(half, sign, source, across, part=0, of="all"):
        target = -sign if source == 0 else FAR
        return ("yx"[half], sign), slot(half, source, across), slot(half, target, across), part, of

    def final(*which):
        return [outer(*which, part, "columns") for part in HALVES]

    halves, signs = HALVES, SIGNS
    return [
        [inner(A, sign, 0, -sign) for sign in signs],
        [inner(B, sign, 0, -sign) for sign in signs],
        [outer(half, sign, 0, 0) for half in (B, A) for sign in signs],
        [inner(half, sign, -sign, FAR, int(sign < 0), "rows") for half in halves for sign in signs]
        + [outer(half, sign, 0, across) for across in NEXT for half in halves for sign in signs],
        [outer(half, 1, -1, 0) for half in halves],
        [outer(half, sign, 0, FAR) for half in halves for sign in signs],
        [copy for half in halves for copy in final(half, 1, -1, -1)],
        [outer(half, -1, 1, 1) for half in halves],
        [copy for half in halves for copy in final(half, -1, 1, FAR)],
    ]


PLAN = _plan()
COPIES = [c for group in PLAN for c in group]
_ENDS = (6, 10, 12, 16, 20, 24, 28, len(SLOTS))
EVENTS = [(SLOTS[a:b], k + 3 if k + 3 < len(PLAN) else None) for k, (a, b) in enumerate(zip((0, *_ENDS), _ENDS))]


def _gather_kernel(x_ref, gain_ref, *refs, side, finish, counts, twins):
    refs = iter(refs)
    take = lambda n: [next(refs) for _ in range(n)]
    extra_refs, w_refs, shared = (take(n) for n in counts[:3])
    (out_ref,), shelves = take(1), take(2 * len(shared))
    g, gain, w, stage, sems_x, sems_w, sems_o, send, recv = take(9)
    more = take(counts[3])
    carry = _Carry(side, twins, shared[0], shelves, *refs) if shared else None
    rows, depth = x_ref.shape
    size = rows // 2
    tiles = sum(ref.shape[1] for ref in w_refs) // w.shape[2]
    ring = min(w.shape[0], tiles)
    loads = tiles if tiles <= ring else len(EVENTS) * tiles

    def weights(s, start):
        finish.weights(w_refs, lax.rem(s, tiles), w, lax.rem(s, ring), sems_w, "start" if start else "wait")

    def remote(number):
        link, src, dst, part, of = COPIES[number]
        height = size // 2 if of == "rows" else size
        width = depth // 2 if of == "columns" else depth
        above, left = (part * height, 0) if of == "rows" else (0, part * width)
        here = [g.at[pl.ds(slot * size + above, height), pl.ds(left, width)] for slot in (src, dst)]
        return _copy(side, link, *here, send.at[number], recv.at[dst, part])

    def begin(group):
        first = sum(len(p) for p in PLAN[:group])
        for number in range(first, first + len(PLAN[group])):
            remote(number).start()

    def arrived(slots, parts=HALVES):
        for number, (_, _, dst, part, _) in enumerate(COPIES):
            if SLOTS[dst] in slots and part in parts:
                remote(number).wait_recv()

    met = _meet(side, bool(carry and twins))
    own = [pltpu.make_async_copy(x_ref.at[here], g.at[here], sems_x.at[half]) for half in HALVES for here in [pl.ds(half * size, size)]]
    gains = pltpu.make_async_copy(gain_ref, gain, sems_x.at[2])
    for c in (own[A], gains, own[B]):
        c.start()

    def norm(i, _):
        here = _tile(i, 16)
        wide = g[here, :].astype(jnp.float32)
        scale = lax.rsqrt(jnp.mean(wide * wide, -1, keepdims=True) + 1e-6)
        g[here, :] = (wide * scale * gain[...].astype(jnp.float32)[None]).astype(jnp.bfloat16)

    gains.wait()
    if carry:
        met()
        carry.begin()
    for half in HALVES:
        own[half].wait()
        lax.fori_loop(half * size // 16, (half + 1) * size // 16, norm, None)
        if half == A:
            carry.proceed() if carry else met()
        begin(half)
    begin(2)
    for s in range(ring - 1):
        weights(s, True)
    if finish.prepare:
        finish.prepare(extra_refs, more)
    if carry:
        for k in HALVES:
            carry.hand(k)

    def block(b, _):
        for k, (slots, group) in enumerate(EVENTS):

            @pl.when(b == k)
            def _(slots=slots, group=group):
                arrived(slots)
                if group is not None:
                    begin(group)
        def tile(n, _):
            s = b * tiles + n

            @pl.when(s + (ring - 1) < loads)
            def _():
                weights(s + (ring - 1), True)

            @pl.when(s < loads)
            def _():
                weights(s, False)

            product(b, n, s, g.at[_tile(b, BLOCK)], w.at[lax.rem(s, ring)])

        lax.fori_loop(0, tiles, tile, None)

    def product(b, n, s, lhs, rhs, *partial):
        to = lax.rem(s, 2)

        @pl.when(s >= 2)
        def _():
            finish.store(stage, out_ref, sems_o, to, b, n, size, side, start=False)

        finish.compute(lhs, rhs, stage.at[to], b, n, more, *partial)
        finish.store(stage, out_ref, sems_o, to, b, n, size, side, start=True)

    final = len(EVENTS) - 1
    whole = final if finish.in_parts else len(EVENTS)
    lax.fori_loop(0, whole, block, None)
    if whole == final:
        for part in HALVES:
            arrived(EVENTS[final][0], [part])
            here = pl.ds(part * (depth // 2), depth // 2)
            lhs = g.at[pl.ds(final * BLOCK, BLOCK), here]

            def tile(n, _, part=part, here=here, lhs=lhs):
                partial, *_ = more
                if part == A:
                    partial[n] = _dot(lhs[...], w[n, here, :])
                else:
                    product(final, n, final * tiles + n, lhs, w.at[n, here], partial)

            lax.fori_loop(0, tiles, tile, None)
    for to in range(2):
        finish.store(stage, out_ref, sems_o, to, 0, 0, size, side, start=False)
    for number in range(len(COPIES)):
        remote(number).wait_send()
    if carry:
        carry.end()


class _Carry:
    SHELF = {-1: 0, 1: 1, FAR: 2}

    def __init__(self, side, twins, w_ref, shelves, send, recv, give, got):
        self.side, self.twins, self.w_ref, self.shelves = side, twins, w_ref, shelves
        self.send, self.recv, self.give, self.got = send, recv, give, got

    def carrier(self, body):
        if self.twins:
            pl.when(lax.rem(lax.axis_index("dp"), 2) == 0)(body)
        else:
            body()

    def copies(self, step):
        for t, shelf in enumerate(self.shelves):
            for sign in SIGNS:
                depth, width = shelf.shape[1:]
                here = pl.ds((int(sign < 0) ^ (step == 1)) * (depth // 2), depth // 2)
                if step == 2:
                    src, dst = shelf.at[self.SHELF[-sign], here], shelf.at[self.SHELF[FAR], here]
                else:
                    src, dst = self.w_ref.at[here, pl.ds(t * width, width)], shelf.at[self.SHELF[-sign], here]
                sem = t, int(sign < 0), step
                yield _copy(self.side, ("xy"[t], sign), src, dst, self.send.at[sem], self.recv.at[sem])

    def handed(self, k):
        for t, shelf in enumerate(self.shelves):
            for at in ((0, 1), (2,))[k]:
                yield pltpu.make_async_remote_copy(src_ref=shelf.at[at], dst_ref=shelf.at[at], send_sem=self.give.at[t, at],
                                                   recv_sem=self.got.at[t, at], device_id=_twin(), device_id_type=MESH)

    def all(self, copies, what):
        for c in copies:
            getattr(c, what)()

    def begin(self):
        @self.carrier
        def _():
            for step in HALVES:
                self.all(self.copies(step), "start")

    def proceed(self):
        @self.carrier
        def _():
            self.all(self.copies(0), "wait_recv")
            self.all(self.copies(2), "start")

    def hand(self, k):
        @self.carrier
        def _():
            self.all(self.copies(k + 1), "wait_recv")
            if self.twins:
                self.all(self.handed(k), "start")

    def end(self):
        @self.carrier
        def _():
            for step in range(3):
                self.all(self.copies(step), "wait_send")
            if self.twins:
                for k in HALVES:
                    self.all(self.handed(k), "wait_send")

        if self.twins:

            @pl.when(lax.rem(lax.axis_index("dp"), 2) == 1)
            def _():
                for k in HALVES:
                    self.all(self.handed(k), "wait_recv")


class _Heads:
    in_parts = True

    def __init__(self, turned_steps):
        self.turned_steps = turned_steps

    def weights(self, refs, n, w, slot, sems, what):
        for at, ref in enumerate(refs):

            @pl.when(n == at)
            def _(ref=ref):
                getattr(pltpu.make_async_copy(ref, w.at[slot], sems.at[slot, 0]), what)()

    def prepare(self, extra_refs, more):
        (table_ref,) = extra_refs
        _, table, sems = more
        size = table.shape[0] // len(SLOTS)
        side = int(round((len(SLOTS) // 2) ** 0.5))
        copies = []
        for n, (half, dx, dy) in enumerate(SLOTS):
            row = _device(side, dx, dy) * (2 * size) + half * size
            copies.append(pltpu.make_async_copy(table_ref.at[pl.ds(pl.multiple_of(row, size), size)], table.at[pl.ds(n * size, size)],
                                                sems.at[n]))
        for what in ("start", "wait"):
            for c in copies:
                getattr(c, what)()

    def compute(self, lhs, w, to, at, n, more, partial=None):
        _, table, _ = more
        got = _dot(lhs[...], w[...])
        got = (got if partial is None else got + partial[n]).astype(jnp.bfloat16)

        @pl.when(n < self.turned_steps)
        def _():
            t = table[_tile(at, BLOCK), :]
            swapped = pltpu.roll(t, HEAD // 2, 1)
            low = lax.broadcasted_iota(jnp.int32, t.shape, 1) < HEAD // 2
            cos, sin = jnp.where(low, t, swapped), jnp.where(low, -swapped, t)
            for i in range(0, w.shape[1], HEAD):
                one = got[:, i : i + HEAD].astype(jnp.float32)
                to[:, i : i + HEAD] = (one * cos + pltpu.roll(one, HEAD // 2, 1) * sin).astype(jnp.bfloat16)

        @pl.when(n >= self.turned_steps)
        def _():
            to[...] = got

    def store(self, stage, out_ref, sems, to, at, n, size, side, start):
        per = BLOCK // size

        heads = stage.shape[2] // HEAD

        def copies(pieces):
            for p, (half, dx, dy) in enumerate(pieces):
                row = pl.multiple_of(_device(side, dx, dy) * (2 * size) + half * size, size)
                for i in range(heads):
                    yield pltpu.make_async_copy(stage.at[to, pl.ds(p * size, size), pl.ds(i * HEAD, HEAD)],
                                                out_ref.at[n * heads + i, pl.ds(row, size)], sems.at[to, p * heads + i])

        if not start:
            for c in copies(SLOTS[:per]):
                c.wait()
            return
        for k in range(len(SLOTS) // per):

            @pl.when(at == k)
            def _(k=k):
                for c in copies(SLOTS[k * per : (k + 1) * per]):
                    c.start()


class _Hidden:
    prepare = None
    in_parts = False

    def weights(self, refs, n, w, slot, sems, what):
        for at, ref in enumerate(refs):
            here = _tile(n, BLOCK)
            getattr(pltpu.make_async_copy(ref.at[:, here], w.at[slot, :, pl.ds(at * BLOCK, BLOCK)], sems.at[slot, at]), what)()

    def compute(self, lhs, w, to, at, n, more):
        got = _dot(lhs[...], w[...])
        to[...] = (jax.nn.silu(got[:, :BLOCK]) * got[:, BLOCK:]).astype(jnp.bfloat16)

    def store(self, stage, out_ref, sems, to, at, n, size, side, start):
        c = pltpu.make_async_copy(stage.at[to], out_ref.at[_tile(at, BLOCK),
                                                           _tile(n, BLOCK)], sems.at[to, 0])
        c.start() if start else c.wait()


def gathered(x, gain, weights, finish, stored, out_shape, number, name, extra=(), scratch=(), share=None, twins=False):
    rows, depth = x.shape
    n = lax.axis_size("tp")
    side = int(round(n**0.5))
    width = sum(w.shape[1] for w in weights)
    anywhere, dma = pl.BlockSpec(memory_space=pl.ANY), pltpu.SemaphoreType.DMA
    shared = [] if share is None else [share]
    shelves = [jax.ShapeDtypeStruct((side - 1, w.shape[0], w.shape[1] // 2), w.dtype) for w in 2 * shared]
    operands = [x, gain, *extra, *weights, *shared]
    return pl.pallas_call(
        functools.partial(_gather_kernel, side=side, finish=finish, counts=(len(extra), len(weights), len(shared), len(scratch)), twins=twins),
        out_shape=[out_shape, *shelves] if shared else out_shape,
        in_specs=[anywhere] * len(operands),
        out_specs=[anywhere] * 3 if shared else anywhere,
        scratch_shapes=[
            pltpu.VMEM((n * rows, depth), jnp.bfloat16),
            pltpu.VMEM((depth,), jnp.bfloat16),
            pltpu.VMEM((3, depth, 2 * BLOCK), jnp.bfloat16),
            pltpu.VMEM((2, BLOCK, stored), jnp.bfloat16),
            dma((3,)), dma((3, 2)), dma((2, len(SLOTS))), dma((len(COPIES),)), dma((len(SLOTS), 2)),
            *scratch,
            *([dma((2, 2, 3))] * 2 + [dma((2, 3))] * 2 if shared else []),
        ],
        compiler_params=pltpu.CompilerParams(collective_id=number, has_side_effects=True, vmem_limit_bytes=VMEM),
        cost_estimate=_cost(n * rows, depth, width, len(EVENTS)),
        name=name,
    )(*operands)


class _Sum:
    def __init__(self, side, pair, late, keep, own, r_pair, r_late, s_pair, s_late, t_pair, t_late):
        self.side, self.pair, self.late, self.keep, self.own = side, pair, late, keep, own
        self.r_pair, self.r_late, self.s_pair, self.s_late, self.t_pair, self.t_late = r_pair, r_late, s_pair, s_late, t_pair, t_late
        self.low = keep.shape[2]

    def copies(self, j, src, dst, s_sem, t_sem):
        a, b = lax.rem(j, 2), lax.rem(j, dst.shape[0])
        return [_copy(self.side, link, src.at[a, l], dst.at[b, l], s_sem.at[a, l], t_sem.at[b, l]) for l, link in enumerate(LINKS)]

    def early(self, j, what):
        for c in self.copies(j, self.pair, self.r_pair, self.s_pair, self.t_pair):
            getattr(c, what)()

    def merged(self, j, what):
        for c in self.copies(j, self.late, self.r_late, self.s_late, self.t_late):
            getattr(c, what)()

    def freed(self, j):
        self.early(j, "wait_send")

    def gone(self, j):
        self.merged(j, "wait_send")

    def put(self, j, t, l, pieces):
        a, low = lax.rem(j, 2), self.low
        self.own[lax.rem(j, 4), t] = pieces[0]
        self.pair[a, l] = jnp.stack([pieces[FAR][:low], pieces[1][low:]]).astype(self.pair.dtype)
        self.pair[a, l + 1] = jnp.stack([pieces[FAR][low:], pieces[-1][:low]]).astype(self.pair.dtype)
        self.keep[a, l] = pieces[1][:low]
        self.keep[a, l + 1] = pieces[-1][low:]

    def leave(self, j):
        self.early(j, "start")

    def merge(self, j):
        a, b = lax.rem(j, 2), lax.rem(j, self.r_pair.shape[0])
        self.early(j, "wait_recv")
        for l in range(len(LINKS)):
            self.late[a, l] = (self.keep[a, l] + self.r_pair[b, l, 0].astype(jnp.float32)).astype(self.late.dtype)
        self.merged(j, "start")

    def arrived(self, j):
        self.merged(j, "wait_recv")

    def total(self, j, t, l):
        b = lax.rem(j, self.r_pair.shape[0])
        up = jnp.concatenate([self.r_late[b, l], self.r_pair[b, l, 1]]).astype(jnp.float32)
        down = jnp.concatenate([self.r_pair[b, l + 1, 1], self.r_late[b, l + 1]]).astype(jnp.float32)
        return self.own[lax.rem(j, 4), t] + up + down

    @staticmethod
    def scratch(rings, low, tile):
        bf, f32, dma = jnp.bfloat16, jnp.float32, pltpu.SemaphoreType.DMA
        return [pltpu.VMEM((2, 4, 2, low, tile), bf), pltpu.VMEM((2, 4, low, tile), bf), pltpu.VMEM((2, 4, low, tile), f32),
                pltpu.VMEM((4, 2, 2 * low, tile), f32), pltpu.VMEM((rings, 4, 2, low, tile), bf), pltpu.VMEM((rings, 4, low, tile), bf),
                *[dma((2, 4))] * 2, *[dma((rings, 4))] * 2]


def _scatter_kernel(rows_ref, x_ref, w_ref, out, hid, res, w, far, plain, summed, r_far, r_plain, r_summed, sems_h, sems_x, sems_w,
                    s_far, s_plain, s_summed, t_far, t_plain, t_summed, *second, side):
    rows, width = out.shape
    size = rows // 2
    tile = w.shape[2]
    tiles = width // tile
    ring = r_far.shape[0]
    group = hid.shape[0] // 4

    def fetch(n):
        return pltpu.make_async_copy(rows_ref.at[pl.ds(SLOT[ORDER[n]] * size, size)], hid.at[pl.ds(n * size, size)], sems_h.at[n])

    def weights(j):
        slot = lax.rem(j, 4)
        return pltpu.make_async_copy(w_ref.at[:, _tile(j, tile)], w.at[slot], sems_w.at[slot])

    def terms(g, j, count=1):
        return _dot(hid[pl.ds(g * group, count * group), :], w[lax.rem(j, 4)]).reshape(-1, size, tile)

    def pairs(src, dst, s_sem, t_sem, j):
        a, b = lax.rem(j, 2), lax.rem(j, ring)
        return [_copy(side, LINKS[l], src.at[a, pl.ds(2 * l, 2)], dst.at[b, pl.ds(2 * l, 2)], s_sem.at[a, l], t_sem.at[b, l])
                for l in range(4)]

    ring2 = _Sum(side, *second)

    def each(copies, what):
        for c in copies:
            getattr(c, what)()

    weights(0).start()
    for n in range(len(ORDER)):
        fetch(n).start()
    residual = pltpu.make_async_copy(x_ref, res, sems_x.at[0])
    residual.start()
    _meet(side)()
    for n in range(len(ORDER)):
        fetch(n).wait()
    residual.wait()

    def step(i, _):
        @_during(i, 2, tiles)
        def _():
            each(pairs(far, r_far, s_far, t_far, i - 2), "wait_send")
            each(pairs(plain, r_plain, s_plain, t_plain, i - 2), "wait_send")

        @_during(i, 0, tiles)
        def _():
            j = i

            @pl.when(j + 1 < tiles)
            def _():
                weights(j + 1).start()

            weights(j).wait()
            got = terms(0, j, 2).astype(jnp.bfloat16)
            far[lax.rem(j, 2)] = got[:8]
            plain[lax.rem(j, 2)] = got[8:]
            each(pairs(far, r_far, s_far, t_far, j), "start")
            each(pairs(plain, r_plain, s_plain, t_plain, j), "start")

        @_during(i, 3, tiles)
        def _():
            each(pairs(summed, r_summed, s_summed, t_summed, i - 3), "wait_send")

        @_during(i, 1, tiles)
        def _():
            j = i - 1
            each(pairs(far, r_far, s_far, t_far, j), "wait_recv")
            summed[lax.rem(j, 2)] = (terms(2, j) + r_far[lax.rem(j, ring)].astype(jnp.float32)).astype(jnp.bfloat16)
            each(pairs(summed, r_summed, s_summed, t_summed, j), "start")

        @_during(i, 4, tiles)
        def _():
            ring2.freed(i - 4)

        @_during(i, 2, tiles)
        def _():
            j = i - 2
            b = lax.rem(j, ring)
            each(pairs(plain, r_plain, s_plain, t_plain, j), "wait_recv")
            each(pairs(summed, r_summed, s_summed, t_summed, j), "wait_recv")
            mine = terms(3, j)
            for half in HALVES:
                l = 2 * half
                up, down = pl.ds(2 * l, 2), pl.ds(2 * l + 2, 2)
                from_up = jnp.concatenate([r_summed[b, up], r_plain[b, up]]).astype(jnp.float32)
                from_down = jnp.concatenate([r_plain[b, down], r_summed[b, down]]).astype(jnp.float32)
                both_ways = mine[4 * half : 4 * half + 4] + from_up + from_down
                sums = {across: both_ways[k] for k, across in enumerate(UP + DOWN)}
                ring2.put(j, half, 2 - l, sums)
            ring2.leave(j)

        @_during(i, 5, tiles)
        def _():
            ring2.gone(i - 5)

        @_during(i, 3, tiles)
        def _():
            ring2.merge(i - 3)

        @pl.when(i >= 4)
        def _():
            j = i - 4

            ring2.arrived(j)
            here = _tile(j, tile)
            for half in HALVES:
                mine = pl.ds(half * size, size)
                out[mine, here] = (res[mine, here].astype(jnp.float32) + ring2.total(j, half, 2 - 2 * half)).astype(jnp.bfloat16)

    lax.fori_loop(0, tiles + 4, step, None)
    ring2.gone(tiles - 1)


def scattered(terms, x, w, number, name):
    rows, width = x.shape
    depth = w.shape[0]
    n = lax.axis_size("tp")
    side = int(round(n**0.5))
    size, low = rows // 2, rows // 4
    tile = min(TILE, width)
    tiles = width // tile
    bf, dma = jnp.bfloat16, pltpu.SemaphoreType.DMA
    return pl.pallas_call(
        functools.partial(_scatter_kernel, side=side),
        out_shape=jax.ShapeDtypeStruct((rows, width), bf),
        in_specs=[pl.BlockSpec(memory_space=pl.ANY)] * 3,
        out_specs=pl.BlockSpec(memory_space=pltpu.VMEM),
        scratch_shapes=[
            pltpu.VMEM((n * rows, depth), bf),
            pltpu.VMEM((rows, width), bf),
            pltpu.VMEM((4, depth, tile), bf),
            pltpu.VMEM((2, 8, size, tile), bf),
            pltpu.VMEM((2, 8, size, tile), bf),
            pltpu.VMEM((2, 8, size, tile), bf),
            pltpu.VMEM((RING, 8, size, tile), bf),
            pltpu.VMEM((RING, 8, size, tile), bf),
            pltpu.VMEM((RING, 8, size, tile), bf),
            dma((len(ORDER),)), dma((1,)), dma((4,)),
            *[dma((2, 4))] * 3, *[dma((RING, 4))] * 3,
            *_Sum.scratch(RING, low, tile),
        ],
        compiler_params=pltpu.CompilerParams(collective_id=number, has_side_effects=True, vmem_limit_bytes=LAST_VMEM),
        cost_estimate=_cost(n * rows, depth, width),
        name=name,
    )(terms, x, w)


AROUND = (0, 1, -1, FAR)
ORIGIN = (0, -1, 1, FAR)
TURNS = (FAR, 1, -1, 0)


def _attend(qkv, mine, o, top_s, mix_s):
    size, d = o.shape[0], qkv.shape[2]
    heads = qkv.shape[0] // 3
    e = d**-0.5 * LOG2E
    top_s[...] = jnp.full(top_s.shape, NEG, jnp.float32)
    mix_s[...] = jnp.zeros(mix_s.shape, jnp.float32)
    ones = jnp.ones((8, size), qkv.dtype)

    def block(j, masked):
        here = _tile(j, size)
        scores = [_dot(qkv[heads + i, here, :], qkv[i, _tile(mine, size), :], 1, 1) for i in range(heads)]
        if masked:
            seen = lax.broadcasted_iota(jnp.int32, (size, size), 1) >= lax.broadcasted_iota(jnp.int32, (size, size), 0)
        weights, keeps = [], []
        for i, s in enumerate(scores):
            s = jnp.where(seen, s, HIDDEN) if masked else s
            old = top_s[i : i + 1, :]
            top = jnp.maximum(old, s.max(axis=0, keepdims=True))
            top_s[i : i + 1, :] = top
            weights.append(jnp.exp2((s - top) * e).astype(qkv.dtype))
            keeps.append(jnp.exp2((old - top) * e))
        for i, (p, keep) in enumerate(zip(weights, keeps)):
            values = jnp.concatenate([qkv[2 * heads + i, here, :].T, ones], axis=0)
            mix_s[i] = mix_s[i] * keep + _dot(values, p, 1, 0)

    lax.fori_loop(0, mine, lambda j, _: block(j, False), None)
    block(mine, True)
    for i in range(heads):
        total = mix_s[i, d : d + 1, :]
        o[:, i * d : (i + 1) * d] = (mix_s[i, :d, :] * (1 / total)).T.astype(o.dtype)


def _share_kernel(qkv_ref, x_ref, w_ref, left_ref, right_ref, out_ref, qkv, seen, top_s, mix_s, s, relay, w, res, out, sems_q, sems_x, sems_w,
                  sems_o, s_next, s_far, s_pass, t_next, t_far, t_pass, *second, side):
    rows, width = out_ref.shape
    depth, tile = w_ref.shape[0], w.shape[3]
    half, tiles = width // 2, width // 2 // tile
    slots = w.shape[0]
    ring = _Sum(side, *second)
    x, y = _place(side)

    def block(t, along, across):
        dx, dy = (along, across) if t == 0 else (across, along)
        return seen.at[TURNS.index(dx), _tile(lax.rem(y + (dy + side), side), rows)]

    def place(t, across, origin):
        return s.at[t, _tile(AROUND.index(across), rows), _tile(ORIGIN.index(origin), depth)]

    ways = [(t, n, sign) for t in HALVES for n, sign in enumerate(SIGNS)]

    def far(t, along, across):
        n, i = divmod(AROUND.index(across), 2)
        sign = 1 - 2 * n
        return _copy(side, ("xy"[t], sign), block(t, FAR, across), relay.at[t, n, i], s_far.at[t, n, i], t_far.at[t, n, i])

    def passed(t, across):
        n, i = divmod(AROUND.index(across), 2)
        return _copy(side, ("xy"[t], 1 - 2 * n), relay.at[t, n, i], place(t, across, FAR), s_pass.at[t, n, i], t_pass.at[t, n, i])

    def next_to(t, sign, across):
        at = t, int(sign < 0), AROUND.index(across)
        return _copy(side, ("xy"[t], sign), block(t, sign, across), place(t, across, -sign), s_next.at[at], t_next.at[at])

    def sends(t, along, across):
        if along:
            (far if along == FAR else next_to)(t, along, across).start()
        else:
            place(t, across, 0)[...] = block(t, 0, across)[...]

    def each(what, copies):
        for c in copies:
            getattr(c, what)()

    def weights(j):
        got = []
        for t, shelf in enumerate((left_ref, right_ref)):
            for i in range(side):
                src = shelf.at[i - 1, :, _tile(j, tile)] if i else w_ref.at[:, _tile(t * tiles + j, tile)]
                got.append(pltpu.make_async_copy(src, w.at[lax.rem(j, slots), t, pl.ds(i * depth, depth)], sems_w.at[lax.rem(j, slots), t, i]))
        return got

    def out_copy(t, j):
        here = _tile(t * tiles + j, tile)
        return pltpu.make_async_copy(out.at[:, here], out_ref.at[:, here], sems_o.at[t, j])

    met = _meet(side)
    heads = qkv.shape[0] // 3
    parts = [pltpu.make_async_copy(qkv_ref.at[here], qkv.at[here], sems_q.at[n]) for n in range(3) for here in [pl.ds(n * heads, heads)]]
    each("start", parts)
    for j in range(slots - 1):
        each("start", weights(j))
    residual = pltpu.make_async_copy(x_ref, res, sems_x.at[0])
    residual.start()
    each("wait", parts)
    met()

    def turn(n, _):
        _attend(qkv, lax.rem(x + (FAR + len(TURNS) * 2) - lax.div(n * (n + 1), 2), side), seen.at[n], top_s, mix_s)
        for k, dx in enumerate(TURNS):

            @pl.when(n == k)
            def _(dx=dx):
                for other in AROUND:
                    sends(0, dx, other)
                    sends(1, other, dx)

    lax.fori_loop(0, len(TURNS), turn, None)
    for t in HALVES:
        for across in TURNS:
            far(t, FAR, across).wait_recv()
            passed(t, across).start()
    for t, n, sign in ways:
        each("wait_recv", [next_to(t, sign, across) for across in AROUND])
    residual.wait()
    for t in HALVES:
        each("wait_recv", [passed(t, across) for across in AROUND])

    def step(i, _):
        @_during(i, 2, tiles)
        def _():
            ring.freed(i - 2)

        @_during(i, 0, tiles)
        def _():
            j = i

            @pl.when(j + (slots - 1) < tiles)
            def _():
                each("start", weights(j + (slots - 1)))

            each("wait", weights(j))
            for t in HALVES:
                got = _dot(s[t], w[lax.rem(j, slots), t])
                ring.put(j, t, 2 * t, {across: got[k * rows : (k + 1) * rows] for k, across in enumerate(AROUND)})
            ring.leave(j)

        @_during(i, 3, tiles)
        def _():
            ring.gone(i - 3)

        @_during(i, 1, tiles)
        def _():
            ring.merge(i - 1)

        @pl.when(i >= 2)
        def _():
            j = i - 2
            ring.arrived(j)
            for t in HALVES:
                here = _tile(t * tiles + j, tile)
                out[:, here] = (res[:, here].astype(jnp.float32) + ring.total(j, t, 2 * t)).astype(jnp.bfloat16)
                out_copy(t, j).start()

    lax.fori_loop(0, tiles + 2, step, None)
    ring.gone(tiles - 1)
    for t, n, sign in ways:
        each("wait_send", [next_to(t, sign, across) for across in AROUND])
    for t in HALVES:
        each("wait_send", [copy for across in AROUND for copy in (far(t, FAR, across), passed(t, across))])
        for j in range(tiles):
            out_copy(t, j).wait()


def projected(qkv, x, w, left, right, number, name):
    rows, width = x.shape
    depth = w.shape[0]
    n = lax.axis_size("tp")
    side = int(round(n**0.5))
    tile = min(TILE, width // 2)
    tiles = width // 2 // tile
    bf, dma = jnp.bfloat16, pltpu.SemaphoreType.DMA
    anywhere = pl.BlockSpec(memory_space=pl.ANY)
    return pl.pallas_call(
        functools.partial(_share_kernel, side=side),
        out_shape=jax.ShapeDtypeStruct((rows, width), bf),
        in_specs=[anywhere] * 5,
        out_specs=anywhere,
        scratch_shapes=[
            pltpu.VMEM(qkv.shape, bf),
            pltpu.VMEM((side, side * rows, depth), bf),
            pltpu.VMEM((qkv.shape[0] // 3, side * rows), jnp.float32),
            pltpu.VMEM((qkv.shape[0] // 3, HEAD + 8, side * rows), jnp.float32),
            pltpu.VMEM((2, side * rows, side * depth), bf),
            pltpu.VMEM((2, 2, 2, rows, depth), bf),
            pltpu.VMEM((3, 2, side * depth, tile), bf),
            pltpu.VMEM((rows, width), bf),
            pltpu.VMEM((rows, width), bf),
            dma((3,)), dma((1,)), dma((3, 2, side)), dma((2, tiles)),
            *[dma((2, 2, 4)), dma((2, 2, 2)), dma((2, 2, 2))] * 2,
            *_Sum.scratch(tiles, rows // 2, tile),
        ],
        compiler_params=pltpu.CompilerParams(collective_id=number, has_side_effects=True, vmem_limit_bytes=VMEM),
        cost_estimate=_cost(n * rows, depth, width, side),
        name=name,
    )(qkv, x, w, left, right)


def _angles(tokens):
    half = HEAD // 2
    rate = np.power(np.float32(THETA), -np.arange(half, dtype=np.float32) / np.float32(half)).astype(np.float32)
    angle = (np.arange(tokens, dtype=np.float32)[:, None] * rate).astype(np.float64)
    return np.concatenate([np.cos(angle), np.sin(angle)], 1).astype(np.float32)


def solution(mesh):
    n = mesh.shape["tp"]

    def step(x, gain_a, wq, wk, wv, wo, gain_m, w_gate, w_up, w_down):
        rows = n * x.shape[0]
        heads = wq.shape[1] // HEAD
        qkv, left, right = gathered(
            x, gain_a, (wq, wk, wv), _Heads(2), 2 * BLOCK, jax.ShapeDtypeStruct((3 * heads, rows, HEAD), jnp.bfloat16), 0, "gather_qkv",
            extra=(jnp.asarray(_angles(rows)),),
            scratch=(pltpu.VMEM((3, BLOCK, 2 * BLOCK), jnp.float32), pltpu.VMEM((rows, HEAD), jnp.float32),
                     pltpu.SemaphoreType.DMA((len(SLOTS),))),
            share=wo, twins=mesh.shape["dp"] % 2 == 0,
        )
        h = projected(qkv, x, wo, left, right, 1, "project")
        hidden = gathered(h, gain_m, (w_gate, w_up), _Hidden(), BLOCK, jax.ShapeDtypeStruct((rows, w_gate.shape[1]), jnp.bfloat16), 2,
                          "gather_hidden")
        return scattered(hidden, h, w_down, 3, "scatter_down")

    tokens, columns, rows_of = P(("dp", "tp"), None), P(None, "tp"), P("tp", None)
    return jax.shard_map(
        step,
        mesh=mesh,
        in_specs=(tokens, P(None), columns, columns, columns, rows_of, P(None), columns, columns, rows_of),
        out_specs=tokens,
        check_vma=False,
    )
```

```python
import functools

import jax
import jax.numpy as jnp
import numpy as np
from jax import lax
from jax.experimental import pallas as pl
from jax.experimental.pallas import tpu as pltpu
from jax.sharding import PartitionSpec as P

MESH = pl.DeviceIdType.MESH
HEAD = 128
THETA = 10000
NEG = -1e30
HIDDEN = 2 * NEG
LOG2E = 1.4426950408889634
VMEM = 62 << 20
LAST_VMEM = 48 << 20
BLOCK = 256
TILE = 512
RING = 6

A, B = 0, 1
FAR = 2
UP, DOWN = (0, -1), (1, FAR)
LINKS = (("y", 1), ("y", -1), ("x", 1), ("x", -1))


def piece(half, along, across):
    return (half, across, along) if half == A else (half, along, across)


def both(along, across):
    return [piece(A, along, across), piece(B, along, across)]


NEXT, SIGNS, HALVES = (-1, 1), (1, -1), (A, B)
SLOTS = [
    p
    for group in (
        [both(0, 0)],
        [[piece(half, 0, d) for d in NEXT] for half in HALVES],
        [[piece(half, d, 0) for d in NEXT] for half in HALVES],
        [both(0, FAR)],
        *([[piece(half, d, across) for d in NEXT] for half in HALVES] for across in NEXT),
        [both(FAR, 0), both(1, FAR), both(-1, FAR), both(FAR, 1), both(FAR, -1), both(FAR, FAR)],
    )
    for some in group
    for p in some
]
SLOT = {p: n for n, p in enumerate(SLOTS)}

def _by_link(along, pick):
    return [
        piece(half, along if along == 2 else sign * along, across)
        for (axis, sign) in LINKS
        for half in [A if axis == "y" else B]
        for across in (UP if (sign > 0) == pick else DOWN)
    ]


ORDER = _by_link(2, True) + _by_link(1, False) + _by_link(1, True) + [piece(half, 0, across) for half in HALVES for across in UP + DOWN]


def _place(side):
    me = lax.axis_index("tp")
    return lax.div(me, side), lax.rem(me, side)


def _device(side, dx, dy):
    x, y = _place(side)
    return lax.rem(x + (dx + side), side) * side + lax.rem(y + (dy + side), side)


def _meet(side, twin=False):
    barrier = pltpu.get_barrier_semaphore()
    others = [{"tp": _device(side, *_step(link))} for link in LINKS] + ([_twin()] if twin else [])
    for other in others:
        pl.semaphore_signal(barrier, inc=1, device_id=other, device_id_type=MESH)
    return lambda: pl.semaphore_wait(barrier, len(others))


def _twin():
    group = lax.axis_index("dp")
    return {"dp": group + 1 - 2 * lax.rem(group, 2), "tp": lax.axis_index("tp")}


def _step(link):
    axis, sign = link
    return (sign, 0) if axis == "x" else (0, sign)


def _copy(side, link, src, dst, send_sem, recv_sem):
    return pltpu.make_async_remote_copy(src_ref=src, dst_ref=dst, send_sem=send_sem, recv_sem=recv_sem,
                                        device_id={"tp": _device(side, *_step(link))}, device_id_type=MESH)


def _cost(rows, depth, width, passes=1):
    return pl.CostEstimate(flops=2 * rows * depth * width, transcendentals=0, bytes_accessed=2 * passes * depth * width)


def _tile(i, size):
    return pl.ds(pl.multiple_of(i * size, size), size)


def _during(i, late, count):
    return pl.when((i >= late) & (i < count + late))


def _dot(a, b, ca=1, cb=0):
    return lax.dot_general(a, b, (((ca,), (cb,)), ((), ())), preferred_element_type=jnp.float32)


def _plan():
    slot = lambda half, along, across: SLOT[piece(half, along, across)]

    def inner(half, sign, source, target, part=0, of="all"):
        return ("xy"[half], sign), slot(half, 0, source), slot(half, 0, target), part, of

    def outer(half, sign, source, across, part=0, of="all"):
        target = -sign if source == 0 else FAR
        return ("yx"[half], sign), slot(half, source, across), slot(half, target, across), part, of

    def final(*which):
        return [outer(*which, part, "columns") for part in HALVES]

    halves, signs = HALVES, SIGNS
    return [
        [inner(A, sign, 0, -sign) for sign in signs],
        [inner(B, sign, 0, -sign) for sign in signs],
        [outer(half, sign, 0, 0) for half in (B, A) for sign in signs],
        [inner(half, sign, -sign, FAR, int(sign < 0), "rows") for half in halves for sign in signs]
        + [outer(half, sign, 0, across) for across in NEXT for half in halves for sign in signs],
        [outer(half, 1, -1, 0) for half in halves],
        [outer(half, sign, 0, FAR) for half in halves for sign in signs],
        [copy for half in halves for copy in final(half, 1, -1, -1)],
        [outer(half, -1, 1, 1) for half in halves],
        [copy for half in halves for copy in final(half, -1, 1, FAR)],
    ]


PLAN = _plan()
COPIES = [c for group in PLAN for c in group]
_ENDS = (6, 10, 12, 16, 20, 24, 28, len(SLOTS))
EVENTS = [(SLOTS[a:b], k + 3 if k + 3 < len(PLAN) else None) for k, (a, b) in enumerate(zip((0, *_ENDS), _ENDS))]


def _gather_kernel(x_ref, gain_ref, *refs, side, finish, counts, twins):
    refs = iter(refs)
    take = lambda n: [next(refs) for _ in range(n)]
    extra_refs, w_refs, shared = (take(n) for n in counts[:3])
    (out_ref,), shelves = take(1), take(2 * len(shared))
    g, gain, w, stage, sems_x, sems_w, sems_o, send, recv = take(9)
    more = take(counts[3])
    carry = _Carry(side, twins, shared[0], shelves, *refs) if shared else None
    rows, depth = x_ref.shape
    size = rows // 2
    tiles = sum(ref.shape[1] for ref in w_refs) // w.shape[2]
    ring = min(w.shape[0], tiles)
    loads = tiles if tiles <= ring else len(EVENTS) * tiles

    def weights(s, start):
        finish.weights(w_refs, lax.rem(s, tiles), w, lax.rem(s, ring), sems_w, "start" if start else "wait")

    def remote(number):
        link, src, dst, part, of = COPIES[number]
        height = size // 2 if of == "rows" else size
        width = depth // 2 if of == "columns" else depth
        above, left = (part * height, 0) if of == "rows" else (0, part * width)
        here = [g.at[pl.ds(slot * size + above, height), pl.ds(left, width)] for slot in (src, dst)]
        return _copy(side, link, *here, send.at[number], recv.at[dst, part])

    def begin(group):
        first = sum(len(p) for p in PLAN[:group])
        for number in range(first, first + len(PLAN[group])):
            remote(number).start()

    def arrived(slots, parts=HALVES):
        for number, (_, _, dst, part, _) in enumerate(COPIES):
            if SLOTS[dst] in slots and part in parts:
                remote(number).wait_recv()

    met = _meet(side, bool(carry and twins))
    own = [pltpu.make_async_copy(x_ref.at[here], g.at[here], sems_x.at[half]) for half in HALVES for here in [pl.ds(half * size, size)]]
    gains = pltpu.make_async_copy(gain_ref, gain, sems_x.at[2])
    for c in (own[A], gains, own[B]):
        c.start()

    def norm(i, _):
        here = _tile(i, 16)
        wide = g[here, :].astype(jnp.float32)
        scale = lax.rsqrt(jnp.mean(wide * wide, -1, keepdims=True) + 1e-6)
        g[here, :] = (wide * scale * gain[...].astype(jnp.float32)[None]).astype(jnp.bfloat16)

    gains.wait()
    if carry:
        met()
        carry.begin()
    for half in HALVES:
        own[half].wait()
        lax.fori_loop(half * size // 16, (half + 1) * size // 16, norm, None)
        if half == A:
            carry.proceed() if carry else met()
        begin(half)
    begin(2)
    for s in range(ring - 1):
        weights(s, True)
    if finish.prepare:
        finish.prepare(extra_refs, more)
    if carry:
        for k in HALVES:
            carry.hand(k)

    def block(b, _):
        for k, (slots, group) in enumerate(EVENTS):

            @pl.when(b == k)
            def _(slots=slots, group=group):
                arrived(slots)
                if group is not None:
                    begin(group)
        def tile(n, _):
            s = b * tiles + n

            @pl.when(s + (ring - 1) < loads)
            def _():
                weights(s + (ring - 1), True)

            @pl.when(s < loads)
            def _():
                weights(s, False)

            product(b, n, s, g.at[_tile(b, BLOCK)], w.at[lax.rem(s, ring)])

        lax.fori_loop(0, tiles, tile, None)

    def product(b, n, s, lhs, rhs, *partial):
        to = lax.rem(s, 2)

        @pl.when(s >= 2)
        def _():
            finish.store(stage, out_ref, sems_o, to, b, n, size, side, start=False)

        finish.compute(lhs, rhs, stage.at[to], b, n, more, *partial)
        finish.store(stage, out_ref, sems_o, to, b, n, size, side, start=True)

    final = len(EVENTS) - 1
    whole = final if finish.in_parts else len(EVENTS)
    lax.fori_loop(0, whole, block, None)
    if whole == final:
        for part in HALVES:
            arrived(EVENTS[final][0], [part])
            here = pl.ds(part * (depth // 2), depth // 2)
            lhs = g.at[pl.ds(final * BLOCK, BLOCK), here]

            def tile(n, _, part=part, here=here, lhs=lhs):
                partial, *_ = more
                if part == A:
                    partial[n] = _dot(lhs[...], w[n, here, :])
                else:
                    product(final, n, final * tiles + n, lhs, w.at[n, here], partial)

            lax.fori_loop(0, tiles, tile, None)
    for to in range(2):
        finish.store(stage, out_ref, sems_o, to, 0, 0, size, side, start=False)
    for number in range(len(COPIES)):
        remote(number).wait_send()
    if carry:
        carry.end()


class _Carry:
    SHELF = {-1: 0, 1: 1, FAR: 2}

    def __init__(self, side, twins, w_ref, shelves, send, recv, give, got):
        self.side, self.twins, self.w_ref, self.shelves = side, twins, w_ref, shelves
        self.send, self.recv, self.give, self.got = send, recv, give, got

    def carrier(self, body):
        if self.twins:
            pl.when(lax.rem(lax.axis_index("dp"), 2) == 1)(body)
        else:
            body()

    def copies(self, step):
        for t, shelf in enumerate(self.shelves):
            for sign in SIGNS:
                depth, width = shelf.shape[1:]
                here = pl.ds((int(sign < 0) ^ (step == 1)) * (depth // 2), depth // 2)
                if step == 2:
                    src, dst = shelf.at[self.SHELF[-sign], here], shelf.at[self.SHELF[FAR], here]
                else:
                    src, dst = self.w_ref.at[here, pl.ds(t * width, width)], shelf.at[self.SHELF[-sign], here]
                sem = t, int(sign < 0), step
                yield _copy(self.side, ("xy"[t], sign), src, dst, self.send.at[sem], self.recv.at[sem])

    def handed(self, k):
        for t, shelf in enumerate(self.shelves):
            for at in ((0, 1), (2,))[k]:
                yield pltpu.make_async_remote_copy(src_ref=shelf.at[at], dst_ref=shelf.at[at], send_sem=self.give.at[t, at],
                                                   recv_sem=self.got.at[t, at], device_id=_twin(), device_id_type=MESH)

    def all(self, copies, what):
        for c in copies:
            getattr(c, what)()

    def begin(self):
        @self.carrier
        def _():
            for step in HALVES:
                self.all(self.copies(step), "start")

    def proceed(self):
        @self.carrier
        def _():
            self.all(self.copies(0), "wait_recv")
            self.all(self.copies(2), "start")

    def hand(self, k):
        @self.carrier
        def _():
            self.all(self.copies(k + 1), "wait_recv")
            if self.twins:
                self.all(self.handed(k), "start")

    def end(self):
        @self.carrier
        def _():
            for step in range(3):
                self.all(self.copies(step), "wait_send")
            if self.twins:
                for k in HALVES:
                    self.all(self.handed(k), "wait_send")

        if self.twins:

            @pl.when(lax.rem(lax.axis_index("dp"), 2) == 0)
            def _():
                for k in HALVES:
                    self.all(self.handed(k), "wait_recv")


class _Heads:
    in_parts = True

    def __init__(self, turned_steps):
        self.turned_steps = turned_steps

    def weights(self, refs, n, w, slot, sems, what):
        for at, ref in enumerate(refs):

            @pl.when(n == at)
            def _(ref=ref):
                getattr(pltpu.make_async_copy(ref, w.at[slot], sems.at[slot, 0]), what)()

    def prepare(self, extra_refs, more):
        (table_ref,) = extra_refs
        _, table, sems = more
        size = table.shape[0] // len(SLOTS)
        side = int(round((len(SLOTS) // 2) ** 0.5))
        copies = []
        for n, (half, dx, dy) in enumerate(SLOTS):
            row = _device(side, dx, dy) * (2 * size) + half * size
            copies.append(pltpu.make_async_copy(table_ref.at[pl.ds(pl.multiple_of(row, size), size)], table.at[pl.ds(n * size, size)],
                                                sems.at[n]))
        for what in ("start", "wait"):
            for c in copies:
                getattr(c, what)()

    def compute(self, lhs, w, to, at, n, more, partial=None):
        _, table, _ = more
        got = _dot(lhs[...], w[...])
        got = (got if partial is None else got + partial[n]).astype(jnp.bfloat16)

        @pl.when(n < self.turned_steps)
        def _():
            t = table[_tile(at, BLOCK), :]
            swapped = pltpu.roll(t, HEAD // 2, 1)
            low = lax.broadcasted_iota(jnp.int32, t.shape, 1) < HEAD // 2
            cos, sin = jnp.where(low, t, swapped), jnp.where(low, -swapped, t)
            for i in range(0, w.shape[1], HEAD):
                one = got[:, i : i + HEAD].astype(jnp.float32)
                to[:, i : i + HEAD] = (one * cos + pltpu.roll(one, HEAD // 2, 1) * sin).astype(jnp.bfloat16)

        @pl.when(n >= self.turned_steps)
        def _():
            to[...] = got

    def store(self, stage, out_ref, sems, to, at, n, size, side, start):
        per = BLOCK // size

        heads = stage.shape[2] // HEAD

        def copies(pieces):
            for p, (half, dx, dy) in enumerate(pieces):
                row = pl.multiple_of(_device(side, dx, dy) * (2 * size) + half * size, size)
                for i in range(heads):
                    yield pltpu.make_async_copy(stage.at[to, pl.ds(p * size, size), pl.ds(i * HEAD, HEAD)],
                                                out_ref.at[n * heads + i, pl.ds(row, size)], sems.at[to, p * heads + i])

        if not start:
            for c in copies(SLOTS[:per]):
                c.wait()
            return
        for k in range(len(SLOTS) // per):

            @pl.when(at == k)
            def _(k=k):
                for c in copies(SLOTS[k * per : (k + 1) * per]):
                    c.start()


class _Hidden:
    prepare = None
    in_parts = False

    def weights(self, refs, n, w, slot, sems, what):
        for at, ref in enumerate(refs):
            here = _tile(n, BLOCK)
            getattr(pltpu.make_async_copy(ref.at[:, here], w.at[slot, :, pl.ds(at * BLOCK, BLOCK)], sems.at[slot, at]), what)()

    def compute(self, lhs, w, to, at, n, more):
        got = _dot(lhs[...], w[...])
        to[...] = (jax.nn.silu(got[:, :BLOCK]) * got[:, BLOCK:]).astype(jnp.bfloat16)

    def store(self, stage, out_ref, sems, to, at, n, size, side, start):
        c = pltpu.make_async_copy(stage.at[to], out_ref.at[_tile(at, BLOCK),
                                                           _tile(n, BLOCK)], sems.at[to, 0])
        c.start() if start else c.wait()


def gathered(x, gain, weights, finish, stored, out_shape, number, name, extra=(), scratch=(), share=None, twins=False):
    rows, depth = x.shape
    n = lax.axis_size("tp")
    side = int(round(n**0.5))
    width = sum(w.shape[1] for w in weights)
    anywhere, dma = pl.BlockSpec(memory_space=pl.ANY), pltpu.SemaphoreType.DMA
    shared = [] if share is None else [share]
    shelves = [jax.ShapeDtypeStruct((side - 1, w.shape[0], w.shape[1] // 2), w.dtype) for w in 2 * shared]
    operands = [x, gain, *extra, *weights, *shared]
    return pl.pallas_call(
        functools.partial(_gather_kernel, side=side, finish=finish, counts=(len(extra), len(weights), len(shared), len(scratch)), twins=twins),
        out_shape=[out_shape, *shelves] if shared else out_shape,
        in_specs=[anywhere] * len(operands),
        out_specs=[anywhere] * 3 if shared else anywhere,
        scratch_shapes=[
            pltpu.VMEM((n * rows, depth), jnp.bfloat16),
            pltpu.VMEM((depth,), jnp.bfloat16),
            pltpu.VMEM((3, depth, 2 * BLOCK), jnp.bfloat16),
            pltpu.VMEM((2, BLOCK, stored), jnp.bfloat16),
            dma((3,)), dma((3, 2)), dma((2, len(SLOTS))), dma((len(COPIES),)), dma((len(SLOTS), 2)),
            *scratch,
            *([dma((2, 2, 3))] * 2 + [dma((2, 3))] * 2 if shared else []),
        ],
        compiler_params=pltpu.CompilerParams(collective_id=number, has_side_effects=True, vmem_limit_bytes=VMEM),
        cost_estimate=_cost(n * rows, depth, width, len(EVENTS)),
        name=name,
    )(*operands)


class _Sum:
    def __init__(self, side, near, keep, own, r_half, r_near, s_half, s_near, t_half, t_near):
        self.side, self.near, self.keep, self.own = side, near, keep, own
        self.r_half, self.r_near, self.s_half, self.s_near, self.t_half, self.t_near = r_half, r_near, s_half, s_near, t_half, t_near
        self.low = keep.shape[2]

    def halves(self, j):
        a, b = lax.rem(j, 2), lax.rem(j, self.r_half.shape[0])
        return [_copy(self.side, link, self.near.at[a, 0, l], self.r_half.at[b, l], self.s_half.at[a, l], self.t_half.at[b, l])
                for l, link in enumerate(LINKS)]

    def lasts(self, j, part):
        a, b = lax.rem(j, 2), lax.rem(j, self.r_near.shape[0])
        got = []
        for l, link in enumerate(LINKS):
            at = l % 2 if part else 1 - l % 2
            got.append(_copy(self.side, link, self.near.at[a, 1 + part, l], self.r_near.at[b, l, pl.ds(at * self.low, self.low)],
                             self.s_near.at[a, part, l], self.t_near.at[b, part, l]))
        return got

    def each(self, what, *groups):
        for c in sum(groups, []):
            getattr(c, what)()

    def freed(self, j):
        self.each("wait_send", self.halves(j), self.lasts(j, 0))

    def gone(self, j):
        self.each("wait_send", self.lasts(j, 1))

    def put(self, j, t, l, pieces):
        a, low, bf = lax.rem(j, 2), self.low, jnp.bfloat16
        self.own[lax.rem(j, 4), t] = pieces[0]
        self.near[a, 0, l] = pieces[FAR][:low].astype(bf)
        self.near[a, 0, l + 1] = pieces[FAR][low:].astype(bf)
        self.near[a, 1, l] = pieces[1][low:].astype(bf)
        self.near[a, 1, l + 1] = pieces[-1][:low].astype(bf)
        self.keep[a, l] = pieces[1][:low]
        self.keep[a, l + 1] = pieces[-1][low:]

    def leave(self, j):
        self.each("start", self.halves(j), self.lasts(j, 0))

    def merge(self, j):
        a, b = lax.rem(j, 2), lax.rem(j, self.r_half.shape[0])
        self.each("wait_recv", self.halves(j))
        for l in range(len(LINKS)):
            self.near[a, 2, l] = (self.keep[a, l] + self.r_half[b, l].astype(jnp.float32)).astype(jnp.bfloat16)
        self.each("start", self.lasts(j, 1))

    def arrived(self, j):
        self.each("wait_recv", self.lasts(j, 0), self.lasts(j, 1))

    def total(self, j, t, l):
        b = lax.rem(j, self.r_near.shape[0])
        return self.own[lax.rem(j, 4), t] + self.r_near[b, l].astype(jnp.float32) + self.r_near[b, l + 1].astype(jnp.float32)

    @staticmethod
    def scratch(rings, low, tile):
        bf, f32, dma = jnp.bfloat16, jnp.float32, pltpu.SemaphoreType.DMA
        return [pltpu.VMEM((2, 3, 4, low, tile), bf), pltpu.VMEM((2, 4, low, tile), f32), pltpu.VMEM((4, 2, 2 * low, tile), f32),
                pltpu.VMEM((rings, 4, low, tile), bf), pltpu.VMEM((rings, 4, 2 * low, tile), bf),
                dma((2, 4)), dma((2, 2, 4)), dma((rings, 4)), dma((rings, 2, 4))]


def _scatter_kernel(rows_ref, x_ref, w_ref, out, hid, res, w, far, plain, summed, r_far, r_plain, r_summed, sems_h, sems_x, sems_w,
                    s_far, s_plain, s_summed, t_far, t_plain, t_summed, *second, side):
    rows, width = out.shape
    size = rows // 2
    tile = w.shape[2]
    tiles = width // tile
    ring = r_far.shape[0]
    group = hid.shape[0] // 4

    def fetch(n):
        return pltpu.make_async_copy(rows_ref.at[pl.ds(SLOT[ORDER[n]] * size, size)], hid.at[pl.ds(n * size, size)], sems_h.at[n])

    def weights(j):
        slot = lax.rem(j, 4)
        return pltpu.make_async_copy(w_ref.at[:, _tile(j, tile)], w.at[slot], sems_w.at[slot])

    def terms(g, j, count=1):
        return _dot(hid[pl.ds(g * group, count * group), :], w[lax.rem(j, 4)]).reshape(-1, size, tile)

    def pairs(src, dst, s_sem, t_sem, j):
        a, b = lax.rem(j, 2), lax.rem(j, ring)
        return [_copy(side, LINKS[l], src.at[a, pl.ds(2 * l, 2)], dst.at[b, pl.ds(2 * l, 2)], s_sem.at[a, l], t_sem.at[b, l])
                for l in range(4)]

    ring2 = _Sum(side, *second)

    def each(copies, what):
        for c in copies:
            getattr(c, what)()

    weights(0).start()
    for n in range(len(ORDER)):
        fetch(n).start()
    residual = pltpu.make_async_copy(x_ref, res, sems_x.at[0])
    residual.start()
    _meet(side)()
    for n in range(len(ORDER)):
        fetch(n).wait()
    residual.wait()

    def step(i, _):
        @_during(i, 2, tiles)
        def _():
            each(pairs(far, r_far, s_far, t_far, i - 2), "wait_send")
            each(pairs(plain, r_plain, s_plain, t_plain, i - 2), "wait_send")

        @_during(i, 0, tiles)
        def _():
            j = i

            @pl.when(j + 1 < tiles)
            def _():
                weights(j + 1).start()

            weights(j).wait()
            got = terms(0, j, 2).astype(jnp.bfloat16)
            far[lax.rem(j, 2)] = got[:8]
            plain[lax.rem(j, 2)] = got[8:]
            each(pairs(far, r_far, s_far, t_far, j), "start")
            each(pairs(plain, r_plain, s_plain, t_plain, j), "start")

        @_during(i, 3, tiles)
        def _():
            each(pairs(summed, r_summed, s_summed, t_summed, i - 3), "wait_send")

        @_during(i, 1, tiles)
        def _():
            j = i - 1
            each(pairs(far, r_far, s_far, t_far, j), "wait_recv")
            summed[lax.rem(j, 2)] = (terms(2, j) + r_far[lax.rem(j, ring)].astype(jnp.float32)).astype(jnp.bfloat16)
            each(pairs(summed, r_summed, s_summed, t_summed, j), "start")

        @_during(i, 4, tiles)
        def _():
            ring2.freed(i - 4)

        @_during(i, 2, tiles)
        def _():
            j = i - 2
            b = lax.rem(j, ring)
            each(pairs(plain, r_plain, s_plain, t_plain, j), "wait_recv")
            each(pairs(summed, r_summed, s_summed, t_summed, j), "wait_recv")
            mine = terms(3, j)
            for half in HALVES:
                l = 2 * half
                up, down = pl.ds(2 * l, 2), pl.ds(2 * l + 2, 2)
                from_up = jnp.concatenate([r_summed[b, up], r_plain[b, up]]).astype(jnp.float32)
                from_down = jnp.concatenate([r_plain[b, down], r_summed[b, down]]).astype(jnp.float32)
                both_ways = mine[4 * half : 4 * half + 4] + from_up + from_down
                sums = {across: both_ways[k] for k, across in enumerate(UP + DOWN)}
                ring2.put(j, half, 2 - l, sums)
            ring2.leave(j)

        @_during(i, 5, tiles)
        def _():
            ring2.gone(i - 5)

        @_during(i, 3, tiles)
        def _():
            ring2.merge(i - 3)

        @pl.when(i >= 4)
        def _():
            j = i - 4

            ring2.arrived(j)
            here = _tile(j, tile)
            for half in HALVES:
                mine = pl.ds(half * size, size)
                out[mine, here] = (res[mine, here].astype(jnp.float32) + ring2.total(j, half, 2 - 2 * half)).astype(jnp.bfloat16)

    lax.fori_loop(0, tiles + 4, step, None)
    ring2.gone(tiles - 1)


def scattered(terms, x, w, number, name):
    rows, width = x.shape
    depth = w.shape[0]
    n = lax.axis_size("tp")
    side = int(round(n**0.5))
    size, low = rows // 2, rows // 4
    tile = min(TILE, width)
    tiles = width // tile
    bf, dma = jnp.bfloat16, pltpu.SemaphoreType.DMA
    return pl.pallas_call(
        functools.partial(_scatter_kernel, side=side),
        out_shape=jax.ShapeDtypeStruct((rows, width), bf),
        in_specs=[pl.BlockSpec(memory_space=pl.ANY)] * 3,
        out_specs=pl.BlockSpec(memory_space=pltpu.VMEM),
        scratch_shapes=[
            pltpu.VMEM((n * rows, depth), bf),
            pltpu.VMEM((rows, width), bf),
            pltpu.VMEM((4, depth, tile), bf),
            pltpu.VMEM((2, 8, size, tile), bf),
            pltpu.VMEM((2, 8, size, tile), bf),
            pltpu.VMEM((2, 8, size, tile), bf),
            pltpu.VMEM((RING, 8, size, tile), bf),
            pltpu.VMEM((RING, 8, size, tile), bf),
            pltpu.VMEM((RING, 8, size, tile), bf),
            dma((len(ORDER),)), dma((1,)), dma((4,)),
            *[dma((2, 4))] * 3, *[dma((RING, 4))] * 3,
            *_Sum.scratch(RING, low, tile),
        ],
        compiler_params=pltpu.CompilerParams(collective_id=number, has_side_effects=True, vmem_limit_bytes=LAST_VMEM),
        cost_estimate=_cost(n * rows, depth, width),
        name=name,
    )(terms, x, w)


AROUND = (0, 1, -1, FAR)
ORIGIN = (0, -1, 1, FAR)
TURNS = (FAR, 1, -1, 0)


def _attend(qkv, mine, o, top_s, mix_s):
    size, d = o.shape[0], qkv.shape[2]
    heads = qkv.shape[0] // 3
    e = d**-0.5 * LOG2E
    top_s[...] = jnp.full(top_s.shape, NEG, jnp.float32)
    mix_s[...] = jnp.zeros(mix_s.shape, jnp.float32)
    ones = jnp.ones((8, size), qkv.dtype)

    def block(j, masked):
        here = _tile(j, size)
        scores = [_dot(qkv[heads + i, here, :], qkv[i, _tile(mine, size), :], 1, 1) for i in range(heads)]
        if masked:
            seen = lax.broadcasted_iota(jnp.int32, (size, size), 1) >= lax.broadcasted_iota(jnp.int32, (size, size), 0)
        weights, keeps = [], []
        for i, s in enumerate(scores):
            s = jnp.where(seen, s, HIDDEN) if masked else s
            old = top_s[i : i + 1, :]
            top = jnp.maximum(old, s.max(axis=0, keepdims=True))
            top_s[i : i + 1, :] = top
            weights.append(jnp.exp2((s - top) * e).astype(qkv.dtype))
            keeps.append(jnp.exp2((old - top) * e))
        for i, (p, keep) in enumerate(zip(weights, keeps)):
            values = jnp.concatenate([qkv[2 * heads + i, here, :].T, ones], axis=0)
            mix_s[i] = mix_s[i] * keep + _dot(values, p, 1, 0)

    lax.fori_loop(0, mine, lambda j, _: block(j, False), None)
    block(mine, True)
    for i in range(heads):
        total = mix_s[i, d : d + 1, :]
        o[:, i * d : (i + 1) * d] = (mix_s[i, :d, :] * (1 / total)).T.astype(o.dtype)


def _share_kernel(qkv_ref, x_ref, w_ref, left_ref, right_ref, out_ref, qkv, seen, top_s, mix_s, s, relay, w, res, out, sems_q, sems_x, sems_w,
                  sems_o, s_next, s_far, s_pass, t_next, t_far, t_pass, *second, side):
    rows, width = out_ref.shape
    depth, tile = w_ref.shape[0], w.shape[3]
    half, tiles = width // 2, width // 2 // tile
    slots = w.shape[0]
    ring = _Sum(side, *second)
    x, y = _place(side)

    def block(t, along, across):
        dx, dy = (along, across) if t == 0 else (across, along)
        return seen.at[TURNS.index(dx), _tile(lax.rem(y + (dy + side), side), rows)]

    def place(t, across, origin):
        return s.at[t, _tile(AROUND.index(across), rows), _tile(ORIGIN.index(origin), depth)]

    ways = [(t, n, sign) for t in HALVES for n, sign in enumerate(SIGNS)]

    def far(t, along, across):
        n, i = divmod(AROUND.index(across), 2)
        sign = 1 - 2 * n
        return _copy(side, ("xy"[t], sign), block(t, FAR, across), relay.at[t, n, i], s_far.at[t, n, i], t_far.at[t, n, i])

    def passed(t, across):
        n, i = divmod(AROUND.index(across), 2)
        return _copy(side, ("xy"[t], 1 - 2 * n), relay.at[t, n, i], place(t, across, FAR), s_pass.at[t, n, i], t_pass.at[t, n, i])

    def next_to(t, sign, across):
        at = t, int(sign < 0), AROUND.index(across)
        return _copy(side, ("xy"[t], sign), block(t, sign, across), place(t, across, -sign), s_next.at[at], t_next.at[at])

    def sends(t, along, across):
        if along:
            (far if along == FAR else next_to)(t, along, across).start()
        else:
            place(t, across, 0)[...] = block(t, 0, across)[...]

    def each(what, copies):
        for c in copies:
            getattr(c, what)()

    def weights(j):
        got = []
        for t, shelf in enumerate((left_ref, right_ref)):
            for i in range(side):
                src = shelf.at[i - 1, :, _tile(j, tile)] if i else w_ref.at[:, _tile(t * tiles + j, tile)]
                got.append(pltpu.make_async_copy(src, w.at[lax.rem(j, slots), t, pl.ds(i * depth, depth)], sems_w.at[lax.rem(j, slots), t, i]))
        return got

    def out_copy(t, j):
        here = _tile(t * tiles + j, tile)
        return pltpu.make_async_copy(out.at[:, here], out_ref.at[:, here], sems_o.at[t, j])

    met = _meet(side)
    heads = qkv.shape[0] // 3
    parts = [pltpu.make_async_copy(qkv_ref.at[here], qkv.at[here], sems_q.at[n]) for n in range(3) for here in [pl.ds(n * heads, heads)]]
    each("start", parts)
    for j in range(slots - 1):
        each("start", weights(j))
    residual = pltpu.make_async_copy(x_ref, res, sems_x.at[0])
    residual.start()
    each("wait", parts)
    met()

    def turn(n, _):
        _attend(qkv, lax.rem(x + (FAR + len(TURNS) * 2) - lax.div(n * (n + 1), 2), side), seen.at[n], top_s, mix_s)
        for k, dx in enumerate(TURNS):

            @pl.when(n == k)
            def _(dx=dx):
                for other in AROUND:
                    sends(0, dx, other)
                    sends(1, other, dx)

    lax.fori_loop(0, len(TURNS), turn, None)
    for t in HALVES:
        for across in TURNS:
            far(t, FAR, across).wait_recv()
            passed(t, across).start()
    for t, n, sign in ways:
        each("wait_recv", [next_to(t, sign, across) for across in AROUND])
    residual.wait()
    for t in HALVES:
        each("wait_recv", [passed(t, across) for across in AROUND])

    def step(i, _):
        @_during(i, 2, tiles)
        def _():
            ring.freed(i - 2)

        @_during(i, 0, tiles)
        def _():
            j = i

            @pl.when(j + (slots - 1) < tiles)
            def _():
                each("start", weights(j + (slots - 1)))

            each("wait", weights(j))
            for t in HALVES:
                got = _dot(s[t], w[lax.rem(j, slots), t])
                ring.put(j, t, 2 * t, {across: got[k * rows : (k + 1) * rows] for k, across in enumerate(AROUND)})
            ring.leave(j)

        @_during(i, 3, tiles)
        def _():
            ring.gone(i - 3)

        @_during(i, 1, tiles)
        def _():
            ring.merge(i - 1)

        @pl.when(i >= 2)
        def _():
            j = i - 2
            ring.arrived(j)
            for t in HALVES:
                here = _tile(t * tiles + j, tile)
                out[:, here] = (res[:, here].astype(jnp.float32) + ring.total(j, t, 2 * t)).astype(jnp.bfloat16)
                out_copy(t, j).start()

    lax.fori_loop(0, tiles + 2, step, None)
    ring.gone(tiles - 1)
    for t, n, sign in ways:
        each("wait_send", [next_to(t, sign, across) for across in AROUND])
    for t in HALVES:
        each("wait_send", [copy for across in AROUND for copy in (far(t, FAR, across), passed(t, across))])
        for j in range(tiles):
            out_copy(t, j).wait()


def projected(qkv, x, w, left, right, number, name):
    rows, width = x.shape
    depth = w.shape[0]
    n = lax.axis_size("tp")
    side = int(round(n**0.5))
    tile = min(TILE, width // 2)
    tiles = width // 2 // tile
    bf, dma = jnp.bfloat16, pltpu.SemaphoreType.DMA
    anywhere = pl.BlockSpec(memory_space=pl.ANY)
    return pl.pallas_call(
        functools.partial(_share_kernel, side=side),
        out_shape=jax.ShapeDtypeStruct((rows, width), bf),
        in_specs=[anywhere] * 5,
        out_specs=anywhere,
        scratch_shapes=[
            pltpu.VMEM(qkv.shape, bf),
            pltpu.VMEM((side, side * rows, depth), bf),
            pltpu.VMEM((qkv.shape[0] // 3, side * rows), jnp.float32),
            pltpu.VMEM((qkv.shape[0] // 3, HEAD + 8, side * rows), jnp.float32),
            pltpu.VMEM((2, side * rows, side * depth), bf),
            pltpu.VMEM((2, 2, 2, rows, depth), bf),
            pltpu.VMEM((3, 2, side * depth, tile), bf),
            pltpu.VMEM((rows, width), bf),
            pltpu.VMEM((rows, width), bf),
            dma((3,)), dma((1,)), dma((3, 2, side)), dma((2, tiles)),
            *[dma((2, 2, 4)), dma((2, 2, 2)), dma((2, 2, 2))] * 2,
            *_Sum.scratch(tiles, rows // 2, tile),
        ],
        compiler_params=pltpu.CompilerParams(collective_id=number, has_side_effects=True, vmem_limit_bytes=VMEM),
        cost_estimate=_cost(n * rows, depth, width, side),
        name=name,
    )(qkv, x, w, left, right)


def _angles(tokens):
    half = HEAD // 2
    rate = np.power(np.float32(THETA), -np.arange(half, dtype=np.float32) / np.float32(half)).astype(np.float32)
    angle = (np.arange(tokens, dtype=np.float32)[:, None] * rate).astype(np.float64)
    return np.concatenate([np.cos(angle), np.sin(angle)], 1).astype(np.float32)


def solution(mesh):
    n = mesh.shape["tp"]

    def step(x, gain_a, wq, wk, wv, wo, gain_m, w_gate, w_up, w_down):
        rows = n * x.shape[0]
        heads = wq.shape[1] // HEAD
        qkv, left, right = gathered(
            x, gain_a, (wq, wk, wv), _Heads(2), 2 * BLOCK, jax.ShapeDtypeStruct((3 * heads, rows, HEAD), jnp.bfloat16), 0, "gather_qkv",
            extra=(jnp.asarray(_angles(rows)),),
            scratch=(pltpu.VMEM((3, BLOCK, 2 * BLOCK), jnp.float32), pltpu.VMEM((rows, HEAD), jnp.float32),
                     pltpu.SemaphoreType.DMA((len(SLOTS),))),
            share=wo, twins=mesh.shape["dp"] % 2 == 0,
        )
        h = projected(qkv, x, wo, left, right, 1, "project")
        hidden = gathered(h, gain_m, (w_gate, w_up), _Hidden(), BLOCK, jax.ShapeDtypeStruct((rows, w_gate.shape[1]), jnp.bfloat16), 2,
                          "gather_hidden")
        return scattered(hidden, h, w_down, 3, "scatter_down")

    tokens, columns, rows_of = P(("dp", "tp"), None), P(None, "tp"), P("tp", None)
    return jax.shard_map(
        step,
        mesh=mesh,
        in_specs=(tokens, P(None), columns, columns, columns, rows_of, P(None), columns, columns, rows_of),
        out_specs=tokens,
        check_vma=False,
    )
```

```python
import functools

import jax
import jax.numpy as jnp
import numpy as np
from jax import lax
from jax.experimental import pallas as pl
from jax.experimental.pallas import tpu as pltpu
from jax.sharding import PartitionSpec as P

MESH = pl.DeviceIdType.MESH
HEAD = 128
THETA = 10000
NEG = -1e30
HIDDEN = 2 * NEG
LOG2E = 1.4426950408889634
VMEM = 62 << 20
LAST_VMEM = 50 << 20
BLOCK = 256
TILE = 512
RING = 6

A, B = 0, 1
FAR = 2
UP, DOWN = (0, -1), (1, FAR)
LINKS = (("y", 1), ("y", -1), ("x", 1), ("x", -1))


def piece(half, along, across):
    return (half, across, along) if half == A else (half, along, across)


def both(along, across):
    return [piece(A, along, across), piece(B, along, across)]


NEXT, SIGNS, HALVES = (-1, 1), (1, -1), (A, B)
SLOTS = [
    p
    for group in (
        [both(0, 0)],
        [[piece(half, 0, d) for d in NEXT] for half in HALVES],
        [[piece(half, d, 0) for d in NEXT] for half in HALVES],
        [both(0, FAR)],
        *([[piece(half, d, across) for d in NEXT] for half in HALVES] for across in NEXT),
        [both(FAR, 0), both(1, FAR), both(-1, FAR), both(FAR, 1), both(FAR, -1), both(FAR, FAR)],
    )
    for some in group
    for p in some
]
SLOT = {p: n for n, p in enumerate(SLOTS)}

def _by_link(along, pick):
    return [
        piece(half, along if along == 2 else sign * along, across)
        for (axis, sign) in LINKS
        for half in [A if axis == "y" else B]
        for across in (UP if (sign > 0) == pick else DOWN)
    ]


ORDER = _by_link(2, True) + _by_link(1, False) + _by_link(1, True) + [piece(half, 0, across) for half in HALVES for across in UP + DOWN]


def _place(side):
    me = lax.axis_index("tp")
    return lax.div(me, side), lax.rem(me, side)


def _device(side, dx, dy):
    x, y = _place(side)
    return lax.rem(x + (dx + side), side) * side + lax.rem(y + (dy + side), side)


def _meet(side, twin=False):
    barrier = pltpu.get_barrier_semaphore()
    others = [{"tp": _device(side, *_step(link))} for link in LINKS] + ([_twin()] if twin else [])
    for other in others:
        pl.semaphore_signal(barrier, inc=1, device_id=other, device_id_type=MESH)
    return lambda: pl.semaphore_wait(barrier, len(others))


def _twin():
    group = lax.axis_index("dp")
    return {"dp": group + 1 - 2 * lax.rem(group, 2), "tp": lax.axis_index("tp")}


def _step(link):
    axis, sign = link
    return (sign, 0) if axis == "x" else (0, sign)


def _copy(side, link, src, dst, send_sem, recv_sem):
    return pltpu.make_async_remote_copy(src_ref=src, dst_ref=dst, send_sem=send_sem, recv_sem=recv_sem,
                                        device_id={"tp": _device(side, *_step(link))}, device_id_type=MESH)


def _cost(rows, depth, width, passes=1):
    return pl.CostEstimate(flops=2 * rows * depth * width, transcendentals=0, bytes_accessed=2 * passes * depth * width)


def _tile(i, size):
    return pl.ds(pl.multiple_of(i * size, size), size)


def _during(i, late, count):
    return pl.when((i >= late) & (i < count + late))


def _dot(a, b, ca=1, cb=0):
    return lax.dot_general(a, b, (((ca,), (cb,)), ((), ())), preferred_element_type=jnp.float32)


def _plan():
    slot = lambda half, along, across: SLOT[piece(half, along, across)]

    def inner(half, sign, source, target, part=0, of="all"):
        return ("xy"[half], sign), slot(half, 0, source), slot(half, 0, target), part, of

    def outer(half, sign, source, across, part=0, of="all"):
        target = -sign if source == 0 else FAR
        return ("yx"[half], sign), slot(half, source, across), slot(half, target, across), part, of

    def final(*which):
        return [outer(*which, part, "columns") for part in HALVES]

    halves, signs = HALVES, SIGNS
    return [
        [inner(A, sign, 0, -sign) for sign in signs],
        [inner(B, sign, 0, -sign) for sign in signs],
        [outer(half, sign, 0, 0) for half in (B, A) for sign in signs],
        [inner(half, sign, -sign, FAR, int(sign < 0), "rows") for half in halves for sign in signs]
        + [outer(half, sign, 0, across) for across in NEXT for half in halves for sign in signs],
        [outer(half, 1, -1, 0) for half in halves],
        [outer(half, sign, 0, FAR) for half in halves for sign in signs],
        [copy for half in halves for copy in final(half, 1, -1, -1)],
        [outer(half, -1, 1, 1) for half in halves],
        [copy for half in halves for copy in final(half, -1, 1, FAR)],
    ]


PLAN = _plan()
COPIES = [c for group in PLAN for c in group]
_ENDS = (6, 10, 12, 16, 20, 24, 28, len(SLOTS))
EVENTS = [(SLOTS[a:b], k + 3 if k + 3 < len(PLAN) else None) for k, (a, b) in enumerate(zip((0, *_ENDS), _ENDS))]


def _gather_kernel(x_ref, gain_ref, *refs, side, finish, counts, twins):
    refs = iter(refs)
    take = lambda n: [next(refs) for _ in range(n)]
    extra_refs, w_refs, shared = (take(n) for n in counts[:3])
    (out_ref,), shelves = take(1), take(2 * len(shared))
    g, gain, w, stage, sems_x, sems_w, sems_o, send, recv = take(9)
    more = take(counts[3])
    carry = _Carry(side, twins, shared[0], shelves, *refs) if shared else None
    rows, depth = x_ref.shape
    size = rows // 2
    tiles = sum(ref.shape[1] for ref in w_refs) // w.shape[2]
    ring = min(w.shape[0], tiles)
    loads = tiles if tiles <= ring else len(EVENTS) * tiles

    def weights(s, start):
        finish.weights(w_refs, lax.rem(s, tiles), w, lax.rem(s, ring), sems_w, "start" if start else "wait")

    def remote(number):
        link, src, dst, part, of = COPIES[number]
        height = size // 2 if of == "rows" else size
        width = depth // 2 if of == "columns" else depth
        above, left = (part * height, 0) if of == "rows" else (0, part * width)
        here = [g.at[pl.ds(slot * size + above, height), pl.ds(left, width)] for slot in (src, dst)]
        return _copy(side, link, *here, send.at[number], recv.at[dst, part])

    def begin(group):
        first = sum(len(p) for p in PLAN[:group])
        for number in range(first, first + len(PLAN[group])):
            remote(number).start()

    def arrived(slots, parts=HALVES):
        for number, (_, _, dst, part, _) in enumerate(COPIES):
            if SLOTS[dst] in slots and part in parts:
                remote(number).wait_recv()

    met = _meet(side, bool(carry and twins))
    own = [pltpu.make_async_copy(x_ref.at[here], g.at[here], sems_x.at[half]) for half in HALVES for here in [pl.ds(half * size, size)]]
    gains = pltpu.make_async_copy(gain_ref, gain, sems_x.at[2])
    for c in (own[A], gains, own[B]):
        c.start()

    def norm(i, _):
        here = _tile(i, 16)
        wide = g[here, :].astype(jnp.float32)
        scale = lax.rsqrt(jnp.mean(wide * wide, -1, keepdims=True) + 1e-6)
        g[here, :] = (wide * scale * gain[...].astype(jnp.float32)[None]).astype(jnp.bfloat16)

    gains.wait()
    if carry:
        met()
        carry.begin()
    for half in HALVES:
        own[half].wait()
        lax.fori_loop(half * size // 16, (half + 1) * size // 16, norm, None)
        if half == A:
            carry.proceed() if carry else met()
        begin(half)
    begin(2)
    for s in range(ring - 1):
        weights(s, True)
    if finish.prepare:
        finish.prepare(extra_refs, more)
    if carry:
        for k in HALVES:
            carry.hand(k)

    def block(b, _):
        for k, (slots, group) in enumerate(EVENTS):

            @pl.when(b == k)
            def _(slots=slots, group=group):
                arrived(slots)
                if group is not None:
                    begin(group)
        def tile(n, _):
            s = b * tiles + n

            @pl.when(s + (ring - 1) < loads)
            def _():
                weights(s + (ring - 1), True)

            @pl.when(s < loads)
            def _():
                weights(s, False)

            product(b, n, s, g.at[_tile(b, BLOCK)], w.at[lax.rem(s, ring)])

        lax.fori_loop(0, tiles, tile, None)

    def product(b, n, s, lhs, rhs, *partial):
        to = lax.rem(s, 2)

        @pl.when(s >= 2)
        def _():
            finish.store(stage, out_ref, sems_o, to, b, n, size, side, start=False)

        finish.compute(lhs, rhs, stage.at[to], b, n, more, *partial)
        finish.store(stage, out_ref, sems_o, to, b, n, size, side, start=True)

    final = len(EVENTS) - 1
    whole = final if finish.in_parts else len(EVENTS)
    lax.fori_loop(0, whole, block, None)
    if whole == final:
        for part in HALVES:
            arrived(EVENTS[final][0], [part])
            here = pl.ds(part * (depth // 2), depth // 2)
            lhs = g.at[pl.ds(final * BLOCK, BLOCK), here]

            def tile(n, _, part=part, here=here, lhs=lhs):
                partial, *_ = more
                if part == A:
                    partial[n] = _dot(lhs[...], w[n, here, :])
                else:
                    product(final, n, final * tiles + n, lhs, w.at[n, here], partial)

            lax.fori_loop(0, tiles, tile, None)
    for to in range(2):
        finish.store(stage, out_ref, sems_o, to, 0, 0, size, side, start=False)
    for number in range(len(COPIES)):
        remote(number).wait_send()
    if carry:
        carry.end()


class _Carry:
    SHELF = {-1: 0, 1: 1, FAR: 2}

    def __init__(self, side, twins, w_ref, shelves, send, recv, give, got):
        self.side, self.twins, self.w_ref, self.shelves = side, twins, w_ref, shelves
        self.send, self.recv, self.give, self.got = send, recv, give, got

    def carrier(self, body):
        if self.twins:
            pl.when(lax.rem(lax.axis_index("dp"), 2) == 0)(body)
        else:
            body()

    def copies(self, step):
        for t, shelf in enumerate(self.shelves):
            for sign in SIGNS:
                depth, width = shelf.shape[1:]
                here = pl.ds((int(sign < 0) ^ (step == 1)) * (depth // 2), depth // 2)
                if step == 2:
                    src, dst = shelf.at[self.SHELF[-sign], here], shelf.at[self.SHELF[FAR], here]
                else:
                    src, dst = self.w_ref.at[here, pl.ds(t * width, width)], shelf.at[self.SHELF[-sign], here]
                sem = t, int(sign < 0), step
                yield _copy(self.side, ("xy"[t], sign), src, dst, self.send.at[sem], self.recv.at[sem])

    def handed(self, k):
        for t, shelf in enumerate(self.shelves):
            for at in ((0, 1), (2,))[k]:
                yield pltpu.make_async_remote_copy(src_ref=shelf.at[at], dst_ref=shelf.at[at], send_sem=self.give.at[t, at],
                                                   recv_sem=self.got.at[t, at], device_id=_twin(), device_id_type=MESH)

    def all(self, copies, what):
        for c in copies:
            getattr(c, what)()

    def begin(self):
        @self.carrier
        def _():
            for step in HALVES:
                self.all(self.copies(step), "start")

    def proceed(self):
        @self.carrier
        def _():
            self.all(self.copies(0), "wait_recv")
            self.all(self.copies(2), "start")

    def hand(self, k):
        @self.carrier
        def _():
            self.all(self.copies(k + 1), "wait_recv")
            if self.twins:
                self.all(self.handed(k), "start")

    def end(self):
        @self.carrier
        def _():
            for step in range(3):
                self.all(self.copies(step), "wait_send")
            if self.twins:
                for k in HALVES:
                    self.all(self.handed(k), "wait_send")

        if self.twins:

            @pl.when(lax.rem(lax.axis_index("dp"), 2) == 1)
            def _():
                for k in HALVES:
                    self.all(self.handed(k), "wait_recv")


class _Heads:
    in_parts = True

    def __init__(self, turned_steps):
        self.turned_steps = turned_steps

    def weights(self, refs, n, w, slot, sems, what):
        for at, ref in enumerate(refs):

            @pl.when(n == at)
            def _(ref=ref):
                getattr(pltpu.make_async_copy(ref, w.at[slot], sems.at[slot, 0]), what)()

    def prepare(self, extra_refs, more):
        (table_ref,) = extra_refs
        _, table, sems = more
        size = table.shape[0] // len(SLOTS)
        side = int(round((len(SLOTS) // 2) ** 0.5))
        copies = []
        for n, (half, dx, dy) in enumerate(SLOTS):
            row = _device(side, dx, dy) * (2 * size) + half * size
            copies.append(pltpu.make_async_copy(table_ref.at[pl.ds(pl.multiple_of(row, size), size)], table.at[pl.ds(n * size, size)],
                                                sems.at[n]))
        for what in ("start", "wait"):
            for c in copies:
                getattr(c, what)()

    def compute(self, lhs, w, to, at, n, more, partial=None):
        _, table, _ = more
        got = _dot(lhs[...], w[...])
        got = (got if partial is None else got + partial[n]).astype(jnp.bfloat16)

        @pl.when(n < self.turned_steps)
        def _():
            t = table[_tile(at, BLOCK), :]
            swapped = pltpu.roll(t, HEAD // 2, 1)
            low = lax.broadcasted_iota(jnp.int32, t.shape, 1) < HEAD // 2
            cos, sin = jnp.where(low, t, swapped), jnp.where(low, -swapped, t)
            for i in range(0, w.shape[1], HEAD):
                one = got[:, i : i + HEAD].astype(jnp.float32)
                to[:, i : i + HEAD] = (one * cos + pltpu.roll(one, HEAD // 2, 1) * sin).astype(jnp.bfloat16)

        @pl.when(n >= self.turned_steps)
        def _():
            to[...] = got

    def store(self, stage, out_ref, sems, to, at, n, size, side, start):
        per = BLOCK // size

        heads = stage.shape[2] // HEAD

        def copies(pieces):
            for p, (half, dx, dy) in enumerate(pieces):
                row = pl.multiple_of(_device(side, dx, dy) * (2 * size) + half * size, size)
                for i in range(heads):
                    yield pltpu.make_async_copy(stage.at[to, pl.ds(p * size, size), pl.ds(i * HEAD, HEAD)],
                                                out_ref.at[n * heads + i, pl.ds(row, size)], sems.at[to, p * heads + i])

        if not start:
            for c in copies(SLOTS[:per]):
                c.wait()
            return
        for k in range(len(SLOTS) // per):

            @pl.when(at == k)
            def _(k=k):
                for c in copies(SLOTS[k * per : (k + 1) * per]):
                    c.start()


class _Hidden:
    prepare = None
    in_parts = False

    def weights(self, refs, n, w, slot, sems, what):
        for at, ref in enumerate(refs):
            here = _tile(n, BLOCK)
            getattr(pltpu.make_async_copy(ref.at[:, here], w.at[slot, :, pl.ds(at * BLOCK, BLOCK)], sems.at[slot, at]), what)()

    def compute(self, lhs, w, to, at, n, more):
        got = _dot(lhs[...], w[...])
        to[...] = (jax.nn.silu(got[:, :BLOCK]) * got[:, BLOCK:]).astype(jnp.bfloat16)

    def store(self, stage, out_ref, sems, to, at, n, size, side, start):
        c = pltpu.make_async_copy(stage.at[to], out_ref.at[_tile(at, BLOCK),
                                                           _tile(n, BLOCK)], sems.at[to, 0])
        c.start() if start else c.wait()


def gathered(x, gain, weights, finish, stored, out_shape, number, name, extra=(), scratch=(), share=None, twins=False):
    rows, depth = x.shape
    n = lax.axis_size("tp")
    side = int(round(n**0.5))
    width = sum(w.shape[1] for w in weights)
    anywhere, dma = pl.BlockSpec(memory_space=pl.ANY), pltpu.SemaphoreType.DMA
    shared = [] if share is None else [share]
    shelves = [jax.ShapeDtypeStruct((side - 1, w.shape[0], w.shape[1] // 2), w.dtype) for w in 2 * shared]
    operands = [x, gain, *extra, *weights, *shared]
    return pl.pallas_call(
        functools.partial(_gather_kernel, side=side, finish=finish, counts=(len(extra), len(weights), len(shared), len(scratch)), twins=twins),
        out_shape=[out_shape, *shelves] if shared else out_shape,
        in_specs=[anywhere] * len(operands),
        out_specs=[anywhere] * 3 if shared else anywhere,
        scratch_shapes=[
            pltpu.VMEM((n * rows, depth), jnp.bfloat16),
            pltpu.VMEM((depth,), jnp.bfloat16),
            pltpu.VMEM((3, depth, 2 * BLOCK), jnp.bfloat16),
            pltpu.VMEM((2, BLOCK, stored), jnp.bfloat16),
            dma((3,)), dma((3, 2)), dma((2, len(SLOTS))), dma((len(COPIES),)), dma((len(SLOTS), 2)),
            *scratch,
            *([dma((2, 2, 3))] * 2 + [dma((2, 3))] * 2 if shared else []),
        ],
        compiler_params=pltpu.CompilerParams(collective_id=number, has_side_effects=True, vmem_limit_bytes=VMEM),
        cost_estimate=_cost(n * rows, depth, width, len(EVENTS)),
        name=name,
    )(*operands)


class _Sum:
    def __init__(self, side, near, keep, own, r_half, r_near, s_half, s_near, t_half, t_near):
        self.side, self.near, self.keep, self.own = side, near, keep, own
        self.r_half, self.r_near, self.s_half, self.s_near, self.t_half, self.t_near = r_half, r_near, s_half, s_near, t_half, t_near
        self.low = keep.shape[2]

    def halves(self, j):
        a, b = lax.rem(j, 2), lax.rem(j, self.r_half.shape[0])
        return [_copy(self.side, link, self.near.at[a, 0, l], self.r_half.at[b, l], self.s_half.at[a, l], self.t_half.at[b, l])
                for l, link in enumerate(LINKS)]

    def lasts(self, j, part):
        a, b = lax.rem(j, 2), lax.rem(j, self.r_near.shape[0])
        got = []
        for l, link in enumerate(LINKS):
            at = l % 2 if part else 1 - l % 2
            got.append(_copy(self.side, link, self.near.at[a, 1 + part, l], self.r_near.at[b, l, pl.ds(at * self.low, self.low)],
                             self.s_near.at[a, part, l], self.t_near.at[b, part, l]))
        return got

    def each(self, what, *groups):
        for c in sum(groups, []):
            getattr(c, what)()

    def freed(self, j):
        self.each("wait_send", self.halves(j), self.lasts(j, 0))

    def gone(self, j):
        self.each("wait_send", self.lasts(j, 1))

    def put(self, j, t, l, pieces):
        a, low, bf = lax.rem(j, 2), self.low, jnp.bfloat16
        self.own[lax.rem(j, 4), t] = pieces[0]
        self.near[a, 0, l] = pieces[FAR][:low].astype(bf)
        self.near[a, 0, l + 1] = pieces[FAR][low:].astype(bf)
        self.near[a, 1, l] = pieces[1][low:].astype(bf)
        self.near[a, 1, l + 1] = pieces[-1][:low].astype(bf)
        self.keep[a, l] = pieces[1][:low]
        self.keep[a, l + 1] = pieces[-1][low:]

    def leave(self, j):
        self.each("start", self.halves(j), self.lasts(j, 0))

    def merge(self, j):
        a, b = lax.rem(j, 2), lax.rem(j, self.r_half.shape[0])
        self.each("wait_recv", self.halves(j))
        for l in range(len(LINKS)):
            self.near[a, 2, l] = (self.keep[a, l] + self.r_half[b, l].astype(jnp.float32)).astype(jnp.bfloat16)
        self.each("start", self.lasts(j, 1))

    def arrived(self, j):
        self.each("wait_recv", self.lasts(j, 0), self.lasts(j, 1))

    def total(self, j, t, l):
        b = lax.rem(j, self.r_near.shape[0])
        return self.own[lax.rem(j, 4), t] + self.r_near[b, l].astype(jnp.float32) + self.r_near[b, l + 1].astype(jnp.float32)

    @staticmethod
    def scratch(rings, low, tile):
        bf, f32, dma = jnp.bfloat16, jnp.float32, pltpu.SemaphoreType.DMA
        return [pltpu.VMEM((2, 3, 4, low, tile), bf), pltpu.VMEM((2, 4, low, tile), f32), pltpu.VMEM((4, 2, 2 * low, tile), f32),
                pltpu.VMEM((rings, 4, low, tile), bf), pltpu.VMEM((rings, 4, 2 * low, tile), bf),
                dma((2, 4)), dma((2, 2, 4)), dma((rings, 4)), dma((rings, 2, 4))]


def _scatter_kernel(rows_ref, x_ref, w_ref, out, hid, res, w, far, plain, summed, r_far, r_plain, r_summed, sems_h, sems_x, sems_w,
                    s_far, s_plain, s_summed, t_far, t_plain, t_summed, *second, side):
    rows, width = out.shape
    size = rows // 2
    tile = w.shape[2]
    tiles = width // tile
    ring = r_far.shape[0]
    group = hid.shape[0] // 4

    def fetch(n):
        return pltpu.make_async_copy(rows_ref.at[pl.ds(SLOT[ORDER[n]] * size, size)], hid.at[pl.ds(n * size, size)], sems_h.at[n])

    def weights(j):
        slot = lax.rem(j, 4)
        return pltpu.make_async_copy(w_ref.at[:, _tile(j, tile)], w.at[slot], sems_w.at[slot])

    def terms(g, j, count=1):
        return _dot(hid[pl.ds(g * group, count * group), :], w[lax.rem(j, 4)]).reshape(-1, size, tile)

    def pairs(src, dst, s_sem, t_sem, j):
        a, b = lax.rem(j, 2), lax.rem(j, ring)
        return [_copy(side, LINKS[l], src.at[a, pl.ds(2 * l, 2)], dst.at[b, pl.ds(2 * l, 2)], s_sem.at[a, l], t_sem.at[b, l])
                for l in range(4)]

    ring2 = _Sum(side, *second)

    def each(copies, what):
        for c in copies:
            getattr(c, what)()

    weights(0).start()
    for n in range(len(ORDER)):
        fetch(n).start()
    residual = pltpu.make_async_copy(x_ref, res, sems_x.at[0])
    residual.start()
    _meet(side)()
    for n in range(len(ORDER)):
        fetch(n).wait()
    residual.wait()

    def step(i, _):
        @_during(i, 2, tiles)
        def _():
            each(pairs(far, r_far, s_far, t_far, i - 2), "wait_send")
            each(pairs(plain, r_plain, s_plain, t_plain, i - 2), "wait_send")

        @_during(i, 0, tiles)
        def _():
            j = i

            @pl.when(j + 1 < tiles)
            def _():
                weights(j + 1).start()

            weights(j).wait()
            got = terms(0, j, 2).astype(jnp.bfloat16)
            far[lax.rem(j, 2)] = got[:8]
            plain[lax.rem(j, 2)] = got[8:]
            each(pairs(far, r_far, s_far, t_far, j), "start")
            each(pairs(plain, r_plain, s_plain, t_plain, j), "start")

        @_during(i, 3, tiles)
        def _():
            each(pairs(summed, r_summed, s_summed, t_summed, i - 3), "wait_send")

        @_during(i, 1, tiles)
        def _():
            j = i - 1
            each(pairs(far, r_far, s_far, t_far, j), "wait_recv")
            summed[lax.rem(j, 2)] = (terms(2, j) + r_far[lax.rem(j, ring)].astype(jnp.float32)).astype(jnp.bfloat16)
            each(pairs(summed, r_summed, s_summed, t_summed, j), "start")

        @_during(i, 4, tiles)
        def _():
            ring2.freed(i - 4)

        @_during(i, 2, tiles)
        def _():
            j = i - 2
            b = lax.rem(j, ring)
            each(pairs(plain, r_plain, s_plain, t_plain, j), "wait_recv")
            each(pairs(summed, r_summed, s_summed, t_summed, j), "wait_recv")
            mine = terms(3, j)
            for half in HALVES:
                l = 2 * half
                up, down = pl.ds(2 * l, 2), pl.ds(2 * l + 2, 2)
                from_up = jnp.concatenate([r_summed[b, up], r_plain[b, up]]).astype(jnp.float32)
                from_down = jnp.concatenate([r_plain[b, down], r_summed[b, down]]).astype(jnp.float32)
                both_ways = mine[4 * half : 4 * half + 4] + from_up + from_down
                sums = {across: both_ways[k] for k, across in enumerate(UP + DOWN)}
                ring2.put(j, half, 2 - l, sums)
            ring2.leave(j)

        @_during(i, 5, tiles)
        def _():
            ring2.gone(i - 5)

        @_during(i, 3, tiles)
        def _():
            ring2.merge(i - 3)

        @pl.when(i >= 4)
        def _():
            j = i - 4

            ring2.arrived(j)
            here = _tile(j, tile)
            for half in HALVES:
                mine = pl.ds(half * size, size)
                out[mine, here] = (res[mine, here].astype(jnp.float32) + ring2.total(j, half, 2 - 2 * half)).astype(jnp.bfloat16)

    lax.fori_loop(0, tiles + 4, step, None)
    ring2.gone(tiles - 1)


def scattered(terms, x, w, number, name):
    rows, width = x.shape
    depth = w.shape[0]
    n = lax.axis_size("tp")
    side = int(round(n**0.5))
    size, low = rows // 2, rows // 4
    tile = min(TILE, width)
    tiles = width // tile
    bf, dma = jnp.bfloat16, pltpu.SemaphoreType.DMA
    return pl.pallas_call(
        functools.partial(_scatter_kernel, side=side),
        out_shape=jax.ShapeDtypeStruct((rows, width), bf),
        in_specs=[pl.BlockSpec(memory_space=pl.ANY)] * 3,
        out_specs=pl.BlockSpec(memory_space=pltpu.VMEM),
        scratch_shapes=[
            pltpu.VMEM((n * rows, depth), bf),
            pltpu.VMEM((rows, width), bf),
            pltpu.VMEM((4, depth, tile), bf),
            pltpu.VMEM((2, 8, size, tile), bf),
            pltpu.VMEM((2, 8, size, tile), bf),
            pltpu.VMEM((2, 8, size, tile), bf),
            pltpu.VMEM((RING, 8, size, tile), bf),
            pltpu.VMEM((RING, 8, size, tile), bf),
            pltpu.VMEM((RING, 8, size, tile), bf),
            dma((len(ORDER),)), dma((1,)), dma((4,)),
            *[dma((2, 4))] * 3, *[dma((RING, 4))] * 3,
            *_Sum.scratch(RING, low, tile),
        ],
        compiler_params=pltpu.CompilerParams(collective_id=number, has_side_effects=True, vmem_limit_bytes=LAST_VMEM),
        cost_estimate=_cost(n * rows, depth, width),
        name=name,
    )(terms, x, w)


AROUND = (0, 1, -1, FAR)
ORIGIN = (0, -1, 1, FAR)
TURNS = (FAR, 1, -1, 0)


def _attend(qkv, mine, o, top_s, mix_s):
    size, d = o.shape[0], qkv.shape[2]
    heads = qkv.shape[0] // 3
    e = d**-0.5 * LOG2E
    top_s[...] = jnp.full(top_s.shape, NEG, jnp.float32)
    mix_s[...] = jnp.zeros(mix_s.shape, jnp.float32)
    ones = jnp.ones((8, size), qkv.dtype)

    def block(j, masked):
        here = _tile(j, size)
        scores = [_dot(qkv[heads + i, here, :], qkv[i, _tile(mine, size), :], 1, 1) for i in range(heads)]
        if masked:
            seen = lax.broadcasted_iota(jnp.int32, (size, size), 1) >= lax.broadcasted_iota(jnp.int32, (size, size), 0)
        weights, keeps = [], []
        for i, s in enumerate(scores):
            s = jnp.where(seen, s, HIDDEN) if masked else s
            old = top_s[i : i + 1, :]
            top = jnp.maximum(old, s.max(axis=0, keepdims=True))
            top_s[i : i + 1, :] = top
            weights.append(jnp.exp2((s - top) * e).astype(qkv.dtype))
            keeps.append(jnp.exp2((old - top) * e))
        for i, (p, keep) in enumerate(zip(weights, keeps)):
            values = jnp.concatenate([qkv[2 * heads + i, here, :].T, ones], axis=0)
            mix_s[i] = mix_s[i] * keep + _dot(values, p, 1, 0)

    lax.fori_loop(0, mine, lambda j, _: block(j, False), None)
    block(mine, True)
    for i in range(heads):
        total = mix_s[i, d : d + 1, :]
        o[:, i * d : (i + 1) * d] = (mix_s[i, :d, :] * (1 / total)).T.astype(o.dtype)


def _share_kernel(qkv_ref, x_ref, w_ref, left_ref, right_ref, out_ref, qkv, seen, top_s, mix_s, s, relay, w, res, out, sems_q, sems_x, sems_w,
                  sems_o, s_next, s_far, s_pass, t_next, t_far, t_pass, *second, side):
    rows, width = out_ref.shape
    depth, tile = w_ref.shape[0], w.shape[3]
    half, tiles = width // 2, width // 2 // tile
    slots = w.shape[0]
    ring = _Sum(side, *second)
    x, y = _place(side)

    def block(t, along, across):
        dx, dy = (along, across) if t == 0 else (across, along)
        return seen.at[TURNS.index(dx), _tile(lax.rem(y + (dy + side), side), rows)]

    def place(t, across, origin):
        return s.at[t, _tile(AROUND.index(across), rows), _tile(ORIGIN.index(origin), depth)]

    ways = [(t, n, sign) for t in HALVES for n, sign in enumerate(SIGNS)]

    def far(t, along, across):
        n, i = divmod(AROUND.index(across), 2)
        sign = 1 - 2 * n
        return _copy(side, ("xy"[t], sign), block(t, FAR, across), relay.at[t, n, i], s_far.at[t, n, i], t_far.at[t, n, i])

    def passed(t, across):
        n, i = divmod(AROUND.index(across), 2)
        return _copy(side, ("xy"[t], 1 - 2 * n), relay.at[t, n, i], place(t, across, FAR), s_pass.at[t, n, i], t_pass.at[t, n, i])

    def next_to(t, sign, across):
        at = t, int(sign < 0), AROUND.index(across)
        return _copy(side, ("xy"[t], sign), block(t, sign, across), place(t, across, -sign), s_next.at[at], t_next.at[at])

    def sends(t, along, across):
        if along:
            (far if along == FAR else next_to)(t, along, across).start()
        else:
            place(t, across, 0)[...] = block(t, 0, across)[...]

    def each(what, copies):
        for c in copies:
            getattr(c, what)()

    def weights(j):
        got = []
        for t, shelf in enumerate((left_ref, right_ref)):
            for i in range(side):
                src = shelf.at[i - 1, :, _tile(j, tile)] if i else w_ref.at[:, _tile(t * tiles + j, tile)]
                got.append(pltpu.make_async_copy(src, w.at[lax.rem(j, slots), t, pl.ds(i * depth, depth)], sems_w.at[lax.rem(j, slots), t, i]))
        return got

    def out_copy(t, j):
        here = _tile(t * tiles + j, tile)
        return pltpu.make_async_copy(out.at[:, here], out_ref.at[:, here], sems_o.at[t, j])

    met = _meet(side)
    heads = qkv.shape[0] // 3
    parts = [pltpu.make_async_copy(qkv_ref.at[here], qkv.at[here], sems_q.at[n]) for n in range(3) for here in [pl.ds(n * heads, heads)]]
    each("start", parts)
    for j in range(slots - 1):
        each("start", weights(j))
    residual = pltpu.make_async_copy(x_ref, res, sems_x.at[0])
    residual.start()
    each("wait", parts)
    met()

    def turn(n, _):
        _attend(qkv, lax.rem(x + (FAR + len(TURNS) * 2) - lax.div(n * (n + 1), 2), side), seen.at[n], top_s, mix_s)
        for k, dx in enumerate(TURNS):

            @pl.when(n == k)
            def _(dx=dx):
                for other in AROUND:
                    sends(0, dx, other)
                    sends(1, other, dx)

    lax.fori_loop(0, len(TURNS), turn, None)
    for t in HALVES:
        for across in TURNS:
            far(t, FAR, across).wait_recv()
            passed(t, across).start()
    for t, n, sign in ways:
        each("wait_recv", [next_to(t, sign, across) for across in AROUND])
    residual.wait()
    for t in HALVES:
        each("wait_recv", [passed(t, across) for across in AROUND])

    def step(i, _):
        @_during(i, 2, tiles)
        def _():
            ring.freed(i - 2)

        @_during(i, 0, tiles)
        def _():
            j = i

            @pl.when(j + (slots - 1) < tiles)
            def _():
                each("start", weights(j + (slots - 1)))

            each("wait", weights(j))
            for t in HALVES:
                got = _dot(s[t], w[lax.rem(j, slots), t])
                ring.put(j, t, 2 * t, {across: got[k * rows : (k + 1) * rows] for k, across in enumerate(AROUND)})
            ring.leave(j)

        @_during(i, 3, tiles)
        def _():
            ring.gone(i - 3)

        @_during(i, 1, tiles)
        def _():
            ring.merge(i - 1)

        @pl.when(i >= 2)
        def _():
            j = i - 2
            ring.arrived(j)
            for t in HALVES:
                here = _tile(t * tiles + j, tile)
                out[:, here] = (res[:, here].astype(jnp.float32) + ring.total(j, t, 2 * t)).astype(jnp.bfloat16)
                out_copy(t, j).start()

    lax.fori_loop(0, tiles + 2, step, None)
    ring.gone(tiles - 1)
    for t, n, sign in ways:
        each("wait_send", [next_to(t, sign, across) for across in AROUND])
    for t in HALVES:
        each("wait_send", [copy for across in AROUND for copy in (far(t, FAR, across), passed(t, across))])
        for j in range(tiles):
            out_copy(t, j).wait()


def projected(qkv, x, w, left, right, number, name):
    rows, width = x.shape
    depth = w.shape[0]
    n = lax.axis_size("tp")
    side = int(round(n**0.5))
    tile = min(TILE, width // 2)
    tiles = width // 2 // tile
    bf, dma = jnp.bfloat16, pltpu.SemaphoreType.DMA
    anywhere = pl.BlockSpec(memory_space=pl.ANY)
    return pl.pallas_call(
        functools.partial(_share_kernel, side=side),
        out_shape=jax.ShapeDtypeStruct((rows, width), bf),
        in_specs=[anywhere] * 5,
        out_specs=anywhere,
        scratch_shapes=[
            pltpu.VMEM(qkv.shape, bf),
            pltpu.VMEM((side, side * rows, depth), bf),
            pltpu.VMEM((qkv.shape[0] // 3, side * rows), jnp.float32),
            pltpu.VMEM((qkv.shape[0] // 3, HEAD + 8, side * rows), jnp.float32),
            pltpu.VMEM((2, side * rows, side * depth), bf),
            pltpu.VMEM((2, 2, 2, rows, depth), bf),
            pltpu.VMEM((3, 2, side * depth, tile), bf),
            pltpu.VMEM((rows, width), bf),
            pltpu.VMEM((rows, width), bf),
            dma((3,)), dma((1,)), dma((3, 2, side)), dma((2, tiles)),
            *[dma((2, 2, 4)), dma((2, 2, 2)), dma((2, 2, 2))] * 2,
            *_Sum.scratch(tiles, rows // 2, tile),
        ],
        compiler_params=pltpu.CompilerParams(collective_id=number, has_side_effects=True, vmem_limit_bytes=VMEM),
        cost_estimate=_cost(n * rows, depth, width, side),
        name=name,
    )(qkv, x, w, left, right)


def _angles(tokens):
    half = HEAD // 2
    rate = np.power(np.float32(THETA), -np.arange(half, dtype=np.float32) / np.float32(half)).astype(np.float32)
    angle = (np.arange(tokens, dtype=np.float32)[:, None] * rate).astype(np.float64)
    return np.concatenate([np.cos(angle), np.sin(angle)], 1).astype(np.float32)


def solution(mesh):
    n = mesh.shape["tp"]

    def step(x, gain_a, wq, wk, wv, wo, gain_m, w_gate, w_up, w_down):
        rows = n * x.shape[0]
        heads = wq.shape[1] // HEAD
        qkv, left, right = gathered(
            x, gain_a, (wq, wk, wv), _Heads(2), 2 * BLOCK, jax.ShapeDtypeStruct((3 * heads, rows, HEAD), jnp.bfloat16), 0, "gather_qkv",
            extra=(jnp.asarray(_angles(rows)),),
            scratch=(pltpu.VMEM((3, BLOCK, 2 * BLOCK), jnp.float32), pltpu.VMEM((rows, HEAD), jnp.float32),
                     pltpu.SemaphoreType.DMA((len(SLOTS),))),
            share=wo, twins=mesh.shape["dp"] % 2 == 0,
        )
        h = projected(qkv, x, wo, left, right, 1, "project")
        hidden = gathered(h, gain_m, (w_gate, w_up), _Hidden(), BLOCK, jax.ShapeDtypeStruct((rows, w_gate.shape[1]), jnp.bfloat16), 2,
                          "gather_hidden")
        return scattered(hidden, h, w_down, 3, "scatter_down")

    tokens, columns, rows_of = P(("dp", "tp"), None), P(None, "tp"), P("tp", None)
    return jax.shard_map(
        step,
        mesh=mesh,
        in_specs=(tokens, P(None), columns, columns, columns, rows_of, P(None), columns, columns, rows_of),
        out_specs=tokens,
        check_vma=False,
    )
```
